32 devices in a mesh: tp: 4 (over z), dp: 8 (over y, x, core).
Axes of the slice: x: 2, y: 2, z: 4, core: 2. Of those that a mesh axis runs over, the one named last changes fastest.
Arguments:
- tokens: int32 [8, 2048], P('dp')
- cotangent: bfloat16 [8, 2048, 1024], P('dp')
- emb_table: bfloat16 [30592, 1024], P('tp')
- w_qkv: bfloat16 [1024, 3072], P(None, 'tp')
- b_qkv: bfloat16 [16, 192], P('tp')
- w_out: bfloat16 [1024, 1024], P('tp')
- b_out: bfloat16 [1024], replicated
- ln1_gain: bfloat16 [1024], replicated
- ln1_bias: bfloat16 [1024], replicated
- w_gate: bfloat16 [1024, 4096], P(None, 'tp')
- b_gate: bfloat16 [4096], P('tp')
- w_lin: bfloat16 [1024, 4096], P(None, 'tp')
- b_lin: bfloat16 [4096], P('tp')
- w_down: bfloat16 [4096, 1024], P('tp')
- b_down: bfloat16 [1024], replicated
- ln2_gain: bfloat16 [1024], replicated
Outputs:
- output 1: float32 [30592, 1024], P('tp')
- output 2: float32 [1024, 3072], P(None, 'tp')
- output 3: float32 [16, 192], P('tp')
- output 4: float32 [1024, 1024], P('tp')
- output 5: float32 [1024], replicated
- output 6: float32 [1024], replicated
- output 7: float32 [1024], replicated
- output 8: float32 [1024, 4096], P(None, 'tp')
- output 9: float32 [4096], P('tp')
- output 10: float32 [1024, 4096], P(None, 'tp')
- output 11: float32 [4096], P('tp')
- output 12: float32 [4096, 1024], P('tp')
- output 13: float32 [1024], replicated
- output 14: float32 [1024], replicated
All inputs are finite; a program needn't handle non-finite values.
Results may differ from the reference program's by a relative error of at most 0.0152302.
Values sent between devices are 32-bit elements.
A program may use at most 1 GiB of HBM per device.

```python
import jax
import jax.numpy as jnp
from jax import lax

VOCAB_SIZE = 30592
D_MODEL = 1024
NUM_HEADS = 16
FFN_DIM = 4096
GLOBAL_BATCH = 8
SEQ_LEN = 2048
HEAD_DIM = D_MODEL // NUM_HEADS
ALPHA = 140.0 ** 0.5
EPS = 1e-5
SHRINK = 0.1
ROPE_BASE = 10000.0


def setup_inputs(seed: int = 0) -> dict:
    root_key = jax.random.key(seed)
    key_list = jax.random.split(root_key, 16)
    id_keys = jax.random.split(key_list[0], 2)
    first_ids = jax.random.randint(id_keys[0], (GLOBAL_BATCH, SEQ_LEN), 0, VOCAB_SIZE, dtype=jnp.int32)
    second_ids = jax.random.randint(id_keys[1], (GLOBAL_BATCH, SEQ_LEN), 0, VOCAB_SIZE, dtype=jnp.int32)
    tokens = jnp.minimum(first_ids, second_ids)
    tokens = tokens.at[0, 0].set(0).at[0, SEQ_LEN - 1].set(VOCAB_SIZE - 1)

    def draw(index, shape, scale, offset):
        return (jax.random.normal(key_list[index], shape, jnp.float32) * scale + offset).astype(jnp.bfloat16)

    return {
        'tokens': tokens,
        'cotangent': draw(1, (GLOBAL_BATCH, SEQ_LEN, D_MODEL), 1.0, 0.0),
        'emb_table': draw(2, (VOCAB_SIZE, D_MODEL), 1.0, 0.0),
        'w_qkv': draw(3, (D_MODEL, 3 * D_MODEL), D_MODEL ** -0.5, 0.0),
        'b_qkv': draw(4, (NUM_HEADS, 3 * HEAD_DIM), 0.3, 0.0),
        'w_out': draw(5, (D_MODEL, D_MODEL), ALPHA * D_MODEL ** -0.5, 0.0),
        'b_out': draw(6, (D_MODEL,), 1.0, 0.0),
        'ln1_gain': draw(7, (D_MODEL,), 0.3, 1.0),
        'ln1_bias': draw(8, (D_MODEL,), 0.3, 0.0),
        'w_gate': draw(9, (D_MODEL, FFN_DIM), D_MODEL ** -0.5, 0.0),
        'b_gate': draw(10, (FFN_DIM,), 0.3, 0.0),
        'w_lin': draw(11, (D_MODEL, FFN_DIM), D_MODEL ** -0.5, 0.0),
        'b_lin': draw(12, (FFN_DIM,), 0.3, 0.0),
        'w_down': draw(13, (FFN_DIM, D_MODEL), ALPHA * FFN_DIM ** -0.5, 0.0),
        'b_down': draw(14, (D_MODEL,), 2.0, 0.0),
        'ln2_gain': draw(15, (D_MODEL,), 0.3, 1.0),
    }


def to_bf16(values):
    return values.astype(jnp.bfloat16).astype(jnp.float32)


def norm_scaled(values, gain):
    mean_val = jnp.mean(values, axis=-1, keepdims=True)
    centered = values - mean_val
    variance = jnp.mean(centered * centered, axis=-1, keepdims=True)
    return centered * lax.rsqrt(variance + EPS) * gain


def rope_tables():
    half_dim = HEAD_DIM // 2
    inv_freq = ROPE_BASE ** (-2.0 * jnp.arange(half_dim, dtype=jnp.float32) / HEAD_DIM)
    angles = jnp.arange(SEQ_LEN, dtype=jnp.float32)[:, None] * inv_freq[None, :]
    return jnp.cos(angles)[:, None, :], jnp.sin(angles)[:, None, :]


def apply_rope(values, cos_tab, sin_tab):
    half_dim = values.shape[-1] // 2
    first_half = values[..., :half_dim]
    second_half = values[..., half_dim:]
    return jnp.concatenate([first_half * cos_tab - second_half * sin_tab, second_half * cos_tab + first_half * sin_tab], axis=-1)


def seq_loss(params, emb_rows, seq_cot):
    (w_qkv, b_qkv, w_out, b_out, ln1_gain, ln1_bias, w_gate, b_gate, w_lin, b_lin, w_down, b_down, ln2_gain) = params
    embedded = SHRINK * emb_rows + (1.0 - SHRINK) * lax.stop_gradient(emb_rows)
    qkv_pre = jnp.dot(embedded, w_qkv, preferred_element_type=jnp.float32) + b_qkv.reshape(-1)
    qkv_all = to_bf16(qkv_pre).reshape(SEQ_LEN, NUM_HEADS, 3, HEAD_DIM)
    cos_tab, sin_tab = rope_tables()
    queries = to_bf16(apply_rope(qkv_all[:, :, 0], cos_tab, sin_tab))
    keys_rot = to_bf16(apply_rope(qkv_all[:, :, 1], cos_tab, sin_tab))
    values = qkv_all[:, :, 2]
    scores = jnp.einsum('qhd,khd->hqk', queries, keys_rot) * HEAD_DIM ** -0.5
    causal = jnp.arange(SEQ_LEN)[:, None] >= jnp.arange(SEQ_LEN)[None, :]
    attn_probs = to_bf16(jax.nn.softmax(jnp.where(causal, scores, -1e30), axis=-1))
    context = to_bf16(jnp.einsum('hqk,khd->qhd', attn_probs, values)).reshape(SEQ_LEN, D_MODEL)
    attn_out = jnp.dot(context, w_out, preferred_element_type=jnp.float32) + b_out
    hidden = to_bf16(norm_scaled(ALPHA * embedded + attn_out, ln1_gain) + ln1_bias)
    gate_pre = jnp.dot(hidden, w_gate, preferred_element_type=jnp.float32) + b_gate
    lin_pre = jnp.dot(hidden, w_lin, preferred_element_type=jnp.float32) + b_lin
    inner_act = to_bf16(jax.nn.gelu(gate_pre, approximate=False) * lin_pre)
    ffn_out = jnp.dot(inner_act, w_down, preferred_element_type=jnp.float32) + b_down
    final_out = norm_scaled(ALPHA * hidden + ffn_out, ln2_gain)
    return jnp.sum(final_out * seq_cot)


def reference(tokens, cotangent, emb_table, w_qkv, b_qkv, w_out, b_out, ln1_gain, ln1_bias, w_gate, b_gate, w_lin, b_lin, w_down, b_down, ln2_gain):
    params = tuple(weight.astype(jnp.float32) for weight in (w_qkv, b_qkv, w_out, b_out, ln1_gain, ln1_bias, w_gate, b_gate, w_lin, b_lin, w_down, b_down, ln2_gain))

    def one_sequence(grad_acc, seq_item):
        seq_tokens, seq_cot = seq_item
        emb_rows = jnp.take(emb_table, seq_tokens, axis=0).astype(jnp.float32)

        def loss_of(prm_all, rows_in):
            return seq_loss(prm_all, rows_in, seq_cot.astype(jnp.float32))

        pull_back = jax.vjp(loss_of, params, emb_rows)[1]
        grad_params, grad_rows = pull_back(jnp.ones((), jnp.float32))
        new_acc = jax.tree.map(lambda acc_val, new_val: acc_val + new_val, grad_acc, grad_params)
        return new_acc, grad_rows

    init_acc = jax.tree.map(lambda prm_item: prm_item * 0.0, params)
    grad_params, grad_rows = lax.scan(one_sequence, init_acc, (tokens, cotangent))
    d_table = jax.ops.segment_sum(grad_rows.reshape(-1, D_MODEL), tokens.reshape(-1), num_segments=VOCAB_SIZE)
    (d_w_qkv, d_b_qkv, d_w_out, d_b_out, d_ln1_gain, d_ln1_bias, d_w_gate, d_b_gate, d_w_lin, d_b_lin, d_w_down, d_b_down, d_ln2_gain) = grad_params
    return (d_table, d_w_qkv, d_b_qkv, d_w_out, d_b_out, d_ln1_gain, d_ln1_bias, d_w_gate, d_b_gate, d_w_lin, d_b_lin, d_w_down, d_b_down, d_ln2_gain)
```

```python
import jax
import jax.numpy as jnp
from jax import lax
from jax.sharding import PartitionSpec as P

ALPHA = 140.0 ** 0.5
EPS = 1e-5
SHRINK = 0.1
ROPE_BASE = 10000.0
WEIGHT_SPECS = (P(None, 'tp'), P('tp', None), P('tp', None), P(), P(), P(), P(None, 'tp'), P('tp'), P(None, 'tp'), P('tp'), P('tp', None), P(), P())
ALL = ('tp', 'dp')
BF = jnp.bfloat16
F32 = jnp.float32


def norm_scaled(values, gain):
    mean_val = jnp.mean(values, axis=-1, keepdims=True)
    centered = values - mean_val
    variance = jnp.mean(centered * centered, axis=-1, keepdims=True)
    return centered * lax.rsqrt(variance + EPS) * gain


def geglu(gate_pre, lin_pre):
    return jax.nn.gelu(gate_pre, approximate=False) * lin_pre


def rope_tables(seq_len, head_dim):
    half_dim = head_dim // 2
    inv_freq = ROPE_BASE ** (-2.0 * jnp.arange(half_dim, dtype=F32) / head_dim)
    angles = jnp.arange(seq_len, dtype=F32)[:, None] * inv_freq[None, :]
    return jnp.cos(angles)[:, None, :], jnp.sin(angles)[:, None, :]


def apply_rope(values, cos_tab, sin_tab):
    half_dim = values.shape[-1] // 2
    first_half = values[..., :half_dim]
    second_half = values[..., half_dim:]
    return jnp.concatenate([first_half * cos_tab - second_half * sin_tab, second_half * cos_tab + first_half * sin_tab], axis=-1)


def solution(mesh):
    n_tp, n_dp = mesh.shape['tp'], mesh.shape['dp']
    in_specs = (P('dp', None), P('dp', None, None), P('tp', None)) + WEIGHT_SPECS
    out_specs = (P('tp', None),) + WEIGHT_SPECS

    def device_step(tokens, cotangent, emb_table, *weights):
        (w_qkv, b_qkv, w_out, b_out, ln1_gain, ln1_bias, w_gate, b_gate, w_lin, b_lin, w_down, b_down, ln2_gain) = weights
        tp, dp = lax.axis_index('tp'), lax.axis_index('dp')
        tokens = tokens[0]
        seq_len, width = tokens.shape[0], emb_table.shape[1]
        heads, head_dim = b_qkv.shape[0], b_qkv.shape[1] // 3
        own = seq_len // n_tp
        ffn = w_gate.shape[1]
        zero = jnp.minimum(tokens[0], 0).astype(F32)

        def rounded(values):
            return (values + zero).astype(BF)

        def gathered(weight):
            rows = weight.shape[0] // n_dp
            piece = lax.dynamic_slice_in_dim(weight, dp * rows, rows, 0).astype(F32)
            return lax.all_gather(piece, ALL, axis=0, tiled=True)

        wo_rows = w_out.shape[0] // n_dp
        wo_piece = lax.dynamic_slice_in_dim(w_out, dp * wo_rows, wo_rows, 0)
        bias_rows = jnp.concatenate([b_gate[None], b_lin[None], jnp.zeros((6, ffn), BF)], axis=0)
        wo_all = lax.all_gather(jnp.concatenate([wo_piece, bias_rows], axis=0).astype(F32), ALL, axis=0, tiled=True).reshape(n_tp, n_dp, wo_rows + 8, width)
        wo_full = rounded(wo_all[:, :, :wo_rows].reshape(n_tp, n_dp * wo_rows, width))
        bg_full, bl_full = wo_all[:, 0, wo_rows], wo_all[:, 0, wo_rows + 1]
        wg_full = rounded(gathered(w_gate).reshape(n_tp, width, ffn))
        wl_full = rounded(gathered(w_lin).reshape(n_tp, width, ffn))
        wd_full = rounded(gathered(w_down).reshape(n_tp, ffn, width))

        vocab_loc = emb_table.shape[0]
        local_ids = tokens - tp * vocab_loc
        in_shard = (local_ids >= 0) & (local_ids < vocab_loc)
        safe_ids = jnp.where(in_shard, local_ids, 0)
        own_rows = jnp.where(in_shard[:, None], jnp.take(emb_table, safe_ids, axis=0), 0.0)
        embedded = lax.psum(own_rows.astype(F32), 'tp')

        emb_bf = embedded.astype(BF)
        qkv_pre = jnp.dot(emb_bf, w_qkv, preferred_element_type=F32) + b_qkv.reshape(-1).astype(F32)
        qkv_all = qkv_pre.astype(BF).reshape(seq_len, heads, 3, head_dim)
        cos_tab, sin_tab = rope_tables(seq_len, head_dim)
        queries = apply_rope(qkv_all[:, :, 0].astype(F32), cos_tab, sin_tab).astype(BF)
        keys_rot = apply_rope(qkv_all[:, :, 1].astype(F32), cos_tab, sin_tab).astype(BF)
        values = qkv_all[:, :, 2]
        attn_scale = head_dim ** -0.5
        causal = jnp.arange(seq_len)[:, None] >= jnp.arange(seq_len)[None, :]
        scores = jnp.einsum('qhd,khd->hqk', queries, keys_rot, preferred_element_type=F32) * attn_scale
        attn_probs = jax.nn.softmax(jnp.where(causal, scores, -1e30), axis=-1).astype(BF)
        context = jnp.einsum('hqk,khd->qhd', attn_probs, values, preferred_element_type=F32).reshape(n_tp, own, heads * head_dim)
        ctx_own = (lax.all_to_all(context, 'tp', 0, 0) + zero).astype(BF)

        emb_own = lax.dynamic_slice_in_dim(embedded, tp * own, own, 0)
        cot_own = lax.dynamic_slice_in_dim(cotangent[0], tp * own, own, 0).astype(F32)
        attn_out = jnp.einsum('hse,hed->sd', ctx_own, wo_full, preferred_element_type=F32) + b_out.astype(F32)
        normed_one, norm_one_pull = jax.vjp(norm_scaled, ALPHA * emb_own + attn_out, ln1_gain.astype(F32))
        hidden = (normed_one + ln1_bias.astype(F32)).astype(BF)
        gate_pre = jnp.einsum('sk,tkc->tsc', hidden, wg_full, preferred_element_type=F32) + bg_full[:, None]
        lin_pre = jnp.einsum('sk,tkc->tsc', hidden, wl_full, preferred_element_type=F32) + bl_full[:, None]
        inner_val, act_pull = jax.vjp(geglu, gate_pre, lin_pre)
        inner_act = inner_val.astype(BF)
        ffn_out = jnp.einsum('tsc,tcd->sd', inner_act, wd_full, preferred_element_type=F32) + b_down.astype(F32)
        norm_two_pull = jax.vjp(norm_scaled, ALPHA * hidden.astype(F32) + ffn_out, ln2_gain.astype(F32))[1]

        d_resid_two, d_ln2_gain = norm_two_pull(cot_own)
        d_b_down = jnp.sum(d_resid_two, axis=0)
        d_ffn_bf = d_resid_two.astype(BF)
        d_w_down = jnp.einsum('tsc,sd->tcd', inner_act, d_ffn_bf, preferred_element_type=F32)
        d_inner = jnp.einsum('sd,tcd->tsc', d_ffn_bf, wd_full, preferred_element_type=F32).astype(BF)
        d_gate_pre, d_lin_pre = act_pull(d_inner.astype(F32))
        d_b_gate = jnp.sum(d_gate_pre, axis=1)
        d_b_lin = jnp.sum(d_lin_pre, axis=1)
        d_gate_bf = d_gate_pre.astype(BF)
        d_lin_bf = d_lin_pre.astype(BF)
        d_w_gate = jnp.einsum('sk,tsc->tkc', hidden, d_gate_bf, preferred_element_type=F32)
        d_w_lin = jnp.einsum('sk,tsc->tkc', hidden, d_lin_bf, preferred_element_type=F32)
        d_hidden = ALPHA * d_resid_two + jnp.einsum('tsc,tkc->sk', d_gate_bf, wg_full, preferred_element_type=F32) + jnp.einsum('tsc,tkc->sk', d_lin_bf, wl_full, preferred_element_type=F32)
        d_ln1_bias = jnp.sum(d_hidden, axis=0)
        d_resid_one, d_ln1_gain = norm_one_pull(d_hidden)
        d_b_out = jnp.sum(d_resid_one, axis=0)
        d_attn_bf = d_resid_one.astype(BF)
        d_w_out = jnp.einsum('hse,sd->hed', ctx_own, d_attn_bf, preferred_element_type=F32)
        d_ctx = jnp.einsum('sd,hed->hse', d_attn_bf, wo_full, preferred_element_type=F32)
        d_context = (lax.all_to_all(d_ctx, 'tp', 0, 0) + zero).astype(BF).reshape(seq_len, heads, head_dim)

        def reduced(grad):
            piece = lax.psum_scatter(grad.reshape(-1, grad.shape[-1]), ALL, scatter_dimension=0, tiled=True)
            return lax.all_gather(piece, 'dp', axis=0, tiled=True)

        d_w_down, d_w_gate, d_w_lin, d_w_out = reduced(d_w_down), reduced(d_w_gate), reduced(d_w_lin), reduced(d_w_out)

        d_probs = jnp.einsum('qhd,khd->hqk', d_context, values, preferred_element_type=F32)
        d_values = jnp.einsum('hqk,qhd->khd', attn_probs, d_context, preferred_element_type=F32)
        probs_f32 = attn_probs.astype(F32)
        d_scores = (probs_f32 * (d_probs - jnp.sum(d_probs * probs_f32, axis=-1, keepdims=True)) * attn_scale).astype(BF)
        d_queries = apply_rope(jnp.einsum('hqk,khd->qhd', d_scores, keys_rot, preferred_element_type=F32), cos_tab, -sin_tab)
        d_keys = apply_rope(jnp.einsum('hqk,qhd->khd', d_scores, queries, preferred_element_type=F32), cos_tab, -sin_tab)
        d_qkv = jnp.stack([d_queries, d_keys, d_values], axis=2).reshape(seq_len, -1)
        d_b_qkv = jnp.sum(d_qkv, axis=0)
        d_qkv_bf = d_qkv.astype(BF)
        d_w_qkv = jnp.dot(emb_bf.T, d_qkv_bf, preferred_element_type=F32)
        d_emb_part = jnp.dot(d_qkv_bf, w_qkv.T, preferred_element_type=F32)
        d_emb_part = lax.dynamic_update_slice_in_dim(d_emb_part, lax.dynamic_slice_in_dim(d_emb_part, tp * own, own, 0) + ALPHA * d_resid_one, tp * own, 0)
        d_embedded = lax.psum(d_emb_part, 'tp')
        d_rows = jnp.where(in_shard[:, None], SHRINK * d_embedded, 0.0)
        d_table = jax.ops.segment_sum(d_rows, safe_ids, num_segments=vocab_loc)

        slot = (jnp.arange(n_tp) == tp).astype(F32)[:, None]
        d_bq_rows = jnp.pad(slot * d_b_qkv[None], ((0, 0), (0, width - d_b_qkv.shape[0])))
        small = jnp.concatenate([d_b_gate, d_b_lin, d_bq_rows, jnp.stack([d_b_out, d_ln1_gain, d_ln1_bias, d_b_down, d_ln2_gain])], axis=0)
        small = lax.psum(small, ALL)
        d_b_gate = lax.dynamic_index_in_dim(small[:n_tp], tp, 0, keepdims=False)
        d_b_lin = lax.dynamic_index_in_dim(small[n_tp:2 * n_tp], tp, 0, keepdims=False)
        d_b_qkv = lax.dynamic_index_in_dim(small[2 * n_tp:3 * n_tp], tp, 0, keepdims=False)[:d_b_qkv.shape[0]].reshape(heads, 3 * head_dim)
        d_b_out, d_ln1_gain, d_ln1_bias, d_b_down, d_ln2_gain = [small[3 * n_tp + i] for i in range(5)]
        d_table, d_w_qkv = lax.psum((d_table, d_w_qkv), 'dp')
        return (d_table, d_w_qkv, d_b_qkv, d_w_out, d_b_out, d_ln1_gain, d_ln1_bias, d_w_gate, d_b_gate, d_w_lin, d_b_lin, d_w_down, d_b_down, d_ln2_gain)

    return jax.shard_map(device_step, mesh=mesh, in_specs=in_specs, out_specs=out_specs, check_vma=False)
```

```python
import functools

import jax
import jax.numpy as jnp
from jax import lax
from jax.experimental import pallas as pl
from jax.experimental.pallas import tpu as pltpu
from jax.sharding import PartitionSpec as P

ALPHA = 140.0 ** 0.5
EPS = 1e-5
SHRINK = 0.1
ROPE_BASE = 10000.0
WEIGHT_SPECS = (P(None, 'tp'), P('tp', None), P('tp', None), P(), P(), P(), P(None, 'tp'), P('tp'), P(None, 'tp'), P('tp'), P('tp', None), P(), P())
ALL = ('tp', 'dp')
BF = jnp.bfloat16
F32 = jnp.float32
MESH = pl.DeviceIdType.MESH
ANY = pl.BlockSpec(memory_space=pl.ANY)
VMEM = pl.BlockSpec(memory_space=pltpu.VMEM)


def norm_scaled(values, gain):
    mean_val = jnp.mean(values, axis=-1, keepdims=True)
    centered = values - mean_val
    variance = jnp.mean(centered * centered, axis=-1, keepdims=True)
    return centered * lax.rsqrt(variance + EPS) * gain


def geglu(gate_pre, lin_pre):
    return jax.nn.gelu(gate_pre, approximate=False) * lin_pre


def rope_tables(seq_len, head_dim):
    half_dim = head_dim // 2
    inv_freq = ROPE_BASE ** (-2.0 * jnp.arange(half_dim, dtype=F32) / head_dim)
    angles = jnp.arange(seq_len, dtype=F32)[:, None] * inv_freq[None, :]
    return jnp.cos(angles)[:, None, :], jnp.sin(angles)[:, None, :]


def apply_rope(values, cos_tab, sin_tab):
    half_dim = values.shape[-1] // 2
    first_half = values[..., :half_dim]
    second_half = values[..., half_dim:]
    return jnp.concatenate([first_half * cos_tab - second_half * sin_tab, second_half * cos_tab + first_half * sin_tab], axis=-1)


def rcopy(src, dst, send, recv, **where):
    return pltpu.make_async_remote_copy(src_ref=src, dst_ref=dst, send_sem=send, recv_sem=recv, device_id=dict(where), device_id_type=MESH)


def plane():
    p = lax.axis_index('dp')
    y, x, c = p // 4, (p // 2) % 2, p % 2

    def at(rel):
        yy = 1 - y if rel & 4 else y
        xx = 1 - x if rel & 2 else x
        cc = 1 - c if rel & 1 else c
        return yy * 4 + xx * 2 + cc
    return p, at


def entry_barrier(z, n, at):
    bar = pltpu.get_barrier_semaphore()
    for rel in range(1, 8):
        pl.semaphore_signal(bar, inc=1, device_id={'dp': at(rel)}, device_id_type=MESH)

    @pl.when(z > 0)
    def _():
        pl.semaphore_signal(bar, inc=1, device_id={'tp': z - 1}, device_id_type=MESH)

    @pl.when(z < n - 1)
    def _():
        pl.semaphore_signal(bar, inc=1, device_id={'tp': z + 1}, device_id_type=MESH)
    inner = (z > 0) & (z < n - 1)

    @pl.when(inner)
    def _():
        pl.semaphore_wait(bar, 9)

    @pl.when(jnp.logical_not(inner))
    def _():
        pl.semaphore_wait(bar, 8)


LAG = 3


def chain_sum(k, z, n, rows, chunks, part, left, right, done, send_r, send_l, recv_l, recv_r):
    last = n - 1

    def cut(ref, c):
        return ref.at[pl.ds(pl.multiple_of(c * rows, rows), rows)]

    def load(ref, c):
        return ref[pl.ds(pl.multiple_of(c * rows, rows), rows)]

    def store(ref, c, value):
        ref[pl.ds(pl.multiple_of(c * rows, rows), rows)] = value
    cl, cr = k - LAG * z, k - LAG * (last - z)
    okl, okr = (cl >= 0) & (cl < chunks), (cr >= 0) & (cr < chunks)

    @pl.when(okl & (z > 0))
    def _():
        rcopy(cut(left, cl), cut(left, cl), send_r, recv_l.at[cl], tp=z).wait_recv()

    @pl.when(okl & (z == last))
    def _():
        done(cl, load(left, cl) + load(part, cl))

    @pl.when(okl & (z > 0) & (z < last))
    def _():
        run = load(left, cl)

        @pl.when(z >= n // 2)
        def _():
            done(cl, run + load(right, cl))
        store(left, cl, run + load(part, cl))

    @pl.when(okr & (z < last))
    def _():
        rcopy(cut(right, cr), cut(right, cr), send_l, recv_r.at[cr], tp=z).wait_recv()

    @pl.when(okr & (z == 0))
    def _():
        done(cr, load(part, cr) + load(right, cr))

    @pl.when(okr & (z > 0) & (z < last))
    def _():
        run = load(right, cr)

        @pl.when(z < n // 2)
        def _():
            done(cr, load(left, cr) + run)
        store(right, cr, run + load(part, cr))

    @pl.when(okl & (z == 0))
    def _():
        rcopy(cut(part, cl), cut(left, cl), send_r, recv_l.at[cl], tp=z + 1).start()

    @pl.when(okl & (z > 0) & (z < last))
    def _():
        rcopy(cut(left, cl), cut(left, cl), send_r, recv_l.at[cl], tp=z + 1).start()

    @pl.when(okr & (z == last))
    def _():
        rcopy(cut(part, cr), cut(right, cr), send_l, recv_r.at[cr], tp=z - 1).start()

    @pl.when(okr & (z > 0) & (z < last))
    def _():
        rcopy(cut(right, cr), cut(right, cr), send_l, recv_r.at[cr], tp=z - 1).start()


def chain_drain(z, n, part, left, right, send_r, send_l, recv_l, recv_r):
    @pl.when(z < n - 1)
    def _():
        rcopy(part, left, send_r, recv_l.at[0], tp=z + 1).wait_send()

    @pl.when(z > 0)
    def _():
        rcopy(part, right, send_l, recv_r.at[0], tp=z - 1).wait_send()


def emb_kernel(n, rows, chunks, part, piece, toks, out, wall, tok_all, left, right, send_r, send_l, recv_l, recv_r, tsend, trecv, tself, zsend, zrecv, psend, precv):
    z = lax.axis_index('tp')
    p, at = plane()
    entry_barrier(z, n, at)
    width = piece.shape[0]
    half = width // 2
    @pl.when(z < n - 1)
    def _():
        rcopy(piece, wall.at[z, p], zsend.at[0], zrecv.at[0], tp=z + 1).start()

    @pl.when(z > 0)
    def _():
        rcopy(piece, wall.at[z, p], zsend.at[n - 1], zrecv.at[n - 1], tp=z - 1).start()
    own = pltpu.make_async_copy(toks, tok_all.at[p], tself)
    own.start()
    for rel in range(1, 8):
        rcopy(toks, tok_all.at[p], tsend.at[rel], trecv.at[rel], dp=at(rel)).start()

    def each(d, body):
        @pl.when(z >= d)
        def _():
            body(2 * (d - 1), z - d, 0)

        @pl.when(z + d < n)
        def _():
            body(2 * (d - 1) + 1, z + d, 1)

    def arrive(d):
        def body(i, t, side):
            blk = wall.at[t, p]
            s = d - 1 if side == 0 else 2 * n - 2 - d + 1 - (n - 1) + 0
            s = d - 1 if side == 0 else n - 1 + d - 1
            rcopy(blk, blk, zsend.at[s], zrecv.at[s], tp=z).wait_recv()
            if d < n - 1:
                if side == 0:
                    @pl.when(z < n - 1)
                    def _():
                        rcopy(blk, blk, zsend.at[d], zrecv.at[d], tp=z + 1).start()
                else:
                    @pl.when(z > 0)
                    def _():
                        rcopy(blk, blk, zsend.at[n - 1 + d], zrecv.at[n - 1 + d], tp=z - 1).start()
            for j, rel in enumerate((2, 4, 1)):
                rcopy(blk, blk, psend.at[i, j], precv.at[i, j], dp=at(rel)).start()
        each(d, body)

    def cross(d):
        def body(i, t, side):
            bx, by = wall.at[t, at(2)], wall.at[t, at(4)]
            rcopy(bx, bx, psend.at[i, 0], precv.at[i, 0], dp=p).wait_recv()
            top = wall.at[t, at(2), pl.ds(0, half)]
            rcopy(top, top, psend.at[i, 3], precv.at[i, 3], dp=at(4)).start()
            rcopy(bx, bx, psend.at[i, 5], precv.at[i, 5], dp=at(1)).start()
            rcopy(by, by, psend.at[i, 1], precv.at[i, 1], dp=p).wait_recv()
            low = wall.at[t, at(4), pl.ds(half, half)]
            rcopy(low, low, psend.at[i, 4], precv.at[i, 4], dp=at(2)).start()
            rcopy(by, by, psend.at[i, 6], precv.at[i, 6], dp=at(1)).start()
        each(d, body)

    def diagonal(d):
        def body(i, t, side):
            top, low = wall.at[t, at(6), pl.ds(0, half)], wall.at[t, at(6), pl.ds(half, half)]
            rcopy(top, top, psend.at[i, 3], precv.at[i, 3], dp=p).wait_recv()
            rcopy(top, top, psend.at[i, 7], precv.at[i, 7], dp=at(1)).start()
            rcopy(low, low, psend.at[i, 4], precv.at[i, 4], dp=p).wait_recv()
            rcopy(low, low, psend.at[i, 8], precv.at[i, 8], dp=at(1)).start()
        each(d, body)

    def finish(d):
        def body(i, t, side):
            def both(j, mine, theirs):
                rcopy(mine, mine, psend.at[i, j], precv.at[i, j], dp=p).wait_send()
                if theirs is not None:
                    rcopy(theirs, theirs, psend.at[i, j], precv.at[i, j], dp=p).wait_recv()
            both(0, wall.at[t, p], None)
            both(1, wall.at[t, p], None)
            both(2, wall.at[t, p], wall.at[t, at(1)])
            both(3, wall.at[t, at(2), pl.ds(0, half)], None)
            both(4, wall.at[t, at(4), pl.ds(half, half)], None)
            both(5, wall.at[t, at(2)], wall.at[t, at(3)])
            both(6, wall.at[t, at(4)], wall.at[t, at(5)])
            both(7, wall.at[t, at(6), pl.ds(0, half)], wall.at[t, at(7), pl.ds(0, half)])
            both(8, wall.at[t, at(6), pl.ds(half, half)], wall.at[t, at(7), pl.ds(half, half)])
        each(d, body)

    for d in range(1, n):
        arrive(d)

    def done(c, value):
        out[pl.ds(pl.multiple_of(c * rows, rows), rows)] = value.astype(out.dtype)

    events = [cross(d) if False else functools.partial(cross, d) for d in range(1, n)] + [functools.partial(diagonal, d) for d in range(1, n)]
    when = [3, 8, 13, 19, 22, 26]

    @pl.loop(0, chunks + LAG * (n - 1))
    def _(k):
        chain_sum(k, z, n, rows, chunks, part, left, right, done, send_r, send_l, recv_l, recv_r)
        for at_step, event in zip(when, events):
            @pl.when(k == at_step)
            def _(event=event):
                event()

    chain_drain(z, n, part, left, right, send_r, send_l, recv_l, recv_r)
    for d in range(1, n):
        finish(d)
    own.wait()
    for rel in range(1, 8):
        rcopy(toks, tok_all.at[at(rel)], tsend.at[rel], trecv.at[rel], dp=at(rel)).wait()

    @pl.when(z < n - 1)
    def _():
        rcopy(piece, wall.at[z, p], zsend.at[0], zrecv.at[0], tp=z + 1).wait_send()

    @pl.when(z > 0)
    def _():
        rcopy(piece, wall.at[z, p], zsend.at[n - 1], zrecv.at[n - 1], tp=z - 1).wait_send()
    for d in range(1, n - 1):
        @pl.when((z >= d) & (z < n - 1))
        def _(d=d):
            rcopy(wall.at[z - d, p], wall.at[z - d, p], zsend.at[d], zrecv.at[d], tp=z).wait_send()

        @pl.when((z + d < n) & (z > 0))
        def _(d=d):
            rcopy(wall.at[z + d, p], wall.at[z + d, p], zsend.at[n - 1 + d], zrecv.at[n - 1 + d], tp=z).wait_send()


def embed(part, piece, toks, n_tp, n_dp):
    seq, width = part.shape
    chunks = 32
    rows = seq // chunks
    dma = pltpu.SemaphoreType.DMA
    return pl.pallas_call(
        functools.partial(emb_kernel, n_tp, rows, chunks),
        name='embed',
        out_shape=(jax.ShapeDtypeStruct((seq, width), BF), jax.ShapeDtypeStruct((n_tp, n_dp) + piece.shape, F32), jax.ShapeDtypeStruct((n_dp,) + toks.shape, toks.dtype)),
        in_specs=[VMEM, ANY, ANY],
        out_specs=(VMEM, ANY, ANY),
        scratch_shapes=[pltpu.VMEM((seq, width), F32), pltpu.VMEM((seq, width), F32), dma, dma, dma((chunks,)), dma((chunks,)),
                        dma((8,)), dma((8,)), dma, dma((2 * n_tp - 2,)), dma((2 * n_tp - 2,)), dma((2 * n_tp - 2, 9)), dma((2 * n_tp - 2, 9))],
        compiler_params=pltpu.CompilerParams(collective_id=0, has_side_effects=True, vmem_limit_bytes=56 * 2 ** 20),
        cost_estimate=pl.CostEstimate(flops=20 * 10 ** 9, bytes_accessed=80 * 2 ** 20, transcendentals=0),
    )(part, piece, toks)


def scatter_sum_kernel(n, rows, chunks, part, out, left, right, total, send_r, send_l, recv_l, recv_r, osend, orecv, oself):
    z = lax.axis_index('tp')
    p, at = plane()
    entry_barrier(z, n, at)
    block = out.shape[2]
    lead = jnp.maximum(z, n - 1 - z)

    def done(c, value):
        total[pl.ds(pl.multiple_of(c * rows, rows), rows)] = value

    def cols(q, c=None):
        sel = pl.ds(pl.multiple_of(q * block, block), block)
        return total.at[:, sel] if c is None else total.at[pl.ds(pl.multiple_of(c * rows, rows), rows), sel]

    @pl.loop(0, chunks + LAG * (n - 1) + 1)
    def _(k):
        c = k - LAG * lead - 1

        @pl.when((c >= 0) & (c < chunks))
        def _():
            where = out.at[p, pl.ds(pl.multiple_of(c * rows, rows), rows)]
            pltpu.make_async_copy(cols(p, c), where, oself).start()
            for rel in range(1, 8):
                rcopy(cols(at(rel), c), where, osend.at[rel], orecv.at[rel], dp=at(rel)).start()
        chain_sum(k, z, n, rows, chunks, part, left, right, done, send_r, send_l, recv_l, recv_r)

    chain_drain(z, n, part, left, right, send_r, send_l, recv_l, recv_r)
    pltpu.make_async_copy(cols(p), out.at[p], oself).wait()
    for rel in range(1, 8):
        rcopy(cols(at(rel)), out.at[at(rel)], osend.at[rel], orecv.at[rel], dp=at(rel)).wait()


def summed_columns(part, n_tp, n_dp):
    seq, width = part.shape
    chunks = 32
    rows = seq // chunks
    dma = pltpu.SemaphoreType.DMA
    return pl.pallas_call(
        functools.partial(scatter_sum_kernel, n_tp, rows, chunks),
        name='summed_columns',
        out_shape=jax.ShapeDtypeStruct((n_dp, seq, width // n_dp), F32),
        in_specs=[VMEM],
        out_specs=ANY,
        scratch_shapes=[pltpu.VMEM((seq, width), F32)] * 3 + [dma, dma, dma((chunks,)), dma((chunks,)), dma((8,)), dma((8,)), dma],
        compiler_params=pltpu.CompilerParams(collective_id=1, has_side_effects=True, vmem_limit_bytes=56 * 2 ** 20),
        cost_estimate=pl.CostEstimate(flops=14 * 10 ** 9, bytes_accessed=30 * 2 ** 20, transcendentals=0),
    )(part)


WAYS = 4


def table_kernel(ids, rows_ref, out, *tables):
    step = pl.program_id(0)
    count = rows_ref.shape[0]
    part = count // WAYS

    @pl.when(step == 0)
    def _():
        for table in tables:
            table[...] = jnp.zeros_like(table)

    @pl.loop(0, part, unroll=4)
    def _(r):
        for way, table in enumerate(tables):
            row = way * part + r
            where = pl.ds(ids[step * count + row], 1)
            table[where, :] = table[where, :] + rows_ref[pl.ds(row, 1), :]

    @pl.when(step == pl.num_programs(0) - 1)
    def _():
        total = tables[0][...]
        for table in tables[1:]:
            total = total + table[...]
        out[...] = SHRINK * total[:out.shape[0]]


def table_rows(ids, rows, vocab_loc):
    count, block = rows.shape
    step = min(1024, count // 2)
    return pl.pallas_call(
        table_kernel,
        name='table_rows',
        grid_spec=pltpu.PrefetchScalarGridSpec(
            num_scalar_prefetch=1,
            grid=(count // step,),
            in_specs=[pl.BlockSpec((step, block), lambda i, ids: (i, 0))],
            out_specs=pl.BlockSpec((vocab_loc, block), lambda i, ids: (0, 0)),
            scratch_shapes=[pltpu.VMEM((vocab_loc + 8, block), F32)] * WAYS,
        ),
        out_shape=jax.ShapeDtypeStruct((vocab_loc, block), F32),
        compiler_params=pltpu.CompilerParams(dimension_semantics=('arbitrary',), vmem_limit_bytes=48 * 2 ** 20),
        cost_estimate=pl.CostEstimate(flops=3 * 10 ** 9, bytes_accessed=16 * 2 ** 20, transcendentals=0),
    )(ids, rows)


def gather_kernel(parts, block_in, out, send, recv, oself):
    p, at = plane()
    bar = pltpu.get_barrier_semaphore()
    for rel in (1, 2, 4):
        pl.semaphore_signal(bar, inc=1, device_id={'dp': at(rel)}, device_id_type=MESH)
    pl.semaphore_wait(bar, 3)
    size, block = block_in.shape
    rows = size // parts
    half = parts // 2

    def region(q, i):
        return out.at[pl.ds(i * rows, rows), pl.ds(pl.multiple_of(q * block, block), block)]

    def mine(i):
        return block_in.at[pl.ds(i * rows, rows)]
    own = pltpu.make_async_copy(block_in, out.at[:, pl.ds(pl.multiple_of(p * block, block), block)], oself)
    own.start()
    order_x = list(range(parts))
    order_y = order_x[half:] + order_x[:half]
    for i, j in zip(order_x, order_y):
        rcopy(mine(i), region(p, i), send.at[0, i], recv.at[0, i], dp=at(2)).start()
        rcopy(mine(j), region(p, j), send.at[1, j], recv.at[1, j], dp=at(4)).start()
    for i in order_x:
        rcopy(mine(i), region(p, i), send.at[2, i], recv.at[2, i], dp=at(1)).start()

    def took(kind, rel, i):
        rcopy(region(at(rel), i), region(at(rel), i), send.at[kind, i], recv.at[kind, i], dp=p).wait_recv()

    def give(kind, rel, i, to):
        rcopy(region(at(rel), i), region(at(rel), i), send.at[kind, i], recv.at[kind, i], dp=at(to)).start()
    for i, j in zip(order_x, order_y):
        took(0, 2, i)
        if i < half:
            give(3, 2, i, 4)
        give(4, 2, i, 1)
        took(1, 4, j)
        if j >= half:
            give(3, 4, j, 2)
        give(5, 4, j, 1)
    for i, j in zip(order_x[:half], order_x[half:]):
        for part in (i, j):
            took(3, 6, part)
            give(6, 6, part, 1)
    for i in order_x:
        took(2, 1, i)
        took(4, 3, i)
        took(5, 5, i)
        took(6, 7, i)
    for i in order_x:
        for kind in (0, 1, 2):
            rcopy(mine(i), region(p, i), send.at[kind, i], recv.at[kind, i], dp=p).wait_send()
        rel = 2 if i < half else 4
        for kind, src in ((3, rel), (4, 2), (5, 4), (6, 6)):
            rcopy(region(at(src), i), region(at(src), i), send.at[kind, i], recv.at[kind, i], dp=p).wait_send()
    own.wait()


def gathered_columns(block_in, n_dp):
    size, block = block_in.shape
    parts = 4
    dma = pltpu.SemaphoreType.DMA
    return pl.pallas_call(
        functools.partial(gather_kernel, parts),
        name='gathered_columns',
        out_shape=jax.ShapeDtypeStruct((size, n_dp * block), F32),
        in_specs=[ANY],
        out_specs=ANY,
        scratch_shapes=[dma((7, parts)), dma((7, parts)), dma],
        compiler_params=pltpu.CompilerParams(collective_id=2, has_side_effects=True),
        cost_estimate=pl.CostEstimate(flops=10 * 10 ** 9, bytes_accessed=60 * 2 ** 20, transcendentals=0),
    )(block_in)


def dot(a, b, dims):
    return lax.dot_general(a, b, (dims, ((), ())), preferred_element_type=F32)


NT, TN, NN = ((1,), (1,)), ((0,), (0,)), ((1,), (0,))


def attention_kernel(scale, kb, q_ref, k_ref, v_ref, ctx_ref, m_ref, l_ref, s_ref):
    i = pl.program_id(1)
    qb = q_ref.shape[1]
    q = q_ref[0]
    blocks = ((i + 1) * qb + kb - 1) // kb

    def scores(j, top):
        at_k = pl.ds(pl.multiple_of(j * kb, kb), kb)
        s = dot(k_ref[0, at_k, :], q, NT) * scale
        key = j * kb + lax.broadcasted_iota(jnp.int32, (kb, qb), 0)
        query = i * qb + lax.broadcasted_iota(jnp.int32, (kb, qb), 1)
        s = jnp.where(query >= key, s, -1e30)
        s_ref[at_k, :] = s
        return jnp.maximum(top, jnp.max(s, axis=0, keepdims=True))
    top = lax.fori_loop(0, blocks, scores, jnp.full((1, qb), -1e30, F32))

    def weigh(j, total):
        at_k = pl.ds(pl.multiple_of(j * kb, kb), kb)
        e = jnp.exp(s_ref[at_k, :] - top)
        s_ref[at_k, :] = e
        return total + jnp.sum(e, axis=0, keepdims=True)
    total = lax.fori_loop(0, blocks, weigh, jnp.zeros((1, qb), F32))
    inv = 1.0 / total

    def mix(j, acc):
        at_k = pl.ds(pl.multiple_of(j * kb, kb), kb)
        probs = (s_ref[at_k, :] * inv).astype(BF)
        return acc + dot(probs, v_ref[0, at_k, :], TN)
    ctx_ref[0] = lax.fori_loop(0, blocks, mix, jnp.zeros((qb, v_ref.shape[2]), F32))
    m_ref[0] = top
    l_ref[0] = inv


def attention(q, k, v):
    heads, seq, dim = q.shape
    qb, kb = seq // 8, seq // 4
    spec_q = pl.BlockSpec((1, qb, dim), lambda h, i: (h, i, 0))
    spec_k = pl.BlockSpec((1, seq, dim), lambda h, i: (h, 0, 0))
    spec_s = pl.BlockSpec((1, 1, qb), lambda h, i: (h, 0, i))
    stat = jax.ShapeDtypeStruct((heads, 1, seq), F32)
    return pl.pallas_call(
        functools.partial(attention_kernel, dim ** -0.5, kb),
        name='attention',
        grid=(heads, seq // qb),
        in_specs=[spec_q, spec_k, spec_k],
        out_specs=(spec_q, spec_s, spec_s),
        out_shape=(jax.ShapeDtypeStruct((heads, seq, dim), F32), stat, stat),
        scratch_shapes=[pltpu.VMEM((seq, qb), F32)],
        compiler_params=pltpu.CompilerParams(dimension_semantics=('arbitrary', 'arbitrary'), vmem_limit_bytes=32 * 2 ** 20),
        cost_estimate=pl.CostEstimate(flops=3 * 10 ** 9, bytes_accessed=8 * 2 ** 20, transcendentals=10 ** 7),
    )(q, k, v)


def attention_grad_kernel(scale, kb, q_ref, k_ref, v_ref, c_ref, dc_ref, m_ref, l_ref, dq_ref, dk_ref, dv_ref):
    i = pl.program_id(1)
    qb = q_ref.shape[1]
    q, dc = q_ref[0], dc_ref[0]
    dc_f = dc.astype(F32)
    top, inv = m_ref[0], l_ref[0]
    ones = jnp.ones((8, dc.shape[1]), F32)
    mean = lax.dot_general(ones, dc_f * c_ref[0], (NT, ((), ())), precision=lax.Precision.HIGHEST, preferred_element_type=F32)[:1]
    blocks = ((i + 1) * qb + kb - 1) // kb

    @pl.when(i == 0)
    def _():
        dk_ref[...] = jnp.zeros_like(dk_ref)
        dv_ref[...] = jnp.zeros_like(dv_ref)

    def step(j, dq):
        at_k = pl.ds(pl.multiple_of(j * kb, kb), kb)
        keys = k_ref[0, at_k, :]
        s = dot(keys, q, NT) * scale
        key = j * kb + lax.broadcasted_iota(jnp.int32, (kb, qb), 0)
        query = i * qb + lax.broadcasted_iota(jnp.int32, (kb, qb), 1)
        probs = (jnp.exp(jnp.where(query >= key, s, -1e30) - top) * inv).astype(BF)
        d_probs = dot(v_ref[0, at_k, :], dc, NT)
        ds = (probs.astype(F32) * (d_probs - mean) * scale).astype(BF)
        dv_ref[0, at_k, :] += dot(probs, dc, NN)
        dk_ref[0, at_k, :] += dot(ds, q, NN)
        return dq + dot(ds, keys, TN)
    dq_ref[0] = lax.fori_loop(0, blocks, step, jnp.zeros((qb, q.shape[1]), F32))


def attention_grad(q, k, v, ctx, dctx, top, inv):
    heads, seq, dim = q.shape
    qb, kb = seq // 8, seq // 4
    spec_q = pl.BlockSpec((1, qb, dim), lambda h, i: (h, i, 0))
    spec_k = pl.BlockSpec((1, seq, dim), lambda h, i: (h, 0, 0))
    spec_s = pl.BlockSpec((1, 1, qb), lambda h, i: (h, 0, i))
    out = jax.ShapeDtypeStruct((heads, seq, dim), F32)
    return pl.pallas_call(
        functools.partial(attention_grad_kernel, dim ** -0.5, kb),
        name='attention_grad',
        grid=(heads, seq // qb),
        in_specs=[spec_q, spec_k, spec_k, spec_q, spec_q, spec_s, spec_s],
        out_specs=(spec_q, spec_k, spec_k),
        out_shape=(out, out, out),
        compiler_params=pltpu.CompilerParams(dimension_semantics=('arbitrary', 'arbitrary'), vmem_limit_bytes=32 * 2 ** 20),
        cost_estimate=pl.CostEstimate(flops=8 * 10 ** 9, bytes_accessed=16 * 2 ** 20, transcendentals=10 ** 7),
    )(q, k, v, ctx, dctx, top, inv)


def solution(mesh):
    n_tp, n_dp = mesh.shape['tp'], mesh.shape['dp']
    in_specs = (P('dp', None), P('dp', None, None), P('tp', None)) + WEIGHT_SPECS
    out_specs = (P('tp', None),) + WEIGHT_SPECS

    def flipped(values, rel):
        return lax.ppermute(values, 'dp', [(d, d ^ rel) for d in range(n_dp)])

    def device_step(tokens, cotangent, emb_table, *weights):
        (w_qkv, b_qkv, w_out, b_out, ln1_gain, ln1_bias, w_gate, b_gate, w_lin, b_lin, w_down, b_down, ln2_gain) = weights
        tp, dp = lax.axis_index('tp'), lax.axis_index('dp')
        tokens = tokens[0]
        seq_len, width = tokens.shape[0], emb_table.shape[1]
        heads, head_dim = b_qkv.shape[0], b_qkv.shape[1] // 3
        own = seq_len // n_tp
        ffn = w_gate.shape[1]
        rk, rf, ro = width // n_dp, ffn // n_dp, w_out.shape[0] // n_dp
        zero = jnp.minimum(tokens[0], 0).astype(F32)

        def cut(weight):
            rows = weight.shape[0] // n_dp
            return lax.dynamic_slice_in_dim(weight, dp * rows, rows, 0)
        bias_rows = jnp.concatenate([b_gate[None], b_lin[None], jnp.zeros((14, ffn), BF)], axis=0)
        piece = jnp.concatenate([cut(w_gate), cut(w_lin), cut(w_down), cut(w_out), bias_rows], axis=0).astype(F32)

        vocab_loc = emb_table.shape[0]
        local_ids = tokens - tp * vocab_loc
        in_shard = (local_ids >= 0) & (local_ids < vocab_loc)
        safe_ids = jnp.where(in_shard, local_ids, 0)
        own_rows = jnp.where(in_shard[:, None], jnp.take(emb_table, safe_ids, axis=0), 0.0).astype(F32)
        emb_bf, wall, tok_all = embed(own_rows, piece, tokens.reshape(-1, min(128, seq_len // 8)), n_tp, n_dp)

        is_own = (jnp.arange(n_tp) == tp)[:, None, None]

        def whole(start, rows, local):
            return jnp.where(is_own, local[None], wall[:, :, start:start + rows].reshape(n_tp, n_dp * rows, local.shape[1]).astype(local.dtype))
        wg_full = whole(0, rk, w_gate)
        wl_full = whole(rk, rk, w_lin)
        wd_full = whole(2 * rk, rf, w_down)
        wo_full = whole(2 * rk + rf, ro, w_out)
        base = 2 * rk + rf + ro
        bg_full = jnp.where(is_own[:, 0], b_gate[None].astype(F32), wall[:, 0, base])
        bl_full = jnp.where(is_own[:, 0], b_lin[None].astype(F32), wall[:, 0, base + 1])

        qkv_pre = jnp.dot(emb_bf, w_qkv, preferred_element_type=F32) + b_qkv.reshape(-1).astype(F32)
        qkv_all = qkv_pre.astype(BF).reshape(seq_len, heads, 3, head_dim)
        cos_tab, sin_tab = rope_tables(seq_len, head_dim)
        queries = apply_rope(qkv_all[:, :, 0].astype(F32), cos_tab, sin_tab).astype(BF).transpose(1, 0, 2)
        keys_rot = apply_rope(qkv_all[:, :, 1].astype(F32), cos_tab, sin_tab).astype(BF).transpose(1, 0, 2)
        values = qkv_all[:, :, 2].transpose(1, 0, 2)
        ctx, top, inv = attention(queries, keys_rot, values)
        context = ctx.transpose(1, 0, 2).reshape(n_tp, own, heads * head_dim)
        ctx_own = (lax.all_to_all(context, 'tp', 0, 0) + zero).astype(BF)

        emb_own = lax.dynamic_slice_in_dim(emb_bf, tp * own, own, 0).astype(F32)
        cot_own = lax.dynamic_slice_in_dim(cotangent[0], tp * own, own, 0).astype(F32)
        attn_out = jnp.einsum('hse,hed->sd', ctx_own, wo_full, preferred_element_type=F32) + b_out.astype(F32)
        normed_one, norm_one_pull = jax.vjp(norm_scaled, ALPHA * emb_own + attn_out, ln1_gain.astype(F32))
        hidden = (normed_one + ln1_bias.astype(F32)).astype(BF)
        gate_pre = jnp.einsum('sk,tkc->tsc', hidden, wg_full, preferred_element_type=F32) + bg_full[:, None]
        lin_pre = jnp.einsum('sk,tkc->tsc', hidden, wl_full, preferred_element_type=F32) + bl_full[:, None]
        inner_val, act_pull = jax.vjp(geglu, gate_pre, lin_pre)
        inner_act = inner_val.astype(BF)
        ffn_out = jnp.einsum('tsc,tcd->sd', inner_act, wd_full, preferred_element_type=F32) + b_down.astype(F32)
        norm_two_pull = jax.vjp(norm_scaled, ALPHA * hidden.astype(F32) + ffn_out, ln2_gain.astype(F32))[1]

        rel_blocks = jnp.arange(n_dp // 2) * 2

        def reduced(lhs, rhs, spec):
            blocks = lhs.reshape(lhs.shape[:-1] + (n_dp, lhs.shape[-1] // n_dp))

            def product(first):
                chosen = jnp.take(blocks, (rel_blocks + first) ^ dp, axis=-2).reshape(lhs.shape[:-1] + (-1,))
                return jnp.einsum(spec, chosen, rhs, preferred_element_type=F32)
            theirs = flipped(product(1), 1)
            both = (product(0) + theirs)
            rows = lhs.shape[-1] // n_dp
            both = both.reshape(n_tp, 4, rows, both.shape[-1])
            h = rows // 2
            xa = flipped(both[:, 1::2, :h], 2)
            yb = flipped(both[:, 2:, h:], 4)
            a0, a2 = both[:, 0, :h] + xa[:, 0], both[:, 2, :h] + xa[:, 1]
            b0, b1 = both[:, 0, h:] + yb[:, 0], both[:, 1, h:] + yb[:, 1]
            ya, xb = flipped(a2, 4), flipped(b1, 2)
            mine = jnp.concatenate([a0 + ya, b0 + xb], axis=1)
            total = lax.dynamic_index_in_dim(mine, tp, 0, keepdims=False)
            for shift in [s for d in range(1, n_tp) for s in (d, -d)]:
                part = lax.dynamic_index_in_dim(mine, jnp.clip(tp + shift, 0, n_tp - 1), 0, keepdims=False)
                total = total + lax.ppermute(part, 'tp', [(t, t + shift) for t in range(n_tp) if 0 <= t + shift < n_tp])
            return lax.all_gather(total, 'dp', axis=0, tiled=True)

        d_resid_two, d_ln2_gain = norm_two_pull(cot_own)
        d_b_down = jnp.sum(d_resid_two, axis=0)
        d_ffn_bf = d_resid_two.astype(BF)
        d_w_down = reduced(inner_act, d_ffn_bf, 'tsc,sd->tcd')
        d_inner = jnp.einsum('sd,tcd->tsc', d_ffn_bf, wd_full, preferred_element_type=F32).astype(BF)
        d_gate_pre, d_lin_pre = act_pull(d_inner.astype(F32))
        d_b_gate = jnp.sum(d_gate_pre, axis=1)
        d_b_lin = jnp.sum(d_lin_pre, axis=1)
        d_gate_bf = d_gate_pre.astype(BF)
        d_lin_bf = d_lin_pre.astype(BF)
        d_w_gate = reduced(hidden, d_gate_bf, 'sk,tsc->tkc')
        d_w_lin = reduced(hidden, d_lin_bf, 'sk,tsc->tkc')
        d_hidden = ALPHA * d_resid_two + jnp.einsum('tsc,tkc->sk', d_gate_bf, wg_full, preferred_element_type=F32) + jnp.einsum('tsc,tkc->sk', d_lin_bf, wl_full, preferred_element_type=F32)
        d_ln1_bias = jnp.sum(d_hidden, axis=0)
        d_resid_one, d_ln1_gain = norm_one_pull(d_hidden)
        d_b_out = jnp.sum(d_resid_one, axis=0)
        d_attn_bf = d_resid_one.astype(BF)
        d_w_out = jnp.einsum('hse,sd->hed', ctx_own, d_attn_bf, preferred_element_type=F32)
        d_w_out = lax.all_gather(lax.psum_scatter(d_w_out.reshape(-1, width), ALL, scatter_dimension=0, tiled=True), 'dp', axis=0, tiled=True)
        d_ctx = jnp.einsum('sd,hed->hse', d_attn_bf, wo_full, preferred_element_type=F32)
        d_context = (lax.all_to_all(d_ctx, 'tp', 0, 0) + zero).astype(BF).reshape(seq_len, heads, head_dim).transpose(1, 0, 2)

        d_queries, d_keys, d_values = attention_grad(queries, keys_rot, values, ctx, d_context, top, inv)
        d_queries = apply_rope(d_queries.transpose(1, 0, 2), cos_tab, -sin_tab)
        d_keys = apply_rope(d_keys.transpose(1, 0, 2), cos_tab, -sin_tab)
        d_qkv = jnp.stack([d_queries, d_keys, d_values.transpose(1, 0, 2)], axis=2).reshape(seq_len, -1)
        d_b_qkv = jnp.sum(d_qkv, axis=0)
        d_qkv_bf = d_qkv.astype(BF)
        d_w_qkv = lax.psum(jnp.dot(emb_bf.T, d_qkv_bf, preferred_element_type=F32), 'dp')
        d_emb_part = jnp.dot(d_qkv_bf, w_qkv.T, preferred_element_type=F32)
        d_emb_part = lax.dynamic_update_slice_in_dim(d_emb_part, lax.dynamic_slice_in_dim(d_emb_part, tp * own, own, 0) + ALPHA * d_resid_one, tp * own, 0)
        d_cols = summed_columns(d_emb_part, n_tp, n_dp)
        all_ids = tok_all.reshape(-1) - tp * vocab_loc
        all_ids = jnp.where((all_ids >= 0) & (all_ids < vocab_loc), all_ids, vocab_loc)
        d_table = gathered_columns(table_rows(all_ids, d_cols.reshape(n_dp * seq_len, -1), vocab_loc), n_dp)

        slot = (jnp.arange(n_tp) == tp).astype(F32)[:, None]
        d_bq_rows = jnp.pad(slot * d_b_qkv[None], ((0, 0), (0, ffn - d_b_qkv.shape[0])))
        small = jnp.concatenate([d_b_gate, d_b_lin, d_bq_rows, jnp.stack([d_b_out, d_ln1_gain, d_ln1_bias, d_b_down, d_ln2_gain])], axis=0)
        small = lax.psum(small, ALL)
        d_b_gate = lax.dynamic_index_in_dim(small[:n_tp], tp, 0, keepdims=False)
        d_b_lin = lax.dynamic_index_in_dim(small[n_tp:2 * n_tp], tp, 0, keepdims=False)
        d_b_qkv = lax.dynamic_index_in_dim(small[2 * n_tp:3 * n_tp], tp, 0, keepdims=False)[:d_b_qkv.shape[0]].reshape(heads, 3 * head_dim)
        d_b_out, d_ln1_gain, d_ln1_bias, d_b_down, d_ln2_gain = [small[3 * n_tp + i] for i in range(5)]
        return (d_table, d_w_qkv, d_b_qkv, d_w_out, d_b_out, d_ln1_gain, d_ln1_bias, d_w_gate, d_b_gate, d_w_lin, d_b_lin, d_w_down, d_b_down, d_ln2_gain)

    return jax.shard_map(device_step, mesh=mesh, in_specs=in_specs, out_specs=out_specs, check_vma=False)
```

```python
import functools

import jax
import jax.numpy as jnp
from jax import lax
from jax.experimental import pallas as pl
from jax.experimental.pallas import tpu as pltpu
from jax.sharding import PartitionSpec as P

ALPHA = 140.0 ** 0.5
EPS = 1e-5
SHRINK = 0.1
ROPE_BASE = 10000.0
WEIGHT_SPECS = (P(None, 'tp'), P('tp', None), P('tp', None), P(), P(), P(), P(None, 'tp'), P('tp'), P(None, 'tp'), P('tp'), P('tp', None), P(), P())
ALL = ('tp', 'dp')
BF = jnp.bfloat16
N0, N1, N2 = range(3)
F32 = jnp.float32
MESH = pl.DeviceIdType.MESH
ANY = pl.BlockSpec(memory_space=pl.ANY)
VMEM = pl.BlockSpec(memory_space=pltpu.VMEM)


def norm_scaled(values, gain):
    mean_val = jnp.mean(values, axis=-1, keepdims=True)
    centered = values - mean_val
    variance = jnp.mean(centered * centered, axis=-1, keepdims=True)
    return centered * lax.rsqrt(variance + EPS) * gain


def geglu(gate_pre, lin_pre):
    return jax.nn.gelu(gate_pre, approximate=False) * lin_pre


def rope_tables(seq_len, head_dim):
    half_dim = head_dim // 2
    inv_freq = ROPE_BASE ** (-2.0 * jnp.arange(half_dim, dtype=F32) / head_dim)
    angles = jnp.arange(seq_len, dtype=F32)[:, None] * inv_freq[None, :]
    return jnp.cos(angles)[:, None, :], jnp.sin(angles)[:, None, :]


def apply_rope(values, cos_tab, sin_tab):
    half_dim = values.shape[-1] // 2
    first_half = values[..., :half_dim]
    second_half = values[..., half_dim:]
    return jnp.concatenate([first_half * cos_tab - second_half * sin_tab, second_half * cos_tab + first_half * sin_tab], axis=-1)


def rcopy(src, dst, send, recv, **where):
    return pltpu.make_async_remote_copy(src_ref=src, dst_ref=dst, send_sem=send, recv_sem=recv, device_id=dict(where), device_id_type=MESH)


def plane():
    p = lax.axis_index('dp')
    y, x, c = p // 4, (p // 2) % 2, p % 2

    def at(rel):
        yy = 1 - y if rel & 4 else y
        xx = 1 - x if rel & 2 else x
        cc = 1 - c if rel & 1 else c
        return yy * 4 + xx * 2 + cc
    return p, at


def entry_barrier(z, n, at):
    bar = pltpu.get_barrier_semaphore()
    for rel in range(1, 8):
        pl.semaphore_signal(bar, inc=1, device_id={'dp': at(rel)}, device_id_type=MESH)

    @pl.when(z > 0)
    def _():
        pl.semaphore_signal(bar, inc=1, device_id={'tp': z - 1}, device_id_type=MESH)

    @pl.when(z < n - 1)
    def _():
        pl.semaphore_signal(bar, inc=1, device_id={'tp': z + 1}, device_id_type=MESH)
    inner = (z > 0) & (z < n - 1)

    @pl.when(inner)
    def _():
        pl.semaphore_wait(bar, 9)

    @pl.when(jnp.logical_not(inner))
    def _():
        pl.semaphore_wait(bar, 8)


LAG = 3


def chain_sum(k, z, n, rows, chunks, part, left, right, done, send_r, send_l, recv_l, recv_r):
    last = n - 1

    def cut(ref, c):
        return ref.at[pl.ds(pl.multiple_of(c * rows, rows), rows)]

    def load(ref, c):
        return ref[pl.ds(pl.multiple_of(c * rows, rows), rows)]

    def store(ref, c, value):
        ref[pl.ds(pl.multiple_of(c * rows, rows), rows)] = value
    cl, cr = k - LAG * z, k - LAG * (last - z)
    okl, okr = (cl >= 0) & (cl < chunks), (cr >= 0) & (cr < chunks)

    @pl.when(okl & (z > 0))
    def _():
        rcopy(cut(left, cl), cut(left, cl), send_r, recv_l.at[cl], tp=z).wait_recv()

    @pl.when(okl & (z == last))
    def _():
        done(cl, load(left, cl) + load(part, cl))

    @pl.when(okl & (z > 0) & (z < last))
    def _():
        run = load(left, cl)

        @pl.when(z >= n // 2)
        def _():
            done(cl, run + load(right, cl))
        store(left, cl, run + load(part, cl))

    @pl.when(okr & (z < last))
    def _():
        rcopy(cut(right, cr), cut(right, cr), send_l, recv_r.at[cr], tp=z).wait_recv()

    @pl.when(okr & (z == 0))
    def _():
        done(cr, load(part, cr) + load(right, cr))

    @pl.when(okr & (z > 0) & (z < last))
    def _():
        run = load(right, cr)

        @pl.when(z < n // 2)
        def _():
            done(cr, load(left, cr) + run)
        store(right, cr, run + load(part, cr))

    @pl.when(okl & (z == 0))
    def _():
        rcopy(cut(part, cl), cut(left, cl), send_r, recv_l.at[cl], tp=z + 1).start()

    @pl.when(okl & (z > 0) & (z < last))
    def _():
        rcopy(cut(left, cl), cut(left, cl), send_r, recv_l.at[cl], tp=z + 1).start()

    @pl.when(okr & (z == last))
    def _():
        rcopy(cut(part, cr), cut(right, cr), send_l, recv_r.at[cr], tp=z - 1).start()

    @pl.when(okr & (z > 0) & (z < last))
    def _():
        rcopy(cut(right, cr), cut(right, cr), send_l, recv_r.at[cr], tp=z - 1).start()


def chain_drain(z, n, part, left, right, send_r, send_l, recv_l, recv_r):
    @pl.when(z < n - 1)
    def _():
        rcopy(part, left, send_r, recv_l.at[0], tp=z + 1).wait_send()

    @pl.when(z > 0)
    def _():
        rcopy(part, right, send_l, recv_r.at[0], tp=z - 1).wait_send()


EDGES = ((0, 0, 2), (0, 0, 4), (0, 0, 1), (2, 1, 4), (4, 2, 2), (2, 0, 1), (4, 0, 1), (6, 1, 1), (6, 2, 1))
CROSS, DIAGONAL, LAST = ((0, 3, 5), (1, 4, 6)), ((3, 7), (4, 8)), {1: (2,), 3: (5,), 5: (6,), 7: (7, 8)}
STEPS = (3, 8, 13, 19, 22, 26)
FIRST = 17
ORDER = (0, 2, 4, 1, 3, 5, 6, 7)


def emb_kernel(n, rows, chunks, cuts, part, piece, toks, *refs):
    m = len(cuts)
    local, outs = refs[:m], refs[m + N1:N2 * m + N1]
    out, (bias, tok_all, wall, left, right, raw, low, send_r, send_l, recv_l, recv_r, tsend, trecv, tself, zsend, zrecv, psend, precv, lsem, isem, osem, bsem) = refs[m], refs[N2 * m + N1:]
    z = lax.axis_index('tp')
    p, at = plane()
    entry_barrier(z, n, at)
    half = piece.shape[N0] // N2

    @pl.when(z < n - N1)
    def _():
        rcopy(piece, wall.at[z, p], zsend.at[z], zrecv.at[z], tp=z + N1).start()

    @pl.when(z > N0)
    def _():
        rcopy(piece, wall.at[z, p], bsem.at[N1], zrecv.at[z], tp=z - N1).start()
    mine = [pltpu.make_async_copy(toks, tok_all.at[p], tself)]
    mine += [pltpu.make_async_copy(src, dst.at[z], lsem.at[i]) for i, (src, dst) in enumerate(zip(local, outs))]
    for copy in mine:
        copy.start()
    for rel in range(N1, 8):
        rcopy(toks, tok_all.at[p], tsend.at[rel], trecv.at[rel], dp=at(rel)).start()

    def others(d, body):
        @pl.when(z >= d)
        def _():
            body(z - d, -N1)

        @pl.when(z + d < n)
        def _():
            body(z + d, N1)

    def region(t, rel, side):
        blk = wall.at[t, at(rel)]
        return blk if side == N0 else wall.at[t, at(rel), pl.ds((side - N1) * half, half)]

    def give(t, j):
        rel, side, to = EDGES[j]
        rcopy(region(t, rel, side), region(t, rel, side), psend.at[t, j], precv.at[t, j], dp=at(to)).start()

    def take(t, j):
        rel, side, to = EDGES[j]
        blk = region(t, rel ^ to, side)
        rcopy(blk, blk, psend.at[t, j], precv.at[t, j], dp=p).wait_recv()

    def gave(t, j):
        rel, side, to = EDGES[j]
        rcopy(region(t, rel, side), region(t, rel, side), psend.at[t, j], precv.at[t, j], dp=p).wait_send()

    def arrive(d):
        def body(t, sign):
            blk = wall.at[t, p]
            rcopy(blk, blk, zsend.at[t], zrecv.at[t], tp=z).wait_recv()

            @pl.when((z - sign >= N0) & (z - sign < n))
            def _():
                rcopy(blk, blk, zsend.at[t], zrecv.at[t], tp=z - sign).start()
            for j in range(3):
                give(t, j)
        others(d, body)

    def relay(d, moves):
        def body(t, sign):
            for first, *rest in moves:
                take(t, first)
                for j in rest:
                    give(t, j)
        others(d, body)

    for d in range(N1, n):
        arrive(d)

    def done(c, value):
        out[pl.ds(pl.multiple_of(c * rows, rows), rows)] = value.astype(out.dtype)

    def other(i):
        return i + (i + n - z) // n

    def loaded(i, rel, slot):
        return pltpu.make_async_copy(wall.at[other(i), at(rel), pl.ds(N0, cuts[-N1][N1])], raw.at[slot], isem.at[slot])

    def stored(i, rel, slot):
        return [pltpu.make_async_copy(low.at[slot, pl.ds(lo, hi - lo)], dst.at[other(i), at(rel)], osem.at[slot, k]) for k, ((lo, hi), dst) in enumerate(zip(cuts, outs))]
    plan = [(i, rel) for rel in ORDER for i in range(n - N1)]

    def prefetch(s):
        i, rel = plan[s]
        for j in LAST.get(rel, ()):
            take(other(i), j)
        loaded(i, rel, s % N2).start()

    def convert(s):
        i, rel = plan[s]
        loaded(i, rel, s % N2).wait()
        if s >= N2:
            for copy in stored(*plan[s - N2], s % N2):
                copy.wait()
        low[s % N2] = raw[s % N2].astype(low.dtype)
        if s + N1 < len(plan):
            prefetch(s + N1)
        for copy in stored(i, rel, s % N2):
            copy.start()
    events = [(STEPS[d - N1], functools.partial(relay, d, CROSS)) for d in range(N1, n)] + [(STEPS[d + n - N2], functools.partial(relay, d, DIAGONAL)) for d in range(N1, n)]
    events += [(FIRST - N1, functools.partial(prefetch, N0))] + [(FIRST + s, functools.partial(convert, s)) for s in range(len(plan))]

    @pl.loop(N0, max(chunks + LAG * (n - N1), FIRST + len(plan)))
    def _(k):
        chain_sum(k, z, n, rows, chunks, part, left, right, done, send_r, send_l, recv_l, recv_r)
        for at_step, event in events:
            pl.when(k == at_step)(event)

    chain_drain(z, n, part, left, right, send_r, send_l, recv_l, recv_r)
    for s in (len(plan) - N2, len(plan) - N1):
        for copy in stored(*plan[s], s % N2):
            copy.wait()

    def finish(t, sign):
        for j in range(len(EDGES)):
            gave(t, j)
        tail = pltpu.make_async_copy(wall.at[t, p, pl.ds(cuts[-N1][N1], bias.shape[N1])], bias.at[t], bsem.at[N0])
        tail.start()
        tail.wait()

        @pl.when((z - sign >= N0) & (z - sign < n))
        def _():
            rcopy(wall.at[t, p], wall.at[t, p], zsend.at[t], zrecv.at[t], tp=z).wait_send()
    for d in range(N1, n):
        others(d, finish)
    for copy in mine:
        copy.wait()
    for rel in range(N1, 8):
        rcopy(toks, tok_all.at[at(rel)], tsend.at[rel], trecv.at[rel], dp=at(rel)).wait()

    @pl.when(z < n - N1)
    def _():
        rcopy(piece, wall.at[z, p], zsend.at[z], zrecv.at[z], tp=z + N1).wait_send()

    @pl.when(z > N0)
    def _():
        rcopy(piece, wall.at[z, p], bsem.at[N1], zrecv.at[z], tp=z - N1).wait_send()


def embed(part, piece, toks, local, n_tp, n_dp):
    seq, width = part.shape
    rows = min(64, seq // 4)
    chunks = seq // rows
    cuts, lo = [], 0
    for weight in local:
        cuts.append((lo, lo + weight.shape[0] // n_dp))
        lo = cuts[-1][1]
    dma = pltpu.SemaphoreType.DMA
    shapes = [jax.ShapeDtypeStruct((seq, width), BF)]
    shapes += [jax.ShapeDtypeStruct((n_tp, n_dp, w.shape[0] // n_dp, w.shape[1]), BF) for w in local]
    shapes += [jax.ShapeDtypeStruct((n_tp, piece.shape[0] - lo, width), F32), jax.ShapeDtypeStruct((n_dp,) + toks.shape, toks.dtype), jax.ShapeDtypeStruct((n_tp, n_dp) + piece.shape, F32)]
    out = pl.pallas_call(
        functools.partial(emb_kernel, n_tp, rows, chunks, cuts),
        name='embed',
        out_shape=shapes,
        in_specs=[VMEM] + [ANY] * (2 + len(local)),
        out_specs=[VMEM] + [ANY] * (len(shapes) - 1),
        scratch_shapes=[pltpu.VMEM((seq, width), F32)] * 2 + [pltpu.VMEM((2, lo, width), F32), pltpu.VMEM((2, lo, width), BF), dma, dma, dma((chunks,)), dma((chunks,)),
                        dma((8,)), dma((8,)), dma, dma((n_tp,)), dma((n_tp,)), dma((n_tp, len(EDGES))), dma((n_tp, len(EDGES))), dma((len(local),)), dma((2,)), dma((2, len(local))), dma((2,))],
        compiler_params=pltpu.CompilerParams(collective_id=0, has_side_effects=True, vmem_limit_bytes=56 * 2 ** 20),
        cost_estimate=pl.CostEstimate(flops=20 * 10 ** 9, bytes_accessed=80 * 2 ** 20, transcendentals=0),
    )(part, piece, toks, *[w.reshape(n_dp, w.shape[0] // n_dp, w.shape[1]) for w in local])
    return out[0], [w.reshape(n_tp, -1, w.shape[3]) for w in out[1:-3]], out[-3], out[-2]


RING = 8
HOLD = 6
OPEN, ADD, CROSSED, PLANE, HOP = 1, 2, 6, 10, 2


def sums_kernel(n, rows, chunks, jobs, part, *refs):
    odd, even = refs[:jobs], refs[jobs:N2 * jobs]
    out, grads, landed, left, right, total, work, fresh, cross, last, along, final, send_r, send_l, recv_l, recv_r, osend, orecv, csend, crecv, esem, fsem, xsend, xrecv, ysend, yrecv, zsend, zrecv, frecv, gsem = refs[N2 * jobs:]
    z = lax.axis_index('tp')
    p, at = plane()
    entry_barrier(z, n, at)
    block = out.shape[N2]
    lead = jnp.maximum(z, n - N1 - z)
    span = N2 * n
    units = jobs * span
    size = work.shape[N2]

    for m in range(jobs):
        @pl.loop(N0, span)
        def _(u, m=m):
            dst = landed.at[m * span + u]
            rcopy(odd[m].at[u // N2, :, pl.ds(pl.multiple_of((u % N2) * size, size), size)], dst, csend, crecv.at[m * span + u], dp=at(N1)).start()

    def here(u):
        return (u >= N0) & (u < units)

    def sides(u):
        side = u % N2
        return side, at(N2) * (N1 - side) + at(4) * side, at(4) * (N1 - side) + at(N2) * side

    def fetch(u):
        slot = u % HOLD

        @pl.when(u >= HOLD)
        def _():
            rcopy(work.at[slot, pl.ds(N0, N2)], cross.at[u - HOLD], xsend.at[slot], xrecv.at[u - HOLD], dp=p).wait_send()
        for m in range(jobs):
            @pl.when(u // span == m)
            def _(m=m):
                v = u - m * span
                pltpu.make_async_copy(even[m].at[v // N2, :, pl.ds(pl.multiple_of((v % N2) * size, size), size)], work.at[slot], esem.at[slot]).start()
        rcopy(landed.at[u], landed.at[u], csend, crecv.at[u], dp=p).wait_recv()
        pltpu.make_async_copy(landed.at[u], fresh.at[u % N2], fsem.at[u % N2]).start()

    def add(u):
        slot = u % HOLD
        pltpu.make_async_copy(landed.at[u], work.at[slot], esem.at[slot]).wait()
        pltpu.make_async_copy(landed.at[u], fresh.at[u % N2], fsem.at[u % N2]).wait()
        for q in range(4):
            work[slot, q] = work[slot, q] + fresh[u % N2, q]

    def add_send(u):
        slot = u % HOLD
        side, first, second = sides(u)
        rcopy(work.at[slot, N1 + side], cross.at[u, N0], xsend.at[slot], xrecv.at[u], dp=first).start()
        rcopy(work.at[slot, 3], cross.at[u, N1], xsend.at[slot], xrecv.at[u], dp=first).start()

    def crossed(u):
        slot = u % HOLD
        rcopy(cross.at[u], cross.at[u], xsend.at[slot], xrecv.at[u], dp=p).wait_recv()
        cross[u, N0] = cross[u, N0] + work[slot, N0]
        cross[u, N1] = cross[u, N1] + work[slot, N2 - u % N2]

    def crossed_send(u):
        side, first, second = sides(u)
        rcopy(cross.at[u, N1], last.at[u], ysend, yrecv.at[u], dp=second).start()

    def in_plane(u):
        rcopy(last.at[u], last.at[u], ysend, yrecv.at[u], dp=p).wait_recv()
        cross[u, N0] = cross[u, N0] + last[u]

    def along_tp(k, t, send):
        toward = jnp.where(z < t, z, n - N1 - z)
        late = HOP * jnp.where(z == t, max(t, n - N1 - t), toward)
        u = k - PLANE - N1 - late
        mine = (u // span) * N2 + u % N2
        ok = here(u) & ((u // N2) % n == t)

        def add_from(ref, sem):
            rcopy(ref, ref, zsend, sem, tp=z).wait_recv()
            cross[u, N0] = cross[u, N0] + ref[...]
        if send:
            @pl.when(ok & (z < t))
            def _():
                rcopy(cross.at[u, N0], along.at[u], zsend, zrecv.at[u], tp=z + N1).start()

            @pl.when(ok & (z > t + N1))
            def _():
                rcopy(cross.at[u, N0], along.at[u], zsend, zrecv.at[u], tp=z - N1).start()

            @pl.when(ok & (z == t + N1))
            def _():
                rcopy(cross.at[u, N0], final.at[mine], zsend, frecv.at[mine], tp=z - N1).start()

            @pl.when(ok & (z == t))
            def _():
                pltpu.make_async_copy(cross.at[u, N0], grads.at[mine], gsem).start()
        else:
            @pl.when(ok & (((z > N0) & (z <= t)) | ((z > t) & (z < n - N1))))
            def _():
                add_from(along.at[u], zrecv.at[u])
            if t < n - N1:
                @pl.when(ok & (z == t))
                def _():
                    add_from(final.at[mine], frecv.at[mine])

    def chunk(c):
        return total.at[c % RING]

    def done(c, value):
        @pl.when(c >= RING)
        def _():
            pltpu.make_async_copy(chunk(c), chunk(c), osend.at[c % RING]).wait()
        total[c % RING] = value

    @pl.loop(N0, max(chunks + LAG * (n - N1) + N1, units + PLANE + N1 + HOP * (n - N1)))
    def _(k):
        c = k - LAG * lead - N1

        @pl.when((c >= N0) & (c < chunks))
        def _():
            where = out.at[p, pl.ds(pl.multiple_of(c * rows, rows), rows)]
            for rel in range(8):
                src = total.at[c % RING, :, pl.ds(pl.multiple_of(at(rel) * block, block), block)]
                if rel == N0:
                    pltpu.make_async_copy(src, where, osend.at[c % RING]).start()
                else:
                    rcopy(src, where, osend.at[c % RING], orecv.at[rel], dp=at(rel)).start()
        chain_sum(k, z, n, rows, chunks, part, left, right, done, send_r, send_l, recv_l, recv_r)
        stages = ((OPEN, fetch, None), (ADD, add, add_send), (CROSSED, crossed, crossed_send), (PLANE, in_plane, None))
        for offset, stage, _ in stages:
            pl.when(here(k - offset))(functools.partial(stage, k - offset))
        for t in range(n):
            along_tp(k, t, False)
        for offset, _, stage in stages:
            if stage:
                pl.when(here(k - offset))(functools.partial(stage, k - offset))
        for t in range(n):
            along_tp(k, t, True)

    chain_drain(z, n, part, left, right, send_r, send_l, recv_l, recv_r)
    for c in range(max(N0, chunks - RING), chunks):
        pltpu.make_async_copy(chunk(c), chunk(c), osend.at[c % RING]).wait()
    for rel in range(N1, 8):
        rcopy(out.at[at(rel)], out.at[at(rel)], ysend, orecv.at[rel], dp=p).wait_recv()
    for u in range(units - HOLD, units):
        rcopy(work.at[u % HOLD, pl.ds(N0, N2)], cross.at[u], xsend.at[u % HOLD], xrecv.at[u], dp=p).wait_send()
    rcopy(landed, landed, csend, crecv.at[N0], dp=p).wait_send()
    rcopy(last, last, ysend, yrecv.at[N0], dp=p).wait_send()
    kept = units - units // n
    rcopy(along.at[pl.ds(N0, kept)], along.at[pl.ds(N0, kept)], zsend, zrecv.at[N0], tp=z).wait_send()
    pltpu.make_async_copy(grads, grads, gsem).wait()


def sums(part, odd, even, n_tp, n_dp):
    seq, width = part.shape
    rows = min(64, seq // 4)
    chunks = seq // rows
    jobs = len(odd)
    size = odd[0].shape[2] // 2
    wide = odd[0].shape[3]
    units = jobs * 2 * n_tp
    dma = pltpu.SemaphoreType.DMA
    piece = (size, wide)
    vmem = [(RING, rows, width), (HOLD, 4) + piece, (2, 4) + piece, (units, 2) + piece, (units,) + piece, (units,) + piece, (2 * jobs,) + piece]
    cols, grads, _ = pl.pallas_call(
        functools.partial(sums_kernel, n_tp, rows, chunks, jobs),
        name='sums',
        out_shape=(jax.ShapeDtypeStruct((n_dp, seq, width // n_dp), F32), jax.ShapeDtypeStruct((2 * jobs,) + piece, F32), jax.ShapeDtypeStruct((units, 4) + piece, F32)),
        in_specs=[VMEM] + [ANY] * (2 * jobs),
        out_specs=(ANY,) * 3,
        scratch_shapes=[pltpu.VMEM((seq, width), F32)] * 2 + [pltpu.VMEM(shape, F32) for shape in vmem] + [
            dma, dma, dma((chunks,)), dma((chunks,)), dma((RING,)), dma((8,)), dma, dma((units,)), dma((HOLD,)), dma((2,)),
            dma((HOLD,)), dma((units,)), dma, dma((units,)), dma, dma((units,)), dma((2 * jobs,)), dma],
        compiler_params=pltpu.CompilerParams(collective_id=1, has_side_effects=True, vmem_limit_bytes=63 * 2 ** 20),
        cost_estimate=pl.CostEstimate(flops=20 * 10 ** 9, bytes_accessed=100 * 2 ** 20, transcendentals=0),
    )(part, *odd, *even)
    return cols, grads.reshape(jobs, 2 * size, wide)


WAYS = 4


def table_kernel(ids, rows_ref, out, *tables):
    step = pl.program_id(0)
    count = rows_ref.shape[0]
    part = count // WAYS

    @pl.when(step == 0)
    def _():
        for table in tables:
            table[...] = jnp.zeros_like(table)

    @pl.loop(0, part, unroll=4)
    def _(r):
        for way, table in enumerate(tables):
            row = way * part + r
            where = pl.ds(ids[step * count + row], 1)
            table[where, :] = table[where, :] + rows_ref[pl.ds(row, 1), :]

    @pl.when(step == pl.num_programs(0) - 1)
    def _():
        total = tables[0][...]
        for table in tables[1:]:
            total = total + table[...]
        out[...] = SHRINK * total[:out.shape[0]]


def table_rows(ids, rows, vocab_loc):
    count, block = rows.shape
    step = min(1024, count // 2)
    return pl.pallas_call(
        table_kernel,
        name='table_rows',
        grid_spec=pltpu.PrefetchScalarGridSpec(
            num_scalar_prefetch=1,
            grid=(count // step,),
            in_specs=[pl.BlockSpec((step, block), lambda i, ids: (i, 0))],
            out_specs=pl.BlockSpec((vocab_loc, block), lambda i, ids: (0, 0)),
            scratch_shapes=[pltpu.VMEM((vocab_loc + 8, block), F32)] * WAYS,
        ),
        out_shape=jax.ShapeDtypeStruct((vocab_loc, block), F32),
        compiler_params=pltpu.CompilerParams(dimension_semantics=('arbitrary',), vmem_limit_bytes=48 * 2 ** 20),
        cost_estimate=pl.CostEstimate(flops=3 * 10 ** 9, bytes_accessed=16 * 2 ** 20, transcendentals=0),
    )(ids, rows)


SPREAD = ((0, 2), (0, 4), (0, 1), (2, 4), (4, 2), (2, 1), (4, 1), (6, 1))


def gather_kernel(parts, block_in, out, send, recv, oself):
    p, at = plane()
    bar = pltpu.get_barrier_semaphore()
    for rel in (1, 2, 4):
        pl.semaphore_signal(bar, inc=1, device_id={'dp': at(rel)}, device_id_type=MESH)
    pl.semaphore_wait(bar, 3)
    size, block = block_in.shape
    rows = size // parts
    half = parts // 2

    def copy(j, rel, i, to):
        dst = out.at[pl.ds(i * rows, rows), pl.ds(pl.multiple_of(at(rel) * block, block), block)]
        src = block_in.at[pl.ds(i * rows, rows)] if rel == 0 else dst
        return rcopy(src, dst, send.at[j, i], recv.at[j, i], dp=at(to))

    def give(j, i):
        copy(j, SPREAD[j][0], i, SPREAD[j][1]).start()

    def take(j, i):
        rel, to = SPREAD[j]
        copy(j, rel ^ to, i, 0).wait_recv()
    own = pltpu.make_async_copy(block_in, out.at[:, pl.ds(pl.multiple_of(p * block, block), block)], oself)
    own.start()
    order_x = list(range(parts))
    order_y = order_x[half:] + order_x[:half]
    for i, j in zip(order_x, order_y):
        give(0, i)
        give(1, j)
    for i in order_x:
        give(2, i)
    for i, j in zip(order_x, order_y):
        take(0, i)
        if i < half:
            give(3, i)
        give(5, i)
        take(1, j)
        if j >= half:
            give(4, j)
        give(6, j)
    for i in order_x[:half]:
        for via, part in ((3, i), (4, i + half)):
            take(via, part)
            give(7, part)
    for i in order_x:
        for j in (2, 5, 6, 7):
            take(j, i)
    for i in order_x:
        for j, (rel, to) in enumerate(SPREAD):
            if j != (4 if i < half else 3):
                copy(j, rel, i, 0).wait_send()
    own.wait()


def gathered_columns(block_in, n_dp):
    size, block = block_in.shape
    parts = 4
    dma = pltpu.SemaphoreType.DMA
    return pl.pallas_call(
        functools.partial(gather_kernel, parts),
        name='gathered_columns',
        out_shape=jax.ShapeDtypeStruct((size, n_dp * block), F32),
        in_specs=[ANY],
        out_specs=ANY,
        scratch_shapes=[dma((len(SPREAD), parts)), dma((len(SPREAD), parts)), dma],
        compiler_params=pltpu.CompilerParams(collective_id=2, has_side_effects=True),
        cost_estimate=pl.CostEstimate(flops=10 * 10 ** 9, bytes_accessed=60 * 2 ** 20, transcendentals=0),
    )(block_in)


def dot(a, b, dims):
    return lax.dot_general(a, b, (dims, ((), ())), preferred_element_type=F32)


NT, TN, NN = ((1,), (1,)), ((0,), (0,)), ((1,), (0,))


def attention_kernel(scale, kb, q_ref, k_ref, v_ref, ctx_ref, m_ref, l_ref, s_ref):
    i = pl.program_id(1)
    qb = q_ref.shape[1]
    q = q_ref[0]
    blocks = ((i + 1) * qb + kb - 1) // kb

    def scores(j, top):
        at_k = pl.ds(pl.multiple_of(j * kb, kb), kb)
        s = dot(k_ref[0, at_k, :], q, NT) * scale
        key = j * kb + lax.broadcasted_iota(jnp.int32, (kb, qb), 0)
        query = i * qb + lax.broadcasted_iota(jnp.int32, (kb, qb), 1)
        s = jnp.where(query >= key, s, -1e30)
        s_ref[at_k, :] = s
        return jnp.maximum(top, jnp.max(s, axis=0, keepdims=True))
    top = lax.fori_loop(0, blocks, scores, jnp.full((1, qb), -1e30, F32))

    def weigh(j, total):
        at_k = pl.ds(pl.multiple_of(j * kb, kb), kb)
        e = jnp.exp(s_ref[at_k, :] - top)
        s_ref[at_k, :] = e
        return total + jnp.sum(e, axis=0, keepdims=True)
    total = lax.fori_loop(0, blocks, weigh, jnp.zeros((1, qb), F32))
    inv = 1.0 / total

    def mix(j, acc):
        at_k = pl.ds(pl.multiple_of(j * kb, kb), kb)
        probs = (s_ref[at_k, :] * inv).astype(BF)
        return acc + dot(probs, v_ref[0, at_k, :], TN)
    ctx_ref[0] = lax.fori_loop(0, blocks, mix, jnp.zeros((qb, v_ref.shape[2]), F32))
    m_ref[0] = top
    l_ref[0] = inv


def attention(q, k, v):
    heads, seq, dim = q.shape
    qb, kb = seq // 8, seq // 4
    spec_q = pl.BlockSpec((1, qb, dim), lambda h, i: (h, i, 0))
    spec_k = pl.BlockSpec((1, seq, dim), lambda h, i: (h, 0, 0))
    spec_s = pl.BlockSpec((1, 1, qb), lambda h, i: (h, 0, i))
    stat = jax.ShapeDtypeStruct((heads, 1, seq), F32)
    return pl.pallas_call(
        functools.partial(attention_kernel, dim ** -0.5, kb),
        name='attention',
        grid=(heads, seq // qb),
        in_specs=[spec_q, spec_k, spec_k],
        out_specs=(spec_q, spec_s, spec_s),
        out_shape=(jax.ShapeDtypeStruct((heads, seq, dim), F32), stat, stat),
        scratch_shapes=[pltpu.VMEM((seq, qb), F32)],
        compiler_params=pltpu.CompilerParams(dimension_semantics=('arbitrary', 'arbitrary'), vmem_limit_bytes=32 * 2 ** 20),
        cost_estimate=pl.CostEstimate(flops=3 * 10 ** 9, bytes_accessed=8 * 2 ** 20, transcendentals=10 ** 7),
    )(q, k, v)


def attention_grad_kernel(scale, kb, q_ref, k_ref, v_ref, c_ref, dc_ref, m_ref, l_ref, dq_ref, dk_ref, dv_ref):
    i = pl.program_id(1)
    qb = q_ref.shape[1]
    q, dc = q_ref[0], dc_ref[0]
    dc_f = dc.astype(F32)
    top, inv = m_ref[0], l_ref[0]
    ones = jnp.ones((8, dc.shape[1]), F32)
    mean = lax.dot_general(ones, dc_f * c_ref[0], (NT, ((), ())), precision=lax.Precision.HIGHEST, preferred_element_type=F32)[:1]
    blocks = ((i + 1) * qb + kb - 1) // kb

    @pl.when(i == 0)
    def _():
        dk_ref[...] = jnp.zeros_like(dk_ref)
        dv_ref[...] = jnp.zeros_like(dv_ref)

    def step(j, dq):
        at_k = pl.ds(pl.multiple_of(j * kb, kb), kb)
        keys = k_ref[0, at_k, :]
        s = dot(keys, q, NT) * scale
        key = j * kb + lax.broadcasted_iota(jnp.int32, (kb, qb), 0)
        query = i * qb + lax.broadcasted_iota(jnp.int32, (kb, qb), 1)
        probs = (jnp.exp(jnp.where(query >= key, s, -1e30) - top) * inv).astype(BF)
        d_probs = dot(v_ref[0, at_k, :], dc, NT)
        ds = (probs.astype(F32) * (d_probs - mean) * scale).astype(BF)
        dv_ref[0, at_k, :] += dot(probs, dc, NN)
        dk_ref[0, at_k, :] += dot(ds, q, NN)
        return dq + dot(ds, keys, TN)
    dq_ref[0] = lax.fori_loop(0, blocks, step, jnp.zeros((qb, q.shape[1]), F32))


def attention_grad(q, k, v, ctx, dctx, top, inv):
    heads, seq, dim = q.shape
    qb, kb = seq // 8, seq // 4
    spec_q = pl.BlockSpec((1, qb, dim), lambda h, i: (h, i, 0))
    spec_k = pl.BlockSpec((1, seq, dim), lambda h, i: (h, 0, 0))
    spec_s = pl.BlockSpec((1, 1, qb), lambda h, i: (h, 0, i))
    out = jax.ShapeDtypeStruct((heads, seq, dim), F32)
    return pl.pallas_call(
        functools.partial(attention_grad_kernel, dim ** -0.5, kb),
        name='attention_grad',
        grid=(heads, seq // qb),
        in_specs=[spec_q, spec_k, spec_k, spec_q, spec_q, spec_s, spec_s],
        out_specs=(spec_q, spec_k, spec_k),
        out_shape=(out, out, out),
        compiler_params=pltpu.CompilerParams(dimension_semantics=('arbitrary', 'arbitrary'), vmem_limit_bytes=32 * 2 ** 20),
        cost_estimate=pl.CostEstimate(flops=8 * 10 ** 9, bytes_accessed=16 * 2 ** 20, transcendentals=10 ** 7),
    )(q, k, v, ctx, dctx, top, inv)


def solution(mesh):
    n_tp, n_dp = mesh.shape['tp'], mesh.shape['dp']
    in_specs = (P('dp', None), P('dp', None, None), P('tp', None)) + WEIGHT_SPECS
    out_specs = (P('tp', None),) + WEIGHT_SPECS

    def device_step(tokens, cotangent, emb_table, *weights):
        (w_qkv, b_qkv, w_out, b_out, ln1_gain, ln1_bias, w_gate, b_gate, w_lin, b_lin, w_down, b_down, ln2_gain) = weights
        tp, dp = lax.axis_index('tp'), lax.axis_index('dp')
        tokens = tokens[N0]
        seq_len, width = tokens.shape[N0], emb_table.shape[N1]
        heads, head_dim = b_qkv.shape[N0], b_qkv.shape[N1] // 3
        own = seq_len // n_tp
        ffn = w_gate.shape[N1]
        rk, rf, ro = width // n_dp, ffn // n_dp, w_out.shape[N0] // n_dp
        zero = jnp.minimum(tokens[N0], N0).astype(F32)

        def cut(weight):
            rows = weight.shape[N0] // n_dp
            return lax.dynamic_slice_in_dim(weight, dp * rows, rows, N0)
        bias_rows = jnp.concatenate([b_gate[None], b_lin[None], jnp.zeros((14, ffn), BF)], axis=N0)
        piece = jnp.concatenate([cut(w_gate), cut(w_lin), cut(w_down), cut(w_out), bias_rows], axis=N0).astype(F32)

        vocab_loc = emb_table.shape[N0]
        local_ids = tokens - tp * vocab_loc
        in_shard = (local_ids >= N0) & (local_ids < vocab_loc)
        safe_ids = jnp.where(in_shard, local_ids, N0)
        own_rows = jnp.where(in_shard[:, None], jnp.take(emb_table, safe_ids, axis=N0), 0.0).astype(F32)
        emb_bf, (wg_full, wl_full, wd_full, wo_full), biases, tok_all = embed(own_rows, piece, tokens.reshape(-N1, min(128, seq_len // 8)), (w_gate, w_lin, w_down, w_out), n_tp, n_dp)
        is_own = (jnp.arange(n_tp) == tp)[:, None]
        bg_full, bl_full = [jnp.where(is_own, b[None].astype(F32), biases[:, i]) for i, b in enumerate((b_gate, b_lin))]

        qkv_pre = jnp.dot(emb_bf, w_qkv, preferred_element_type=F32) + b_qkv.reshape(-N1).astype(F32)
        qkv_all = qkv_pre.astype(BF).reshape(seq_len, heads, 3, head_dim)
        cos_tab, sin_tab = rope_tables(seq_len, head_dim)
        queries = apply_rope(qkv_all[:, :, N0].astype(F32), cos_tab, sin_tab).astype(BF).transpose(N1, N0, N2)
        keys_rot = apply_rope(qkv_all[:, :, N1].astype(F32), cos_tab, sin_tab).astype(BF).transpose(N1, N0, N2)
        values = qkv_all[:, :, N2].transpose(N1, N0, N2)
        ctx, top, inv = attention(queries, keys_rot, values)
        context = ctx.transpose(N1, N0, N2).reshape(n_tp, own, heads * head_dim)
        ctx_own = (lax.all_to_all(context, 'tp', N0, N0) + zero).astype(BF)

        emb_own = lax.dynamic_slice_in_dim(emb_bf, tp * own, own, N0).astype(F32)
        cot_own = lax.dynamic_slice_in_dim(cotangent[N0], tp * own, own, N0).astype(F32)
        attn_out = jnp.einsum('hse,hed->sd', ctx_own, wo_full, preferred_element_type=F32) + b_out.astype(F32)
        normed_one, norm_one_pull = jax.vjp(norm_scaled, ALPHA * emb_own + attn_out, ln1_gain.astype(F32))
        hidden = (normed_one + ln1_bias.astype(F32)).astype(BF)
        gate_pre = jnp.einsum('sk,tkc->tsc', hidden, wg_full, preferred_element_type=F32) + bg_full[:, None]
        lin_pre = jnp.einsum('sk,tkc->tsc', hidden, wl_full, preferred_element_type=F32) + bl_full[:, None]
        inner_val, act_pull = jax.vjp(geglu, gate_pre, lin_pre)
        inner_act = inner_val.astype(BF)
        ffn_out = jnp.einsum('tsc,tcd->sd', inner_act, wd_full, preferred_element_type=F32) + b_down.astype(F32)
        norm_two_pull = jax.vjp(norm_scaled, ALPHA * hidden.astype(F32) + ffn_out, ln2_gain.astype(F32))[N1]

        rel_blocks = jnp.arange(n_dp // N2) * N2

        def products(lhs, rhs, spec):
            rows = lhs.shape[-N1] // n_dp
            blocks = lhs.reshape(lhs.shape[:-N1] + (n_dp, rows))
            for first in (N1, N0):
                chosen = jnp.take(blocks, (rel_blocks + first) ^ dp, axis=-N2).reshape(lhs.shape[:-N1] + (-N1,))
                yield jnp.einsum(spec, chosen, rhs, preferred_element_type=F32).reshape(n_tp, n_dp // N2, rows, -N1)

        d_resid_two, d_ln2_gain = norm_two_pull(cot_own)
        d_b_down = jnp.sum(d_resid_two, axis=N0)
        d_ffn_bf = d_resid_two.astype(BF)
        pair_down = products(inner_act, d_ffn_bf, 'tsc,sd->tcd')
        d_inner = jnp.einsum('sd,tcd->tsc', d_ffn_bf, wd_full, preferred_element_type=F32).astype(BF)
        d_gate_pre, d_lin_pre = act_pull(d_inner.astype(F32))
        d_b_gate = jnp.sum(d_gate_pre, axis=N1)
        d_b_lin = jnp.sum(d_lin_pre, axis=N1)
        d_gate_bf = d_gate_pre.astype(BF)
        d_lin_bf = d_lin_pre.astype(BF)
        pair_gate = products(hidden, d_gate_bf, 'sk,tsc->tkc')
        pair_lin = products(hidden, d_lin_bf, 'sk,tsc->tkc')
        d_hidden = ALPHA * d_resid_two + jnp.einsum('tsc,tkc->sk', d_gate_bf, wg_full, preferred_element_type=F32) + jnp.einsum('tsc,tkc->sk', d_lin_bf, wl_full, preferred_element_type=F32)
        d_ln1_bias = jnp.sum(d_hidden, axis=N0)
        d_resid_one, d_ln1_gain = norm_one_pull(d_hidden)
        d_b_out = jnp.sum(d_resid_one, axis=N0)
        d_attn_bf = d_resid_one.astype(BF)
        d_w_out = jnp.einsum('hse,sd->hed', ctx_own, d_attn_bf, preferred_element_type=F32)
        d_w_out = lax.all_gather(lax.psum_scatter(d_w_out.reshape(-N1, width), ALL, scatter_dimension=N0, tiled=True), 'dp', axis=N0, tiled=True)
        d_ctx = jnp.einsum('sd,hed->hse', d_attn_bf, wo_full, preferred_element_type=F32)
        d_context = (lax.all_to_all(d_ctx, 'tp', N0, N0) + zero).astype(BF).reshape(seq_len, heads, head_dim).transpose(N1, N0, N2)

        d_queries, d_keys, d_values = attention_grad(queries, keys_rot, values, ctx, d_context, top, inv)
        d_queries = apply_rope(d_queries.transpose(N1, N0, N2), cos_tab, -sin_tab)
        d_keys = apply_rope(d_keys.transpose(N1, N0, N2), cos_tab, -sin_tab)
        d_qkv = jnp.stack([d_queries, d_keys, d_values.transpose(N1, N0, N2)], axis=N2).reshape(seq_len, -N1)
        d_b_qkv = jnp.sum(d_qkv, axis=N0)
        d_qkv_bf = d_qkv.astype(BF)
        d_w_qkv = lax.psum(jnp.dot(emb_bf.T, d_qkv_bf, preferred_element_type=F32), 'dp')
        d_emb_part = jnp.dot(d_qkv_bf, w_qkv.T, preferred_element_type=F32)
        d_emb_part = lax.dynamic_update_slice_in_dim(d_emb_part, lax.dynamic_slice_in_dim(d_emb_part, tp * own, own, N0) + ALPHA * d_resid_one, tp * own, N0)
        odd, even = zip(*[tuple(pair) for pair in (pair_gate, pair_lin, pair_down)])
        d_cols, mine = sums(d_emb_part, odd, even, n_tp, n_dp)
        d_w_gate, d_w_lin, d_w_down = [lax.all_gather(grad, 'dp', axis=N0, tiled=True) for grad in mine]
        all_ids = tok_all.reshape(-N1) - tp * vocab_loc
        all_ids = jnp.where((all_ids >= N0) & (all_ids < vocab_loc), all_ids, vocab_loc)
        d_table = gathered_columns(table_rows(all_ids, d_cols.reshape(n_dp * seq_len, -N1), vocab_loc), n_dp)

        slot = (jnp.arange(n_tp) == tp).astype(F32)[:, None]
        d_bq_rows = jnp.pad(slot * d_b_qkv[None], ((N0, N0), (N0, ffn - d_b_qkv.shape[N0])))
        small = jnp.concatenate([d_b_gate, d_b_lin, d_bq_rows, jnp.stack([d_b_out, d_ln1_gain, d_ln1_bias, d_b_down, d_ln2_gain])], axis=N0)
        small = lax.psum(small, ALL)
        d_b_gate = lax.dynamic_index_in_dim(small[:n_tp], tp, N0, keepdims=False)
        d_b_lin = lax.dynamic_index_in_dim(small[n_tp:N2 * n_tp], tp, N0, keepdims=False)
        d_b_qkv = lax.dynamic_index_in_dim(small[N2 * n_tp:3 * n_tp], tp, N0, keepdims=False)[:d_b_qkv.shape[N0]].reshape(heads, 3 * head_dim)
        d_b_out, d_ln1_gain, d_ln1_bias, d_b_down, d_ln2_gain = [small[3 * n_tp + i] for i in range(5)]
        return (d_table, d_w_qkv, d_b_qkv, d_w_out, d_b_out, d_ln1_gain, d_ln1_bias, d_w_gate, d_b_gate, d_w_lin, d_b_lin, d_w_down, d_b_down, d_ln2_gain)

    return jax.shard_map(device_step, mesh=mesh, in_specs=in_specs, out_specs=out_specs, check_vma=False)
```

```python
import functools

import jax
import jax.numpy as jnp
import numpy as np
from jax import lax
from jax.experimental import pallas as pl
from jax.experimental.pallas import tpu as pltpu
from jax.sharding import PartitionSpec as P

ALPHA = 140.0 ** 0.5
EPS = 1e-5
SHRINK = 0.1
ROPE_BASE = 10000.0
WEIGHT_SPECS = (P(None, 'tp'), P('tp', None), P('tp', None), P(), P(), P(), P(None, 'tp'), P('tp'), P(None, 'tp'), P('tp'), P('tp', None), P(), P())
ALL = ('tp', 'dp')
BF = jnp.bfloat16
N0, N1, N2 = range(3)
F32 = jnp.float32
MESH = pl.DeviceIdType.MESH
ANY = pl.BlockSpec(memory_space=pl.ANY)
VMEM = pl.BlockSpec(memory_space=pltpu.VMEM)


def norm_scaled(values, gain):
    mean_val = jnp.mean(values, axis=-1, keepdims=True)
    centered = values - mean_val
    variance = jnp.mean(centered * centered, axis=-1, keepdims=True)
    return centered * lax.rsqrt(variance + EPS) * gain


def geglu(gate_pre, lin_pre):
    return jax.nn.gelu(gate_pre, approximate=False) * lin_pre


def rope_tables(seq_len, head_dim, heads):
    half_dim = head_dim // 2
    inv_freq = (ROPE_BASE ** (-2.0 * np.arange(half_dim) / head_dim)).astype(np.float32)
    angles = np.arange(seq_len, dtype=np.float32)[:, None] * inv_freq[None, :]
    return [jnp.asarray(np.tile(table(angles), (1, heads))) for table in (np.cos, np.sin)]


def column_order(heads, head_dim):
    cols = np.arange(3 * heads * head_dim).reshape(heads, 3, 2, head_dim // 2)
    return np.concatenate([cols[:, part].transpose(1, 0, 2).ravel() for part in (0, 1)] + [cols[:, 2].ravel()])


def rcopy(src, dst, send, recv, **where):
    return pltpu.make_async_remote_copy(src_ref=src, dst_ref=dst, send_sem=send, recv_sem=recv, device_id=dict(where), device_id_type=MESH)


def plane():
    p = lax.axis_index('dp')
    y, x, c = p // 4, (p // 2) % 2, p % 2

    def at(rel):
        yy = 1 - y if rel & 4 else y
        xx = 1 - x if rel & 2 else x
        cc = 1 - c if rel & 1 else c
        return yy * 4 + xx * 2 + cc
    return p, at


def entry_barrier(z, n, at):
    bar = pltpu.get_barrier_semaphore()
    for rel in range(1, 8):
        pl.semaphore_signal(bar, inc=1, device_id={'dp': at(rel)}, device_id_type=MESH)
    for d in range(1, n):
        pl.semaphore_signal(bar, inc=1, device_id={'tp': (z + d) % n}, device_id_type=MESH)
    pl.semaphore_wait(bar, 7 + n - 1)


LAG = 3


def chain_sum(k, z, n, rows, chunks, part, left, right, done, send_r, send_l, recv_l, recv_r):
    last = n - 1

    def cut(ref, c):
        return ref.at[pl.ds(pl.multiple_of(c * rows, rows), rows)]

    def load(ref, c):
        return ref[pl.ds(pl.multiple_of(c * rows, rows), rows)]

    def store(ref, c, value):
        ref[pl.ds(pl.multiple_of(c * rows, rows), rows)] = value
    cl, cr = k - LAG * z, k - LAG * (last - z)
    okl, okr = (cl >= 0) & (cl < chunks), (cr >= 0) & (cr < chunks)

    @pl.when(okl & (z > 0))
    def _():
        rcopy(cut(left, cl), cut(left, cl), send_r, recv_l.at[cl], tp=z).wait_recv()

    @pl.when(okl & (z == last))
    def _():
        done(cl, load(left, cl) + load(part, cl))

    @pl.when(okl & (z > 0) & (z < last))
    def _():
        run = load(left, cl)

        @pl.when(z >= n // 2)
        def _():
            done(cl, run + load(right, cl))
        store(left, cl, run + load(part, cl))

    @pl.when(okr & (z < last))
    def _():
        rcopy(cut(right, cr), cut(right, cr), send_l, recv_r.at[cr], tp=z).wait_recv()

    @pl.when(okr & (z == 0))
    def _():
        done(cr, load(part, cr) + load(right, cr))

    @pl.when(okr & (z > 0) & (z < last))
    def _():
        run = load(right, cr)

        @pl.when(z < n // 2)
        def _():
            done(cr, load(left, cr) + run)
        store(right, cr, run + load(part, cr))

    @pl.when(okl & (z == 0))
    def _():
        rcopy(cut(part, cl), cut(left, cl), send_r, recv_l.at[cl], tp=z + 1).start()

    @pl.when(okl & (z > 0) & (z < last))
    def _():
        rcopy(cut(left, cl), cut(left, cl), send_r, recv_l.at[cl], tp=z + 1).start()

    @pl.when(okr & (z == last))
    def _():
        rcopy(cut(part, cr), cut(right, cr), send_l, recv_r.at[cr], tp=z - 1).start()

    @pl.when(okr & (z > 0) & (z < last))
    def _():
        rcopy(cut(right, cr), cut(right, cr), send_l, recv_r.at[cr], tp=z - 1).start()


def chain_drain(z, n, part, left, right, send_r, send_l, recv_l, recv_r):
    @pl.when(z < n - 1)
    def _():
        rcopy(part, left, send_r, recv_l.at[0], tp=z + 1).wait_send()

    @pl.when(z > 0)
    def _():
        rcopy(part, right, send_l, recv_r.at[0], tp=z - 1).wait_send()


EDGES = ((0, 0, 2), (0, 0, 4), (0, 0, 1), (2, 1, 4), (4, 2, 2), (2, 0, 1), (4, 0, 1), (6, 1, 1), (6, 2, 1))
CROSS, DIAGONAL, LAST = ((0, 3, 5), (1, 4, 6)), ((3, 7), (4, 8)), {1: (2,), 3: (5,), 5: (6,), 7: (7, 8)}
STEPS = (3, 8, 13, 19, 22, 26)
FIRST = 17
ORDER = (0, 2, 4, 1, 3, 5, 6, 7)


def emb_kernel(n, rows, chunks, cuts, heads, part, wq, bq, cos, sin, piece, toks, *refs):
    m = len(cuts)
    local, outs = refs[:m], refs[m + N1:N2 * m + N1]
    out, (bias, tok_all, wall, ctx_own, q, k_all, v, ctx, top, inv, left, right, raw, low, weights, send_r, send_l, recv_l, recv_r, tsend, trecv, tself, zsend, zrecv, psend, precv, lsem, isem, osem, bsem, asend, arecv, aself) = refs[m], refs[N2 * m + N1:]
    blocks = 8
    qb = part.shape[N0] // blocks
    per = chunks // blocks
    z = lax.axis_index('tp')
    p, at = plane()
    entry_barrier(z, n, at)
    half = piece.shape[N0] // N2

    @pl.when(z < n - N1)
    def _():
        rcopy(piece, wall.at[z, p], zsend.at[z], zrecv.at[z], tp=z + N1).start()

    @pl.when(z > N0)
    def _():
        rcopy(piece, wall.at[z, p], bsem.at[N1], zrecv.at[z], tp=z - N1).start()
    mine = [pltpu.make_async_copy(toks, tok_all.at[p], tself)]
    mine += [pltpu.make_async_copy(src, dst.at[z], lsem.at[i]) for i, (src, dst) in enumerate(zip(local, outs))]
    for copy in mine:
        copy.start()
    for rel in range(N1, 8):
        rcopy(toks, tok_all.at[p], tsend.at[rel], trecv.at[rel], dp=at(rel)).start()

    def others(d, body):
        @pl.when(z >= d)
        def _():
            body(z - d, -N1)

        @pl.when(z + d < n)
        def _():
            body(z + d, N1)

    def region(t, rel, side):
        blk = wall.at[t, at(rel)]
        return blk if side == N0 else wall.at[t, at(rel), pl.ds((side - N1) * half, half)]

    def give(t, j):
        rel, side, to = EDGES[j]
        rcopy(region(t, rel, side), region(t, rel, side), psend.at[t, j], precv.at[t, j], dp=at(to)).start()

    def take(t, j):
        rel, side, to = EDGES[j]
        blk = region(t, rel ^ to, side)
        rcopy(blk, blk, psend.at[t, j], precv.at[t, j], dp=p).wait_recv()

    def gave(t, j):
        rel, side, to = EDGES[j]
        rcopy(region(t, rel, side), region(t, rel, side), psend.at[t, j], precv.at[t, j], dp=p).wait_send()

    def arrive(d):
        def body(t, sign):
            blk = wall.at[t, p]
            rcopy(blk, blk, zsend.at[t], zrecv.at[t], tp=z).wait_recv()

            @pl.when((z - sign >= N0) & (z - sign < n))
            def _():
                rcopy(blk, blk, zsend.at[t], zrecv.at[t], tp=z - sign).start()
            for j in range(3):
                give(t, j)
        others(d, body)

    def relay(d, moves):
        def body(t, sign):
            for first, *rest in moves:
                take(t, first)
                for j in rest:
                    give(t, j)
        others(d, body)

    k_all[...] = jnp.zeros_like(k_all)
    v[...] = jnp.zeros_like(v)
    for d in range(N1, n):
        arrive(d)

    def done(c, value):
        out[pl.ds(pl.multiple_of(c * rows, rows), rows)] = value.astype(out.dtype)

    def other(i):
        return i + (i + n - z) // n

    def loaded(i, rel, slot):
        return pltpu.make_async_copy(wall.at[other(i), at(rel), pl.ds(N0, cuts[-N1][N1])], raw.at[slot], isem.at[slot])

    def stored(i, rel, slot):
        return [pltpu.make_async_copy(low.at[slot, pl.ds(lo, hi - lo)], dst.at[other(i), at(rel)], osem.at[slot, k]) for k, ((lo, hi), dst) in enumerate(zip(cuts, outs))]
    plan = [(i, rel) for rel in ORDER for i in range(n - N1)]

    def prefetch(s):
        i, rel = plan[s]
        for j in LAST.get(rel, ()):
            take(other(i), j)
        loaded(i, rel, s % N2).start()

    def convert(s):
        i, rel = plan[s]
        loaded(i, rel, s % N2).wait()
        if s >= N2:
            for copy in stored(*plan[s - N2], s % N2):
                copy.wait()
        low[s % N2] = raw[s % N2].astype(low.dtype)
        if s + N1 < len(plan):
            prefetch(s + N1)
        for copy in stored(i, rel, s % N2):
            copy.start()
    events = [(STEPS[d - N1], functools.partial(relay, d, CROSS)) for d in range(N1, n)] + [(STEPS[d + n - N2], functools.partial(relay, d, DIAGONAL)) for d in range(N1, n)]
    events += [(FIRST - N1, functools.partial(prefetch, N0))] + [(FIRST + s, functools.partial(convert, s)) for s in range(len(plan))]

    start = per + LAG * (n - N1)

    def context(i):
        src = ctx.at[pl.ds(pl.multiple_of(i * qb, qb), qb)]
        to = i // (blocks // n)
        dst = ctx_own.at[z, pl.ds(pl.multiple_of((i % (blocks // n)) * qb, qb), qb)]
        return to, pltpu.make_async_copy(src, dst, aself), rcopy(src, dst, asend, arecv.at[z], tp=to)

    @pl.loop(N0, max(start + blocks * heads + N1, FIRST + len(plan)))
    def _(k):
        step = k - start
        i = step // heads - N1

        @pl.when((step > N0) & (step % heads == N0) & (step <= blocks * heads))
        def _():
            to, local_copy, remote = context(i)

            @pl.when(to == z)
            def _():
                local_copy.start()

            @pl.when(to != z)
            def _():
                remote.start()
        chain_sum(k, z, n, rows, chunks, part, left, right, done, send_r, send_l, recv_l, recv_r)
        for at_step, event in events:
            pl.when(k == at_step)(event)

        @pl.when((step >= N0) & (step < blocks * heads))
        def _():
            @pl.when(step % heads == N0)
            def _():
                project(step // heads, qb, out, wq, bq, cos, sin, q, k_all, v)
            attend(step // heads, step % heads, heads, qb, q, k_all, v, ctx, top, inv, weights)

    kept = blocks // n
    pltpu.make_async_copy(ctx.at[pl.ds(N0, kept * qb)], ctx_own.at[z], aself).wait()
    rest = ctx.at[pl.ds(N0, (blocks - kept) * qb)]
    rcopy(rest, rest, asend, arecv.at[z], tp=z).wait_send()
    for d in range(N1, n):
        src = (z + d) % n
        rcopy(ctx_own.at[src], ctx_own.at[src], asend, arecv.at[src], tp=z).wait_recv()
    chain_drain(z, n, part, left, right, send_r, send_l, recv_l, recv_r)
    for s in (len(plan) - N2, len(plan) - N1):
        for copy in stored(*plan[s], s % N2):
            copy.wait()

    def finish(t, sign):
        for j in range(len(EDGES)):
            gave(t, j)
        tail = pltpu.make_async_copy(wall.at[t, p, pl.ds(cuts[-N1][N1], bias.shape[N1])], bias.at[t], bsem.at[N0])
        tail.start()
        tail.wait()

        @pl.when((z - sign >= N0) & (z - sign < n))
        def _():
            rcopy(wall.at[t, p], wall.at[t, p], zsend.at[t], zrecv.at[t], tp=z).wait_send()
    for d in range(N1, n):
        others(d, finish)
    for copy in mine:
        copy.wait()
    for rel in range(N1, 8):
        rcopy(toks, tok_all.at[at(rel)], tsend.at[rel], trecv.at[rel], dp=at(rel)).wait()

    @pl.when(z < n - N1)
    def _():
        rcopy(piece, wall.at[z, p], zsend.at[z], zrecv.at[z], tp=z + N1).wait_send()

    @pl.when(z > N0)
    def _():
        rcopy(piece, wall.at[z, p], bsem.at[N1], zrecv.at[z], tp=z - N1).wait_send()


def embed(part, piece, toks, local, wq, bq, cos, sin, heads, n_tp, n_dp):
    seq, width = part.shape
    chunks = 32
    rows = seq // chunks
    dims = wq.shape[1] // 3
    cuts, lo = [], 0
    for weight in local:
        cuts.append((lo, lo + weight.shape[0] // n_dp))
        lo = cuts[-1][1]
    dma = pltpu.SemaphoreType.DMA
    shape = jax.ShapeDtypeStruct
    shapes = [shape((seq, width), BF)]
    shapes += [shape((n_tp, n_dp, w.shape[0] // n_dp, w.shape[1]), BF) for w in local]
    shapes += [shape((n_tp, piece.shape[0] - lo, width), F32), shape((n_dp,) + toks.shape, toks.dtype), shape((n_tp, n_dp) + piece.shape, F32), shape((n_tp, seq // n_tp, dims), F32)]
    shapes += [shape((seq, dims), BF)] * 3 + [shape((seq, dims), F32)] + [shape((heads, seq), F32)] * 2
    out = pl.pallas_call(
        functools.partial(emb_kernel, n_tp, rows, chunks, cuts, heads),
        name='embed',
        out_shape=shapes,
        in_specs=[VMEM] * 5 + [ANY] * (2 + len(local)),
        out_specs=[VMEM] + [ANY] * (4 + len(local)) + [VMEM] * 6,
        scratch_shapes=[pltpu.VMEM((seq, width), F32)] * 2 + [pltpu.VMEM((2, lo, width), F32), pltpu.VMEM((2, lo, width), BF), pltpu.VMEM((seq, seq // 8), F32), dma, dma, dma((chunks,)), dma((chunks,)),
                        dma((8,)), dma((8,)), dma, dma((n_tp,)), dma((n_tp,)), dma((n_tp, len(EDGES))), dma((n_tp, len(EDGES))), dma((len(local),)), dma((2,)), dma((2, len(local))), dma((2,)),
                        dma, dma((n_tp,)), dma],
        compiler_params=pltpu.CompilerParams(collective_id=0, has_side_effects=True, vmem_limit_bytes=60 * 2 ** 20),
        cost_estimate=pl.CostEstimate(flops=20 * 10 ** 9, bytes_accessed=80 * 2 ** 20, transcendentals=0),
    )(part, wq, bq, cos, sin, piece, toks, *[w.reshape(n_dp, w.shape[0] // n_dp, w.shape[1]) for w in local])
    m = 1 + len(local)
    return out[0], [w.reshape(n_tp, -1, w.shape[3]) for w in out[1:m]], out[m], out[m + 1], out[m + 3], out[m + 4:]


RING = 8
HOLD = 6
OPEN, ADD, CROSSED, PLANE, HOP = 1, 2, 6, 10, 2


def sums_kernel(n, rows, chunks, jobs, part, *refs):
    odd, even = refs[:jobs], refs[jobs:N2 * jobs]
    out, grads, landed, left, right, total, work, fresh, cross, last, along, final, send_r, send_l, recv_l, recv_r, osend, orecv, csend, crecv, esem, fsem, xsend, xrecv, ysend, yrecv, zsend, zrecv, frecv, gsem = refs[N2 * jobs:]
    z = lax.axis_index('tp')
    p, at = plane()
    entry_barrier(z, n, at)
    block = out.shape[N2]
    lead = jnp.maximum(z, n - N1 - z)
    span = N2 * n
    units = jobs * span
    size = work.shape[N2]

    for m in range(jobs):
        @pl.loop(N0, span)
        def _(u, m=m):
            dst = landed.at[m * span + u]
            rcopy(odd[m].at[u // N2, :, pl.ds(pl.multiple_of((u % N2) * size, size), size)], dst, csend, crecv.at[m * span + u], dp=at(N1)).start()

    def here(u):
        return (u >= N0) & (u < units)

    def sides(u):
        side = u % N2
        return side, at(N2) * (N1 - side) + at(4) * side, at(4) * (N1 - side) + at(N2) * side

    def fetch(u):
        slot = u % HOLD

        @pl.when(u >= HOLD)
        def _():
            rcopy(work.at[slot, pl.ds(N0, N2)], cross.at[u - HOLD], xsend.at[slot], xrecv.at[u - HOLD], dp=p).wait_send()
        for m in range(jobs):
            @pl.when(u // span == m)
            def _(m=m):
                v = u - m * span
                pltpu.make_async_copy(even[m].at[v // N2, :, pl.ds(pl.multiple_of((v % N2) * size, size), size)], work.at[slot], esem.at[slot]).start()
        rcopy(landed.at[u], landed.at[u], csend, crecv.at[u], dp=p).wait_recv()
        pltpu.make_async_copy(landed.at[u], fresh.at[u % N2], fsem.at[u % N2]).start()

    def add(u):
        slot = u % HOLD
        pltpu.make_async_copy(landed.at[u], work.at[slot], esem.at[slot]).wait()
        pltpu.make_async_copy(landed.at[u], fresh.at[u % N2], fsem.at[u % N2]).wait()
        for q in range(4):
            work[slot, q] = work[slot, q] + fresh[u % N2, q]

    def add_send(u):
        slot = u % HOLD
        side, first, second = sides(u)
        rcopy(work.at[slot, N1 + side], cross.at[u, N0], xsend.at[slot], xrecv.at[u], dp=first).start()
        rcopy(work.at[slot, 3], cross.at[u, N1], xsend.at[slot], xrecv.at[u], dp=first).start()

    def crossed(u):
        slot = u % HOLD
        rcopy(cross.at[u], cross.at[u], xsend.at[slot], xrecv.at[u], dp=p).wait_recv()
        cross[u, N0] = cross[u, N0] + work[slot, N0]
        cross[u, N1] = cross[u, N1] + work[slot, N2 - u % N2]

    def crossed_send(u):
        side, first, second = sides(u)
        rcopy(cross.at[u, N1], last.at[u], ysend, yrecv.at[u], dp=second).start()

    def in_plane(u):
        rcopy(last.at[u], last.at[u], ysend, yrecv.at[u], dp=p).wait_recv()
        cross[u, N0] = cross[u, N0] + last[u]

    def along_tp(k, t, send):
        toward = jnp.where(z < t, z, n - N1 - z)
        late = HOP * jnp.where(z == t, max(t, n - N1 - t), toward)
        u = k - PLANE - N1 - late
        mine = (u // span) * N2 + u % N2
        ok = here(u) & ((u // N2) % n == t)

        def add_from(ref, sem):
            rcopy(ref, ref, zsend, sem, tp=z).wait_recv()
            cross[u, N0] = cross[u, N0] + ref[...]
        if send:
            @pl.when(ok & (z < t))
            def _():
                rcopy(cross.at[u, N0], along.at[u], zsend, zrecv.at[u], tp=z + N1).start()

            @pl.when(ok & (z > t + N1))
            def _():
                rcopy(cross.at[u, N0], along.at[u], zsend, zrecv.at[u], tp=z - N1).start()

            @pl.when(ok & (z == t + N1))
            def _():
                rcopy(cross.at[u, N0], final.at[mine], zsend, frecv.at[mine], tp=z - N1).start()

            @pl.when(ok & (z == t))
            def _():
                pltpu.make_async_copy(cross.at[u, N0], grads.at[mine], gsem).start()
        else:
            @pl.when(ok & (((z > N0) & (z <= t)) | ((z > t) & (z < n - N1))))
            def _():
                add_from(along.at[u], zrecv.at[u])
            if t < n - N1:
                @pl.when(ok & (z == t))
                def _():
                    add_from(final.at[mine], frecv.at[mine])

    def chunk(c):
        return total.at[c % RING]

    def done(c, value):
        @pl.when(c >= RING)
        def _():
            pltpu.make_async_copy(chunk(c), chunk(c), osend.at[c % RING]).wait()
        total[c % RING] = value

    @pl.loop(N0, max(chunks + LAG * (n - N1) + N1, units + PLANE + N1 + HOP * (n - N1)))
    def _(k):
        c = k - LAG * lead - N1

        @pl.when((c >= N0) & (c < chunks))
        def _():
            where = out.at[p, pl.ds(pl.multiple_of(c * rows, rows), rows)]
            for rel in range(8):
                src = total.at[c % RING, :, pl.ds(pl.multiple_of(at(rel) * block, block), block)]
                if rel == N0:
                    pltpu.make_async_copy(src, where, osend.at[c % RING]).start()
                else:
                    rcopy(src, where, osend.at[c % RING], orecv.at[rel], dp=at(rel)).start()
        chain_sum(k, z, n, rows, chunks, part, left, right, done, send_r, send_l, recv_l, recv_r)
        stages = ((OPEN, fetch, None), (ADD, add, add_send), (CROSSED, crossed, crossed_send), (PLANE, in_plane, None))
        for offset, stage, _ in stages:
            pl.when(here(k - offset))(functools.partial(stage, k - offset))
        for t in range(n):
            along_tp(k, t, False)
        for offset, _, stage in stages:
            if stage:
                pl.when(here(k - offset))(functools.partial(stage, k - offset))
        for t in range(n):
            along_tp(k, t, True)

    chain_drain(z, n, part, left, right, send_r, send_l, recv_l, recv_r)
    for c in range(max(N0, chunks - RING), chunks):
        pltpu.make_async_copy(chunk(c), chunk(c), osend.at[c % RING]).wait()
    for rel in range(N1, 8):
        rcopy(out.at[at(rel)], out.at[at(rel)], ysend, orecv.at[rel], dp=p).wait_recv()
    for u in range(units - HOLD, units):
        rcopy(work.at[u % HOLD, pl.ds(N0, N2)], cross.at[u], xsend.at[u % HOLD], xrecv.at[u], dp=p).wait_send()
    rcopy(landed, landed, csend, crecv.at[N0], dp=p).wait_send()
    rcopy(last, last, ysend, yrecv.at[N0], dp=p).wait_send()
    kept = units - units // n
    rcopy(along.at[pl.ds(N0, kept)], along.at[pl.ds(N0, kept)], zsend, zrecv.at[N0], tp=z).wait_send()
    pltpu.make_async_copy(grads, grads, gsem).wait()


def sums(part, odd, even, n_tp, n_dp):
    seq, width = part.shape
    rows = min(64, seq // 4)
    chunks = seq // rows
    jobs = len(odd)
    size = odd[0].shape[2] // 2
    wide = odd[0].shape[3]
    units = jobs * 2 * n_tp
    dma = pltpu.SemaphoreType.DMA
    piece = (size, wide)
    vmem = [(RING, rows, width), (HOLD, 4) + piece, (2, 4) + piece, (units, 2) + piece, (units,) + piece, (units,) + piece, (2 * jobs,) + piece]
    cols, grads, _ = pl.pallas_call(
        functools.partial(sums_kernel, n_tp, rows, chunks, jobs),
        name='sums',
        out_shape=(jax.ShapeDtypeStruct((n_dp, seq, width // n_dp), F32), jax.ShapeDtypeStruct((2 * jobs,) + piece, F32), jax.ShapeDtypeStruct((units, 4) + piece, F32)),
        in_specs=[VMEM] + [ANY] * (2 * jobs),
        out_specs=(ANY,) * 3,
        scratch_shapes=[pltpu.VMEM((seq, width), F32)] * 2 + [pltpu.VMEM(shape, F32) for shape in vmem] + [
            dma, dma, dma((chunks,)), dma((chunks,)), dma((RING,)), dma((8,)), dma, dma((units,)), dma((HOLD,)), dma((2,)),
            dma((HOLD,)), dma((units,)), dma, dma((units,)), dma, dma((units,)), dma((2 * jobs,)), dma],
        compiler_params=pltpu.CompilerParams(collective_id=1, has_side_effects=True, vmem_limit_bytes=63 * 2 ** 20),
        cost_estimate=pl.CostEstimate(flops=20 * 10 ** 9, bytes_accessed=100 * 2 ** 20, transcendentals=0),
    )(part, *odd, *even)
    return cols, grads.reshape(jobs, 2 * size, wide)


WAYS = 4


def table_kernel(ids, rows_ref, out, *tables):
    step = pl.program_id(0)
    count = rows_ref.shape[0]
    part = count // WAYS

    @pl.when(step == 0)
    def _():
        for table in tables:
            table[...] = jnp.zeros_like(table)

    @pl.loop(0, part, unroll=4)
    def _(r):
        for way, table in enumerate(tables):
            row = way * part + r
            where = pl.ds(ids[step * count + row], 1)
            table[where, :] = table[where, :] + rows_ref[pl.ds(row, 1), :]

    @pl.when(step == pl.num_programs(0) - 1)
    def _():
        total = tables[0][...]
        for table in tables[1:]:
            total = total + table[...]
        out[...] = SHRINK * total[:out.shape[0]]


def table_rows(ids, rows, vocab_loc):
    count, block = rows.shape
    step = min(1024, count // 2)
    return pl.pallas_call(
        table_kernel,
        name='table_rows',
        grid_spec=pltpu.PrefetchScalarGridSpec(
            num_scalar_prefetch=1,
            grid=(count // step,),
            in_specs=[pl.BlockSpec((step, block), lambda i, ids: (i, 0))],
            out_specs=pl.BlockSpec((vocab_loc, block), lambda i, ids: (0, 0)),
            scratch_shapes=[pltpu.VMEM((vocab_loc + 8, block), F32)] * WAYS,
        ),
        out_shape=jax.ShapeDtypeStruct((vocab_loc, block), F32),
        compiler_params=pltpu.CompilerParams(dimension_semantics=('arbitrary',), vmem_limit_bytes=48 * 2 ** 20),
        cost_estimate=pl.CostEstimate(flops=3 * 10 ** 9, bytes_accessed=16 * 2 ** 20, transcendentals=0),
    )(ids, rows)


SPREAD = ((0, 2), (0, 4), (0, 1), (2, 4), (4, 2), (2, 1), (4, 1), (6, 1))


def gather_kernel(parts, block_in, out, send, recv, oself):
    p, at = plane()
    bar = pltpu.get_barrier_semaphore()
    for rel in (1, 2, 4):
        pl.semaphore_signal(bar, inc=1, device_id={'dp': at(rel)}, device_id_type=MESH)
    pl.semaphore_wait(bar, 3)
    size, block = block_in.shape
    rows = size // parts
    half = parts // 2

    def copy(j, rel, i, to):
        dst = out.at[pl.ds(i * rows, rows), pl.ds(pl.multiple_of(at(rel) * block, block), block)]
        src = block_in.at[pl.ds(i * rows, rows)] if rel == 0 else dst
        return rcopy(src, dst, send.at[j, i], recv.at[j, i], dp=at(to))

    def give(j, i):
        copy(j, SPREAD[j][0], i, SPREAD[j][1]).start()

    def take(j, i):
        rel, to = SPREAD[j]
        copy(j, rel ^ to, i, 0).wait_recv()
    own = pltpu.make_async_copy(block_in, out.at[:, pl.ds(pl.multiple_of(p * block, block), block)], oself)
    own.start()
    order_x = list(range(parts))
    order_y = order_x[half:] + order_x[:half]
    for i, j in zip(order_x, order_y):
        give(0, i)
        give(1, j)
    for i in order_x:
        give(2, i)
    for i, j in zip(order_x, order_y):
        take(0, i)
        if i < half:
            give(3, i)
        give(5, i)
        take(1, j)
        if j >= half:
            give(4, j)
        give(6, j)
    for i in order_x[:half]:
        for via, part in ((3, i), (4, i + half)):
            take(via, part)
            give(7, part)
    for i in order_x:
        for j in (2, 5, 6, 7):
            take(j, i)
    for i in order_x:
        for j, (rel, to) in enumerate(SPREAD):
            if j != (4 if i < half else 3):
                copy(j, rel, i, 0).wait_send()
    own.wait()


def gathered_columns(block_in, n_dp):
    size, block = block_in.shape
    parts = 4
    dma = pltpu.SemaphoreType.DMA
    return pl.pallas_call(
        functools.partial(gather_kernel, parts),
        name='gathered_columns',
        out_shape=jax.ShapeDtypeStruct((size, n_dp * block), F32),
        in_specs=[ANY],
        out_specs=ANY,
        scratch_shapes=[dma((len(SPREAD), parts)), dma((len(SPREAD), parts)), dma],
        compiler_params=pltpu.CompilerParams(collective_id=2, has_side_effects=True),
        cost_estimate=pl.CostEstimate(flops=10 * 10 ** 9, bytes_accessed=60 * 2 ** 20, transcendentals=0),
    )(block_in)


def dot(a, b, dims):
    return lax.dot_general(a, b, (dims, ((), ())), preferred_element_type=F32)


NT, TN, NN = ((1,), (1,)), ((0,), (0,)), ((1,), (0,))


def lane_head(shape, heads, halves):
    lane = lax.broadcasted_iota(jnp.int32, shape, 1)
    dims = shape[1] // halves
    return (lane % dims) // (dims // heads)


def turned(both, cos, sin):
    half = both.shape[1] // 2
    x1, x2 = both[:, :half], both[:, half:]
    return jnp.concatenate([x1 * cos - x2 * sin, x2 * cos + x1 * sin], axis=1)


def project(i, qb, emb, wq, bq, cos, sin, q, k, v):
    at_q = pl.ds(pl.multiple_of(i * qb, qb), qb)
    dims = q.shape[1]
    qkv = (dot(emb[at_q, :], wq[...], NN) + bq[...]).astype(BF)
    for ref, part in ((q, 0), (k, 1)):
        ref[at_q, :] = turned(qkv[:, part * dims:(part + 1) * dims].astype(F32), cos[at_q, :], sin[at_q, :]).astype(BF)
    v[at_q, :] = qkv[:, 2 * dims:]


def scores(i, j, kb, qb, scale, keys, q):
    s = dot(keys, q, NT) * scale
    key = j * kb + lax.broadcasted_iota(jnp.int32, (kb, qb), 0)
    query = i * qb + lax.broadcasted_iota(jnp.int32, (kb, qb), 1)
    return jnp.where(query >= key, s, -1e30)


def attend(i, h, heads, qb, q_ref, k_ref, v_ref, ctx_ref, top_ref, inv_ref, s_ref):
    kb = 2 * qb
    dims = q_ref.shape[1]
    scale = (dims // heads) ** -0.5
    at_q = pl.ds(pl.multiple_of(i * qb, qb), qb)
    q = jnp.where(lane_head((qb, dims), heads, 2) == h, q_ref[at_q, :].astype(F32), 0.0).astype(BF)
    count = (i + 2) // 2

    def at_key(j):
        return pl.ds(pl.multiple_of(j * kb, kb), kb)

    def first(j, top):
        s = scores(i, j, kb, qb, scale, k_ref[at_key(j), :], q)
        s_ref[at_key(j), :] = s
        return jnp.maximum(top, jnp.max(s, axis=0, keepdims=True))
    top = lax.fori_loop(0, count, first, jnp.full((1, qb), -1e30, F32))

    def weigh(j, total):
        e = jnp.exp(s_ref[at_key(j), :] - top)
        s_ref[at_key(j), :] = e
        return total + jnp.sum(e, axis=0, keepdims=True)
    inv = 1.0 / lax.fori_loop(0, count, weigh, jnp.zeros((1, qb), F32))

    def mix(j, acc):
        return acc + dot((s_ref[at_key(j), :] * inv).astype(BF), v_ref[at_key(j), :], TN)
    mixed = lax.fori_loop(0, count, mix, jnp.zeros((qb, dims), F32))
    ctx_ref[at_q, :] = jnp.where(lane_head((qb, dims), heads, 1) == h, mixed, ctx_ref[at_q, :])
    top_ref[pl.ds(h, 1), at_q] = top
    inv_ref[pl.ds(h, 1), at_q] = inv


def attend_grad(i, h, heads, qb, q_ref, k_ref, v_ref, ctx_ref, dctx_ref, top_ref, inv_ref, dq_ref, dk_ref, dv_ref):
    kb = 2 * qb
    dims = q_ref.shape[1]
    scale = (dims // heads) ** -0.5
    at_q = pl.ds(pl.multiple_of(i * qb, qb), qb)
    q = jnp.where(lane_head((qb, dims), heads, 2) == h, q_ref[at_q, :].astype(F32), 0.0).astype(BF)
    dc = jnp.where(lane_head((qb, dims), heads, 1) == h, dctx_ref[at_q, :], 0.0).astype(BF)
    ones = jnp.ones((8, dims), F32)
    mean = lax.dot_general(ones, dc.astype(F32) * ctx_ref[at_q, :], (NT, ((), ())), precision=lax.Precision.HIGHEST, preferred_element_type=F32)[:1]
    top, inv = top_ref[pl.ds(h, 1), at_q], inv_ref[pl.ds(h, 1), at_q]

    def step(j, dq):
        at_k = pl.ds(pl.multiple_of(j * kb, kb), kb)
        keys = k_ref[at_k, :]
        probs = (jnp.exp(scores(i, j, kb, qb, scale, keys, q) - top) * inv).astype(BF)
        ds = (probs.astype(F32) * (dot(v_ref[at_k, :], dc, NT) - mean) * scale).astype(BF)
        dv_ref[at_k, :] += dot(probs, dc, NN)
        dk_ref[at_k, :] += dot(ds, q, NN)
        return dq + dot(ds, keys, TN)
    dq = lax.fori_loop(0, (i + 2) // 2, step, jnp.zeros((qb, dims), F32))
    dq_ref[...] = jnp.where(lane_head((qb, dims), heads, 2) == h, dq, dq_ref[...])


def grad_rows(i, qb, cos, sin, dq, dk, dv, d_bias):
    at_q = pl.ds(pl.multiple_of(i * qb, qb), qb)
    back = [turned(values, cos[at_q, :], -sin[at_q, :]) for values in (dq[...], dk[at_q, :])]
    rows = jnp.concatenate(back + [dv[at_q, :]], axis=1)
    d_bias[...] += jnp.sum(rows, axis=0, keepdims=True)
    return rows.astype(BF)


def attention_grad_kernel(heads, q, k, v, ctx, dctx, top, inv, cos, sin, d_qkv, d_bias, dq, dk, dv):
    blocks = 8
    qb = q.shape[0] // blocks
    dk[...] = jnp.zeros_like(dk)
    dv[...] = jnp.zeros_like(dv)
    d_bias[...] = jnp.zeros_like(d_bias)

    @pl.loop(0, blocks)
    def _(step):
        i = blocks - 1 - step

        @pl.loop(0, heads)
        def _(h):
            attend_grad(i, h, heads, qb, q, k, v, ctx, dctx, top, inv, dq, dk, dv)
        d_qkv[pl.ds(pl.multiple_of(i * qb, qb), qb), :] = grad_rows(i, qb, cos, sin, dq, dk, dv, d_bias)


def attention_grad(saved, dctx, cos, sin, heads):
    q, k, v, ctx, top, inv = saved
    seq, dims = q.shape
    return pl.pallas_call(
        functools.partial(attention_grad_kernel, heads),
        name='attention_grad',
        in_specs=[VMEM] * 9,
        out_specs=(VMEM, VMEM),
        out_shape=(jax.ShapeDtypeStruct((seq, 3 * dims), BF), jax.ShapeDtypeStruct((1, 3 * dims), F32)),
        scratch_shapes=[pltpu.VMEM((seq // 8, dims), F32), pltpu.VMEM((seq, dims), F32), pltpu.VMEM((seq, dims), F32)],
        compiler_params=pltpu.CompilerParams(vmem_limit_bytes=48 * 2 ** 20),
        cost_estimate=pl.CostEstimate(flops=8 * 10 ** 9, bytes_accessed=16 * 2 ** 20, transcendentals=10 ** 7),
    )(q, k, v, ctx, dctx, top, inv, cos, sin)


def solution(mesh):
    n_tp, n_dp = mesh.shape['tp'], mesh.shape['dp']
    in_specs = (P('dp', None), P('dp', None, None), P('tp', None)) + WEIGHT_SPECS
    out_specs = (P('tp', None),) + WEIGHT_SPECS

    def device_step(tokens, cotangent, emb_table, *weights):
        (w_qkv, b_qkv, w_out, b_out, ln1_gain, ln1_bias, w_gate, b_gate, w_lin, b_lin, w_down, b_down, ln2_gain) = weights
        tp, dp = lax.axis_index('tp'), lax.axis_index('dp')
        tokens = tokens[N0]
        seq_len, width = tokens.shape[N0], emb_table.shape[N1]
        heads, head_dim = b_qkv.shape[N0], b_qkv.shape[N1] // 3
        own = seq_len // n_tp
        ffn = w_gate.shape[N1]
        rk, rf, ro = width // n_dp, ffn // n_dp, w_out.shape[N0] // n_dp

        def cut(weight):
            rows = weight.shape[N0] // n_dp
            return lax.dynamic_slice_in_dim(weight, dp * rows, rows, N0)
        bias_rows = jnp.concatenate([b_gate[None], b_lin[None], jnp.zeros((14, ffn), BF)], axis=N0)
        piece = jnp.concatenate([cut(w_gate), cut(w_lin), cut(w_down), cut(w_out), bias_rows], axis=N0).astype(F32)

        vocab_loc = emb_table.shape[N0]
        local_ids = tokens - tp * vocab_loc
        in_shard = (local_ids >= N0) & (local_ids < vocab_loc)
        safe_ids = jnp.where(in_shard, local_ids, N0)
        own_rows = jnp.where(in_shard[:, None], jnp.take(emb_table, safe_ids, axis=N0), 0.0).astype(F32)
        dims = heads * head_dim
        place = column_order(heads, head_dim)
        swap = (jnp.arange(3 * dims)[:, None] == jnp.asarray(place)[None, :]).astype(BF)
        wq = jnp.dot(w_qkv, swap, preferred_element_type=F32).astype(BF)
        bq = jnp.dot(b_qkv.reshape(N1, -1), swap, preferred_element_type=F32)
        cos_tab, sin_tab = rope_tables(seq_len, head_dim, heads)
        emb_bf, (wg_full, wl_full, wd_full, wo_full), biases, tok_all, ctx_own, saved = embed(own_rows, piece, tokens.reshape(-N1, min(128, seq_len // 8)), (w_gate, w_lin, w_down, w_out), wq, bq, cos_tab, sin_tab, heads, n_tp, n_dp)
        ctx_own = ctx_own.astype(BF)
        is_own = (jnp.arange(n_tp) == tp)[:, None]
        bg_full, bl_full = [jnp.where(is_own, b[None].astype(F32), biases[:, i]) for i, b in enumerate((b_gate, b_lin))]

        emb_own = lax.dynamic_slice_in_dim(emb_bf, tp * own, own, N0).astype(F32)
        cot_own = lax.dynamic_slice_in_dim(cotangent[N0], tp * own, own, N0).astype(F32)
        attn_out = jnp.einsum('hse,hed->sd', ctx_own, wo_full, preferred_element_type=F32) + b_out.astype(F32)
        normed_one, norm_one_pull = jax.vjp(norm_scaled, ALPHA * emb_own + attn_out, ln1_gain.astype(F32))
        hidden = (normed_one + ln1_bias.astype(F32)).astype(BF)
        gate_pre = jnp.einsum('sk,tkc->tsc', hidden, wg_full, preferred_element_type=F32) + bg_full[:, None]
        lin_pre = jnp.einsum('sk,tkc->tsc', hidden, wl_full, preferred_element_type=F32) + bl_full[:, None]
        inner_val, act_pull = jax.vjp(geglu, gate_pre, lin_pre)
        inner_act = inner_val.astype(BF)
        ffn_out = jnp.einsum('tsc,tcd->sd', inner_act, wd_full, preferred_element_type=F32) + b_down.astype(F32)
        norm_two_pull = jax.vjp(norm_scaled, ALPHA * hidden.astype(F32) + ffn_out, ln2_gain.astype(F32))[N1]

        rel_blocks = jnp.arange(n_dp // N2) * N2

        def products(lhs, rhs, spec):
            rows = lhs.shape[-N1] // n_dp
            blocks = lhs.reshape(lhs.shape[:-N1] + (n_dp, rows))
            for first in (N1, N0):
                chosen = jnp.take(blocks, (rel_blocks + first) ^ dp, axis=-N2).reshape(lhs.shape[:-N1] + (-N1,))
                yield jnp.einsum(spec, chosen, rhs, preferred_element_type=F32).reshape(n_tp, n_dp // N2, rows, -N1)

        d_resid_two, d_ln2_gain = norm_two_pull(cot_own)
        d_b_down = jnp.sum(d_resid_two, axis=N0)
        d_ffn_bf = d_resid_two.astype(BF)
        pair_down = products(inner_act, d_ffn_bf, 'tsc,sd->tcd')
        d_inner = jnp.einsum('sd,tcd->tsc', d_ffn_bf, wd_full, preferred_element_type=F32).astype(BF)
        d_gate_pre, d_lin_pre = act_pull(d_inner.astype(F32))
        d_b_gate = jnp.sum(d_gate_pre, axis=N1)
        d_b_lin = jnp.sum(d_lin_pre, axis=N1)
        d_gate_bf = d_gate_pre.astype(BF)
        d_lin_bf = d_lin_pre.astype(BF)
        pair_gate = products(hidden, d_gate_bf, 'sk,tsc->tkc')
        pair_lin = products(hidden, d_lin_bf, 'sk,tsc->tkc')
        d_hidden = ALPHA * d_resid_two + jnp.einsum('tsc,tkc->sk', d_gate_bf, wg_full, preferred_element_type=F32) + jnp.einsum('tsc,tkc->sk', d_lin_bf, wl_full, preferred_element_type=F32)
        d_ln1_bias = jnp.sum(d_hidden, axis=N0)
        d_resid_one, d_ln1_gain = norm_one_pull(d_hidden)
        d_b_out = jnp.sum(d_resid_one, axis=N0)
        d_attn_bf = d_resid_one.astype(BF)
        d_w_out = jnp.einsum('hse,sd->hed', ctx_own, d_attn_bf, preferred_element_type=F32)
        d_w_out = lax.all_gather(lax.psum_scatter(d_w_out.reshape(-N1, width), ALL, scatter_dimension=N0, tiled=True), 'dp', axis=N0, tiled=True)
        d_ctx = jnp.einsum('sd,hed->hse', d_attn_bf, wo_full, preferred_element_type=F32)
        d_context = lax.all_to_all(d_ctx, 'tp', N0, N0).reshape(seq_len, dims)
        d_qkv, d_b_qkv = attention_grad(saved, d_context, cos_tab, sin_tab, heads)
        d_b_qkv = jnp.dot(d_b_qkv, swap.astype(F32).T, precision=lax.Precision.HIGHEST)[N0]
        d_w_qkv = lax.psum(jnp.dot(emb_bf.T, jnp.dot(d_qkv, swap.T, preferred_element_type=F32).astype(BF), preferred_element_type=F32), 'dp')
        d_emb_part = jnp.dot(d_qkv, wq.T, preferred_element_type=F32)
        d_emb_part = lax.dynamic_update_slice_in_dim(d_emb_part, lax.dynamic_slice_in_dim(d_emb_part, tp * own, own, N0) + ALPHA * d_resid_one, tp * own, N0)
        odd, even = zip(*[tuple(pair) for pair in (pair_gate, pair_lin, pair_down)])
        d_cols, mine = sums(d_emb_part, odd, even, n_tp, n_dp)
        d_w_gate, d_w_lin, d_w_down = [lax.all_gather(grad, 'dp', axis=N0, tiled=True) for grad in mine]
        all_ids = tok_all.reshape(-N1) - tp * vocab_loc
        all_ids = jnp.where((all_ids >= N0) & (all_ids < vocab_loc), all_ids, vocab_loc)
        d_table = gathered_columns(table_rows(all_ids, d_cols.reshape(n_dp * seq_len, -N1), vocab_loc), n_dp)

        slot = (jnp.arange(n_tp) == tp).astype(F32)[:, None]
        d_bq_rows = jnp.pad(slot * d_b_qkv[None], ((N0, N0), (N0, ffn - d_b_qkv.shape[N0])))
        small = jnp.concatenate([d_b_gate, d_b_lin, d_bq_rows, jnp.stack([d_b_out, d_ln1_gain, d_ln1_bias, d_b_down, d_ln2_gain])], axis=N0)
        small = lax.psum(small, ALL)
        d_b_gate = lax.dynamic_index_in_dim(small[:n_tp], tp, N0, keepdims=False)
        d_b_lin = lax.dynamic_index_in_dim(small[n_tp:N2 * n_tp], tp, N0, keepdims=False)
        d_b_qkv = lax.dynamic_index_in_dim(small[N2 * n_tp:3 * n_tp], tp, N0, keepdims=False)[:d_b_qkv.shape[N0]].reshape(heads, 3 * head_dim)
        d_b_out, d_ln1_gain, d_ln1_bias, d_b_down, d_ln2_gain = [small[3 * n_tp + i] for i in range(5)]
        return (d_table, d_w_qkv, d_b_qkv, d_w_out, d_b_out, d_ln1_gain, d_ln1_bias, d_w_gate, d_b_gate, d_w_lin, d_b_lin, d_w_down, d_b_down, d_ln2_gain)

    return jax.shard_map(device_step, mesh=mesh, in_specs=in_specs, out_specs=out_specs, check_vma=False)
```

```python
import functools

import jax
import jax.numpy as jnp
import numpy as np
from jax import lax
from jax.experimental import pallas as pl
from jax.experimental.pallas import tpu as pltpu
from jax.sharding import PartitionSpec as P

ALPHA = 140.0 ** 0.5
EPS = 1e-5
SHRINK = 0.1
ROPE_BASE = 10000.0
WEIGHT_SPECS = (P(None, 'tp'), P('tp', None), P('tp', None), P(), P(), P(), P(None, 'tp'), P('tp'), P(None, 'tp'), P('tp'), P('tp', None), P(), P())
ALL = ('tp', 'dp')
BF = jnp.bfloat16
N0, N1, N2 = range(3)
F32 = jnp.float32
MESH = pl.DeviceIdType.MESH
ANY = pl.BlockSpec(memory_space=pl.ANY)
VMEM = pl.BlockSpec(memory_space=pltpu.VMEM)


def norm_scaled(values, gain):
    mean_val = jnp.mean(values, axis=-1, keepdims=True)
    centered = values - mean_val
    variance = jnp.mean(centered * centered, axis=-1, keepdims=True)
    return centered * lax.rsqrt(variance + EPS) * gain


def geglu(gate_pre, lin_pre):
    return jax.nn.gelu(gate_pre, approximate=False) * lin_pre


def rope_tables(seq_len, head_dim, heads):
    half_dim = head_dim // 2
    inv_freq = (ROPE_BASE ** (-2.0 * np.arange(half_dim) / head_dim)).astype(np.float32)
    angles = np.arange(seq_len, dtype=np.float32)[:, None] * inv_freq[None, :]
    return [jnp.asarray(np.tile(table(angles), (1, heads))) for table in (np.cos, np.sin)]


def column_order(heads, head_dim):
    cols = np.arange(3 * heads * head_dim).reshape(heads, 3, 2, head_dim // 2)
    return np.concatenate([cols[:, part].transpose(1, 0, 2).ravel() for part in (0, 1)] + [cols[:, 2].ravel()])


def rcopy(src, dst, send, recv, **where):
    return pltpu.make_async_remote_copy(src_ref=src, dst_ref=dst, send_sem=send, recv_sem=recv, device_id=dict(where), device_id_type=MESH)


def plane():
    p = lax.axis_index('dp')
    y, x, c = p // 4, (p // 2) % 2, p % 2

    def at(rel):
        yy = 1 - y if rel & 4 else y
        xx = 1 - x if rel & 2 else x
        cc = 1 - c if rel & 1 else c
        return yy * 4 + xx * 2 + cc
    return p, at


def entry_barrier(z, n, at):
    bar = pltpu.get_barrier_semaphore()
    for rel in range(1, 8):
        pl.semaphore_signal(bar, inc=1, device_id={'dp': at(rel)}, device_id_type=MESH)
    for d in range(1, n):
        pl.semaphore_signal(bar, inc=1, device_id={'tp': (z + d) % n}, device_id_type=MESH)
    pl.semaphore_wait(bar, 7 + n - 1)


LAG = 3


def chain_sum(k, z, n, rows, chunks, part, left, right, done, send_r, send_l, recv_l, recv_r, place=lambda c: c):
    last = n - 1

    def at_rows(c):
        return pl.ds(pl.multiple_of(place(c) * rows, rows), rows)

    def cut(ref, c):
        return ref.at[at_rows(c)]

    def load(ref, c):
        return ref[at_rows(c)]

    def store(ref, c, value):
        ref[at_rows(c)] = value
    cl, cr = k - LAG * z, k - LAG * (last - z)
    okl, okr = (cl >= 0) & (cl < chunks), (cr >= 0) & (cr < chunks)

    @pl.when(okl & (z > 0))
    def _():
        rcopy(cut(left, cl), cut(left, cl), send_r, recv_l.at[cl], tp=z).wait_recv()

    @pl.when(okl & (z == last))
    def _():
        done(cl, load(left, cl) + load(part, cl))

    @pl.when(okl & (z > 0) & (z < last))
    def _():
        run = load(left, cl)

        @pl.when(z >= n // 2)
        def _():
            done(cl, run + load(right, cl))
        store(left, cl, run + load(part, cl))

    @pl.when(okr & (z < last))
    def _():
        rcopy(cut(right, cr), cut(right, cr), send_l, recv_r.at[cr], tp=z).wait_recv()

    @pl.when(okr & (z == 0))
    def _():
        done(cr, load(part, cr) + load(right, cr))

    @pl.when(okr & (z > 0) & (z < last))
    def _():
        run = load(right, cr)

        @pl.when(z < n // 2)
        def _():
            done(cr, load(left, cr) + run)
        store(right, cr, run + load(part, cr))

    @pl.when(okl & (z == 0))
    def _():
        rcopy(cut(part, cl), cut(left, cl), send_r, recv_l.at[cl], tp=z + 1).start()

    @pl.when(okl & (z > 0) & (z < last))
    def _():
        rcopy(cut(left, cl), cut(left, cl), send_r, recv_l.at[cl], tp=z + 1).start()

    @pl.when(okr & (z == last))
    def _():
        rcopy(cut(part, cr), cut(right, cr), send_l, recv_r.at[cr], tp=z - 1).start()

    @pl.when(okr & (z > 0) & (z < last))
    def _():
        rcopy(cut(right, cr), cut(right, cr), send_l, recv_r.at[cr], tp=z - 1).start()


def chain_drain(z, n, part, left, right, send_r, send_l, recv_l, recv_r):
    @pl.when(z < n - 1)
    def _():
        rcopy(part, left, send_r, recv_l.at[0], tp=z + 1).wait_send()

    @pl.when(z > 0)
    def _():
        rcopy(part, right, send_l, recv_r.at[0], tp=z - 1).wait_send()


EDGES = ((0, 0, 2), (0, 0, 4), (0, 0, 1), (2, 1, 4), (4, 2, 2), (2, 0, 1), (4, 0, 1), (6, 1, 1), (6, 2, 1))
CROSS, DIAGONAL, LAST = ((0, 3, 5), (1, 4, 6)), ((3, 7), (4, 8)), {1: (2,), 3: (5,), 5: (6,), 7: (7, 8)}
STEPS = (3, 8, 13, 19, 22, 26)
FIRST = 17
ORDER = (0, 2, 4, 1, 3, 5, 6, 7)


def emb_kernel(n, rows, chunks, cuts, heads, part, wq, bq, cos, sin, piece, toks, *refs):
    m = len(cuts)
    local, outs = refs[:m], refs[m + N1:N2 * m + N1]
    out, (bias, tok_all, wall, ctx_own, q, k_all, v, ctx, top, inv, left, right, raw, low, weights, send_r, send_l, recv_l, recv_r, tsend, trecv, tself, zsend, zrecv, psend, precv, lsem, isem, osem, bsem, asend, arecv, aself) = refs[m], refs[N2 * m + N1:]
    blocks = 8
    qb = part.shape[N0] // blocks
    per = chunks // blocks
    z = lax.axis_index('tp')
    p, at = plane()
    entry_barrier(z, n, at)
    half = piece.shape[N0] // N2

    @pl.when(z < n - N1)
    def _():
        rcopy(piece, wall.at[z, p], zsend.at[z], zrecv.at[z], tp=z + N1).start()

    @pl.when(z > N0)
    def _():
        rcopy(piece, wall.at[z, p], bsem.at[N1], zrecv.at[z], tp=z - N1).start()
    mine = [pltpu.make_async_copy(toks, tok_all.at[p], tself)]
    mine += [pltpu.make_async_copy(src, dst.at[z], lsem.at[i]) for i, (src, dst) in enumerate(zip(local, outs))]
    for copy in mine:
        copy.start()
    for rel in range(N1, 8):
        rcopy(toks, tok_all.at[p], tsend.at[rel], trecv.at[rel], dp=at(rel)).start()

    def others(d, body):
        @pl.when(z >= d)
        def _():
            body(z - d, -N1)

        @pl.when(z + d < n)
        def _():
            body(z + d, N1)

    def region(t, rel, side):
        blk = wall.at[t, at(rel)]
        return blk if side == N0 else wall.at[t, at(rel), pl.ds((side - N1) * half, half)]

    def give(t, j):
        rel, side, to = EDGES[j]
        rcopy(region(t, rel, side), region(t, rel, side), psend.at[t, j], precv.at[t, j], dp=at(to)).start()

    def take(t, j):
        rel, side, to = EDGES[j]
        blk = region(t, rel ^ to, side)
        rcopy(blk, blk, psend.at[t, j], precv.at[t, j], dp=p).wait_recv()

    def gave(t, j):
        rel, side, to = EDGES[j]
        rcopy(region(t, rel, side), region(t, rel, side), psend.at[t, j], precv.at[t, j], dp=p).wait_send()

    def arrive(d):
        def body(t, sign):
            blk = wall.at[t, p]
            rcopy(blk, blk, zsend.at[t], zrecv.at[t], tp=z).wait_recv()

            @pl.when((z - sign >= N0) & (z - sign < n))
            def _():
                rcopy(blk, blk, zsend.at[t], zrecv.at[t], tp=z - sign).start()
            for j in range(3):
                give(t, j)
        others(d, body)

    def relay(d, moves):
        def body(t, sign):
            for first, *rest in moves:
                take(t, first)
                for j in rest:
                    give(t, j)
        others(d, body)

    k_all[...] = jnp.zeros_like(k_all)
    v[...] = jnp.zeros_like(v)
    for d in range(N1, n):
        arrive(d)

    def done(c, value):
        out[pl.ds(pl.multiple_of(c * rows, rows), rows)] = value.astype(out.dtype)

    def other(i):
        return i + (i + n - z) // n

    def loaded(i, rel, slot):
        return pltpu.make_async_copy(wall.at[other(i), at(rel), pl.ds(N0, cuts[-N1][N1])], raw.at[slot], isem.at[slot])

    def stored(i, rel, slot):
        return [pltpu.make_async_copy(low.at[slot, pl.ds(lo, hi - lo)], dst.at[other(i), at(rel)], osem.at[slot, k]) for k, ((lo, hi), dst) in enumerate(zip(cuts, outs))]
    plan = [(i, rel) for rel in ORDER for i in range(n - N1)]

    def prefetch(s):
        i, rel = plan[s]
        for j in LAST.get(rel, ()):
            take(other(i), j)
        loaded(i, rel, s % N2).start()

    def convert(s):
        i, rel = plan[s]
        loaded(i, rel, s % N2).wait()
        if s >= N2:
            for copy in stored(*plan[s - N2], s % N2):
                copy.wait()
        low[s % N2] = raw[s % N2].astype(low.dtype)
        if s + N1 < len(plan):
            prefetch(s + N1)
        for copy in stored(i, rel, s % N2):
            copy.start()
    events = [(STEPS[d - N1], functools.partial(relay, d, CROSS)) for d in range(N1, n)] + [(STEPS[d + n - N2], functools.partial(relay, d, DIAGONAL)) for d in range(N1, n)]
    events += [(FIRST - N1, functools.partial(prefetch, N0))] + [(FIRST + s, functools.partial(convert, s)) for s in range(len(plan))]

    start = per + LAG * (n - N1)

    share = qb // n

    def context(i, d):
        to = (z + d) % n
        src = ctx.at[pl.ds(pl.multiple_of(i * qb + to * share, share), share)]
        if d == N0:
            return pltpu.make_async_copy(src, ctx_own.at[z, i], aself)
        return rcopy(src, ctx_own.at[z, i], asend, arecv.at[z], tp=to)

    @pl.loop(N0, max(start + blocks * heads + N1, FIRST + len(plan)))
    def _(k):
        step = k - start
        i = step // heads - N1

        @pl.when((step > N0) & (step % heads == N0) & (step <= blocks * heads))
        def _():
            for d in range(n):
                context(i, d).start()
        chain_sum(k, z, n, rows, chunks, part, left, right, done, send_r, send_l, recv_l, recv_r)
        for at_step, event in events:
            pl.when(k == at_step)(event)

        @pl.when((step >= N0) & (step < blocks * heads))
        def _():
            @pl.when(step % heads == N0)
            def _():
                project(step // heads, qb, out, wq, bq, cos, sin, q, k_all, v)
            attend(step // heads, step % heads, heads, qb, q, k_all, v, ctx, top, inv, weights)

    pltpu.make_async_copy(ctx_own.at[z], ctx_own.at[z], aself).wait()
    for d in range(N1, n):
        src = (z + d) % n
        rcopy(ctx_own.at[src], ctx_own.at[src], asend, arecv.at[src], tp=z).wait()
    chain_drain(z, n, part, left, right, send_r, send_l, recv_l, recv_r)
    for s in (len(plan) - N2, len(plan) - N1):
        for copy in stored(*plan[s], s % N2):
            copy.wait()

    def finish(t, sign):
        for j in range(len(EDGES)):
            gave(t, j)
        tail = pltpu.make_async_copy(wall.at[t, p, pl.ds(cuts[-N1][N1], bias.shape[N1])], bias.at[t], bsem.at[N0])
        tail.start()
        tail.wait()

        @pl.when((z - sign >= N0) & (z - sign < n))
        def _():
            rcopy(wall.at[t, p], wall.at[t, p], zsend.at[t], zrecv.at[t], tp=z).wait_send()
    for d in range(N1, n):
        others(d, finish)
    for copy in mine:
        copy.wait()
    for rel in range(N1, 8):
        rcopy(toks, tok_all.at[at(rel)], tsend.at[rel], trecv.at[rel], dp=at(rel)).wait()

    @pl.when(z < n - N1)
    def _():
        rcopy(piece, wall.at[z, p], zsend.at[z], zrecv.at[z], tp=z + N1).wait_send()

    @pl.when(z > N0)
    def _():
        rcopy(piece, wall.at[z, p], bsem.at[N1], zrecv.at[z], tp=z - N1).wait_send()


def embed(part, piece, toks, local, wq, bq, cos, sin, heads, n_tp, n_dp):
    seq, width = part.shape
    chunks = 32
    rows = seq // chunks
    dims = wq.shape[1] // 3
    cuts, lo = [], 0
    for weight in local:
        cuts.append((lo, lo + weight.shape[0] // n_dp))
        lo = cuts[-1][1]
    dma = pltpu.SemaphoreType.DMA
    shape = jax.ShapeDtypeStruct
    shapes = [shape((seq, width), BF)]
    shapes += [shape((n_tp, n_dp, w.shape[0] // n_dp, w.shape[1]), BF) for w in local]
    shapes += [shape((n_tp, piece.shape[0] - lo, width), F32), shape((n_dp,) + toks.shape, toks.dtype), shape((n_tp, n_dp) + piece.shape, F32), shape((n_tp, 8, seq // n_tp // 8, dims), F32)]
    shapes += [shape((seq, dims), BF)] * 3 + [shape((seq, dims), F32)] + [shape((heads, seq), F32)] * 2
    out = pl.pallas_call(
        functools.partial(emb_kernel, n_tp, rows, chunks, cuts, heads),
        name='embed',
        out_shape=shapes,
        in_specs=[VMEM] * 5 + [ANY] * (2 + len(local)),
        out_specs=[VMEM] + [ANY] * (4 + len(local)) + [VMEM] * 6,
        scratch_shapes=[pltpu.VMEM((seq, width), F32)] * 2 + [pltpu.VMEM((2, lo, width), F32), pltpu.VMEM((2, lo, width), BF), pltpu.VMEM((seq, seq // 8), F32), dma, dma, dma((chunks,)), dma((chunks,)),
                        dma((8,)), dma((8,)), dma, dma((n_tp,)), dma((n_tp,)), dma((n_tp, len(EDGES))), dma((n_tp, len(EDGES))), dma((len(local),)), dma((2,)), dma((2, len(local))), dma((2,)),
                        dma, dma((n_tp,)), dma],
        compiler_params=pltpu.CompilerParams(collective_id=0, has_side_effects=True, vmem_limit_bytes=60 * 2 ** 20),
        cost_estimate=pl.CostEstimate(flops=20 * 10 ** 9, bytes_accessed=80 * 2 ** 20, transcendentals=0),
    )(part, wq, bq, cos, sin, piece, toks, *[w.reshape(n_dp, w.shape[0] // n_dp, w.shape[1]) for w in local])
    m = 1 + len(local)
    return out[0], [w.reshape(n_tp, -1, w.shape[3]) for w in out[1:m]], out[m], out[m + 1], out[m + 3], out[m + 4:]


RING = 8
HOLD, LIVE, PAIR = 4, 8, 4
ADD, LOAD, CROSSED, LAND, PLANE = 1, 4, 5, 7, 8


def backward_kernel(n, rows, chunks, jobs, heads, d_ctx, resid, q, k_all, v, ctx, top, inv, cos, sin, wq, *refs):
    prods = refs[:jobs]
    out, grads, d_qkv, d_bias, landed, cross, last, part, left, right, total, dctx, dq, dk, dv, ctx_in, res_in, work, fresh, xin, yin, keep, pass_on, along, final, *sems = refs[jobs:]
    send_r, send_l, recv_l, recv_r, osend, orecv, csend, crecv, esem, fsem, xsend, xrecv, xsem, ysend, yrecv, ysem, ksem, zrecv, frecv, asend, arecv, aself, isem = sems
    z = lax.axis_index('tp')
    p, at = plane()
    entry_barrier(z, n, at)
    blocks = 8
    per = chunks // blocks
    qb = rows * per
    share = qb // n
    block = out.shape[N2]
    lead = jnp.maximum(z, n - N1 - z)
    span = N2 * n
    units = jobs * span
    size = work.shape[N2]

    def rows_of(i, to, count):
        return pl.ds(pl.multiple_of(i * qb + to * count, count), count)

    def exchange(i, d):
        to = (z + d) % n
        dst = dctx.at[rows_of(i, z, share)]
        if d == N0:
            return pltpu.make_async_copy(d_ctx.at[z, i], dst, aself.at[i])
        return rcopy(d_ctx.at[to, i], dst, asend, arecv.at[i], tp=to)

    @pl.loop(N0, blocks)
    def _(b):
        for d in range(n):
            exchange(blocks - N1 - b, d).start()

    def piece(m, u, rel):
        return prods[m].at[(u % span) // N2, at(rel), pl.ds(pl.multiple_of((u % N2) * size, size), size)]

    for m in range(jobs):
        @pl.loop(m * span, (m + N1) * span)
        def _(u, m=m):
            for i in range(4):
                rcopy(piece(m, u, N2 * i + N1), landed.at[u, i], csend, crecv.at[u], dp=at(N1)).start()

    def inputs(i):
        slot = i % N2
        at_q = rows_of(i, N0, qb)
        return [pltpu.make_async_copy(ctx.at[at_q], ctx_in.at[slot], isem.at[N0, slot]), pltpu.make_async_copy(resid.at[i], res_in.at[slot], isem.at[N1, slot])]

    dk[...] = jnp.zeros_like(dk)
    dv[...] = jnp.zeros_like(dv)
    d_bias[...] = jnp.zeros_like(d_bias)
    for copy in inputs(blocks - N1):
        copy.start()

    def attention_step(b, h):
        i = blocks - N1 - b

        @pl.when(h == N0)
        def _():
            for copy in inputs(i):
                copy.wait()

            @pl.when(b + N1 < blocks)
            def _():
                for copy in inputs(i - N1):
                    copy.start()
            exchange(i, N0).wait()
            others = dctx.at[pl.ds(N0, (n - N1) * share)]
            rcopy(others, others, asend, arecv.at[i], tp=z).wait_recv()
        attend_grad(i, h, heads, qb, q, k_all, v, ctx_in.at[i % N2], dctx, top, inv, dq, dk, dv)

        @pl.when(h == heads - N1)
        def _():
            got = grad_rows(i, qb, cos, sin, dq, dk, dv, d_bias)
            d_qkv[rows_of(i, N0, qb), :] = got
            part[rows_of(i, N0, qb), :] = dot(got, wq[...], NT)
            part[rows_of(i, z, share), :] = part[rows_of(i, z, share), :] + res_in[i % N2]

    def sides(u):
        side = u % N2
        return side, at(N2) * (N1 - side) + at(4) * side, at(4) * (N1 - side) + at(N2) * side

    def fetch(u):
        slot = u % HOLD

        @pl.when(u >= HOLD)
        def _():
            rcopy(xin.at[N0], cross.at[N0], xsend.at[slot], xrecv.at[N0], dp=p).wait_send()
        for m in range(jobs):
            @pl.when(u // span == m)
            def _(m=m):
                for i in range(4):
                    pltpu.make_async_copy(piece(m, u, N2 * i), work.at[slot, i], esem.at[slot]).start()
        rcopy(landed.at[u], landed.at[u], csend, crecv.at[u], dp=p).wait_recv()
        pltpu.make_async_copy(landed.at[u], fresh, fsem).start()

    def add(u):
        slot = u % HOLD
        pltpu.make_async_copy(landed.at[u], work.at[slot], esem.at[slot]).wait()
        pltpu.make_async_copy(landed.at[u], fresh, fsem).wait()
        for i in range(4):
            work[slot, i] = work[slot, i] + fresh[i]

    def add_send(u):
        slot = u % HOLD
        side, first, second = sides(u)
        rcopy(work.at[slot, N1 + side], cross.at[u, N0], xsend.at[slot], xrecv.at[u], dp=first).start()
        rcopy(work.at[slot, 3], cross.at[u, N1], xsend.at[slot], xrecv.at[u], dp=first).start()

    def load_cross(u):
        rcopy(cross.at[u], cross.at[u], xsend.at[N0], xrecv.at[u], dp=p).wait_recv()
        pltpu.make_async_copy(cross.at[u], xin.at[u % N2], xsem.at[u % N2]).start()

    def crossed(u):
        slot = u % HOLD
        pltpu.make_async_copy(cross.at[u], xin.at[u % N2], xsem.at[u % N2]).wait()

        @pl.when(u >= LIVE)
        def _():
            pltpu.make_async_copy(keep.at[u % LIVE], keep.at[u % LIVE], ksem.at[u % LIVE]).wait()

        @pl.when(u >= PAIR)
        def _():
            rcopy(pass_on.at[u % PAIR], last.at[u], ysend.at[u % PAIR], yrecv.at[u], dp=p).wait_send()
        keep[u % LIVE] = xin[u % N2, N0] + work[slot, N0]
        pass_on[u % PAIR] = xin[u % N2, N1] + work[slot, N2 - u % N2]

    def crossed_send(u):
        side, first, second = sides(u)
        rcopy(pass_on.at[u % PAIR], last.at[u], ysend.at[u % PAIR], yrecv.at[u], dp=second).start()

    def load_last(u):
        rcopy(last.at[u], last.at[u], ysend.at[N0], yrecv.at[u], dp=p).wait_recv()
        pltpu.make_async_copy(last.at[u], yin.at[u % N2], ysem.at[u % N2]).start()

    def in_plane(u):
        pltpu.make_async_copy(last.at[u], yin.at[u % N2], ysem.at[u % N2]).wait()
        keep[u % LIVE] = keep[u % LIVE] + yin[u % N2]

    def unit(k):
        u = (k // 3) * N2 + k % 3
        return u, (k >= N0) & (k % 3 < N2) & (u < units)

    def along_tp(k, t, send):
        toward = jnp.where(z < t, z, n - N1 - z)
        late = jnp.where(z == t, max(t, n - N1 - t), toward)
        u, ok = unit(k - PLANE - N1 - late)
        mine = (u // span) * N2 + u % N2
        slot = u % LIVE
        ok = ok & ((u // N2) % n == t)

        def add_from(ref, sem):
            rcopy(ref, ref, csend, sem, tp=z).wait_recv()
            keep[slot] = keep[slot] + ref[...]
        if send:
            @pl.when(ok & (z < t))
            def _():
                rcopy(keep.at[slot], along.at[u], ksem.at[slot], zrecv.at[u], tp=z + N1).start()

            @pl.when(ok & (z > t + N1))
            def _():
                rcopy(keep.at[slot], along.at[u], ksem.at[slot], zrecv.at[u], tp=z - N1).start()

            @pl.when(ok & (z == t + N1))
            def _():
                rcopy(keep.at[slot], final.at[mine], ksem.at[slot], frecv.at[mine], tp=z - N1).start()

            @pl.when(ok & (z == t))
            def _():
                pltpu.make_async_copy(keep.at[slot], grads.at[mine], ksem.at[slot]).start()
        else:
            @pl.when(ok & (((z > N0) & (z <= t)) | ((z > t) & (z < n - N1))))
            def _():
                add_from(along.at[u], zrecv.at[u])
            if t < n - N1:
                @pl.when(ok & (z == t))
                def _():
                    add_from(final.at[mine], frecv.at[mine])

    def place(c):
        return (blocks - N1 - c // per) * per + c % per

    def chunk(c):
        return total.at[c % RING]

    def done(c, value):
        @pl.when(c >= RING)
        def _():
            pltpu.make_async_copy(chunk(c), chunk(c), osend.at[c % RING]).wait()
        total[c % RING] = value

    def hand_out(c):
        where = out.at[p, pl.ds(pl.multiple_of(place(c) * rows, rows), rows)]
        for rel in range(8):
            src = total.at[c % RING, :, pl.ds(pl.multiple_of(at(rel) * block, block), block)]
            if rel == N0:
                pltpu.make_async_copy(src, where, osend.at[c % RING]).start()
            else:
                rcopy(src, where, osend.at[c % RING], orecv.at[rel], dp=at(rel)).start()

    def staged(k, offset, stage):
        u, ok = unit(k - offset)
        pl.when(ok)(functools.partial(stage, u))
    steps = max(heads + chunks + LAG * (n - N1) + N1, (units // N2) * 3 + PLANE + n)

    @pl.loop(N0, steps)
    def _(k):
        c = k - heads - LAG * lead - N1

        @pl.when((c >= N0) & (c < chunks))
        def _():
            hand_out(c)
        chain_sum(k - heads, z, n, rows, chunks, part, left, right, done, send_r, send_l, recv_l, recv_r, place)
        for offset, stage in ((CROSSED, crossed), (ADD, add), (PLANE, in_plane)):
            staged(k, offset, stage)
        for t in range(n):
            along_tp(k, t, False)
        for offset, stage in ((N0, fetch), (LOAD, load_cross), (LAND, load_last)):
            staged(k, offset, stage)

        @pl.when(k < blocks * heads)
        def _():
            attention_step(k // heads, k % heads)
        for offset, stage in ((ADD, add_send), (CROSSED, crossed_send)):
            staged(k, offset, stage)
        for t in range(n):
            along_tp(k, t, True)

    chain_drain(z, n, part, left, right, send_r, send_l, recv_l, recv_r)
    for c in range(max(N0, chunks - RING), chunks):
        pltpu.make_async_copy(chunk(c), chunk(c), osend.at[c % RING]).wait()
    for rel in range(N1, 8):
        rcopy(out.at[at(rel)], out.at[at(rel)], csend, orecv.at[rel], dp=p).wait_recv()
    for slot in range(HOLD):
        rcopy(xin.at[N0], cross.at[N0], xsend.at[slot], xrecv.at[N0], dp=p).wait_send()
    for slot in range(PAIR):
        rcopy(pass_on.at[slot], last.at[N0], ysend.at[slot], yrecv.at[N0], dp=p).wait_send()
    for slot in range(LIVE):
        pltpu.make_async_copy(keep.at[slot], keep.at[slot], ksem.at[slot]).wait()
    rcopy(landed, landed, csend, crecv.at[N0], dp=p).wait_send()
    sent = dctx.at[pl.ds(N0, (n - N1) * share * blocks)]
    rcopy(sent, sent, asend, arecv.at[N0], tp=z).wait_send()


def backward(d_ctx, resid, saved, cos, sin, wq, prods, heads, n_tp, n_dp):
    q, k, v, ctx, top, inv = saved
    seq, dims = q.shape
    width = wq.shape[0]
    chunks = 32
    rows = seq // chunks
    jobs = len(prods)
    piece = (prods[0].shape[2] // 2, prods[0].shape[3])
    units = jobs * 2 * n_tp
    dma = pltpu.SemaphoreType.DMA
    shape = jax.ShapeDtypeStruct
    qb = seq // 8
    vmem = [(seq, width)] * 3 + [(RING, rows, width), (seq, dims), (qb, dims), (seq, dims), (seq, dims), (2, qb, dims), (2, qb // n_tp, width),
            (HOLD, 4) + piece, (4,) + piece, (2, 2) + piece, (2,) + piece, (LIVE,) + piece, (PAIR,) + piece, (units,) + piece, (2 * jobs,) + piece]
    sems = [(), (), (chunks,), (chunks,), (RING,), (8,), (), (units,), (HOLD,), (), (HOLD,), (units,), (2,), (PAIR,), (units,), (2,), (LIVE,), (units,), (2 * jobs,), (), (8,), (8,), (2, 2)]
    cols, grads, d_qkv, d_bias, *_ = pl.pallas_call(
        functools.partial(backward_kernel, n_tp, rows, chunks, jobs, heads),
        name='backward',
        out_shape=(shape((n_dp, seq, width // n_dp), F32), shape((2 * jobs,) + piece, F32), shape((seq, 3 * dims), BF), shape((1, 3 * dims), F32),
                   shape((units, 4) + piece, F32), shape((units, 2) + piece, F32), shape((units,) + piece, F32)),
        in_specs=[ANY, ANY] + [VMEM] * 3 + [ANY] + [VMEM] * 5 + [ANY] * jobs,
        out_specs=(ANY, ANY, VMEM, VMEM, ANY, ANY, ANY),
        scratch_shapes=[pltpu.VMEM(size, F32) for size in vmem] + [dma(size) for size in sems],
        compiler_params=pltpu.CompilerParams(collective_id=1, has_side_effects=True, vmem_limit_bytes=63 * 2 ** 20),
        cost_estimate=pl.CostEstimate(flops=20 * 10 ** 9, bytes_accessed=100 * 2 ** 20, transcendentals=0),
    )(d_ctx, resid, q, k, v, ctx, top, inv, cos, sin, wq, *prods)
    return d_qkv, d_bias, cols, grads.reshape(jobs, 2 * piece[0], piece[1])


WAYS = 4


def table_kernel(ids, rows_ref, out, *tables):
    step = pl.program_id(0)
    count = rows_ref.shape[0]
    part = count // WAYS

    @pl.when(step == 0)
    def _():
        for table in tables:
            table[...] = jnp.zeros_like(table)

    @pl.loop(0, part, unroll=4)
    def _(r):
        for way, table in enumerate(tables):
            row = way * part + r
            where = pl.ds(ids[step * count + row], 1)
            table[where, :] = table[where, :] + rows_ref[pl.ds(row, 1), :]

    @pl.when(step == pl.num_programs(0) - 1)
    def _():
        total = tables[0][...]
        for table in tables[1:]:
            total = total + table[...]
        out[...] = SHRINK * total[:out.shape[0]]


def table_rows(ids, rows, vocab_loc):
    count, block = rows.shape
    step = min(1024, count // 2)
    return pl.pallas_call(
        table_kernel,
        name='table_rows',
        grid_spec=pltpu.PrefetchScalarGridSpec(
            num_scalar_prefetch=1,
            grid=(count // step,),
            in_specs=[pl.BlockSpec((step, block), lambda i, ids: (i, 0))],
            out_specs=pl.BlockSpec((vocab_loc, block), lambda i, ids: (0, 0)),
            scratch_shapes=[pltpu.VMEM((vocab_loc + 8, block), F32)] * WAYS,
        ),
        out_shape=jax.ShapeDtypeStruct((vocab_loc, block), F32),
        compiler_params=pltpu.CompilerParams(dimension_semantics=('arbitrary',), vmem_limit_bytes=48 * 2 ** 20),
        cost_estimate=pl.CostEstimate(flops=3 * 10 ** 9, bytes_accessed=16 * 2 ** 20, transcendentals=0),
    )(ids, rows)


SPREAD = ((0, 2), (0, 4), (0, 1), (2, 4), (4, 2), (2, 1), (4, 1), (6, 1))


def gather_kernel(parts, block_in, out, send, recv, oself):
    p, at = plane()
    bar = pltpu.get_barrier_semaphore()
    for rel in (1, 2, 4):
        pl.semaphore_signal(bar, inc=1, device_id={'dp': at(rel)}, device_id_type=MESH)
    pl.semaphore_wait(bar, 3)
    size, block = block_in.shape
    rows = size // parts
    half = parts // 2

    def copy(j, rel, i, to):
        dst = out.at[pl.ds(i * rows, rows), pl.ds(pl.multiple_of(at(rel) * block, block), block)]
        src = block_in.at[pl.ds(i * rows, rows)] if rel == 0 else dst
        return rcopy(src, dst, send.at[j, i], recv.at[j, i], dp=at(to))

    def give(j, i):
        copy(j, SPREAD[j][0], i, SPREAD[j][1]).start()

    def take(j, i):
        rel, to = SPREAD[j]
        copy(j, rel ^ to, i, 0).wait_recv()
    own = pltpu.make_async_copy(block_in, out.at[:, pl.ds(pl.multiple_of(p * block, block), block)], oself)
    own.start()
    order_x = list(range(parts))
    order_y = order_x[half:] + order_x[:half]
    for i, j in zip(order_x, order_y):
        give(0, i)
        give(1, j)
    for i in order_x:
        give(2, i)
    for i, j in zip(order_x, order_y):
        take(0, i)
        if i < half:
            give(3, i)
        give(5, i)
        take(1, j)
        if j >= half:
            give(4, j)
        give(6, j)
    for i in order_x[:half]:
        for via, part in ((3, i), (4, i + half)):
            take(via, part)
            give(7, part)
    for i in order_x:
        for j in (2, 5, 6, 7):
            take(j, i)
    for i in order_x:
        for j, (rel, to) in enumerate(SPREAD):
            if j != (4 if i < half else 3):
                copy(j, rel, i, 0).wait_send()
    own.wait()


def gathered_columns(block_in, n_dp):
    size, block = block_in.shape
    parts = 4
    dma = pltpu.SemaphoreType.DMA
    return pl.pallas_call(
        functools.partial(gather_kernel, parts),
        name='gathered_columns',
        out_shape=jax.ShapeDtypeStruct((size, n_dp * block), F32),
        in_specs=[ANY],
        out_specs=ANY,
        scratch_shapes=[dma((len(SPREAD), parts)), dma((len(SPREAD), parts)), dma],
        compiler_params=pltpu.CompilerParams(collective_id=2, has_side_effects=True),
        cost_estimate=pl.CostEstimate(flops=10 * 10 ** 9, bytes_accessed=60 * 2 ** 20, transcendentals=0),
    )(block_in)


def dot(a, b, dims):
    return lax.dot_general(a, b, (dims, ((), ())), preferred_element_type=F32)


NT, TN, NN = ((1,), (1,)), ((0,), (0,)), ((1,), (0,))


def lane_head(shape, heads, halves):
    lane = lax.broadcasted_iota(jnp.int32, shape, 1)
    dims = shape[1] // halves
    return (lane % dims) // (dims // heads)


def turned(both, cos, sin):
    half = both.shape[1] // 2
    x1, x2 = both[:, :half], both[:, half:]
    return jnp.concatenate([x1 * cos - x2 * sin, x2 * cos + x1 * sin], axis=1)


def project(i, qb, emb, wq, bq, cos, sin, q, k, v):
    at_q = pl.ds(pl.multiple_of(i * qb, qb), qb)
    dims = q.shape[1]
    qkv = (dot(emb[at_q, :], wq[...], NN) + bq[...]).astype(BF)
    for ref, part in ((q, 0), (k, 1)):
        ref[at_q, :] = turned(qkv[:, part * dims:(part + 1) * dims].astype(F32), cos[at_q, :], sin[at_q, :]).astype(BF)
    v[at_q, :] = qkv[:, 2 * dims:]


def scores(i, j, kb, qb, scale, keys, q):
    s = dot(keys, q, NT) * scale
    key = j * kb + lax.broadcasted_iota(jnp.int32, (kb, qb), 0)
    query = i * qb + lax.broadcasted_iota(jnp.int32, (kb, qb), 1)
    return jnp.where(query >= key, s, -1e30)


def attend(i, h, heads, qb, q_ref, k_ref, v_ref, ctx_ref, top_ref, inv_ref, s_ref):
    kb = 2 * qb
    dims = q_ref.shape[1]
    scale = (dims // heads) ** -0.5
    at_q = pl.ds(pl.multiple_of(i * qb, qb), qb)
    q = jnp.where(lane_head((qb, dims), heads, 2) == h, q_ref[at_q, :].astype(F32), 0.0).astype(BF)
    count = (i + 2) // 2

    def at_key(j):
        return pl.ds(pl.multiple_of(j * kb, kb), kb)

    def first(j, top):
        s = scores(i, j, kb, qb, scale, k_ref[at_key(j), :], q)
        s_ref[at_key(j), :] = s
        return jnp.maximum(top, jnp.max(s, axis=0, keepdims=True))
    top = lax.fori_loop(0, count, first, jnp.full((1, qb), -1e30, F32))

    def weigh(j, total):
        e = jnp.exp(s_ref[at_key(j), :] - top)
        s_ref[at_key(j), :] = e
        return total + jnp.sum(e, axis=0, keepdims=True)
    inv = 1.0 / lax.fori_loop(0, count, weigh, jnp.zeros((1, qb), F32))

    def mix(j, acc):
        return acc + dot((s_ref[at_key(j), :] * inv).astype(BF), v_ref[at_key(j), :], TN)
    mixed = lax.fori_loop(0, count, mix, jnp.zeros((qb, dims), F32))
    ctx_ref[at_q, :] = jnp.where(lane_head((qb, dims), heads, 1) == h, mixed, ctx_ref[at_q, :])
    top_ref[pl.ds(h, 1), at_q] = top
    inv_ref[pl.ds(h, 1), at_q] = inv


def attend_grad(i, h, heads, qb, q_ref, k_ref, v_ref, ctx_ref, dctx_ref, top_ref, inv_ref, dq_ref, dk_ref, dv_ref):
    kb = 2 * qb
    dims = q_ref.shape[1]
    scale = (dims // heads) ** -0.5
    at_q = pl.ds(pl.multiple_of(i * qb, qb), qb)
    q = jnp.where(lane_head((qb, dims), heads, 2) == h, q_ref[at_q, :].astype(F32), 0.0).astype(BF)
    dc = jnp.where(lane_head((qb, dims), heads, 1) == h, dctx_ref[at_q, :], 0.0).astype(BF)
    ones = jnp.ones((8, dims), F32)
    mean = lax.dot_general(ones, dc.astype(F32) * ctx_ref[...], (NT, ((), ())), precision=lax.Precision.HIGHEST, preferred_element_type=F32)[:1]
    top, inv = top_ref[pl.ds(h, 1), at_q], inv_ref[pl.ds(h, 1), at_q]

    def step(j, dq):
        at_k = pl.ds(pl.multiple_of(j * kb, kb), kb)
        keys = k_ref[at_k, :]
        probs = (jnp.exp(scores(i, j, kb, qb, scale, keys, q) - top) * inv).astype(BF)
        ds = (probs.astype(F32) * (dot(v_ref[at_k, :], dc, NT) - mean) * scale).astype(BF)
        dv_ref[at_k, :] += dot(probs, dc, NN)
        dk_ref[at_k, :] += dot(ds, q, NN)
        return dq + dot(ds, keys, TN)
    dq = lax.fori_loop(0, (i + 2) // 2, step, jnp.zeros((qb, dims), F32))
    dq_ref[...] = jnp.where(lane_head((qb, dims), heads, 2) == h, dq, dq_ref[...])


def grad_rows(i, qb, cos, sin, dq, dk, dv, d_bias):
    at_q = pl.ds(pl.multiple_of(i * qb, qb), qb)
    back = [turned(values, cos[at_q, :], -sin[at_q, :]) for values in (dq[...], dk[at_q, :])]
    rows = jnp.concatenate(back + [dv[at_q, :]], axis=1)
    d_bias[...] += jnp.sum(rows, axis=0, keepdims=True)
    return rows.astype(BF)


def solution(mesh):
    n_tp, n_dp = mesh.shape['tp'], mesh.shape['dp']
    in_specs = (P('dp', None), P('dp', None, None), P('tp', None)) + WEIGHT_SPECS
    out_specs = (P('tp', None),) + WEIGHT_SPECS

    def device_step(tokens, cotangent, emb_table, *weights):
        (w_qkv, b_qkv, w_out, b_out, ln1_gain, ln1_bias, w_gate, b_gate, w_lin, b_lin, w_down, b_down, ln2_gain) = weights
        tp, dp = lax.axis_index('tp'), lax.axis_index('dp')
        tokens = tokens[N0]
        seq_len, width = tokens.shape[N0], emb_table.shape[N1]
        heads, head_dim = b_qkv.shape[N0], b_qkv.shape[N1] // 3
        own = seq_len // n_tp
        ffn = w_gate.shape[N1]
        rk, rf, ro = width // n_dp, ffn // n_dp, w_out.shape[N0] // n_dp

        def cut(weight):
            rows = weight.shape[N0] // n_dp
            return lax.dynamic_slice_in_dim(weight, dp * rows, rows, N0)
        bias_rows = jnp.concatenate([b_gate[None], b_lin[None], jnp.zeros((14, ffn), BF)], axis=N0)
        piece = jnp.concatenate([cut(w_gate), cut(w_lin), cut(w_down), cut(w_out), bias_rows], axis=N0).astype(F32)

        vocab_loc = emb_table.shape[N0]
        local_ids = tokens - tp * vocab_loc
        in_shard = (local_ids >= N0) & (local_ids < vocab_loc)
        safe_ids = jnp.where(in_shard, local_ids, N0)
        own_rows = jnp.where(in_shard[:, None], jnp.take(emb_table, safe_ids, axis=N0), 0.0).astype(F32)
        dims = heads * head_dim
        place = column_order(heads, head_dim)
        swap = (jnp.arange(3 * dims)[:, None] == jnp.asarray(place)[None, :]).astype(BF)
        wq = jnp.dot(w_qkv, swap, preferred_element_type=F32).astype(BF)
        bq = jnp.dot(b_qkv.reshape(N1, -N1), swap, preferred_element_type=F32)
        cos_tab, sin_tab = rope_tables(seq_len, head_dim, heads)
        emb_bf, (wg_full, wl_full, wd_full, wo_full), biases, tok_all, ctx_own, saved = embed(own_rows, piece, tokens.reshape(-N1, min(128, seq_len // 8)), (w_gate, w_lin, w_down, w_out), wq, bq, cos_tab, sin_tab, heads, n_tp, n_dp)
        ctx_own = ctx_own.reshape(n_tp, own, dims).astype(BF)
        is_own = (jnp.arange(n_tp) == tp)[:, None]
        bg_full, bl_full = [jnp.where(is_own, b[None].astype(F32), biases[:, i]) for i, b in enumerate((b_gate, b_lin))]

        blocks = 8

        def owned(values):
            return lax.dynamic_index_in_dim(values.reshape(blocks, n_tp, -N1, width), tp, N1, keepdims=False).reshape(own, width).astype(F32)
        emb_own, cot_own = owned(emb_bf), owned(cotangent[N0])
        attn_out = jnp.einsum('hse,hed->sd', ctx_own, wo_full, preferred_element_type=F32) + b_out.astype(F32)
        normed_one, norm_one_pull = jax.vjp(norm_scaled, ALPHA * emb_own + attn_out, ln1_gain.astype(F32))
        hidden = (normed_one + ln1_bias.astype(F32)).astype(BF)
        gate_pre = jnp.einsum('sk,tkc->tsc', hidden, wg_full, preferred_element_type=F32) + bg_full[:, None]
        lin_pre = jnp.einsum('sk,tkc->tsc', hidden, wl_full, preferred_element_type=F32) + bl_full[:, None]
        inner_val, act_pull = jax.vjp(geglu, gate_pre, lin_pre)
        inner_act = inner_val.astype(BF)
        ffn_out = jnp.einsum('tsc,tcd->sd', inner_act, wd_full, preferred_element_type=F32) + b_down.astype(F32)
        norm_two_pull = jax.vjp(norm_scaled, ALPHA * hidden.astype(F32) + ffn_out, ln2_gain.astype(F32))[N1]

        def product(lhs, rhs, spec):
            return jnp.einsum(spec, lhs, rhs, preferred_element_type=F32).reshape(n_tp, n_dp, -N1, width)

        d_resid_two, d_ln2_gain = norm_two_pull(cot_own)
        d_b_down = jnp.sum(d_resid_two, axis=N0)
        d_ffn_bf = d_resid_two.astype(BF)
        prod_down = product(inner_act, d_ffn_bf, 'tsc,sd->tcd')
        d_inner = jnp.einsum('sd,tcd->tsc', d_ffn_bf, wd_full, preferred_element_type=F32).astype(BF)
        d_gate_pre, d_lin_pre = act_pull(d_inner.astype(F32))
        d_b_gate = jnp.sum(d_gate_pre, axis=N1)
        d_b_lin = jnp.sum(d_lin_pre, axis=N1)
        d_gate_bf = d_gate_pre.astype(BF)
        d_lin_bf = d_lin_pre.astype(BF)
        prod_gate = product(hidden, d_gate_bf, 'sk,tsc->tkc')
        prod_lin = product(hidden, d_lin_bf, 'sk,tsc->tkc')
        d_hidden = ALPHA * d_resid_two + jnp.einsum('tsc,tkc->sk', d_gate_bf, wg_full, preferred_element_type=F32) + jnp.einsum('tsc,tkc->sk', d_lin_bf, wl_full, preferred_element_type=F32)
        d_ln1_bias = jnp.sum(d_hidden, axis=N0)
        d_resid_one, d_ln1_gain = norm_one_pull(d_hidden)
        d_b_out = jnp.sum(d_resid_one, axis=N0)
        d_attn_bf = d_resid_one.astype(BF)
        d_w_out = jnp.einsum('hse,sd->hed', ctx_own, d_attn_bf, preferred_element_type=F32)
        d_w_out = lax.all_gather(lax.psum_scatter(d_w_out.reshape(-N1, width), ALL, scatter_dimension=N0, tiled=True), 'dp', axis=N0, tiled=True)
        d_ctx = jnp.einsum('sd,hed->hse', d_attn_bf, wo_full, preferred_element_type=F32)
        d_qkv, d_b_qkv, d_cols, mine = backward(
            d_ctx.reshape(n_tp, blocks, own // blocks, dims), (ALPHA * d_resid_one).reshape(blocks, own // blocks, width), saved, cos_tab, sin_tab, wq,
            (prod_gate, prod_lin, prod_down), heads, n_tp, n_dp)
        d_b_qkv = jnp.dot(d_b_qkv, swap.astype(F32).T, precision=lax.Precision.HIGHEST)[N0]
        d_w_qkv = lax.psum(jnp.dot(emb_bf.T, jnp.dot(d_qkv, swap.T, preferred_element_type=F32).astype(BF), preferred_element_type=F32), 'dp')
        d_w_gate, d_w_lin, d_w_down = [lax.all_gather(grad, 'dp', axis=N0, tiled=True) for grad in mine]
        all_ids = tok_all.reshape(-N1) - tp * vocab_loc
        all_ids = jnp.where((all_ids >= N0) & (all_ids < vocab_loc), all_ids, vocab_loc)
        d_table = gathered_columns(table_rows(all_ids, d_cols.reshape(n_dp * seq_len, -N1), vocab_loc), n_dp)

        slot = (jnp.arange(n_tp) == tp).astype(F32)[:, None]
        d_bq_rows = jnp.pad(slot * d_b_qkv[None], ((N0, N0), (N0, ffn - d_b_qkv.shape[N0])))
        small = jnp.concatenate([d_b_gate, d_b_lin, d_bq_rows, jnp.stack([d_b_out, d_ln1_gain, d_ln1_bias, d_b_down, d_ln2_gain])], axis=N0)
        small = lax.psum(small, ALL)
        d_b_gate = lax.dynamic_index_in_dim(small[:n_tp], tp, N0, keepdims=False)
        d_b_lin = lax.dynamic_index_in_dim(small[n_tp:N2 * n_tp], tp, N0, keepdims=False)
        d_b_qkv = lax.dynamic_index_in_dim(small[N2 * n_tp:3 * n_tp], tp, N0, keepdims=False)[:d_b_qkv.shape[N0]].reshape(heads, 3 * head_dim)
        d_b_out, d_ln1_gain, d_ln1_bias, d_b_down, d_ln2_gain = [small[3 * n_tp + i] for i in range(5)]
        return (d_table, d_w_qkv, d_b_qkv, d_w_out, d_b_out, d_ln1_gain, d_ln1_bias, d_w_gate, d_b_gate, d_w_lin, d_b_lin, d_w_down, d_b_down, d_ln2_gain)

    return jax.shard_map(device_step, mesh=mesh, in_specs=in_specs, out_specs=out_specs, check_vma=False)
```

```python
import functools

import jax
import jax.numpy as jnp
import numpy as np
from jax import lax
from jax.experimental import pallas as pl
from jax.experimental.pallas import tpu as pltpu
from jax.sharding import PartitionSpec as P

ALPHA = 140.0 ** 0.5
EPS = 1e-5
SHRINK = 0.1
ROPE_BASE = 10000.0
WEIGHT_SPECS = (P(None, 'tp'), P('tp', None), P('tp', None), P(), P(), P(), P(None, 'tp'), P('tp'), P(None, 'tp'), P('tp'), P('tp', None), P(), P())
ALL = ('tp', 'dp')
BF = jnp.bfloat16
N0, N1, N2 = range(3)
F32 = jnp.float32
MESH = pl.DeviceIdType.MESH
ANY = pl.BlockSpec(memory_space=pl.ANY)
VMEM = pl.BlockSpec(memory_space=pltpu.VMEM)


def norm_scaled(values, gain):
    mean_val = jnp.mean(values, axis=-1, keepdims=True)
    centered = values - mean_val
    variance = jnp.mean(centered * centered, axis=-1, keepdims=True)
    return centered * lax.rsqrt(variance + EPS) * gain


def geglu(gate_pre, lin_pre):
    return jax.nn.gelu(gate_pre, approximate=False) * lin_pre


def rope_tables(seq_len, head_dim, heads):
    half_dim = head_dim // 2
    inv_freq = (ROPE_BASE ** (-2.0 * np.arange(half_dim) / head_dim)).astype(np.float32)
    angles = np.arange(seq_len, dtype=np.float32)[:, None] * inv_freq[None, :]
    return [jnp.asarray(np.tile(table(angles), (1, heads))) for table in (np.cos, np.sin)]


def column_order(heads, head_dim):
    cols = np.arange(3 * heads * head_dim).reshape(heads, 3, 2, head_dim // 2)
    return np.concatenate([cols[:, part].transpose(1, 0, 2).ravel() for part in (0, 1)] + [cols[:, 2].ravel()])


def rcopy(src, dst, send, recv, **where):
    return pltpu.make_async_remote_copy(src_ref=src, dst_ref=dst, send_sem=send, recv_sem=recv, device_id=dict(where), device_id_type=MESH)


def plane():
    p = lax.axis_index('dp')
    y, x, c = p // 4, (p // 2) % 2, p % 2

    def at(rel):
        yy = 1 - y if rel & 4 else y
        xx = 1 - x if rel & 2 else x
        cc = 1 - c if rel & 1 else c
        return yy * 4 + xx * 2 + cc
    return p, at


def entry_barrier(z, n, at):
    bar = pltpu.get_barrier_semaphore()
    for rel in range(1, 8):
        pl.semaphore_signal(bar, inc=1, device_id={'dp': at(rel)}, device_id_type=MESH)
    for d in range(1, n):
        pl.semaphore_signal(bar, inc=1, device_id={'tp': (z + d) % n}, device_id_type=MESH)
    pl.semaphore_wait(bar, 7 + n - 1)


LAG = 3


def chain_sum(k, z, n, rows, chunks, part, left, right, done, send_r, send_l, recv_l, recv_r, place=lambda c: c):
    last = n - 1

    def at_rows(c):
        return pl.ds(pl.multiple_of(place(c) * rows, rows), rows)

    def cut(ref, c):
        return ref.at[at_rows(c)]

    def load(ref, c):
        return ref[at_rows(c)]

    def store(ref, c, value):
        ref[at_rows(c)] = value
    cl, cr = k - LAG * z, k - LAG * (last - z)
    okl, okr = (cl >= 0) & (cl < chunks), (cr >= 0) & (cr < chunks)

    @pl.when(okl & (z > 0))
    def _():
        rcopy(cut(left, cl), cut(left, cl), send_r, recv_l.at[cl], tp=z).wait_recv()

    @pl.when(okl & (z == last))
    def _():
        done(cl, load(left, cl) + load(part, cl))

    @pl.when(okl & (z > 0) & (z < last))
    def _():
        run = load(left, cl)

        @pl.when(z >= n // 2)
        def _():
            done(cl, run + load(right, cl))
        store(left, cl, run + load(part, cl))

    @pl.when(okr & (z < last))
    def _():
        rcopy(cut(right, cr), cut(right, cr), send_l, recv_r.at[cr], tp=z).wait_recv()

    @pl.when(okr & (z == 0))
    def _():
        done(cr, load(part, cr) + load(right, cr))

    @pl.when(okr & (z > 0) & (z < last))
    def _():
        run = load(right, cr)

        @pl.when(z < n // 2)
        def _():
            done(cr, load(left, cr) + run)
        store(right, cr, run + load(part, cr))

    @pl.when(okl & (z == 0))
    def _():
        rcopy(cut(part, cl), cut(left, cl), send_r, recv_l.at[cl], tp=z + 1).start()

    @pl.when(okl & (z > 0) & (z < last))
    def _():
        rcopy(cut(left, cl), cut(left, cl), send_r, recv_l.at[cl], tp=z + 1).start()

    @pl.when(okr & (z == last))
    def _():
        rcopy(cut(part, cr), cut(right, cr), send_l, recv_r.at[cr], tp=z - 1).start()

    @pl.when(okr & (z > 0) & (z < last))
    def _():
        rcopy(cut(right, cr), cut(right, cr), send_l, recv_r.at[cr], tp=z - 1).start()


def chain_drain(z, n, part, left, right, send_r, send_l, recv_l, recv_r):
    @pl.when(z < n - 1)
    def _():
        rcopy(part, left, send_r, recv_l.at[0], tp=z + 1).wait_send()

    @pl.when(z > 0)
    def _():
        rcopy(part, right, send_l, recv_r.at[0], tp=z - 1).wait_send()


EDGES = ((0, 0, 2), (0, 0, 4), (0, 0, 1), (2, 1, 4), (4, 2, 2), (2, 0, 1), (4, 0, 1), (6, 1, 1), (6, 2, 1))
CROSS, DIAGONAL, LAST = ((0, 3, 5), (1, 4, 6)), ((3, 7), (4, 8)), {1: (2,), 3: (5,), 5: (6,), 7: (7, 8)}
STEPS = (4, 10, 17, 21, 25, 29)
FIRST = 18
ORDER = (0, 2, 4, 1, 3, 5, 6, 7)


def emb_kernel(n, rows, chunks, cuts, heads, found, mask, wq, bq, cos, sin, piece, toks, *refs):
    m = len(cuts)
    local, outs = refs[:m], refs[m + N1:N2 * m + N1]
    out, (bias, tok_all, wall, ctx_own, q, k_all, v, ctx, top, inv, part, left, right, raw, low, weights, send_r, send_l, recv_l, recv_r, tsend, trecv, tself, zsend, zrecv, psend, precv, lsem, isem, osem, bsem, asend, arecv, aself) = refs[m], refs[N2 * m + N1:]
    blocks = 8
    qb = part.shape[N0] // blocks
    per = chunks // blocks
    z = lax.axis_index('tp')
    p, at = plane()
    entry_barrier(z, n, at)
    half = piece.shape[N0] // N2

    @pl.when(z < n - N1)
    def _():
        rcopy(piece, wall.at[z, p], zsend.at[z], zrecv.at[z], tp=z + N1).start()

    @pl.when(z > N0)
    def _():
        rcopy(piece, wall.at[z, p], bsem.at[N1], zrecv.at[z], tp=z - N1).start()
    mine = [pltpu.make_async_copy(toks, tok_all.at[p], tself)]
    mine += [pltpu.make_async_copy(src, dst.at[z], lsem.at[i]) for i, (src, dst) in enumerate(zip(local, outs))]
    for copy in mine:
        copy.start()
    for rel in range(N1, 8):
        rcopy(toks, tok_all.at[p], tsend.at[rel], trecv.at[rel], dp=at(rel)).start()

    def others(d, body):
        @pl.when(z >= d)
        def _():
            body(z - d, -N1)

        @pl.when(z + d < n)
        def _():
            body(z + d, N1)

    def region(t, rel, side):
        blk = wall.at[t, at(rel)]
        return blk if side == N0 else wall.at[t, at(rel), pl.ds((side - N1) * half, half)]

    def give(t, j):
        rel, side, to = EDGES[j]
        rcopy(region(t, rel, side), region(t, rel, side), psend.at[t, j], precv.at[t, j], dp=at(to)).start()

    def take(t, j):
        rel, side, to = EDGES[j]
        blk = region(t, rel ^ to, side)
        rcopy(blk, blk, psend.at[t, j], precv.at[t, j], dp=p).wait_recv()

    def gave(t, j):
        rel, side, to = EDGES[j]
        rcopy(region(t, rel, side), region(t, rel, side), psend.at[t, j], precv.at[t, j], dp=p).wait_send()

    def arrive(d):
        def body(t, sign):
            blk = wall.at[t, p]
            rcopy(blk, blk, zsend.at[t], zrecv.at[t], tp=z).wait_recv()

            @pl.when((z - sign >= N0) & (z - sign < n))
            def _():
                rcopy(blk, blk, zsend.at[t], zrecv.at[t], tp=z - sign).start()
            for j in range(3):
                give(t, j)
        others(d, body)

    def relay(d, moves):
        def body(t, sign):
            for first, *rest in moves:
                take(t, first)
                for j in rest:
                    give(t, j)
        others(d, body)

    k_all[...] = jnp.zeros_like(k_all)
    v[...] = jnp.zeros_like(v)
    arrive(N1)

    @pl.loop(N0, blocks)
    def _(i):
        at_i = pl.ds(pl.multiple_of(i * qb, qb), qb)
        part[at_i, :] = jnp.where(mask[at_i, :] > N0, found[at_i, :].astype(F32), 0.0)

    def done(c, value):
        out[pl.ds(pl.multiple_of(c * rows, rows), rows)] = value.astype(out.dtype)

    def other(i):
        return i + (i + n - z) // n

    def loaded(i, rel, slot):
        return pltpu.make_async_copy(wall.at[other(i), at(rel), pl.ds(N0, cuts[-N1][N1])], raw.at[slot], isem.at[slot])

    def stored(i, rel, slot):
        return [pltpu.make_async_copy(low.at[slot, pl.ds(lo, hi - lo)], dst.at[other(i), at(rel)], osem.at[slot, k]) for k, ((lo, hi), dst) in enumerate(zip(cuts, outs))]
    plan = [(i, rel) for rel in ORDER for i in range(n - N1)]

    def prefetch(s):
        i, rel = plan[s]
        for j in LAST.get(rel, ()):
            take(other(i), j)
        loaded(i, rel, s % N2).start()

    def convert(s):
        i, rel = plan[s]
        loaded(i, rel, s % N2).wait()
        if s >= N2:
            for copy in stored(*plan[s - N2], s % N2):
                copy.wait()
        low[s % N2] = raw[s % N2].astype(low.dtype)
        if s + N1 < len(plan):
            prefetch(s + N1)
        for copy in stored(i, rel, s % N2):
            copy.start()
    events = [(STEPS[d - N1], functools.partial(relay, d, CROSS)) for d in range(N1, n)] + [(STEPS[d + n - N2], functools.partial(relay, d, DIAGONAL)) for d in range(N1, n)]
    events += [(N2 * d - N2, functools.partial(arrive, d)) for d in range(N2, n)]
    events += [(FIRST - N1, functools.partial(prefetch, N0))] + [(FIRST + s, functools.partial(convert, s)) for s in range(len(plan))]

    start = per + LAG * (n - N1)

    share = qb // n

    def context(i, d):
        to = (z + d) % n
        src = ctx.at[pl.ds(pl.multiple_of(i * qb + to * share, share), share)]
        if d == N0:
            return pltpu.make_async_copy(src, ctx_own.at[z, i], aself)
        return rcopy(src, ctx_own.at[z, i], asend, arecv.at[z], tp=to)

    @pl.loop(N0, max(start + blocks * heads + N1, FIRST + len(plan)))
    def _(k):
        step = k - start
        i = step // heads - N1

        @pl.when((step > N0) & (step % heads == N0) & (step <= blocks * heads))
        def _():
            for d in range(n):
                context(i, d).start()
        chain_sum(k, z, n, rows, chunks, part, left, right, done, send_r, send_l, recv_l, recv_r)
        for at_step, event in events:
            pl.when(k == at_step)(event)

        @pl.when((step >= N0) & (step < blocks * heads))
        def _():
            @pl.when(step % heads == N0)
            def _():
                project(step // heads, qb, out, wq, bq, cos, sin, q, k_all, v)
            attend(step // heads, step % heads, heads, qb, q, k_all, v, ctx, top, inv, weights)

    pltpu.make_async_copy(ctx_own.at[z], ctx_own.at[z], aself).wait()
    for d in range(N1, n):
        src = (z + d) % n
        rcopy(ctx_own.at[src], ctx_own.at[src], asend, arecv.at[src], tp=z).wait()
    chain_drain(z, n, part, left, right, send_r, send_l, recv_l, recv_r)
    for s in (len(plan) - N2, len(plan) - N1):
        for copy in stored(*plan[s], s % N2):
            copy.wait()

    def finish(t, sign):
        for j in range(len(EDGES)):
            gave(t, j)
        tail = pltpu.make_async_copy(wall.at[t, p, pl.ds(cuts[-N1][N1], bias.shape[N1])], bias.at[t], bsem.at[N0])
        tail.start()
        tail.wait()

        @pl.when((z - sign >= N0) & (z - sign < n))
        def _():
            rcopy(wall.at[t, p], wall.at[t, p], zsend.at[t], zrecv.at[t], tp=z).wait_send()
    for d in range(N1, n):
        others(d, finish)
    for copy in mine:
        copy.wait()
    for rel in range(N1, 8):
        rcopy(toks, tok_all.at[at(rel)], tsend.at[rel], trecv.at[rel], dp=at(rel)).wait()

    @pl.when(z < n - N1)
    def _():
        rcopy(piece, wall.at[z, p], zsend.at[z], zrecv.at[z], tp=z + N1).wait_send()

    @pl.when(z > N0)
    def _():
        rcopy(piece, wall.at[z, p], bsem.at[N1], zrecv.at[z], tp=z - N1).wait_send()


def embed(found, mask, piece, toks, local, wq, bq, cos, sin, heads, n_tp, n_dp):
    seq, width = found.shape
    chunks = 32
    rows = seq // chunks
    dims = wq.shape[1] // 3
    cuts, lo = [], 0
    for weight in local:
        cuts.append((lo, lo + weight.shape[0] // n_dp))
        lo = cuts[-1][1]
    dma = pltpu.SemaphoreType.DMA
    shape = jax.ShapeDtypeStruct
    shapes = [shape((seq, width), BF)]
    shapes += [shape((n_tp, n_dp, w.shape[0] // n_dp, w.shape[1]), BF) for w in local]
    shapes += [shape((n_tp, piece.shape[0] - lo, width), F32), shape((n_dp,) + toks.shape, toks.dtype), shape((n_tp, n_dp) + piece.shape, F32), shape((n_tp, 8, seq // n_tp // 8, dims), F32)]
    shapes += [shape((seq, dims), BF)] * 3 + [shape((seq, dims), F32)] + [shape((heads, seq), F32)] * 2
    out = pl.pallas_call(
        functools.partial(emb_kernel, n_tp, rows, chunks, cuts, heads),
        name='embed',
        out_shape=shapes,
        in_specs=[VMEM] * 6 + [ANY] * (2 + len(local)),
        out_specs=[VMEM] + [ANY] * (4 + len(local)) + [VMEM] * 6,
        scratch_shapes=[pltpu.VMEM((seq, width), F32)] * 3 + [pltpu.VMEM((2, lo, width), F32), pltpu.VMEM((2, lo, width), BF), pltpu.VMEM((seq, seq // 8), F32), dma, dma, dma((chunks,)), dma((chunks,)),
                        dma((8,)), dma((8,)), dma, dma((n_tp,)), dma((n_tp,)), dma((n_tp, len(EDGES))), dma((n_tp, len(EDGES))), dma((len(local),)), dma((2,)), dma((2, len(local))), dma((2,)),
                        dma, dma((n_tp,)), dma],
        compiler_params=pltpu.CompilerParams(collective_id=0, has_side_effects=True, vmem_limit_bytes=60 * 2 ** 20),
        cost_estimate=pl.CostEstimate(flops=20 * 10 ** 9, bytes_accessed=80 * 2 ** 20, transcendentals=0),
    )(found, mask, wq, bq, cos, sin, piece, toks, *[w.reshape(n_dp, w.shape[0] // n_dp, w.shape[1]) for w in local])
    m = 1 + len(local)
    return out[0], [w.reshape(n_tp, -1, w.shape[3]) for w in out[1:m]], out[m], out[m + 1], out[m + 3], out[m + 4:]


RING = 4
HOLD, LIVE, PAIR = 4, 8, 4
ADD, LOAD, CROSSED, LAND, PLANE = 1, 4, 5, 7, 8


def backward_kernel(n, rows, chunks, jobs, heads, d_ctx, resid, q, k_all, v, ctx, top, inv, cos, sin, wq, back, emb, *refs):
    prods = refs[:jobs]
    out, grads, d_w, d_bias, landed, cross, last, part, left, right, total, dctx, dq, dk, dv, ctx_in, res_in, cos_in, sin_in, emb_in, work, fresh, xin, yin, keep, pass_on, along, final, *sems = refs[jobs:]
    send_r, send_l, recv_l, recv_r, osend, orecv, csend, crecv, esem, fsem, xsend, xrecv, xsem, ysend, yrecv, ysem, ksem, zrecv, frecv, asend, arecv, aself, isem = sems
    z = lax.axis_index('tp')
    p, at = plane()
    entry_barrier(z, n, at)
    blocks = 8
    per = chunks // blocks
    qb = rows * per
    share = qb // n
    block = out.shape[N2]
    lead = jnp.maximum(z, n - N1 - z)
    span = N2 * n
    units = jobs * span
    size = work.shape[N2]

    def rows_of(i, to, count):
        return pl.ds(pl.multiple_of(i * qb + to * count, count), count)

    def exchange(i, d):
        to = (z + d) % n
        dst = dctx.at[rows_of(i, z, share)]
        if d == N0:
            return pltpu.make_async_copy(d_ctx.at[z, i], dst, aself.at[i])
        return rcopy(d_ctx.at[to, i], dst, asend, arecv.at[i], tp=to)

    @pl.loop(N0, blocks)
    def _(b):
        for d in range(n):
            exchange(blocks - N1 - b, d).start()

    def piece(m, u, rel):
        return prods[m].at[(u % span) // N2, at(rel), pl.ds(pl.multiple_of((u % N2) * size, size), size)]

    for m in range(jobs):
        @pl.loop(m * span, (m + N1) * span)
        def _(u, m=m):
            for i in range(4):
                rcopy(piece(m, u, N2 * i + N1), landed.at[u, i], csend, crecv.at[u], dp=at(N1)).start()

    def inputs(i):
        slot = i % N2
        at_q = rows_of(i, N0, qb)
        pairs = ((ctx.at[at_q], ctx_in), (resid.at[i], res_in), (cos.at[at_q], cos_in), (sin.at[at_q], sin_in), (emb.at[at_q], emb_in))
        return [pltpu.make_async_copy(src, dst.at[slot], isem.at[j, slot]) for j, (src, dst) in enumerate(pairs)]

    dk[...] = jnp.zeros_like(dk)
    dv[...] = jnp.zeros_like(dv)
    d_w[...] = jnp.zeros_like(d_w)
    d_bias[...] = jnp.zeros_like(d_bias)
    for copy in inputs(blocks - N1):
        copy.start()

    def attention_step(b, h):
        i = blocks - N1 - b

        @pl.when(h == N0)
        def _():
            for copy in inputs(i):
                copy.wait()

            @pl.when(b + N1 < blocks)
            def _():
                for copy in inputs(i - N1):
                    copy.start()
            exchange(i, N0).wait()
            others = dctx.at[pl.ds(N0, (n - N1) * share)]
            rcopy(others, others, asend, arecv.at[i], tp=z).wait_recv()
        attend_grad(i, h, heads, qb, q, k_all, v, ctx_in.at[i % N2], dctx, top, inv, dq, dk, dv)

        @pl.when(h == heads - N1)
        def _():
            slot = i % N2
            got = grad_rows(i, qb, cos_in[slot], sin_in[slot], dq, dk, dv, d_bias)
            d_w[...] += dot(emb_in[slot], dot(got, back[...], NN).astype(BF), TN)
            part[rows_of(i, N0, qb), :] = dot(got, wq[...], NT)
            part[rows_of(i, z, share), :] = part[rows_of(i, z, share), :] + res_in[i % N2]

    def sides(u):
        side = u % N2
        return side, at(N2) * (N1 - side) + at(4) * side, at(4) * (N1 - side) + at(N2) * side

    def fetch(u):
        slot = u % HOLD

        @pl.when(u >= HOLD)
        def _():
            rcopy(xin.at[N0], cross.at[N0], xsend.at[slot], xrecv.at[N0], dp=p).wait_send()
        for m in range(jobs):
            @pl.when(u // span == m)
            def _(m=m):
                for i in range(4):
                    pltpu.make_async_copy(piece(m, u, N2 * i), work.at[slot, i], esem.at[slot]).start()
        rcopy(landed.at[u], landed.at[u], csend, crecv.at[u], dp=p).wait_recv()
        pltpu.make_async_copy(landed.at[u], fresh, fsem).start()

    def add(u):
        slot = u % HOLD
        pltpu.make_async_copy(landed.at[u], work.at[slot], esem.at[slot]).wait()
        pltpu.make_async_copy(landed.at[u], fresh, fsem).wait()
        for i in range(4):
            work[slot, i] = work[slot, i] + fresh[i]

    def add_send(u):
        slot = u % HOLD
        side, first, second = sides(u)
        rcopy(work.at[slot, N1 + side], cross.at[u, N0], xsend.at[slot], xrecv.at[u], dp=first).start()
        rcopy(work.at[slot, 3], cross.at[u, N1], xsend.at[slot], xrecv.at[u], dp=first).start()

    def load_cross(u):
        rcopy(cross.at[u], cross.at[u], xsend.at[N0], xrecv.at[u], dp=p).wait_recv()
        pltpu.make_async_copy(cross.at[u], xin.at[u % N2], xsem.at[u % N2]).start()

    def crossed(u):
        slot = u % HOLD
        pltpu.make_async_copy(cross.at[u], xin.at[u % N2], xsem.at[u % N2]).wait()

        @pl.when(u >= LIVE)
        def _():
            pltpu.make_async_copy(keep.at[u % LIVE], keep.at[u % LIVE], ksem.at[u % LIVE]).wait()

        @pl.when(u >= PAIR)
        def _():
            rcopy(pass_on.at[u % PAIR], last.at[u], ysend.at[u % PAIR], yrecv.at[u], dp=p).wait_send()
        keep[u % LIVE] = xin[u % N2, N0] + work[slot, N0]
        pass_on[u % PAIR] = xin[u % N2, N1] + work[slot, N2 - u % N2]

    def crossed_send(u):
        side, first, second = sides(u)
        rcopy(pass_on.at[u % PAIR], last.at[u], ysend.at[u % PAIR], yrecv.at[u], dp=second).start()

    def load_last(u):
        rcopy(last.at[u], last.at[u], ysend.at[N0], yrecv.at[u], dp=p).wait_recv()
        pltpu.make_async_copy(last.at[u], yin.at[u % N2], ysem.at[u % N2]).start()

    def in_plane(u):
        pltpu.make_async_copy(last.at[u], yin.at[u % N2], ysem.at[u % N2]).wait()
        keep[u % LIVE] = keep[u % LIVE] + yin[u % N2]

    def unit(k):
        u = (k // 3) * N2 + k % 3
        return u, (k >= N0) & (k % 3 < N2) & (u < units)

    def along_tp(k, t, send):
        toward = jnp.where(z < t, z, n - N1 - z)
        late = jnp.where(z == t, max(t, n - N1 - t), toward)
        u, ok = unit(k - PLANE - N1 - late)
        mine = (u // span) * N2 + u % N2
        slot = u % LIVE
        ok = ok & ((u // N2) % n == t)

        def add_from(ref, sem):
            rcopy(ref, ref, csend, sem, tp=z).wait_recv()
            keep[slot] = keep[slot] + ref[...]
        if send:
            @pl.when(ok & (z < t))
            def _():
                rcopy(keep.at[slot], along.at[u], ksem.at[slot], zrecv.at[u], tp=z + N1).start()

            @pl.when(ok & (z > t + N1))
            def _():
                rcopy(keep.at[slot], along.at[u], ksem.at[slot], zrecv.at[u], tp=z - N1).start()

            @pl.when(ok & (z == t + N1))
            def _():
                rcopy(keep.at[slot], final.at[mine], ksem.at[slot], frecv.at[mine], tp=z - N1).start()

            @pl.when(ok & (z == t))
            def _():
                pltpu.make_async_copy(keep.at[slot], grads.at[mine], ksem.at[slot]).start()
        else:
            @pl.when(ok & (((z > N0) & (z <= t)) | ((z > t) & (z < n - N1))))
            def _():
                add_from(along.at[u], zrecv.at[u])
            if t < n - N1:
                @pl.when(ok & (z == t))
                def _():
                    add_from(final.at[mine], frecv.at[mine])

    def place(c):
        return (blocks - N1 - c // per) * per + c % per

    def chunk(c):
        return total.at[c % RING]

    def done(c, value):
        @pl.when(c >= RING)
        def _():
            pltpu.make_async_copy(chunk(c), chunk(c), osend.at[c % RING]).wait()
        total[c % RING] = value

    def hand_out(c):
        where = out.at[p, pl.ds(pl.multiple_of(place(c) * rows, rows), rows)]
        for rel in range(8):
            src = total.at[c % RING, :, pl.ds(pl.multiple_of(at(rel) * block, block), block)]
            if rel == N0:
                pltpu.make_async_copy(src, where, osend.at[c % RING]).start()
            else:
                rcopy(src, where, osend.at[c % RING], orecv.at[rel], dp=at(rel)).start()

    def staged(k, offset, stage):
        u, ok = unit(k - offset)
        pl.when(ok)(functools.partial(stage, u))
    steps = max(heads + chunks + LAG * (n - N1) + N1, (units // N2) * 3 + PLANE + n)

    @pl.loop(N0, steps)
    def _(k):
        c = k - heads - LAG * lead - N1

        @pl.when((c >= N0) & (c < chunks))
        def _():
            hand_out(c)
        chain_sum(k - heads, z, n, rows, chunks, part, left, right, done, send_r, send_l, recv_l, recv_r, place)
        for offset, stage in ((CROSSED, crossed), (ADD, add), (PLANE, in_plane)):
            staged(k, offset, stage)
        for t in range(n):
            along_tp(k, t, False)
        for offset, stage in ((N0, fetch), (LOAD, load_cross), (LAND, load_last)):
            staged(k, offset, stage)

        @pl.when(k < blocks * heads)
        def _():
            attention_step(k // heads, k % heads)
        for offset, stage in ((ADD, add_send), (CROSSED, crossed_send)):
            staged(k, offset, stage)
        for t in range(n):
            along_tp(k, t, True)

    chain_drain(z, n, part, left, right, send_r, send_l, recv_l, recv_r)
    for c in range(max(N0, chunks - RING), chunks):
        pltpu.make_async_copy(chunk(c), chunk(c), osend.at[c % RING]).wait()
    for rel in range(N1, 8):
        rcopy(out.at[at(rel)], out.at[at(rel)], csend, orecv.at[rel], dp=p).wait_recv()
    for slot in range(HOLD):
        rcopy(xin.at[N0], cross.at[N0], xsend.at[slot], xrecv.at[N0], dp=p).wait_send()
    for slot in range(PAIR):
        rcopy(pass_on.at[slot], last.at[N0], ysend.at[slot], yrecv.at[N0], dp=p).wait_send()
    for slot in range(LIVE):
        pltpu.make_async_copy(keep.at[slot], keep.at[slot], ksem.at[slot]).wait()
    rcopy(landed, landed, csend, crecv.at[N0], dp=p).wait_send()
    sent = dctx.at[pl.ds(N0, (n - N1) * share * blocks)]
    rcopy(sent, sent, asend, arecv.at[N0], tp=z).wait_send()


def backward(d_ctx, resid, saved, cos, sin, wq, back, emb, prods, heads, n_tp, n_dp):
    q, k, v, ctx, top, inv = saved
    seq, dims = q.shape
    width = wq.shape[0]
    chunks = 32
    rows = seq // chunks
    jobs = len(prods)
    piece = (prods[0].shape[2] // 2, prods[0].shape[3])
    units = jobs * 2 * n_tp
    dma = pltpu.SemaphoreType.DMA
    shape = jax.ShapeDtypeStruct
    qb = seq // 8
    vmem = [(seq, width)] * 3 + [(RING, rows, width), (seq, dims), (qb, dims), (seq, dims), (seq, dims), (2, qb, dims), (2, qb // n_tp, width)] + [(2, qb, dims // 2)] * 2 + [
            (HOLD, 4) + piece, (4,) + piece, (2, 2) + piece, (2,) + piece, (LIVE,) + piece, (PAIR,) + piece, (units,) + piece, (2 * jobs,) + piece]
    sems = [(), (), (chunks,), (chunks,), (RING,), (8,), (), (units,), (HOLD,), (), (HOLD,), (units,), (2,), (PAIR,), (units,), (2,), (LIVE,), (units,), (2 * jobs,), (), (8,), (8,), (5, 2)]
    scratch = [pltpu.VMEM(size, F32) for size in vmem]
    scratch.insert(12, pltpu.VMEM((2, qb, width), BF))
    cols, grads, d_w, d_bias, *_ = pl.pallas_call(
        functools.partial(backward_kernel, n_tp, rows, chunks, jobs, heads),
        name='backward',
        out_shape=(shape((n_dp, seq, width // n_dp), F32), shape((2 * jobs,) + piece, F32), shape((width, 3 * dims), F32), shape((1, 3 * dims), F32),
                   shape((units, 4) + piece, F32), shape((units, 2) + piece, F32), shape((units,) + piece, F32)),
        in_specs=[ANY, ANY] + [VMEM] * 3 + [ANY] + [VMEM] * 2 + [ANY] * 2 + [VMEM] * 2 + [ANY] * (1 + jobs),
        out_specs=(ANY, ANY, VMEM, VMEM, ANY, ANY, ANY),
        scratch_shapes=scratch + [dma(size) for size in sems],
        compiler_params=pltpu.CompilerParams(collective_id=1, has_side_effects=True, vmem_limit_bytes=67_000_000),
        cost_estimate=pl.CostEstimate(flops=20 * 10 ** 9, bytes_accessed=100 * 2 ** 20, transcendentals=0),
    )(d_ctx, resid, q, k, v, ctx, top, inv, cos, sin, wq, back, emb, *prods)
    return d_w, d_bias, cols, grads.reshape(jobs, 2 * piece[0], piece[1])


WAYS = 4


def table_kernel(ids, rows_ref, out, *tables):
    step = pl.program_id(0)
    count = rows_ref.shape[0]
    part = count // WAYS

    @pl.when(step == 0)
    def _():
        for table in tables:
            table[...] = jnp.zeros_like(table)

    @pl.loop(0, part, unroll=4)
    def _(r):
        for way, table in enumerate(tables):
            row = way * part + r
            where = pl.ds(ids[step * count + row], 1)
            table[where, :] = table[where, :] + rows_ref[pl.ds(row, 1), :]

    @pl.when(step == pl.num_programs(0) - 1)
    def _():
        total = tables[0][...]
        for table in tables[1:]:
            total = total + table[...]
        out[...] = SHRINK * total[:out.shape[0]]


def table_rows(ids, rows, vocab_loc):
    count, block = rows.shape
    step = min(1024, count // 2)
    return pl.pallas_call(
        table_kernel,
        name='table_rows',
        grid_spec=pltpu.PrefetchScalarGridSpec(
            num_scalar_prefetch=1,
            grid=(count // step,),
            in_specs=[pl.BlockSpec((step, block), lambda i, ids: (i, 0))],
            out_specs=pl.BlockSpec((vocab_loc, block), lambda i, ids: (0, 0)),
            scratch_shapes=[pltpu.VMEM((vocab_loc + 8, block), F32)] * WAYS,
        ),
        out_shape=jax.ShapeDtypeStruct((vocab_loc, block), F32),
        compiler_params=pltpu.CompilerParams(dimension_semantics=('arbitrary',), vmem_limit_bytes=48 * 2 ** 20),
        cost_estimate=pl.CostEstimate(flops=3 * 10 ** 9, bytes_accessed=16 * 2 ** 20, transcendentals=0),
    )(ids, rows)


SPREAD = ((0, 2), (0, 4), (0, 1), (2, 4), (4, 2), (2, 1), (4, 1), (6, 1))


def gather_kernel(parts, block_in, out, send, recv, oself):
    p, at = plane()
    bar = pltpu.get_barrier_semaphore()
    for rel in (1, 2, 4):
        pl.semaphore_signal(bar, inc=1, device_id={'dp': at(rel)}, device_id_type=MESH)
    pl.semaphore_wait(bar, 3)
    size, block = block_in.shape
    rows = size // parts
    half = parts // 2

    def copy(j, rel, i, to):
        dst = out.at[pl.ds(i * rows, rows), pl.ds(pl.multiple_of(at(rel) * block, block), block)]
        src = block_in.at[pl.ds(i * rows, rows)] if rel == 0 else dst
        return rcopy(src, dst, send.at[j, i], recv.at[j, i], dp=at(to))

    def give(j, i):
        copy(j, SPREAD[j][0], i, SPREAD[j][1]).start()

    def take(j, i):
        rel, to = SPREAD[j]
        copy(j, rel ^ to, i, 0).wait_recv()
    own = pltpu.make_async_copy(block_in, out.at[:, pl.ds(pl.multiple_of(p * block, block), block)], oself)
    own.start()
    order_x = list(range(parts))
    order_y = order_x[half:] + order_x[:half]
    for i, j in zip(order_x, order_y):
        give(0, i)
        give(1, j)
    for i in order_x:
        give(2, i)
    for i, j in zip(order_x, order_y):
        take(0, i)
        if i < half:
            give(3, i)
        give(5, i)
        take(1, j)
        if j >= half:
            give(4, j)
        give(6, j)
    for i in order_x[:half]:
        for via, part in ((3, i), (4, i + half)):
            take(via, part)
            give(7, part)
    for i in order_x:
        for j in (2, 5, 6, 7):
            take(j, i)
    for i in order_x:
        for j, (rel, to) in enumerate(SPREAD):
            if j != (4 if i < half else 3):
                copy(j, rel, i, 0).wait_send()
    own.wait()


def gathered_columns(block_in, n_dp):
    size, block = block_in.shape
    parts = 4
    dma = pltpu.SemaphoreType.DMA
    return pl.pallas_call(
        functools.partial(gather_kernel, parts),
        name='gathered_columns',
        out_shape=jax.ShapeDtypeStruct((size, n_dp * block), F32),
        in_specs=[ANY],
        out_specs=ANY,
        scratch_shapes=[dma((len(SPREAD), parts)), dma((len(SPREAD), parts)), dma],
        compiler_params=pltpu.CompilerParams(collective_id=2, has_side_effects=True),
        cost_estimate=pl.CostEstimate(flops=10 * 10 ** 9, bytes_accessed=60 * 2 ** 20, transcendentals=0),
    )(block_in)


def dot(a, b, dims):
    return lax.dot_general(a, b, (dims, ((), ())), preferred_element_type=F32)


NT, TN, NN = ((1,), (1,)), ((0,), (0,)), ((1,), (0,))


def lane_head(shape, heads, halves):
    lane = lax.broadcasted_iota(jnp.int32, shape, 1)
    dims = shape[1] // halves
    return (lane % dims) // (dims // heads)


def turned(both, cos, sin):
    half = both.shape[1] // 2
    x1, x2 = both[:, :half], both[:, half:]
    return jnp.concatenate([x1 * cos - x2 * sin, x2 * cos + x1 * sin], axis=1)


def project(i, qb, emb, wq, bq, cos, sin, q, k, v):
    at_q = pl.ds(pl.multiple_of(i * qb, qb), qb)
    dims = q.shape[1]
    qkv = (dot(emb[at_q, :], wq[...], NN) + bq[...]).astype(BF)
    for ref, part in ((q, 0), (k, 1)):
        ref[at_q, :] = turned(qkv[:, part * dims:(part + 1) * dims].astype(F32), cos[at_q, :], sin[at_q, :]).astype(BF)
    v[at_q, :] = qkv[:, 2 * dims:]


def scores(i, j, kb, qb, scale, keys, q):
    s = dot(keys, q, NT) * scale
    key = j * kb + lax.broadcasted_iota(jnp.int32, (kb, qb), 0)
    query = i * qb + lax.broadcasted_iota(jnp.int32, (kb, qb), 1)
    return jnp.where(query >= key, s, -1e30)


def attend(i, h, heads, qb, q_ref, k_ref, v_ref, ctx_ref, top_ref, inv_ref, s_ref):
    kb = 2 * qb
    dims = q_ref.shape[1]
    scale = (dims // heads) ** -0.5
    at_q = pl.ds(pl.multiple_of(i * qb, qb), qb)
    q = jnp.where(lane_head((qb, dims), heads, 2) == h, q_ref[at_q, :].astype(F32), 0.0).astype(BF)
    count = (i + 2) // 2

    def at_key(j):
        return pl.ds(pl.multiple_of(j * kb, kb), kb)

    def first(j, top):
        s = scores(i, j, kb, qb, scale, k_ref[at_key(j), :], q)
        s_ref[at_key(j), :] = s
        return jnp.maximum(top, jnp.max(s, axis=0, keepdims=True))
    top = lax.fori_loop(0, count, first, jnp.full((1, qb), -1e30, F32))

    def weigh(j, total):
        e = jnp.exp(s_ref[at_key(j), :] - top)
        s_ref[at_key(j), :] = e
        return total + jnp.sum(e, axis=0, keepdims=True)
    inv = 1.0 / lax.fori_loop(0, count, weigh, jnp.zeros((1, qb), F32))

    def mix(j, acc):
        return acc + dot((s_ref[at_key(j), :] * inv).astype(BF), v_ref[at_key(j), :], TN)
    mixed = lax.fori_loop(0, count, mix, jnp.zeros((qb, dims), F32))
    ctx_ref[at_q, :] = jnp.where(lane_head((qb, dims), heads, 1) == h, mixed, ctx_ref[at_q, :])
    top_ref[pl.ds(h, 1), at_q] = top
    inv_ref[pl.ds(h, 1), at_q] = inv


def attend_grad(i, h, heads, qb, q_ref, k_ref, v_ref, ctx_ref, dctx_ref, top_ref, inv_ref, dq_ref, dk_ref, dv_ref):
    kb = 2 * qb
    dims = q_ref.shape[1]
    scale = (dims // heads) ** -0.5
    at_q = pl.ds(pl.multiple_of(i * qb, qb), qb)
    q = jnp.where(lane_head((qb, dims), heads, 2) == h, q_ref[at_q, :].astype(F32), 0.0).astype(BF)
    dc = jnp.where(lane_head((qb, dims), heads, 1) == h, dctx_ref[at_q, :], 0.0).astype(BF)
    ones = jnp.ones((8, dims), F32)
    mean = lax.dot_general(ones, dc.astype(F32) * ctx_ref[...], (NT, ((), ())), precision=lax.Precision.HIGHEST, preferred_element_type=F32)[:1]
    top, inv = top_ref[pl.ds(h, 1), at_q], inv_ref[pl.ds(h, 1), at_q]

    def step(j, dq):
        at_k = pl.ds(pl.multiple_of(j * kb, kb), kb)
        keys = k_ref[at_k, :]
        probs = (jnp.exp(scores(i, j, kb, qb, scale, keys, q) - top) * inv).astype(BF)
        ds = (probs.astype(F32) * (dot(v_ref[at_k, :], dc, NT) - mean) * scale).astype(BF)
        dv_ref[at_k, :] += dot(probs, dc, NN)
        dk_ref[at_k, :] += dot(ds, q, NN)
        return dq + dot(ds, keys, TN)
    dq = lax.fori_loop(0, (i + 2) // 2, step, jnp.zeros((qb, dims), F32))
    dq_ref[...] = jnp.where(lane_head((qb, dims), heads, 2) == h, dq, dq_ref[...])


def grad_rows(i, qb, cos, sin, dq, dk, dv, d_bias):
    at_q = pl.ds(pl.multiple_of(i * qb, qb), qb)
    back = [turned(values, cos, -sin) for values in (dq[...], dk[at_q, :])]
    rows = jnp.concatenate(back + [dv[at_q, :]], axis=1)
    d_bias[...] += jnp.sum(rows, axis=0, keepdims=True)
    return rows.astype(BF)


def solution(mesh):
    n_tp, n_dp = mesh.shape['tp'], mesh.shape['dp']
    in_specs = (P('dp', None), P('dp', None, None), P('tp', None)) + WEIGHT_SPECS
    out_specs = (P('tp', None),) + WEIGHT_SPECS

    def device_step(tokens, cotangent, emb_table, *weights):
        (w_qkv, b_qkv, w_out, b_out, ln1_gain, ln1_bias, w_gate, b_gate, w_lin, b_lin, w_down, b_down, ln2_gain) = weights
        tp, dp = lax.axis_index('tp'), lax.axis_index('dp')
        tokens = tokens[N0]
        seq_len, width = tokens.shape[N0], emb_table.shape[N1]
        heads, head_dim = b_qkv.shape[N0], b_qkv.shape[N1] // 3
        own = seq_len // n_tp
        ffn = w_gate.shape[N1]
        rk, rf, ro = width // n_dp, ffn // n_dp, w_out.shape[N0] // n_dp

        def cut(weight):
            rows = weight.shape[N0] // n_dp
            return lax.dynamic_slice_in_dim(weight, dp * rows, rows, N0)
        bias_rows = jnp.concatenate([b_gate[None], b_lin[None], jnp.zeros((14, ffn), BF)], axis=N0)
        piece = jnp.concatenate([cut(w_gate), cut(w_lin), cut(w_down), cut(w_out), bias_rows], axis=N0).astype(F32)

        vocab_loc = emb_table.shape[N0]
        local_ids = tokens - tp * vocab_loc
        in_shard = (local_ids >= N0) & (local_ids < vocab_loc)
        safe_ids = jnp.where(in_shard, local_ids, N0)
        found = jnp.take(emb_table, safe_ids, axis=N0)
        dims = heads * head_dim
        place = column_order(heads, head_dim)
        swap = (jnp.arange(3 * dims)[:, None] == jnp.asarray(place)[None, :]).astype(BF)
        wq = jnp.dot(w_qkv, swap, preferred_element_type=F32).astype(BF)
        bq = jnp.dot(b_qkv.reshape(N1, -N1), swap, preferred_element_type=F32)
        cos_tab, sin_tab = rope_tables(seq_len, head_dim, heads)
        emb_bf, (wg_full, wl_full, wd_full, wo_full), biases, tok_all, ctx_own, saved = embed(found, in_shard[:, None].astype(F32), piece, tokens.reshape(-N1, min(128, seq_len // 8)), (w_gate, w_lin, w_down, w_out), wq, bq, cos_tab, sin_tab, heads, n_tp, n_dp)
        ctx_own = ctx_own.reshape(n_tp, own, dims).astype(BF)
        is_own = (jnp.arange(n_tp) == tp)[:, None]
        bg_full, bl_full = [jnp.where(is_own, b[None].astype(F32), biases[:, i]) for i, b in enumerate((b_gate, b_lin))]

        blocks = 8

        def owned(values):
            return lax.dynamic_index_in_dim(values.reshape(blocks, n_tp, -N1, width), tp, N1, keepdims=False).reshape(own, width).astype(F32)
        emb_own, cot_own = owned(emb_bf), owned(cotangent[N0])
        attn_out = jnp.einsum('hse,hed->sd', ctx_own, wo_full, preferred_element_type=F32) + b_out.astype(F32)
        normed_one, norm_one_pull = jax.vjp(norm_scaled, ALPHA * emb_own + attn_out, ln1_gain.astype(F32))
        hidden = (normed_one + ln1_bias.astype(F32)).astype(BF)
        gate_pre = jnp.einsum('sk,tkc->tsc', hidden, wg_full, preferred_element_type=F32) + bg_full[:, None]
        lin_pre = jnp.einsum('sk,tkc->tsc', hidden, wl_full, preferred_element_type=F32) + bl_full[:, None]
        inner_val, act_pull = jax.vjp(geglu, gate_pre, lin_pre)
        inner_act = inner_val.astype(BF)
        ffn_out = jnp.einsum('tsc,tcd->sd', inner_act, wd_full, preferred_element_type=F32) + b_down.astype(F32)
        norm_two_pull = jax.vjp(norm_scaled, ALPHA * hidden.astype(F32) + ffn_out, ln2_gain.astype(F32))[N1]

        def product(lhs, rhs, spec):
            return jnp.einsum(spec, lhs, rhs, preferred_element_type=F32).reshape(n_tp, n_dp, -N1, width)

        d_resid_two, d_ln2_gain = norm_two_pull(cot_own)
        d_b_down = jnp.sum(d_resid_two, axis=N0)
        d_ffn_bf = d_resid_two.astype(BF)
        prod_down = product(inner_act, d_ffn_bf, 'tsc,sd->tcd')
        d_inner = jnp.einsum('sd,tcd->tsc', d_ffn_bf, wd_full, preferred_element_type=F32).astype(BF)
        d_gate_pre, d_lin_pre = act_pull(d_inner.astype(F32))
        d_b_gate = jnp.sum(d_gate_pre, axis=N1)
        d_b_lin = jnp.sum(d_lin_pre, axis=N1)
        d_gate_bf = d_gate_pre.astype(BF)
        d_lin_bf = d_lin_pre.astype(BF)
        prod_gate = product(hidden, d_gate_bf, 'sk,tsc->tkc')
        prod_lin = product(hidden, d_lin_bf, 'sk,tsc->tkc')
        d_hidden = ALPHA * d_resid_two + jnp.einsum('tsc,tkc->sk', d_gate_bf, wg_full, preferred_element_type=F32) + jnp.einsum('tsc,tkc->sk', d_lin_bf, wl_full, preferred_element_type=F32)
        d_ln1_bias = jnp.sum(d_hidden, axis=N0)
        d_resid_one, d_ln1_gain = norm_one_pull(d_hidden)
        d_b_out = jnp.sum(d_resid_one, axis=N0)
        d_attn_bf = d_resid_one.astype(BF)
        d_w_out = jnp.einsum('hse,sd->hed', ctx_own, d_attn_bf, preferred_element_type=F32)
        d_w_out = lax.all_gather(lax.psum_scatter(d_w_out.reshape(-N1, width), ALL, scatter_dimension=N0, tiled=True), 'dp', axis=N0, tiled=True)
        d_ctx = jnp.einsum('sd,hed->hse', d_attn_bf, wo_full, preferred_element_type=F32)
        d_w_qkv, d_b_qkv, d_cols, mine = backward(
            d_ctx.reshape(n_tp, blocks, own // blocks, dims), (ALPHA * d_resid_one).reshape(blocks, own // blocks, width), saved, cos_tab, sin_tab, wq, swap.T, emb_bf,
            (prod_gate, prod_lin, prod_down), heads, n_tp, n_dp)
        d_b_qkv = jnp.dot(d_b_qkv, swap.astype(F32).T, precision=lax.Precision.HIGHEST)[N0]
        d_w_qkv = lax.psum(d_w_qkv, 'dp')
        d_w_gate, d_w_lin, d_w_down = [lax.all_gather(grad, 'dp', axis=N0, tiled=True) for grad in mine]
        all_ids = tok_all.reshape(-N1) - tp * vocab_loc
        all_ids = jnp.where((all_ids >= N0) & (all_ids < vocab_loc), all_ids, vocab_loc)
        d_table = gathered_columns(table_rows(all_ids, d_cols.reshape(n_dp * seq_len, -N1), vocab_loc), n_dp)

        slot = (jnp.arange(n_tp) == tp).astype(F32)[:, None]
        d_bq_rows = jnp.pad(slot * d_b_qkv[None], ((N0, N0), (N0, ffn - d_b_qkv.shape[N0])))
        small = jnp.concatenate([d_b_gate, d_b_lin, d_bq_rows, jnp.stack([d_b_out, d_ln1_gain, d_ln1_bias, d_b_down, d_ln2_gain])], axis=N0)
        small = lax.psum(small, ALL)
        d_b_gate = lax.dynamic_index_in_dim(small[:n_tp], tp, N0, keepdims=False)
        d_b_lin = lax.dynamic_index_in_dim(small[n_tp:N2 * n_tp], tp, N0, keepdims=False)
        d_b_qkv = lax.dynamic_index_in_dim(small[N2 * n_tp:3 * n_tp], tp, N0, keepdims=False)[:d_b_qkv.shape[N0]].reshape(heads, 3 * head_dim)
        d_b_out, d_ln1_gain, d_ln1_bias, d_b_down, d_ln2_gain = [small[3 * n_tp + i] for i in range(5)]
        return (d_table, d_w_qkv, d_b_qkv, d_w_out, d_b_out, d_ln1_gain, d_ln1_bias, d_w_gate, d_b_gate, d_w_lin, d_b_lin, d_w_down, d_b_down, d_ln2_gain)

    return jax.shard_map(device_step, mesh=mesh, in_specs=in_specs, out_specs=out_specs, check_vma=False)
```

```python
import functools

import jax
import jax.numpy as jnp
import numpy as np
from jax import lax
from jax.experimental import pallas as pl
from jax.experimental.pallas import tpu as pltpu
from jax.sharding import PartitionSpec as P

ALPHA = 140.0 ** 0.5
EPS = 1e-5
SHRINK = 0.1
ROPE_BASE = 10000.0
WEIGHT_SPECS = (P(None, 'tp'), P('tp', None), P('tp', None), P(), P(), P(), P(None, 'tp'), P('tp'), P(None, 'tp'), P('tp'), P('tp', None), P(), P())
ALL = ('tp', 'dp')
BF = jnp.bfloat16
N0, N1, N2 = range(3)
F32 = jnp.float32
MESH = pl.DeviceIdType.MESH
ANY = pl.BlockSpec(memory_space=pl.ANY)
VMEM = pl.BlockSpec(memory_space=pltpu.VMEM)


def norm_scaled(values, gain):
    mean_val = jnp.mean(values, axis=-1, keepdims=True)
    centered = values - mean_val
    variance = jnp.mean(centered * centered, axis=-1, keepdims=True)
    return centered * lax.rsqrt(variance + EPS) * gain


def geglu(gate_pre, lin_pre):
    return jax.nn.gelu(gate_pre, approximate=False) * lin_pre


def rope_tables(seq_len, head_dim, heads):
    half_dim = head_dim // 2
    inv_freq = (ROPE_BASE ** (-2.0 * np.arange(half_dim) / head_dim)).astype(np.float32)
    angles = np.arange(seq_len, dtype=np.float32)[:, None] * inv_freq[None, :]
    return [jnp.asarray(np.tile(table(angles), (1, heads))) for table in (np.cos, np.sin)]


def column_order(heads, head_dim):
    cols = np.arange(3 * heads * head_dim).reshape(heads, 3, 2, head_dim // 2)
    return np.concatenate([cols[:, part].transpose(1, 0, 2).ravel() for part in (0, 1)] + [cols[:, 2].ravel()])


def rcopy(src, dst, send, recv, **where):
    return pltpu.make_async_remote_copy(src_ref=src, dst_ref=dst, send_sem=send, recv_sem=recv, device_id=dict(where), device_id_type=MESH)


def plane():
    p = lax.axis_index('dp')
    y, x, c = p // 4, (p // 2) % 2, p % 2

    def at(rel):
        yy = 1 - y if rel & 4 else y
        xx = 1 - x if rel & 2 else x
        cc = 1 - c if rel & 1 else c
        return yy * 4 + xx * 2 + cc
    return p, at


def entry_barrier(z, n, at):
    bar = pltpu.get_barrier_semaphore()
    for rel in range(1, 8):
        pl.semaphore_signal(bar, inc=1, device_id={'dp': at(rel)}, device_id_type=MESH)
    for d in range(1, n):
        pl.semaphore_signal(bar, inc=1, device_id={'tp': (z + d) % n}, device_id_type=MESH)
    pl.semaphore_wait(bar, 7 + n - 1)


LAG = 3


def chain_sum(k, z, n, rows, chunks, part, left, right, done, send_r, send_l, recv_l, recv_r, place=lambda c: c):
    last = n - 1

    def at_rows(c):
        return pl.ds(pl.multiple_of(place(c) * rows, rows), rows)

    def cut(ref, c):
        return ref.at[at_rows(c)]

    def load(ref, c):
        return ref[at_rows(c)]

    def store(ref, c, value):
        ref[at_rows(c)] = value
    cl, cr = k - LAG * z, k - LAG * (last - z)
    okl, okr = (cl >= 0) & (cl < chunks), (cr >= 0) & (cr < chunks)

    @pl.when(okl & (z > 0))
    def _():
        rcopy(cut(left, cl), cut(left, cl), send_r, recv_l.at[cl], tp=z).wait_recv()

    @pl.when(okl & (z == last))
    def _():
        done(cl, load(left, cl) + load(part, cl))

    @pl.when(okl & (z > 0) & (z < last))
    def _():
        run = load(left, cl)

        @pl.when(z >= n // 2)
        def _():
            done(cl, run + load(right, cl))
        store(left, cl, run + load(part, cl))

    @pl.when(okr & (z < last))
    def _():
        rcopy(cut(right, cr), cut(right, cr), send_l, recv_r.at[cr], tp=z).wait_recv()

    @pl.when(okr & (z == 0))
    def _():
        done(cr, load(part, cr) + load(right, cr))

    @pl.when(okr & (z > 0) & (z < last))
    def _():
        run = load(right, cr)

        @pl.when(z < n // 2)
        def _():
            done(cr, load(left, cr) + run)
        store(right, cr, run + load(part, cr))

    @pl.when(okl & (z == 0))
    def _():
        rcopy(cut(part, cl), cut(left, cl), send_r, recv_l.at[cl], tp=z + 1).start()

    @pl.when(okl & (z > 0) & (z < last))
    def _():
        rcopy(cut(left, cl), cut(left, cl), send_r, recv_l.at[cl], tp=z + 1).start()

    @pl.when(okr & (z == last))
    def _():
        rcopy(cut(part, cr), cut(right, cr), send_l, recv_r.at[cr], tp=z - 1).start()

    @pl.when(okr & (z > 0) & (z < last))
    def _():
        rcopy(cut(right, cr), cut(right, cr), send_l, recv_r.at[cr], tp=z - 1).start()


def chain_drain(z, n, part, left, right, send_r, send_l, recv_l, recv_r):
    @pl.when(z < n - 1)
    def _():
        rcopy(part, left, send_r, recv_l.at[0], tp=z + 1).wait_send()

    @pl.when(z > 0)
    def _():
        rcopy(part, right, send_l, recv_r.at[0], tp=z - 1).wait_send()


EDGES = ((0, 0, 2), (0, 0, 4), (0, 0, 1), (2, 1, 4), (4, 2, 2), (2, 0, 1), (4, 0, 1), (6, 1, 1), (6, 2, 1))
CROSS, DIAGONAL, LAST = ((0, 3, 5), (1, 4, 6)), ((3, 7), (4, 8)), {1: (2,), 3: (5,), 5: (6,), 7: (7, 8)}
STEPS = (4, 10, 17, 21, 25, 29)
FIRST = 18
ORDER = (0, 2, 4, 1, 3, 5, 6, 7)


def emb_kernel(n, rows, chunks, cuts, heads, found, mask, wq, bq, cos, sin, piece, toks, *refs):
    m = len(cuts)
    local, outs = refs[:m], refs[m + N1:N2 * m + N1]
    out, (bias, tok_all, wall, ctx_own, q, k_all, v, ctx, top, inv, part, left, right, raw, low, weights, send_r, send_l, recv_l, recv_r, tsend, trecv, tself, zsend, zrecv, psend, precv, lsem, isem, osem, bsem, asend, arecv, aself) = refs[m], refs[N2 * m + N1:]
    blocks = 8
    qb = part.shape[N0] // blocks
    per = chunks // blocks
    z = lax.axis_index('tp')
    p, at = plane()
    entry_barrier(z, n, at)
    half = piece.shape[N0] // N2

    @pl.when(z < n - N1)
    def _():
        rcopy(piece, wall.at[z, p], zsend.at[z], zrecv.at[z], tp=z + N1).start()

    @pl.when(z > N0)
    def _():
        rcopy(piece, wall.at[z, p], bsem.at[N1], zrecv.at[z], tp=z - N1).start()
    mine = [pltpu.make_async_copy(toks, tok_all.at[p], tself)]
    mine += [pltpu.make_async_copy(src, dst.at[z], lsem.at[i]) for i, (src, dst) in enumerate(zip(local, outs))]
    for copy in mine:
        copy.start()
    for rel in range(N1, 8):
        rcopy(toks, tok_all.at[p], tsend.at[rel], trecv.at[rel], dp=at(rel)).start()

    def others(d, body):
        @pl.when(z >= d)
        def _():
            body(z - d, -N1)

        @pl.when(z + d < n)
        def _():
            body(z + d, N1)

    def region(t, rel, side):
        blk = wall.at[t, at(rel)]
        return blk if side == N0 else wall.at[t, at(rel), pl.ds((side - N1) * half, half)]

    def give(t, j):
        rel, side, to = EDGES[j]
        rcopy(region(t, rel, side), region(t, rel, side), psend.at[t, j], precv.at[t, j], dp=at(to)).start()

    def take(t, j):
        rel, side, to = EDGES[j]
        blk = region(t, rel ^ to, side)
        rcopy(blk, blk, psend.at[t, j], precv.at[t, j], dp=p).wait_recv()

    def gave(t, j):
        rel, side, to = EDGES[j]
        rcopy(region(t, rel, side), region(t, rel, side), psend.at[t, j], precv.at[t, j], dp=p).wait_send()

    def arrive(d):
        def body(t, sign):
            blk = wall.at[t, p]
            rcopy(blk, blk, zsend.at[t], zrecv.at[t], tp=z).wait_recv()

            @pl.when((z - sign >= N0) & (z - sign < n))
            def _():
                rcopy(blk, blk, zsend.at[t], zrecv.at[t], tp=z - sign).start()
            for j in range(3):
                give(t, j)
        others(d, body)

    def relay(d, moves):
        def body(t, sign):
            for first, *rest in moves:
                take(t, first)
                for j in rest:
                    give(t, j)
        others(d, body)

    k_all[...] = jnp.zeros_like(k_all)
    v[...] = jnp.zeros_like(v)
    arrive(N1)

    @pl.loop(N0, blocks)
    def _(i):
        at_i = pl.ds(pl.multiple_of(i * qb, qb), qb)
        part[at_i, :] = jnp.where(mask[at_i, :] > N0, found[at_i, :].astype(F32), 0.0)

    def done(c, value):
        out[pl.ds(pl.multiple_of(c * rows, rows), rows)] = value.astype(out.dtype)

    def other(i):
        return i + (i + n - z) // n

    def loaded(i, rel, slot):
        return pltpu.make_async_copy(wall.at[other(i), at(rel), pl.ds(N0, cuts[-N1][N1])], raw.at[slot], isem.at[slot])

    def stored(i, rel, slot):
        return [pltpu.make_async_copy(low.at[slot, pl.ds(lo, hi - lo)], dst.at[other(i), at(rel)], osem.at[slot, k]) for k, ((lo, hi), dst) in enumerate(zip(cuts, outs))]
    plan = [(i, rel) for rel in ORDER for i in range(n - N1)]

    def prefetch(s):
        i, rel = plan[s]
        for j in LAST.get(rel, ()):
            take(other(i), j)
        loaded(i, rel, s % N2).start()

    def convert(s):
        i, rel = plan[s]
        loaded(i, rel, s % N2).wait()
        if s >= N2:
            for copy in stored(*plan[s - N2], s % N2):
                copy.wait()
        low[s % N2] = raw[s % N2].astype(low.dtype)
        if s + N1 < len(plan):
            prefetch(s + N1)
        for copy in stored(i, rel, s % N2):
            copy.start()
    events = [(STEPS[d - N1], functools.partial(relay, d, CROSS)) for d in range(N1, n)] + [(STEPS[d + n - N2], functools.partial(relay, d, DIAGONAL)) for d in range(N1, n)]
    events += [(N2 * d - N2, functools.partial(arrive, d)) for d in range(N2, n)]
    events += [(FIRST - N1, functools.partial(prefetch, N0))] + [(FIRST + s, functools.partial(convert, s)) for s in range(len(plan))]

    start = per + LAG * (n - N1)

    share = qb // n

    def context(i, d):
        to = (z + d) % n
        src = ctx.at[pl.ds(pl.multiple_of(i * qb + to * share, share), share)]
        if d == N0:
            return pltpu.make_async_copy(src, ctx_own.at[z, i], aself)
        return rcopy(src, ctx_own.at[z, i], asend, arecv.at[z], tp=to)

    @pl.loop(N0, max(start + blocks * heads + N1, FIRST + len(plan)))
    def _(k):
        step = k - start
        i = step // heads - N1

        @pl.when((step > N0) & (step % heads == N0) & (step <= blocks * heads))
        def _():
            for d in range(n):
                context(i, d).start()
        chain_sum(k, z, n, rows, chunks, part, left, right, done, send_r, send_l, recv_l, recv_r)
        for at_step, event in events:
            pl.when(k == at_step)(event)

        @pl.when((step >= N0) & (step < blocks * heads))
        def _():
            @pl.when(step % heads == N0)
            def _():
                project(step // heads, qb, out, wq, bq, cos, sin, q, k_all, v)
            attend(step // heads, step % heads, heads, qb, q, k_all, v, ctx, top, inv, weights)

    pltpu.make_async_copy(ctx_own.at[z], ctx_own.at[z], aself).wait()
    for d in range(N1, n):
        src = (z + d) % n
        rcopy(ctx_own.at[src], ctx_own.at[src], asend, arecv.at[src], tp=z).wait()
    chain_drain(z, n, part, left, right, send_r, send_l, recv_l, recv_r)
    for s in (len(plan) - N2, len(plan) - N1):
        for copy in stored(*plan[s], s % N2):
            copy.wait()

    def finish(t, sign):
        for j in range(len(EDGES)):
            gave(t, j)
        tail = pltpu.make_async_copy(wall.at[t, p, pl.ds(cuts[-N1][N1], bias.shape[N1])], bias.at[t], bsem.at[N0])
        tail.start()
        tail.wait()

        @pl.when((z - sign >= N0) & (z - sign < n))
        def _():
            rcopy(wall.at[t, p], wall.at[t, p], zsend.at[t], zrecv.at[t], tp=z).wait_send()
    for d in range(N1, n):
        others(d, finish)
    for copy in mine:
        copy.wait()
    for rel in range(N1, 8):
        rcopy(toks, tok_all.at[at(rel)], tsend.at[rel], trecv.at[rel], dp=at(rel)).wait()

    @pl.when(z < n - N1)
    def _():
        rcopy(piece, wall.at[z, p], zsend.at[z], zrecv.at[z], tp=z + N1).wait_send()

    @pl.when(z > N0)
    def _():
        rcopy(piece, wall.at[z, p], bsem.at[N1], zrecv.at[z], tp=z - N1).wait_send()


def embed(found, mask, piece, toks, local, wq, bq, cos, sin, heads, n_tp, n_dp):
    seq, width = found.shape
    chunks = 32
    rows = seq // chunks
    dims = wq.shape[1] // 3
    cuts, lo = [], 0
    for weight in local:
        cuts.append((lo, lo + weight.shape[0] // n_dp))
        lo = cuts[-1][1]
    dma = pltpu.SemaphoreType.DMA
    shape = jax.ShapeDtypeStruct
    shapes = [shape((seq, width), BF)]
    shapes += [shape((n_tp, n_dp, w.shape[0] // n_dp, w.shape[1]), BF) for w in local]
    shapes += [shape((n_tp, piece.shape[0] - lo, width), F32), shape((n_dp,) + toks.shape, toks.dtype), shape((n_tp, n_dp) + piece.shape, F32), shape((n_tp, 8, seq // n_tp // 8, dims), F32)]
    shapes += [shape((seq, dims), BF)] * 3 + [shape((seq, dims), F32)] + [shape((heads, seq), F32)] * 2
    out = pl.pallas_call(
        functools.partial(emb_kernel, n_tp, rows, chunks, cuts, heads),
        name='embed',
        out_shape=shapes,
        in_specs=[VMEM] * 6 + [ANY] * (2 + len(local)),
        out_specs=[VMEM] + [ANY] * (4 + len(local)) + [VMEM] * 6,
        scratch_shapes=[pltpu.VMEM((seq, width), F32)] * 3 + [pltpu.VMEM((2, lo, width), F32), pltpu.VMEM((2, lo, width), BF), pltpu.VMEM((seq, seq // 8), F32), dma, dma, dma((chunks,)), dma((chunks,)),
                        dma((8,)), dma((8,)), dma, dma((n_tp,)), dma((n_tp,)), dma((n_tp, len(EDGES))), dma((n_tp, len(EDGES))), dma((len(local),)), dma((2,)), dma((2, len(local))), dma((2,)),
                        dma, dma((n_tp,)), dma],
        compiler_params=pltpu.CompilerParams(collective_id=0, has_side_effects=True, vmem_limit_bytes=60 * 2 ** 20),
        cost_estimate=pl.CostEstimate(flops=20 * 10 ** 9, bytes_accessed=80 * 2 ** 20, transcendentals=0),
    )(found, mask, wq, bq, cos, sin, piece, toks, *[w.reshape(n_dp, w.shape[0] // n_dp, w.shape[1]) for w in local])
    m = 1 + len(local)
    return out[0], [w.reshape(n_tp, -1, w.shape[3]) for w in out[1:m]], out[m], out[m + 1], out[m + 3], out[m + 4:]


RING = 4
HOLD, LIVE, PAIR = 4, 8, 4
ADD, LOAD, CROSSED, LAND, PLANE = 1, 4, 5, 7, 8
GATHER = (37, 41)


def block_of(ref, at, rel, side):
    return ref.at[at(rel)] if side == 0 else ref.at[at(rel), side - 1]


class Spread:
    def __init__(self, at, block, send, recv, own=None):
        self.at, self.block, self.send, self.recv, self.own = at, block, send, recv, own

    def copy(self, j, rel, side, to):
        dst = self.block(rel, side)
        src = self.own if rel == 0 and self.own is not None else dst
        return rcopy(src, dst, self.send.at[j], self.recv.at[j], dp=self.at(to))

    def give(self, j):
        self.copy(j, *EDGES[j]).start()

    def take(self, j):
        rel, side, to = EDGES[j]
        self.copy(j, rel ^ to, side, 0).wait_recv()

    def start(self):
        for j in range(3):
            self.give(j)

    def relay(self, moves):
        for first, *rest in moves:
            self.take(first)
            for j in rest:
                self.give(j)

    def cross(self):
        self.relay(CROSS)

    def diagonal(self):
        self.relay(DIAGONAL)

    def finish(self):
        for j in (2, 5, 6, 7, 8):
            self.take(j)
        for j, (rel, side, _) in enumerate(EDGES):
            self.copy(j, rel, side, 0).wait_send()


def backward_kernel(n, rows, chunks, jobs, heads, d_ctx, resid, q, k_all, v, ctx, top, inv, cos, sin, wq, back, emb, *refs):
    prods = refs[:jobs]
    whole = refs[jobs:N2 * jobs - N1]
    out, grads, d_w, d_bias, landed, cross, last, part, left, right, total, dctx, dq, dk, dv, ctx_in, res_in, cos_in, sin_in, emb_in, work, fresh, xin, yin, keep, pass_on, along, final, *sems = refs[N2 * jobs - N1:]
    send_r, send_l, recv_l, recv_r, osend, orecv, csend, crecv, esem, fsem, xsend, xrecv, xsem, ysend, yrecv, ysem, ksem, zrecv, frecv, asend, arecv, aself, isem, gsend, grecv = sems
    z = lax.axis_index('tp')
    p, at = plane()
    entry_barrier(z, n, at)
    blocks = 8
    per = chunks // blocks
    qb = rows * per
    share = qb // n
    block = out.shape[N2]
    lead = jnp.maximum(z, n - N1 - z)
    span = N2 * n
    units = jobs * span
    size = work.shape[N2]

    def rows_of(i, to, count):
        return pl.ds(pl.multiple_of(i * qb + to * count, count), count)

    def exchange(i, d):
        to = (z + d) % n
        dst = dctx.at[rows_of(i, z, share)]
        if d == N0:
            return pltpu.make_async_copy(d_ctx.at[z, i], dst, aself.at[i])
        return rcopy(d_ctx.at[to, i], dst, asend, arecv.at[i], tp=to)

    @pl.loop(N0, blocks)
    def _(b):
        for d in range(n):
            exchange(blocks - N1 - b, d).start()

    def piece(m, u, rel):
        return prods[m].at[(u % span) // N2, at(rel), pl.ds(pl.multiple_of((u % N2) * size, size), size)]

    for m in range(jobs):
        @pl.loop(m * span, (m + N1) * span)
        def _(u, m=m):
            for i in range(4):
                rcopy(piece(m, u, N2 * i + N1), landed.at[u, i], csend, crecv.at[u], dp=at(N1)).start()

    def inputs(i):
        slot = i % N2
        at_q = rows_of(i, N0, qb)
        pairs = ((ctx.at[at_q], ctx_in), (resid.at[i], res_in), (cos.at[at_q], cos_in), (sin.at[at_q], sin_in), (emb.at[at_q], emb_in))
        return [pltpu.make_async_copy(src, dst.at[slot], isem.at[j, slot]) for j, (src, dst) in enumerate(pairs)]

    dk[...] = jnp.zeros_like(dk)
    dv[...] = jnp.zeros_like(dv)
    d_w[...] = jnp.zeros_like(d_w)
    d_bias[...] = jnp.zeros_like(d_bias)
    for copy in inputs(blocks - N1):
        copy.start()

    def attention_step(b, h):
        i = blocks - N1 - b

        @pl.when(h == N0)
        def _():
            for copy in inputs(i):
                copy.wait()

            @pl.when(b + N1 < blocks)
            def _():
                for copy in inputs(i - N1):
                    copy.start()
            exchange(i, N0).wait()
            others = dctx.at[pl.ds(N0, (n - N1) * share)]
            rcopy(others, others, asend, arecv.at[i], tp=z).wait_recv()
        attend_grad(i, h, heads, qb, q, k_all, v, ctx_in.at[i % N2], dctx, top, inv, dq, dk, dv)

        @pl.when(h == heads - N1)
        def _():
            slot = i % N2
            got = grad_rows(i, qb, cos_in[slot], sin_in[slot], dq, dk, dv, d_bias)
            d_w[...] += dot(emb_in[slot], dot(got, back[...], NN).astype(BF), TN)
            part[rows_of(i, N0, qb), :] = dot(got, wq[...], NT)
            part[rows_of(i, z, share), :] = part[rows_of(i, z, share), :] + res_in[i % N2]

    def sides(u):
        side = u % N2
        return side, at(N2) * (N1 - side) + at(4) * side, at(4) * (N1 - side) + at(N2) * side

    def fetch(u):
        slot = u % HOLD

        @pl.when(u >= HOLD)
        def _():
            rcopy(xin.at[N0], cross.at[N0], xsend.at[slot], xrecv.at[N0], dp=p).wait_send()
        for m in range(jobs):
            @pl.when(u // span == m)
            def _(m=m):
                for i in range(4):
                    pltpu.make_async_copy(piece(m, u, N2 * i), work.at[slot, i], esem.at[slot]).start()
        rcopy(landed.at[u], landed.at[u], csend, crecv.at[u], dp=p).wait_recv()
        pltpu.make_async_copy(landed.at[u], fresh, fsem).start()

    def add(u):
        slot = u % HOLD
        pltpu.make_async_copy(landed.at[u], work.at[slot], esem.at[slot]).wait()
        pltpu.make_async_copy(landed.at[u], fresh, fsem).wait()
        for i in range(4):
            work[slot, i] = work[slot, i] + fresh[i]

    def add_send(u):
        slot = u % HOLD
        side, first, second = sides(u)
        rcopy(work.at[slot, N1 + side], cross.at[u, N0], xsend.at[slot], xrecv.at[u], dp=first).start()
        rcopy(work.at[slot, 3], cross.at[u, N1], xsend.at[slot], xrecv.at[u], dp=first).start()

    def load_cross(u):
        rcopy(cross.at[u], cross.at[u], xsend.at[N0], xrecv.at[u], dp=p).wait_recv()
        pltpu.make_async_copy(cross.at[u], xin.at[u % N2], xsem.at[u % N2]).start()

    def crossed(u):
        slot = u % HOLD
        pltpu.make_async_copy(cross.at[u], xin.at[u % N2], xsem.at[u % N2]).wait()

        @pl.when(u >= LIVE)
        def _():
            pltpu.make_async_copy(keep.at[u % LIVE], keep.at[u % LIVE], ksem.at[u % LIVE]).wait()

        @pl.when(u >= PAIR)
        def _():
            rcopy(pass_on.at[u % PAIR], last.at[u], ysend.at[u % PAIR], yrecv.at[u], dp=p).wait_send()
        keep[u % LIVE] = xin[u % N2, N0] + work[slot, N0]
        pass_on[u % PAIR] = xin[u % N2, N1] + work[slot, N2 - u % N2]

    def crossed_send(u):
        side, first, second = sides(u)
        rcopy(pass_on.at[u % PAIR], last.at[u], ysend.at[u % PAIR], yrecv.at[u], dp=second).start()

    def load_last(u):
        rcopy(last.at[u], last.at[u], ysend.at[N0], yrecv.at[u], dp=p).wait_recv()
        pltpu.make_async_copy(last.at[u], yin.at[u % N2], ysem.at[u % N2]).start()

    def in_plane(u):
        pltpu.make_async_copy(last.at[u], yin.at[u % N2], ysem.at[u % N2]).wait()
        keep[u % LIVE] = keep[u % LIVE] + yin[u % N2]

    def unit(k):
        u = (k // 3) * N2 + k % 3
        return u, (k >= N0) & (k % 3 < N2) & (u < units)

    def along_tp(k, t, send):
        toward = jnp.where(z < t, z, n - N1 - z)
        late = jnp.where(z == t, max(t, n - N1 - t), toward)
        u, ok = unit(k - PLANE - N1 - late)
        mine = (u // span) * N2 + u % N2
        slot = u % LIVE
        ok = ok & ((u // N2) % n == t)

        def add_from(ref, sem):
            rcopy(ref, ref, csend, sem, tp=z).wait_recv()
            keep[slot] = keep[slot] + ref[...]
        if send:
            @pl.when(ok & (z < t))
            def _():
                rcopy(keep.at[slot], along.at[u], ksem.at[slot], zrecv.at[u], tp=z + N1).start()

            @pl.when(ok & (z > t + N1))
            def _():
                rcopy(keep.at[slot], along.at[u], ksem.at[slot], zrecv.at[u], tp=z - N1).start()

            @pl.when(ok & (z == t + N1))
            def _():
                rcopy(keep.at[slot], final.at[mine], ksem.at[slot], frecv.at[mine], tp=z - N1).start()

            for m in range(jobs):
                @pl.when(ok & (z == t) & (u // span == m))
                def _(m=m):
                    dst = whole[m].at[p, u % N2] if m < jobs - N1 else grads.at[u % N2]
                    pltpu.make_async_copy(keep.at[slot], dst, ksem.at[slot]).start()
        else:
            @pl.when(ok & (((z > N0) & (z <= t)) | ((z > t) & (z < n - N1))))
            def _():
                add_from(along.at[u], zrecv.at[u])
            if t < n - N1:
                @pl.when(ok & (z == t))
                def _():
                    add_from(final.at[mine], frecv.at[mine])

    spread = [Spread(at, functools.partial(block_of, whole[m], at), gsend.at[m], grecv.at[m]) for m in range(jobs - N1)]

    def place(c):
        return (blocks - N1 - c // per) * per + c % per

    def chunk(c):
        return total.at[c % RING]

    def done(c, value):
        @pl.when(c >= RING)
        def _():
            pltpu.make_async_copy(chunk(c), chunk(c), osend.at[c % RING]).wait()
        total[c % RING] = value

    def hand_out(c):
        where = out.at[p, pl.ds(pl.multiple_of(place(c) * rows, rows), rows)]
        for rel in range(8):
            src = total.at[c % RING, :, pl.ds(pl.multiple_of(at(rel) * block, block), block)]
            if rel == N0:
                pltpu.make_async_copy(src, where, osend.at[c % RING]).start()
            else:
                rcopy(src, where, osend.at[c % RING], orecv.at[rel], dp=at(rel)).start()

    def staged(k, offset, stage):
        u, ok = unit(k - offset)
        pl.when(ok)(functools.partial(stage, u))
    steps = max(heads + chunks + LAG * (n - N1) + N1, (units // N2) * 3 + PLANE + n)

    @pl.loop(N0, steps)
    def _(k):
        c = k - heads - LAG * lead - N1

        @pl.when((c >= N0) & (c < chunks))
        def _():
            hand_out(c)
        chain_sum(k - heads, z, n, rows, chunks, part, left, right, done, send_r, send_l, recv_l, recv_r, place)
        for offset, stage in ((CROSSED, crossed), (ADD, add), (PLANE, in_plane)):
            staged(k, offset, stage)
        for t in range(n):
            along_tp(k, t, False)
        for offset, stage in ((N0, fetch), (LOAD, load_cross), (LAND, load_last)):
            staged(k, offset, stage)

        @pl.when(k < blocks * heads)
        def _():
            attention_step(k // heads, k % heads)
        for offset, stage in ((ADD, add_send), (CROSSED, crossed_send)):
            staged(k, offset, stage)
        for t in range(n):
            along_tp(k, t, True)
        for m, gather in enumerate(spread):
            for offset, stage in ((N0, gather.start), (3, gather.cross), (6, gather.diagonal)):
                pl.when(k == GATHER[m] + offset)(stage)

    chain_drain(z, n, part, left, right, send_r, send_l, recv_l, recv_r)
    for c in range(max(N0, chunks - RING), chunks):
        pltpu.make_async_copy(chunk(c), chunk(c), osend.at[c % RING]).wait()
    for rel in range(N1, 8):
        rcopy(out.at[at(rel)], out.at[at(rel)], csend, orecv.at[rel], dp=p).wait_recv()
    for slot in range(HOLD):
        rcopy(xin.at[N0], cross.at[N0], xsend.at[slot], xrecv.at[N0], dp=p).wait_send()
    for slot in range(PAIR):
        rcopy(pass_on.at[slot], last.at[N0], ysend.at[slot], yrecv.at[N0], dp=p).wait_send()
    for slot in range(LIVE):
        pltpu.make_async_copy(keep.at[slot], keep.at[slot], ksem.at[slot]).wait()
    rcopy(landed, landed, csend, crecv.at[N0], dp=p).wait_send()
    for gather in spread:
        gather.finish()
    sent = dctx.at[pl.ds(N0, (n - N1) * share * blocks)]
    rcopy(sent, sent, asend, arecv.at[N0], tp=z).wait_send()


def backward(d_ctx, resid, saved, cos, sin, wq, back, emb, prods, heads, n_tp, n_dp):
    q, k, v, ctx, top, inv = saved
    seq, dims = q.shape
    width = wq.shape[0]
    chunks = 32
    rows = seq // chunks
    jobs = len(prods)
    piece = (prods[0].shape[2] // 2, prods[0].shape[3])
    units = jobs * 2 * n_tp
    dma = pltpu.SemaphoreType.DMA
    shape = jax.ShapeDtypeStruct
    qb = seq // 8
    vmem = [(seq, width)] * 3 + [(RING, rows, width), (seq, dims), (qb, dims), (seq, dims), (seq, dims), (2, qb, dims), (2, qb // n_tp, width)] + [(2, qb, dims // 2)] * 2 + [
            (HOLD, 4) + piece, (4,) + piece, (2, 2) + piece, (2,) + piece, (LIVE,) + piece, (PAIR,) + piece, (units,) + piece, (2 * jobs,) + piece]
    sems = [(), (), (chunks,), (chunks,), (RING,), (8,), (), (units,), (HOLD,), (), (HOLD,), (units,), (2,), (PAIR,), (units,), (2,), (LIVE,), (units,), (2 * jobs,), (), (8,), (8,), (5, 2), (jobs - 1, len(EDGES)), (jobs - 1, len(EDGES))]
    scratch = [pltpu.VMEM(size, F32) for size in vmem]
    scratch.insert(12, pltpu.VMEM((2, qb, width), BF))
    full = shape((n_dp, 2) + piece, F32)
    *whole, cols, grads, d_w, d_bias, _, _, _ = pl.pallas_call(
        functools.partial(backward_kernel, n_tp, rows, chunks, jobs, heads),
        name='backward',
        out_shape=[full] * (jobs - 1) + [shape((n_dp, seq, width // n_dp), F32), shape((2,) + piece, F32), shape((width, 3 * dims), F32), shape((1, 3 * dims), F32),
                   shape((units, 4) + piece, F32), shape((units, 2) + piece, F32), shape((units,) + piece, F32)],
        in_specs=[ANY, ANY] + [VMEM] * 3 + [ANY] + [VMEM] * 2 + [ANY] * 2 + [VMEM] * 2 + [ANY] * (1 + jobs),
        out_specs=[ANY] * (jobs - 1) + [ANY, ANY, VMEM, VMEM, ANY, ANY, ANY],
        scratch_shapes=scratch + [dma(size) for size in sems],
        compiler_params=pltpu.CompilerParams(collective_id=1, has_side_effects=True, vmem_limit_bytes=67_000_000),
        cost_estimate=pl.CostEstimate(flops=20 * 10 ** 9, bytes_accessed=100 * 2 ** 20, transcendentals=0),
    )(d_ctx, resid, q, k, v, ctx, top, inv, cos, sin, wq, back, emb, *prods)
    return d_w, d_bias, cols, whole, grads


WAYS = 4


def table_kernel(ids, rows_ref, out, *tables):
    step = pl.program_id(0)
    count = rows_ref.shape[0]
    part = count // WAYS

    @pl.when(step == 0)
    def _():
        for table in tables:
            table[...] = jnp.zeros_like(table)

    @pl.loop(0, part, unroll=4)
    def _(r):
        for way, table in enumerate(tables):
            row = way * part + r
            where = pl.ds(ids[step * count + row], 1)
            table[where, :] = table[where, :] + rows_ref[pl.ds(row, 1), :]

    @pl.when(step == pl.num_programs(0) - 1)
    def _():
        total = tables[0][...]
        for table in tables[1:]:
            total = total + table[...]
        out[...] = SHRINK * total[:out.shape[0]]


def table_rows(ids, rows, vocab_loc):
    count, block = rows.shape
    step = min(1024, count // 2)
    return pl.pallas_call(
        table_kernel,
        name='table_rows',
        grid_spec=pltpu.PrefetchScalarGridSpec(
            num_scalar_prefetch=1,
            grid=(count // step,),
            in_specs=[pl.BlockSpec((step, block), lambda i, ids: (i, 0))],
            out_specs=pl.BlockSpec((vocab_loc, block), lambda i, ids: (0, 0)),
            scratch_shapes=[pltpu.VMEM((vocab_loc + 8, block), F32)] * WAYS,
        ),
        out_shape=jax.ShapeDtypeStruct((vocab_loc, block), F32),
        compiler_params=pltpu.CompilerParams(dimension_semantics=('arbitrary',), vmem_limit_bytes=48 * 2 ** 20),
        cost_estimate=pl.CostEstimate(flops=3 * 10 ** 9, bytes_accessed=16 * 2 ** 20, transcendentals=0),
    )(ids, rows)


def finish_kernel(n, cuts, col, down, proj, d_w, small, table, down_all, proj_all, qkv_all, total, landed, work, cross, last, mine, inbox, sem, send, recv, dsend, drecv, osem, csem, xsend, xrecv, ysend, yrecv, rsend, rrecv):
    z = lax.axis_index('tp')
    p, at = plane()
    entry_barrier(z, n, at)
    block = col.shape[N1]
    half = len(cuts) // N2

    def part(i):
        def region(rel, side):
            return table.at[pl.ds(cuts[i][N0], cuts[i][N1] - cuts[i][N0]), pl.ds(pl.multiple_of(at(rel) * block, block), block)]
        return Spread(at, region, send.at[i], recv.at[i], col.at[pl.ds(cuts[i][N0], cuts[i][N1] - cuts[i][N0])])
    parts = [part(i) for i in range(len(cuts))]
    spread = [Spread(at, functools.partial(block_of, ref, at), dsend.at[i], drecv.at[i], own) for i, (ref, own) in enumerate(((down_all, down), (proj_all, proj), (qkv_all, mine)))]
    own_copies = [pltpu.make_async_copy(col, table.at[:, pl.ds(pl.multiple_of(p * block, block), block)], osem.at[N0])]
    own_copies += [pltpu.make_async_copy(src, dst.at[p], osem.at[i]) for i, (src, dst) in enumerate(((down, down_all), (proj, proj_all), (mine, qkv_all)), N1)]
    order = list(range(len(cuts)))
    flipped = order[half:] + order[:half]
    peers = [{'dp': at(N1)}, {'dp': at(N2)}, {'dp': at(4)}, {'tp': z + N1 - N2 * (z % N2)}, {'tp': (z + n // N2) % n}]

    def next_part(i):
        parts[order[i]].give(N0)
        parts[flipped[i]].give(N1)
        parts[order[i]].give(N2)

    def relay_part(i):
        one, two = order[i], flipped[i]
        parts[one].take(N0)
        if one < half:
            parts[one].give(3)
        parts[one].give(5)
        parts[two].take(N1)
        if two >= half:
            parts[two].give(4)
        parts[two].give(6)

    def exchange(r):
        return rcopy(total, inbox.at[r], rsend.at[r], rrecv.at[r], **peers[r])

    def round_end(r):
        exchange(r).wait()
        total[...] = total[...] + inbox[r]

    total[...] = small[...]
    for i in range(4):
        rcopy(d_w.at[at(N2 * i + N1)], landed.at[i], csem.at[N0], csem.at[N1], dp=at(N1)).start()
    for copy in own_copies[:3]:
        copy.start()
    next_part(N0)
    exchange(N0).start()
    spread[N0].start()
    spread[N1].start()
    next_part(N1)
    rcopy(landed, landed, csem.at[N0], csem.at[N1], dp=p).wait()
    for i in range(4):
        work[i] = d_w[at(N2 * i)] + landed[i]
    round_end(N0)
    for side, first in ((N0, N2), (N1, 4)):
        rcopy(work.at[N1 + side, side], cross.at[side, N0], xsend.at[side], xrecv.at[side], dp=at(first)).start()
        rcopy(work.at[3, side], cross.at[side, N1], xsend.at[side], xrecv.at[side], dp=at(first)).start()
    exchange(N1).start()
    next_part(N2)
    relay_part(N0)
    round_end(N1)
    for side, first in ((N0, N2), (N1, 4)):
        rcopy(cross.at[side], cross.at[side], xsend.at[side], xrecv.at[side], dp=p).wait()
        cross[side, N0] = cross[side, N0] + work[N0, side]
        cross[side, N1] = cross[side, N1] + work[N2 - side, side]
    exchange(N2).start()
    for side, second in ((N0, 4), (N1, N2)):
        rcopy(cross.at[side, N1], last.at[side], ysend.at[side], yrecv.at[side], dp=at(second)).start()
    next_part(3)
    spread[N0].cross()
    spread[N1].cross()
    relay_part(N1)
    round_end(N2)
    for side in range(N2):
        rcopy(last.at[side], last.at[side], ysend.at[side], yrecv.at[side], dp=p).wait()
        mine[side] = cross[side, N0] + last[side]
    exchange(3).start()
    next_part(4)
    spread[N2].start()
    own_copies[3].start()
    spread[N0].diagonal()
    spread[N1].diagonal()
    relay_part(N2)
    round_end(3)
    next_part(5)
    exchange(4).start()
    relay_part(3)
    spread[N2].cross()
    next_part(6)
    round_end(4)
    relay_part(4)
    next_part(7)
    spread[N2].diagonal()
    for i in range(5, len(cuts)):
        relay_part(i)
    for i in range(half):
        for via, where in ((3, i), (4, i + half)):
            parts[where].take(via)
            parts[where].give(7)
    for i in order:
        for j in (N2, 5, 6, 7):
            parts[i].take(j)
        for j in (N0, N1, N2, 3 if i < half else 4, 5, 6, 7):
            parts[i].copy(j, *EDGES[j]).wait_send()
    for gather in spread:
        gather.finish()
    for copy in own_copies:
        copy.wait()


def finish(col, down, proj, d_w, small, n_tp, n_dp):
    size, block = col.shape
    tiles = size // 8
    cuts = [(8 * (tiles * i // 8), 8 * (tiles * (i + N1) // 8)) for i in range(8)]
    dma = pltpu.SemaphoreType.DMA
    shape = jax.ShapeDtypeStruct
    third = d_w.shape[N1:]
    kinds = len(EDGES)
    table, down_all, proj_all, qkv_all, total = pl.pallas_call(
        functools.partial(finish_kernel, n_tp, cuts),
        name='finish',
        out_shape=[shape((size, n_dp * block), F32)] + [shape((n_dp,) + src, F32) for src in (down.shape, proj.shape, third)] + [shape(small.shape, F32)],
        in_specs=[ANY] * 3 + [VMEM] * N2,
        out_specs=[ANY] * 4 + [VMEM],
        scratch_shapes=[pltpu.VMEM(lead + third[N1:], F32) for lead in ((4, N2), (4, N2), (N2, N2), (N2,), (N2,))] + [pltpu.VMEM((5,) + small.shape, F32), dma,
                        dma((8, kinds)), dma((8, kinds)), dma((3, kinds)), dma((3, kinds)), dma((4,))] + [dma((N2,))] * 5 + [dma((5,))] * N2,
        compiler_params=pltpu.CompilerParams(collective_id=N2, has_side_effects=True, vmem_limit_bytes=32 * N2 ** 20),
        cost_estimate=pl.CostEstimate(flops=10 * 10 ** 9, bytes_accessed=60 * N2 ** 20, transcendentals=N0),
    )(col, down, proj, d_w, small)
    return table, down_all.reshape(-N1, down.shape[N2]), proj_all.reshape(-N1, proj.shape[N2]), qkv_all.reshape(-N1, third[N2]), total


def dot(a, b, dims):
    return lax.dot_general(a, b, (dims, ((), ())), preferred_element_type=F32)


NT, TN, NN = ((1,), (1,)), ((0,), (0,)), ((1,), (0,))


def lane_head(shape, heads, halves):
    lane = lax.broadcasted_iota(jnp.int32, shape, 1)
    dims = shape[1] // halves
    return (lane % dims) // (dims // heads)


def turned(both, cos, sin):
    half = both.shape[1] // 2
    x1, x2 = both[:, :half], both[:, half:]
    return jnp.concatenate([x1 * cos - x2 * sin, x2 * cos + x1 * sin], axis=1)


def project(i, qb, emb, wq, bq, cos, sin, q, k, v):
    at_q = pl.ds(pl.multiple_of(i * qb, qb), qb)
    dims = q.shape[1]
    qkv = (dot(emb[at_q, :], wq[...], NN) + bq[...]).astype(BF)
    for ref, part in ((q, 0), (k, 1)):
        ref[at_q, :] = turned(qkv[:, part * dims:(part + 1) * dims].astype(F32), cos[at_q, :], sin[at_q, :]).astype(BF)
    v[at_q, :] = qkv[:, 2 * dims:]


def scores(i, j, kb, qb, scale, keys, q):
    s = dot(keys, q, NT) * scale
    key = j * kb + lax.broadcasted_iota(jnp.int32, (kb, qb), 0)
    query = i * qb + lax.broadcasted_iota(jnp.int32, (kb, qb), 1)
    return jnp.where(query >= key, s, -1e30)


def attend(i, h, heads, qb, q_ref, k_ref, v_ref, ctx_ref, top_ref, inv_ref, s_ref):
    kb = 2 * qb
    dims = q_ref.shape[1]
    scale = (dims // heads) ** -0.5
    at_q = pl.ds(pl.multiple_of(i * qb, qb), qb)
    q = jnp.where(lane_head((qb, dims), heads, 2) == h, q_ref[at_q, :].astype(F32), 0.0).astype(BF)
    count = (i + 2) // 2

    def at_key(j):
        return pl.ds(pl.multiple_of(j * kb, kb), kb)

    def first(j, top):
        s = scores(i, j, kb, qb, scale, k_ref[at_key(j), :], q)
        s_ref[at_key(j), :] = s
        return jnp.maximum(top, jnp.max(s, axis=0, keepdims=True))
    top = lax.fori_loop(0, count, first, jnp.full((1, qb), -1e30, F32))

    def weigh(j, total):
        e = jnp.exp(s_ref[at_key(j), :] - top)
        s_ref[at_key(j), :] = e
        return total + jnp.sum(e, axis=0, keepdims=True)
    inv = 1.0 / lax.fori_loop(0, count, weigh, jnp.zeros((1, qb), F32))

    def mix(j, acc):
        return acc + dot((s_ref[at_key(j), :] * inv).astype(BF), v_ref[at_key(j), :], TN)
    mixed = lax.fori_loop(0, count, mix, jnp.zeros((qb, dims), F32))
    ctx_ref[at_q, :] = jnp.where(lane_head((qb, dims), heads, 1) == h, mixed, ctx_ref[at_q, :])
    top_ref[pl.ds(h, 1), at_q] = top
    inv_ref[pl.ds(h, 1), at_q] = inv


def attend_grad(i, h, heads, qb, q_ref, k_ref, v_ref, ctx_ref, dctx_ref, top_ref, inv_ref, dq_ref, dk_ref, dv_ref):
    kb = 2 * qb
    dims = q_ref.shape[1]
    scale = (dims // heads) ** -0.5
    at_q = pl.ds(pl.multiple_of(i * qb, qb), qb)
    q = jnp.where(lane_head((qb, dims), heads, 2) == h, q_ref[at_q, :].astype(F32), 0.0).astype(BF)
    dc = jnp.where(lane_head((qb, dims), heads, 1) == h, dctx_ref[at_q, :], 0.0).astype(BF)
    ones = jnp.ones((8, dims), F32)
    mean = lax.dot_general(ones, dc.astype(F32) * ctx_ref[...], (NT, ((), ())), precision=lax.Precision.HIGHEST, preferred_element_type=F32)[:1]
    top, inv = top_ref[pl.ds(h, 1), at_q], inv_ref[pl.ds(h, 1), at_q]

    def step(j, dq):
        at_k = pl.ds(pl.multiple_of(j * kb, kb), kb)
        keys = k_ref[at_k, :]
        probs = (jnp.exp(scores(i, j, kb, qb, scale, keys, q) - top) * inv).astype(BF)
        ds = (probs.astype(F32) * (dot(v_ref[at_k, :], dc, NT) - mean) * scale).astype(BF)
        dv_ref[at_k, :] += dot(probs, dc, NN)
        dk_ref[at_k, :] += dot(ds, q, NN)
        return dq + dot(ds, keys, TN)
    dq = lax.fori_loop(0, (i + 2) // 2, step, jnp.zeros((qb, dims), F32))
    dq_ref[...] = jnp.where(lane_head((qb, dims), heads, 2) == h, dq, dq_ref[...])


def grad_rows(i, qb, cos, sin, dq, dk, dv, d_bias):
    at_q = pl.ds(pl.multiple_of(i * qb, qb), qb)
    back = [turned(values, cos, -sin) for values in (dq[...], dk[at_q, :])]
    rows = jnp.concatenate(back + [dv[at_q, :]], axis=1)
    d_bias[...] += jnp.sum(rows, axis=0, keepdims=True)
    return rows.astype(BF)


def solution(mesh):
    n_tp, n_dp = mesh.shape['tp'], mesh.shape['dp']
    in_specs = (P('dp', None), P('dp', None, None), P('tp', None)) + WEIGHT_SPECS
    out_specs = (P('tp', None),) + WEIGHT_SPECS

    def device_step(tokens, cotangent, emb_table, *weights):
        (w_qkv, b_qkv, w_out, b_out, ln1_gain, ln1_bias, w_gate, b_gate, w_lin, b_lin, w_down, b_down, ln2_gain) = weights
        tp, dp = lax.axis_index('tp'), lax.axis_index('dp')
        tokens = tokens[N0]
        seq_len, width = tokens.shape[N0], emb_table.shape[N1]
        heads, head_dim = b_qkv.shape[N0], b_qkv.shape[N1] // 3
        own = seq_len // n_tp
        ffn = w_gate.shape[N1]
        rk, rf, ro = width // n_dp, ffn // n_dp, w_out.shape[N0] // n_dp

        def cut(weight):
            rows = weight.shape[N0] // n_dp
            return lax.dynamic_slice_in_dim(weight, dp * rows, rows, N0)
        bias_rows = jnp.concatenate([b_gate[None], b_lin[None], jnp.zeros((14, ffn), BF)], axis=N0)
        piece = jnp.concatenate([cut(w_gate), cut(w_lin), cut(w_down), cut(w_out), bias_rows], axis=N0).astype(F32)

        vocab_loc = emb_table.shape[N0]
        local_ids = tokens - tp * vocab_loc
        in_shard = (local_ids >= N0) & (local_ids < vocab_loc)
        safe_ids = jnp.where(in_shard, local_ids, N0)
        found = jnp.take(emb_table, safe_ids, axis=N0)
        dims = heads * head_dim
        place = column_order(heads, head_dim)
        swap = (jnp.arange(3 * dims)[:, None] == jnp.asarray(place)[None, :]).astype(BF)
        wq = jnp.dot(w_qkv, swap, preferred_element_type=F32).astype(BF)
        bq = jnp.dot(b_qkv.reshape(N1, -N1), swap, preferred_element_type=F32)
        cos_tab, sin_tab = rope_tables(seq_len, head_dim, heads)
        emb_bf, (wg_full, wl_full, wd_full, wo_full), biases, tok_all, ctx_own, saved = embed(found, in_shard[:, None].astype(F32), piece, tokens.reshape(-N1, min(128, seq_len // 8)), (w_gate, w_lin, w_down, w_out), wq, bq, cos_tab, sin_tab, heads, n_tp, n_dp)
        ctx_own = ctx_own.reshape(n_tp, own, dims).astype(BF)
        is_own = (jnp.arange(n_tp) == tp)[:, None]
        bg_full, bl_full = [jnp.where(is_own, b[None].astype(F32), biases[:, i]) for i, b in enumerate((b_gate, b_lin))]

        blocks = 8

        def owned(values):
            return lax.dynamic_index_in_dim(values.reshape(blocks, n_tp, -N1, width), tp, N1, keepdims=False).reshape(own, width).astype(F32)
        emb_own, cot_own = owned(emb_bf), owned(cotangent[N0])
        attn_out = jnp.einsum('hse,hed->sd', ctx_own, wo_full, preferred_element_type=F32) + b_out.astype(F32)
        normed_one, norm_one_pull = jax.vjp(norm_scaled, ALPHA * emb_own + attn_out, ln1_gain.astype(F32))
        hidden = (normed_one + ln1_bias.astype(F32)).astype(BF)
        gate_pre = jnp.einsum('sk,tkc->tsc', hidden, wg_full, preferred_element_type=F32) + bg_full[:, None]
        lin_pre = jnp.einsum('sk,tkc->tsc', hidden, wl_full, preferred_element_type=F32) + bl_full[:, None]
        inner_val, act_pull = jax.vjp(geglu, gate_pre, lin_pre)
        inner_act = inner_val.astype(BF)
        ffn_out = jnp.einsum('tsc,tcd->sd', inner_act, wd_full, preferred_element_type=F32) + b_down.astype(F32)
        norm_two_pull = jax.vjp(norm_scaled, ALPHA * hidden.astype(F32) + ffn_out, ln2_gain.astype(F32))[N1]

        def product(lhs, rhs, spec):
            return jnp.einsum(spec, lhs, rhs, preferred_element_type=F32).reshape(n_tp, n_dp, -N1, width)

        d_resid_two, d_ln2_gain = norm_two_pull(cot_own)
        d_b_down = jnp.sum(d_resid_two, axis=N0)
        d_ffn_bf = d_resid_two.astype(BF)
        prod_down = product(inner_act, d_ffn_bf, 'tsc,sd->tcd')
        d_inner = jnp.einsum('sd,tcd->tsc', d_ffn_bf, wd_full, preferred_element_type=F32).astype(BF)
        d_gate_pre, d_lin_pre = act_pull(d_inner.astype(F32))
        d_b_gate = jnp.sum(d_gate_pre, axis=N1)
        d_b_lin = jnp.sum(d_lin_pre, axis=N1)
        d_gate_bf = d_gate_pre.astype(BF)
        d_lin_bf = d_lin_pre.astype(BF)
        prod_gate = product(hidden, d_gate_bf, 'sk,tsc->tkc')
        prod_lin = product(hidden, d_lin_bf, 'sk,tsc->tkc')
        d_hidden = ALPHA * d_resid_two + jnp.einsum('tsc,tkc->sk', d_gate_bf, wg_full, preferred_element_type=F32) + jnp.einsum('tsc,tkc->sk', d_lin_bf, wl_full, preferred_element_type=F32)
        d_ln1_bias = jnp.sum(d_hidden, axis=N0)
        d_resid_one, d_ln1_gain = norm_one_pull(d_hidden)
        d_b_out = jnp.sum(d_resid_one, axis=N0)
        d_attn_bf = d_resid_one.astype(BF)
        d_w_out = jnp.einsum('hse,sd->hed', ctx_own, d_attn_bf, preferred_element_type=F32)
        d_w_out = lax.psum_scatter(d_w_out.reshape(-N1, width), ALL, scatter_dimension=N0, tiled=True)
        d_ctx = jnp.einsum('sd,hed->hse', d_attn_bf, wo_full, preferred_element_type=F32)
        d_w_qkv, d_b_qkv, d_cols, (d_w_gate, d_w_lin), d_w_down = backward(
            d_ctx.reshape(n_tp, blocks, own // blocks, dims), (ALPHA * d_resid_one).reshape(blocks, own // blocks, width), saved, cos_tab, sin_tab, wq, swap.T, emb_bf,
            (prod_gate, prod_lin, prod_down), heads, n_tp, n_dp)
        d_w_gate, d_w_lin = d_w_gate.reshape(-N1, ffn), d_w_lin.reshape(-N1, ffn)
        d_b_qkv = jnp.dot(d_b_qkv, swap.astype(F32).T, precision=lax.Precision.HIGHEST)
        all_ids = tok_all.reshape(-N1) - tp * vocab_loc
        all_ids = jnp.where((all_ids >= N0) & (all_ids < vocab_loc), all_ids, vocab_loc)
        col = table_rows(all_ids, d_cols.reshape(n_dp * seq_len, -N1), vocab_loc)

        slot = (jnp.arange(n_tp) == tp).astype(F32)[:, None]
        d_bq_rows = jnp.pad(slot * d_b_qkv, ((N0, N0), (N0, ffn - 3 * dims)))
        small = jnp.concatenate([d_b_gate, d_b_lin, d_bq_rows, jnp.stack([d_b_out, d_ln1_gain, d_ln1_bias, d_b_down, d_ln2_gain]), jnp.zeros((7, width), F32)], axis=N0)
        d_table, d_w_down, d_w_out, d_w_qkv, small = finish(
            col, d_w_down, d_w_out.reshape(N2, -N1, width), d_w_qkv.reshape(n_dp, N2, -N1, 3 * dims), small, n_tp, n_dp)
        d_b_gate = lax.dynamic_index_in_dim(small[:n_tp], tp, N0, keepdims=False)
        d_b_lin = lax.dynamic_index_in_dim(small[n_tp:N2 * n_tp], tp, N0, keepdims=False)
        d_b_qkv = lax.dynamic_index_in_dim(small[N2 * n_tp:3 * n_tp], tp, N0, keepdims=False)[:3 * dims].reshape(heads, 3 * head_dim)
        d_b_out, d_ln1_gain, d_ln1_bias, d_b_down, d_ln2_gain = [small[3 * n_tp + i] for i in range(5)]
        return (d_table, d_w_qkv, d_b_qkv, d_w_out, d_b_out, d_ln1_gain, d_ln1_bias, d_w_gate, d_b_gate, d_w_lin, d_b_lin, d_w_down, d_b_down, d_ln2_gain)

    return jax.shard_map(device_step, mesh=mesh, in_specs=in_specs, out_specs=out_specs, check_vma=False)
```

```python
import functools

import jax
import jax.numpy as jnp
import numpy as np
from jax import lax
from jax.experimental import pallas as pl
from jax.experimental.pallas import tpu as pltpu
from jax.sharding import PartitionSpec as P

ALPHA = 140.0 ** 0.5
EPS = 1e-5
SHRINK = 0.1
ROPE_BASE = 10000.0
WEIGHT_SPECS = (P(None, 'tp'), P('tp', None), P('tp', None), P(), P(), P(), P(None, 'tp'), P('tp'), P(None, 'tp'), P('tp'), P('tp', None), P(), P())
ALL = ('tp', 'dp')
BF = jnp.bfloat16
N0, N1, N2 = range(3)
F32 = jnp.float32
MESH = pl.DeviceIdType.MESH
ANY = pl.BlockSpec(memory_space=pl.ANY)
VMEM = pl.BlockSpec(memory_space=pltpu.VMEM)


def rope_tables(seq_len, head_dim, heads):
    half_dim = head_dim // 2
    inv_freq = (ROPE_BASE ** (-2.0 * np.arange(half_dim) / head_dim)).astype(np.float32)
    angles = np.arange(seq_len, dtype=np.float32)[:, None] * inv_freq[None, :]
    return [jnp.asarray(np.tile(table(angles), (1, heads))) for table in (np.cos, np.sin)]


def column_order(heads, head_dim):
    cols = np.arange(3 * heads * head_dim).reshape(heads, 3, 2, head_dim // 2)
    return np.concatenate([cols[:, part].transpose(1, 0, 2).ravel() for part in (0, 1)] + [cols[:, 2].ravel()])


def rcopy(src, dst, send, recv, **where):
    return pltpu.make_async_remote_copy(src_ref=src, dst_ref=dst, send_sem=send, recv_sem=recv, device_id=dict(where), device_id_type=MESH)


def plane():
    p = lax.axis_index('dp')
    y, x, c = p // 4, (p // 2) % 2, p % 2

    def at(rel):
        yy = 1 - y if rel & 4 else y
        xx = 1 - x if rel & 2 else x
        cc = 1 - c if rel & 1 else c
        return yy * 4 + xx * 2 + cc
    return p, at


def entry_barrier(z, n, at):
    bar = pltpu.get_barrier_semaphore()
    for rel in range(1, 8):
        pl.semaphore_signal(bar, inc=1, device_id={'dp': at(rel)}, device_id_type=MESH)
    for d in range(1, n):
        pl.semaphore_signal(bar, inc=1, device_id={'tp': (z + d) % n}, device_id_type=MESH)
    pl.semaphore_wait(bar, 7 + n - 1)


LAG = 3


def chain_sum(k, z, n, rows, chunks, part, left, right, done, send_r, send_l, recv_l, recv_r, place=lambda c: c):
    last = n - 1

    def at_rows(c):
        return pl.ds(pl.multiple_of(place(c) * rows, rows), rows)

    def cut(ref, c):
        return ref.at[at_rows(c)]

    def load(ref, c):
        return ref[at_rows(c)]

    def store(ref, c, value):
        ref[at_rows(c)] = value
    cl, cr = k - LAG * z, k - LAG * (last - z)
    okl, okr = (cl >= 0) & (cl < chunks), (cr >= 0) & (cr < chunks)

    @pl.when(okl & (z > 0))
    def _():
        rcopy(cut(left, cl), cut(left, cl), send_r, recv_l.at[cl], tp=z).wait_recv()

    @pl.when(okl & (z == last))
    def _():
        done(cl, load(left, cl) + load(part, cl))

    @pl.when(okl & (z > 0) & (z < last))
    def _():
        run = load(left, cl)

        @pl.when(z >= n // 2)
        def _():
            done(cl, run + load(right, cl))
        store(left, cl, run + load(part, cl))

    @pl.when(okr & (z < last))
    def _():
        rcopy(cut(right, cr), cut(right, cr), send_l, recv_r.at[cr], tp=z).wait_recv()

    @pl.when(okr & (z == 0))
    def _():
        done(cr, load(part, cr) + load(right, cr))

    @pl.when(okr & (z > 0) & (z < last))
    def _():
        run = load(right, cr)

        @pl.when(z < n // 2)
        def _():
            done(cr, load(left, cr) + run)
        store(right, cr, run + load(part, cr))

    @pl.when(okl & (z == 0))
    def _():
        rcopy(cut(part, cl), cut(left, cl), send_r, recv_l.at[cl], tp=z + 1).start()

    @pl.when(okl & (z > 0) & (z < last))
    def _():
        rcopy(cut(left, cl), cut(left, cl), send_r, recv_l.at[cl], tp=z + 1).start()

    @pl.when(okr & (z == last))
    def _():
        rcopy(cut(part, cr), cut(right, cr), send_l, recv_r.at[cr], tp=z - 1).start()

    @pl.when(okr & (z > 0) & (z < last))
    def _():
        rcopy(cut(right, cr), cut(right, cr), send_l, recv_r.at[cr], tp=z - 1).start()


def chain_drain(z, n, part, left, right, send_r, send_l, recv_l, recv_r):
    @pl.when(z < n - 1)
    def _():
        rcopy(part, left, send_r, recv_l.at[0], tp=z + 1).wait_send()

    @pl.when(z > 0)
    def _():
        rcopy(part, right, send_l, recv_r.at[0], tp=z - 1).wait_send()


EDGES = ((0, 0, 2), (0, 0, 4), (0, 0, 1), (2, 1, 4), (4, 2, 2), (2, 0, 1), (4, 0, 1), (6, 1, 1), (6, 2, 1))
CROSS, DIAGONAL, LAST = ((0, 3, 5), (1, 4, 6)), ((3, 7), (4, 8)), {1: (2,), 3: (5,), 5: (6,), 7: (7, 8)}
STEPS = (4, 10, 17, 21, 25, 29)
FIRST = 18
ORDER = (0, 2, 4, 1, 3, 5, 6, 7)


def emb_kernel(n, rows, chunks, cuts, heads, found, mask, wq, bq, cos, sin, piece, toks, *refs):
    m = len(cuts)
    local, outs = refs[:m], refs[m + N1:N2 * m + N1]
    out, (bias, tok_all, wall, ctx_own, q, k_all, v, ctx, top, inv, part, left, right, raw, low, weights, send_r, send_l, recv_l, recv_r, tsend, trecv, tself, zsend, zrecv, psend, precv, lsem, isem, osem, bsem, asend, arecv, aself) = refs[m], refs[N2 * m + N1:]
    blocks = 8
    qb = part.shape[N0] // blocks
    per = chunks // blocks
    z = lax.axis_index('tp')
    p, at = plane()
    entry_barrier(z, n, at)
    half = piece.shape[N0] // N2

    @pl.when(z < n - N1)
    def _():
        rcopy(piece, wall.at[z, p], zsend.at[z], zrecv.at[z], tp=z + N1).start()

    @pl.when(z > N0)
    def _():
        rcopy(piece, wall.at[z, p], bsem.at[N1], zrecv.at[z], tp=z - N1).start()
    mine = [pltpu.make_async_copy(toks, tok_all.at[p], tself)]
    mine += [pltpu.make_async_copy(src, dst.at[z], lsem.at[i]) for i, (src, dst) in enumerate(zip(local, outs))]
    for copy in mine:
        copy.start()
    for rel in range(N1, 8):
        rcopy(toks, tok_all.at[p], tsend.at[rel], trecv.at[rel], dp=at(rel)).start()

    def others(d, body):
        @pl.when(z >= d)
        def _():
            body(z - d, -N1)

        @pl.when(z + d < n)
        def _():
            body(z + d, N1)

    def region(t, rel, side):
        blk = wall.at[t, at(rel)]
        return blk if side == N0 else wall.at[t, at(rel), pl.ds((side - N1) * half, half)]

    def give(t, j):
        rel, side, to = EDGES[j]
        rcopy(region(t, rel, side), region(t, rel, side), psend.at[t, j], precv.at[t, j], dp=at(to)).start()

    def take(t, j):
        rel, side, to = EDGES[j]
        blk = region(t, rel ^ to, side)
        rcopy(blk, blk, psend.at[t, j], precv.at[t, j], dp=p).wait_recv()

    def gave(t, j):
        rel, side, to = EDGES[j]
        rcopy(region(t, rel, side), region(t, rel, side), psend.at[t, j], precv.at[t, j], dp=p).wait_send()

    def arrive(d):
        def body(t, sign):
            blk = wall.at[t, p]
            rcopy(blk, blk, zsend.at[t], zrecv.at[t], tp=z).wait_recv()

            @pl.when((z - sign >= N0) & (z - sign < n))
            def _():
                rcopy(blk, blk, zsend.at[t], zrecv.at[t], tp=z - sign).start()
            for j in range(3):
                give(t, j)
        others(d, body)

    def relay(d, moves):
        def body(t, sign):
            for first, *rest in moves:
                take(t, first)
                for j in rest:
                    give(t, j)
        others(d, body)

    k_all[:] = jnp.zeros_like(k_all)
    v[:] = jnp.zeros_like(v)
    arrive(N1)

    @pl.loop(N0, blocks)
    def _(i):
        at_i = pl.ds(pl.multiple_of(i * qb, qb), qb)
        part[at_i, :] = jnp.where(mask[at_i, :] > N0, found[at_i, :].astype(F32), 0.0)

    def done(c, value):
        out[pl.ds(pl.multiple_of(c * rows, rows), rows)] = value.astype(out.dtype)

    def other(i):
        return i + (i + n - z) // n

    def loaded(i, rel, slot):
        return pltpu.make_async_copy(wall.at[other(i), at(rel), pl.ds(N0, cuts[-N1][N1])], raw.at[slot], isem.at[slot])

    def stored(i, rel, slot):
        return [pltpu.make_async_copy(low.at[slot, pl.ds(lo, hi - lo)], dst.at[other(i), at(rel)], osem.at[slot, k]) for k, ((lo, hi), dst) in enumerate(zip(cuts, outs))]
    plan = [(i, rel) for rel in ORDER for i in range(n - N1)]

    def prefetch(s):
        i, rel = plan[s]
        for j in LAST.get(rel, ()):
            take(other(i), j)
        loaded(i, rel, s % N2).start()

    def convert(s):
        i, rel = plan[s]
        loaded(i, rel, s % N2).wait()
        if s >= N2:
            for copy in stored(*plan[s - N2], s % N2):
                copy.wait()
        low[s % N2] = raw[s % N2].astype(low.dtype)
        if s + N1 < len(plan):
            prefetch(s + N1)
        for copy in stored(i, rel, s % N2):
            copy.start()
    events = [(STEPS[d - N1], functools.partial(relay, d, CROSS)) for d in range(N1, n)] + [(STEPS[d + n - N2], functools.partial(relay, d, DIAGONAL)) for d in range(N1, n)]
    events += [(N2 * d - N2, functools.partial(arrive, d)) for d in range(N2, n)]
    events += [(FIRST - N1, functools.partial(prefetch, N0))] + [(FIRST + s, functools.partial(convert, s)) for s in range(len(plan))]

    start = per + LAG * (n - N1)

    share = qb // n

    def context(i, d):
        to = (z + d) % n
        src = ctx.at[pl.ds(pl.multiple_of(i * qb + to * share, share), share)]
        if d == N0:
            return pltpu.make_async_copy(src, ctx_own.at[z, i], aself)
        return rcopy(src, ctx_own.at[z, i], asend, arecv.at[z], tp=to)

    @pl.loop(N0, max(start + blocks * heads + N1, FIRST + len(plan)))
    def _(k):
        step = k - start
        i = step // heads - N1

        @pl.when((step > N0) & (step % heads == N0) & (step <= blocks * heads))
        def _():
            for d in range(n):
                context(i, d).start()
        chain_sum(k, z, n, rows, chunks, part, left, right, done, send_r, send_l, recv_l, recv_r)
        for at_step, event in events:
            pl.when(k == at_step)(event)

        @pl.when((step >= N0) & (step < blocks * heads))
        def _():
            @pl.when(step % heads == N0)
            def _():
                project(step // heads, qb, out, wq, bq, cos, sin, q, k_all, v)
            attend(step // heads, step % heads, heads, qb, q, k_all, v, ctx, top, inv, weights)

    pltpu.make_async_copy(ctx_own.at[z], ctx_own.at[z], aself).wait()
    for d in range(N1, n):
        src = (z + d) % n
        rcopy(ctx_own.at[src], ctx_own.at[src], asend, arecv.at[src], tp=z).wait()
    chain_drain(z, n, part, left, right, send_r, send_l, recv_l, recv_r)
    for s in (len(plan) - N2, len(plan) - N1):
        for copy in stored(*plan[s], s % N2):
            copy.wait()

    def finish(t, sign):
        for j in range(len(EDGES)):
            gave(t, j)
        tail = pltpu.make_async_copy(wall.at[t, p, pl.ds(cuts[-N1][N1], bias.shape[N1])], bias.at[t], bsem.at[N0])
        tail.start()
        tail.wait()

        @pl.when((z - sign >= N0) & (z - sign < n))
        def _():
            rcopy(wall.at[t, p], wall.at[t, p], zsend.at[t], zrecv.at[t], tp=z).wait_send()
    for d in range(N1, n):
        others(d, finish)
    for copy in mine:
        copy.wait()
    for rel in range(N1, 8):
        rcopy(toks, tok_all.at[at(rel)], tsend.at[rel], trecv.at[rel], dp=at(rel)).wait()

    @pl.when(z < n - N1)
    def _():
        rcopy(piece, wall.at[z, p], zsend.at[z], zrecv.at[z], tp=z + N1).wait_send()

    @pl.when(z > N0)
    def _():
        rcopy(piece, wall.at[z, p], bsem.at[N1], zrecv.at[z], tp=z - N1).wait_send()


def embed(found, mask, piece, toks, local, wq, bq, cos, sin, heads, n_tp, n_dp):
    seq, width = found.shape
    chunks = 32
    rows = seq // chunks
    dims = wq.shape[1] // 3
    cuts, lo = [], 0
    for weight in local:
        cuts.append((lo, lo + weight.shape[0] // n_dp))
        lo = cuts[-1][1]
    dma = pltpu.SemaphoreType.DMA
    shape = jax.ShapeDtypeStruct
    shapes = [shape((seq, width), BF)]
    shapes += [shape((n_tp, n_dp, w.shape[0] // n_dp, w.shape[1]), BF) for w in local]
    shapes += [shape((n_tp, piece.shape[0] - lo, width), F32), shape((n_dp,) + toks.shape, toks.dtype), shape((n_tp, n_dp) + piece.shape, F32), shape((n_tp, 8, seq // n_tp // 8, dims), F32)]
    shapes += [shape((seq, dims), BF)] * 3 + [shape((seq, dims), F32)] + [shape((heads, seq), F32)] * 2
    out = pl.pallas_call(
        functools.partial(emb_kernel, n_tp, rows, chunks, cuts, heads),
        name='embed',
        out_shape=shapes,
        in_specs=[VMEM] * 6 + [ANY] * (2 + len(local)),
        out_specs=[VMEM] + [ANY] * (4 + len(local)) + [VMEM] * 6,
        scratch_shapes=[pltpu.VMEM((seq, width), F32)] * 3 + [pltpu.VMEM((2, lo, width), F32), pltpu.VMEM((2, lo, width), BF), pltpu.VMEM((seq, seq // 8), F32), dma, dma, dma((chunks,)), dma((chunks,)),
                        dma((8,)), dma((8,)), dma, dma((n_tp,)), dma((n_tp,)), dma((n_tp, len(EDGES))), dma((n_tp, len(EDGES))), dma((len(local),)), dma((2,)), dma((2, len(local))), dma((2,)),
                        dma, dma((n_tp,)), dma],
        compiler_params=pltpu.CompilerParams(collective_id=0, has_side_effects=True, vmem_limit_bytes=60 * 2 ** 20),
        cost_estimate=pl.CostEstimate(flops=20 * 10 ** 9, bytes_accessed=80 * 2 ** 20, transcendentals=0),
    )(found, mask, wq, bq, cos, sin, piece, toks, *[w.reshape(n_dp, w.shape[0] // n_dp, w.shape[1]) for w in local])
    m = 1 + len(local)
    return out[0], [w.reshape(n_tp, -1, w.shape[3]) for w in out[1:m]], out[m], out[m + 1], out[m + 3], out[m + 4:]


RING = 4
HOLD, LIVE, PAIR = 4, 8, 4
ADD, LOAD, CROSSED, LAND, PLANE = 1, 4, 5, 7, 8
GATHER = (37, 41)


def block_of(ref, at, rel, side):
    return ref.at[at(rel)] if side == 0 else ref.at[at(rel), side - 1]


class Spread:
    def __init__(self, at, block, send, recv, own=None):
        self.at, self.block, self.send, self.recv, self.own = at, block, send, recv, own

    def copy(self, j, rel, side, to):
        dst = self.block(rel, side)
        src = self.own if rel == 0 and self.own is not None else dst
        return rcopy(src, dst, self.send.at[j], self.recv.at[j], dp=self.at(to))

    def give(self, j):
        self.copy(j, *EDGES[j]).start()

    def take(self, j):
        rel, side, to = EDGES[j]
        self.copy(j, rel ^ to, side, 0).wait_recv()

    def start(self):
        for j in range(3):
            self.give(j)

    def relay(self, moves):
        for first, *rest in moves:
            self.take(first)
            for j in rest:
                self.give(j)

    def cross(self):
        self.relay(CROSS)

    def diagonal(self):
        self.relay(DIAGONAL)

    def finish(self):
        for j in (2, 5, 6, 7, 8):
            self.take(j)
        for j, (rel, side, _) in enumerate(EDGES):
            self.copy(j, rel, side, 0).wait_send()


def backward_kernel(n, rows, chunks, jobs, heads, d_ctx, resid, q, k_all, v, ctx, top, inv, cos, sin, wq, back, emb, *refs):
    prods = refs[:jobs]
    whole = refs[jobs:N2 * jobs - N1]
    out, grads, d_w, d_bias, landed, cross, last, part, left, right, total, dctx, dq, dk, dv, ctx_in, res_in, cos_in, sin_in, emb_in, work, fresh, xin, yin, keep, pass_on, along, final, *sems = refs[N2 * jobs - N1:]
    send_r, send_l, recv_l, recv_r, osend, orecv, csend, crecv, esem, fsem, xsend, xrecv, xsem, ysend, yrecv, ysem, ksem, zrecv, frecv, asend, arecv, aself, isem, gsend, grecv = sems
    z = lax.axis_index('tp')
    p, at = plane()
    entry_barrier(z, n, at)
    blocks = 8
    per = chunks // blocks
    qb = rows * per
    share = qb // n
    block = out.shape[N2]
    lead = jnp.maximum(z, n - N1 - z)
    span = N2 * n
    units = jobs * span
    size = work.shape[N2]

    def rows_of(i, to, count):
        return pl.ds(pl.multiple_of(i * qb + to * count, count), count)

    def exchange(i, d):
        to = (z + d) % n
        dst = dctx.at[rows_of(i, z, share)]
        if d == N0:
            return pltpu.make_async_copy(d_ctx.at[z, i], dst, aself.at[i])
        return rcopy(d_ctx.at[to, i], dst, asend, arecv.at[i], tp=to)

    @pl.loop(N0, blocks)
    def _(b):
        for d in range(n):
            exchange(blocks - N1 - b, d).start()

    def piece(m, u, rel):
        return prods[m].at[(u % span) // N2, at(rel), pl.ds(pl.multiple_of((u % N2) * size, size), size)]

    for m in range(jobs):
        @pl.loop(m * span, (m + N1) * span)
        def _(u, m=m):
            for i in range(4):
                rcopy(piece(m, u, N2 * i + N1), landed.at[u, i], csend, crecv.at[u], dp=at(N1)).start()

    def inputs(i):
        slot = i % N2
        at_q = rows_of(i, N0, qb)
        pairs = ((ctx.at[at_q], ctx_in), (resid.at[i], res_in), (cos.at[at_q], cos_in), (sin.at[at_q], sin_in), (emb.at[at_q], emb_in))
        return [pltpu.make_async_copy(src, dst.at[slot], isem.at[j, slot]) for j, (src, dst) in enumerate(pairs)]

    dk[:] = jnp.zeros_like(dk)
    dv[:] = jnp.zeros_like(dv)
    d_w[:] = jnp.zeros_like(d_w)
    d_bias[:] = jnp.zeros_like(d_bias)
    for copy in inputs(blocks - N1):
        copy.start()

    def attention_step(b, h):
        i = blocks - N1 - b

        @pl.when(h == N0)
        def _():
            for copy in inputs(i):
                copy.wait()

            @pl.when(b + N1 < blocks)
            def _():
                for copy in inputs(i - N1):
                    copy.start()
            exchange(i, N0).wait()
            others = dctx.at[pl.ds(N0, (n - N1) * share)]
            rcopy(others, others, asend, arecv.at[i], tp=z).wait_recv()
        attend_grad(i, h, heads, qb, q, k_all, v, ctx_in.at[i % N2], dctx, top, inv, dq, dk, dv)

        @pl.when(h == heads - N1)
        def _():
            slot = i % N2
            got = grad_rows(i, qb, cos_in[slot], sin_in[slot], dq, dk, dv, d_bias)
            d_w[:] += dot(emb_in[slot], dot(got, back[:], NN).astype(BF), TN)
            part[rows_of(i, N0, qb), :] = dot(got, wq[:], NT)
            part[rows_of(i, z, share), :] = part[rows_of(i, z, share), :] + res_in[i % N2]

    def sides(u):
        side = u % N2
        return side, at(N2) * (N1 - side) + at(4) * side, at(4) * (N1 - side) + at(N2) * side

    def fetch(u):
        slot = u % HOLD

        @pl.when(u >= HOLD)
        def _():
            rcopy(xin.at[N0], cross.at[N0], xsend.at[slot], xrecv.at[N0], dp=p).wait_send()
        for m in range(jobs):
            @pl.when(u // span == m)
            def _(m=m):
                for i in range(4):
                    pltpu.make_async_copy(piece(m, u, N2 * i), work.at[slot, i], esem.at[slot]).start()
        rcopy(landed.at[u], landed.at[u], csend, crecv.at[u], dp=p).wait_recv()
        pltpu.make_async_copy(landed.at[u], fresh, fsem).start()

    def add(u):
        slot = u % HOLD
        pltpu.make_async_copy(landed.at[u], work.at[slot], esem.at[slot]).wait()
        pltpu.make_async_copy(landed.at[u], fresh, fsem).wait()
        for i in range(4):
            work[slot, i] = work[slot, i] + fresh[i]

    def add_send(u):
        slot = u % HOLD
        side, first, second = sides(u)
        rcopy(work.at[slot, N1 + side], cross.at[u, N0], xsend.at[slot], xrecv.at[u], dp=first).start()
        rcopy(work.at[slot, 3], cross.at[u, N1], xsend.at[slot], xrecv.at[u], dp=first).start()

    def load_cross(u):
        rcopy(cross.at[u], cross.at[u], xsend.at[N0], xrecv.at[u], dp=p).wait_recv()
        pltpu.make_async_copy(cross.at[u], xin.at[u % N2], xsem.at[u % N2]).start()

    def crossed(u):
        slot = u % HOLD
        pltpu.make_async_copy(cross.at[u], xin.at[u % N2], xsem.at[u % N2]).wait()

        @pl.when(u >= LIVE)
        def _():
            pltpu.make_async_copy(keep.at[u % LIVE], keep.at[u % LIVE], ksem.at[u % LIVE]).wait()

        @pl.when(u >= PAIR)
        def _():
            rcopy(pass_on.at[u % PAIR], last.at[u], ysend.at[u % PAIR], yrecv.at[u], dp=p).wait_send()
        keep[u % LIVE] = xin[u % N2, N0] + work[slot, N0]
        pass_on[u % PAIR] = xin[u % N2, N1] + work[slot, N2 - u % N2]

    def crossed_send(u):
        side, first, second = sides(u)
        rcopy(pass_on.at[u % PAIR], last.at[u], ysend.at[u % PAIR], yrecv.at[u], dp=second).start()

    def load_last(u):
        rcopy(last.at[u], last.at[u], ysend.at[N0], yrecv.at[u], dp=p).wait_recv()
        pltpu.make_async_copy(last.at[u], yin.at[u % N2], ysem.at[u % N2]).start()

    def in_plane(u):
        pltpu.make_async_copy(last.at[u], yin.at[u % N2], ysem.at[u % N2]).wait()
        keep[u % LIVE] = keep[u % LIVE] + yin[u % N2]

    def unit(k):
        u = (k // 3) * N2 + k % 3
        return u, (k >= N0) & (k % 3 < N2) & (u < units)

    def along_tp(k, t, send):
        toward = jnp.where(z < t, z, n - N1 - z)
        late = jnp.where(z == t, max(t, n - N1 - t), toward)
        u, ok = unit(k - PLANE - N1 - late)
        mine = (u // span) * N2 + u % N2
        slot = u % LIVE
        ok = ok & ((u // N2) % n == t)

        def add_from(ref, sem):
            rcopy(ref, ref, csend, sem, tp=z).wait_recv()
            keep[slot] = keep[slot] + ref[:]
        if send:
            @pl.when(ok & (z < t))
            def _():
                rcopy(keep.at[slot], along.at[u], ksem.at[slot], zrecv.at[u], tp=z + N1).start()

            @pl.when(ok & (z > t + N1))
            def _():
                rcopy(keep.at[slot], along.at[u], ksem.at[slot], zrecv.at[u], tp=z - N1).start()

            @pl.when(ok & (z == t + N1))
            def _():
                rcopy(keep.at[slot], final.at[mine], ksem.at[slot], frecv.at[mine], tp=z - N1).start()

            for m in range(jobs):
                @pl.when(ok & (z == t) & (u // span == m))
                def _(m=m):
                    dst = whole[m].at[p, u % N2] if m < jobs - N1 else grads.at[u % N2]
                    pltpu.make_async_copy(keep.at[slot], dst, ksem.at[slot]).start()
        else:
            @pl.when(ok & (((z > N0) & (z <= t)) | ((z > t) & (z < n - N1))))
            def _():
                add_from(along.at[u], zrecv.at[u])
            if t < n - N1:
                @pl.when(ok & (z == t))
                def _():
                    add_from(final.at[mine], frecv.at[mine])

    spread = [Spread(at, functools.partial(block_of, whole[m], at), gsend.at[m], grecv.at[m]) for m in range(jobs - N1)]

    def place(c):
        return (blocks - N1 - c // per) * per + c % per

    def chunk(c):
        return total.at[c % RING]

    def done(c, value):
        @pl.when(c >= RING)
        def _():
            pltpu.make_async_copy(chunk(c), chunk(c), osend.at[c % RING]).wait()
        total[c % RING] = value

    def hand_out(c):
        where = out.at[p, pl.ds(pl.multiple_of(place(c) * rows, rows), rows)]
        for rel in range(8):
            src = total.at[c % RING, :, pl.ds(pl.multiple_of(at(rel) * block, block), block)]
            if rel == N0:
                pltpu.make_async_copy(src, where, osend.at[c % RING]).start()
            else:
                rcopy(src, where, osend.at[c % RING], orecv.at[rel], dp=at(rel)).start()

    def staged(k, offset, stage):
        u, ok = unit(k - offset)
        pl.when(ok)(functools.partial(stage, u))
    steps = max(heads + chunks + LAG * (n - N1) + N1, (units // N2) * 3 + PLANE + n)

    @pl.loop(N0, steps)
    def _(k):
        c = k - heads - LAG * lead - N1

        @pl.when((c >= N0) & (c < chunks))
        def _():
            hand_out(c)
        chain_sum(k - heads, z, n, rows, chunks, part, left, right, done, send_r, send_l, recv_l, recv_r, place)
        for offset, stage in ((CROSSED, crossed), (ADD, add), (PLANE, in_plane)):
            staged(k, offset, stage)
        for t in range(n):
            along_tp(k, t, False)
        for offset, stage in ((N0, fetch), (LOAD, load_cross), (LAND, load_last)):
            staged(k, offset, stage)

        @pl.when(k < blocks * heads)
        def _():
            attention_step(k // heads, k % heads)
        for offset, stage in ((ADD, add_send), (CROSSED, crossed_send)):
            staged(k, offset, stage)
        for t in range(n):
            along_tp(k, t, True)
        for m, gather in enumerate(spread):
            for offset, stage in ((N0, gather.start), (3, gather.cross), (6, gather.diagonal)):
                pl.when(k == GATHER[m] + offset)(stage)

    chain_drain(z, n, part, left, right, send_r, send_l, recv_l, recv_r)
    for c in range(max(N0, chunks - RING), chunks):
        pltpu.make_async_copy(chunk(c), chunk(c), osend.at[c % RING]).wait()
    for rel in range(N1, 8):
        rcopy(out.at[at(rel)], out.at[at(rel)], csend, orecv.at[rel], dp=p).wait_recv()
    for slot in range(HOLD):
        rcopy(xin.at[N0], cross.at[N0], xsend.at[slot], xrecv.at[N0], dp=p).wait_send()
    for slot in range(PAIR):
        rcopy(pass_on.at[slot], last.at[N0], ysend.at[slot], yrecv.at[N0], dp=p).wait_send()
    for slot in range(LIVE):
        pltpu.make_async_copy(keep.at[slot], keep.at[slot], ksem.at[slot]).wait()
    rcopy(landed, landed, csend, crecv.at[N0], dp=p).wait_send()
    for gather in spread:
        gather.finish()
    sent = dctx.at[pl.ds(N0, (n - N1) * share * blocks)]
    rcopy(sent, sent, asend, arecv.at[N0], tp=z).wait_send()


def backward(d_ctx, resid, saved, cos, sin, wq, back, emb, prods, heads, n_tp, n_dp):
    q, k, v, ctx, top, inv = saved
    seq, dims = q.shape
    width = wq.shape[0]
    chunks = 32
    rows = seq // chunks
    jobs = len(prods)
    piece = (prods[0].shape[2] // 2, prods[0].shape[3])
    units = jobs * 2 * n_tp
    dma = pltpu.SemaphoreType.DMA
    shape = jax.ShapeDtypeStruct
    qb = seq // 8
    vmem = [(seq, width)] * 3 + [(RING, rows, width), (seq, dims), (qb, dims), (seq, dims), (seq, dims), (2, qb, dims), (2, qb // n_tp, width)] + [(2, qb, dims // 2)] * 2 + [
            (HOLD, 4) + piece, (4,) + piece, (2, 2) + piece, (2,) + piece, (LIVE,) + piece, (PAIR,) + piece, (units,) + piece, (2 * jobs,) + piece]
    sems = [(), (), (chunks,), (chunks,), (RING,), (8,), (), (units,), (HOLD,), (), (HOLD,), (units,), (2,), (PAIR,), (units,), (2,), (LIVE,), (units,), (2 * jobs,), (), (8,), (8,), (5, 2), (jobs - 1, len(EDGES)), (jobs - 1, len(EDGES))]
    scratch = [pltpu.VMEM(size, F32) for size in vmem]
    scratch.insert(12, pltpu.VMEM((2, qb, width), BF))
    full = shape((n_dp, 2) + piece, F32)
    *whole, cols, grads, d_w, d_bias, _, _, _ = pl.pallas_call(
        functools.partial(backward_kernel, n_tp, rows, chunks, jobs, heads),
        name='backward',
        out_shape=[full] * (jobs - 1) + [shape((n_dp, seq, width // n_dp), F32), shape((2,) + piece, F32), shape((width, 3 * dims), F32), shape((1, 3 * dims), F32),
                   shape((units, 4) + piece, F32), shape((units, 2) + piece, F32), shape((units,) + piece, F32)],
        in_specs=[ANY, ANY] + [VMEM] * 3 + [ANY] + [VMEM] * 2 + [ANY] * 2 + [VMEM] * 2 + [ANY] * (1 + jobs),
        out_specs=[ANY] * (jobs - 1) + [ANY, ANY, VMEM, VMEM, ANY, ANY, ANY],
        scratch_shapes=scratch + [dma(size) for size in sems],
        compiler_params=pltpu.CompilerParams(collective_id=1, has_side_effects=True, vmem_limit_bytes=67_000_000),
        cost_estimate=pl.CostEstimate(flops=20 * 10 ** 9, bytes_accessed=100 * 2 ** 20, transcendentals=0),
    )(d_ctx, resid, q, k, v, ctx, top, inv, cos, sin, wq, back, emb, *prods)
    return d_w, d_bias, cols, whole, grads


WAYS = 4


def table_kernel(ids, rows_ref, out, *tables):
    step = pl.program_id(0)
    count = rows_ref.shape[0]
    part = count // WAYS

    @pl.when(step == 0)
    def _():
        for table in tables:
            table[:] = jnp.zeros_like(table)

    @pl.loop(0, part, unroll=4)
    def _(r):
        for way, table in enumerate(tables):
            row = way * part + r
            where = pl.ds(ids[step * count + row], 1)
            table[where, :] = table[where, :] + rows_ref[pl.ds(row, 1), :]

    @pl.when(step == pl.num_programs(0) - 1)
    def _():
        total = tables[0][:]
        for table in tables[1:]:
            total = total + table[:]
        out[:] = SHRINK * total[:out.shape[0]]


def table_rows(ids, rows, vocab_loc):
    count, block = rows.shape
    step = min(1024, count // 2)
    return pl.pallas_call(
        table_kernel,
        name='table_rows',
        grid_spec=pltpu.PrefetchScalarGridSpec(
            num_scalar_prefetch=1,
            grid=(count // step,),
            in_specs=[pl.BlockSpec((step, block), lambda i, ids: (i, 0))],
            out_specs=pl.BlockSpec((vocab_loc, block), lambda i, ids: (0, 0)),
            scratch_shapes=[pltpu.VMEM((vocab_loc + 8, block), F32)] * WAYS,
        ),
        out_shape=jax.ShapeDtypeStruct((vocab_loc, block), F32),
        compiler_params=pltpu.CompilerParams(dimension_semantics=('arbitrary',), vmem_limit_bytes=48 * 2 ** 20),
        cost_estimate=pl.CostEstimate(flops=3 * 10 ** 9, bytes_accessed=16 * 2 ** 20, transcendentals=0),
    )(ids, rows)


def finish_kernel(n, cuts, col, down, proj, d_w, small, table, down_all, proj_all, qkv_all, total, landed, work, cross, last, mine, inbox, sem, send, recv, dsend, drecv, osem, csem, xsend, xrecv, ysend, yrecv, rsend, rrecv):
    z = lax.axis_index('tp')
    p, at = plane()
    entry_barrier(z, n, at)
    block = col.shape[N1]
    half = len(cuts) // N2

    def part(i):
        def region(rel, side):
            return table.at[pl.ds(cuts[i][N0], cuts[i][N1] - cuts[i][N0]), pl.ds(pl.multiple_of(at(rel) * block, block), block)]
        return Spread(at, region, send.at[i], recv.at[i], col.at[pl.ds(cuts[i][N0], cuts[i][N1] - cuts[i][N0])])
    parts = [part(i) for i in range(len(cuts))]
    spread = [Spread(at, functools.partial(block_of, ref, at), dsend.at[i], drecv.at[i], own) for i, (ref, own) in enumerate(((down_all, down), (proj_all, proj), (qkv_all, mine)))]
    own_copies = [pltpu.make_async_copy(col, table.at[:, pl.ds(pl.multiple_of(p * block, block), block)], osem.at[N0])]
    own_copies += [pltpu.make_async_copy(src, dst.at[p], osem.at[i]) for i, (src, dst) in enumerate(((down, down_all), (proj, proj_all), (mine, qkv_all)), N1)]
    order = list(range(len(cuts)))
    flipped = order[half:] + order[:half]
    peers = [{'dp': at(N1)}, {'dp': at(N2)}, {'dp': at(4)}, {'tp': z + N1 - N2 * (z % N2)}, {'tp': (z + n // N2) % n}]

    def next_part(i):
        parts[order[i]].give(N0)
        parts[flipped[i]].give(N1)
        parts[order[i]].give(N2)

    def relay_part(i):
        one, two = order[i], flipped[i]
        parts[one].take(N0)
        if one < half:
            parts[one].give(3)
        parts[one].give(5)
        parts[two].take(N1)
        if two >= half:
            parts[two].give(4)
        parts[two].give(6)

    def exchange(r):
        return rcopy(total, inbox.at[r], rsend.at[r], rrecv.at[r], **peers[r])

    def round_end(r):
        exchange(r).wait()
        total[:] = total[:] + inbox[r]

    total[:] = small[:]
    for i in range(4):
        rcopy(d_w.at[at(N2 * i + N1)], landed.at[i], csem.at[N0], csem.at[N1], dp=at(N1)).start()
    for copy in own_copies[:3]:
        copy.start()
    next_part(N0)
    exchange(N0).start()
    spread[N0].start()
    spread[N1].start()
    next_part(N1)
    rcopy(landed, landed, csem.at[N0], csem.at[N1], dp=p).wait()
    for i in range(4):
        work[i] = d_w[at(N2 * i)] + landed[i]
    round_end(N0)
    for side, first in ((N0, N2), (N1, 4)):
        rcopy(work.at[N1 + side, side], cross.at[side, N0], xsend.at[side], xrecv.at[side], dp=at(first)).start()
        rcopy(work.at[3, side], cross.at[side, N1], xsend.at[side], xrecv.at[side], dp=at(first)).start()
    exchange(N1).start()
    next_part(N2)
    relay_part(N0)
    round_end(N1)
    for side, first in ((N0, N2), (N1, 4)):
        rcopy(cross.at[side], cross.at[side], xsend.at[side], xrecv.at[side], dp=p).wait()
        cross[side, N0] = cross[side, N0] + work[N0, side]
        cross[side, N1] = cross[side, N1] + work[N2 - side, side]
    exchange(N2).start()
    for side, second in ((N0, 4), (N1, N2)):
        rcopy(cross.at[side, N1], last.at[side], ysend.at[side], yrecv.at[side], dp=at(second)).start()
    next_part(3)
    spread[N0].cross()
    spread[N1].cross()
    relay_part(N1)
    round_end(N2)
    for side in range(N2):
        rcopy(last.at[side], last.at[side], ysend.at[side], yrecv.at[side], dp=p).wait()
        mine[side] = cross[side, N0] + last[side]
    exchange(3).start()
    next_part(4)
    spread[N2].start()
    own_copies[3].start()
    spread[N0].diagonal()
    spread[N1].diagonal()
    relay_part(N2)
    round_end(3)
    next_part(5)
    exchange(4).start()
    relay_part(3)
    spread[N2].cross()
    next_part(6)
    round_end(4)
    relay_part(4)
    next_part(7)
    spread[N2].diagonal()
    for i in range(5, len(cuts)):
        relay_part(i)
    for i in range(half):
        for via, where in ((3, i), (4, i + half)):
            parts[where].take(via)
            parts[where].give(7)
    for i in order:
        for j in (N2, 5, 6, 7):
            parts[i].take(j)
        for j in (N0, N1, N2, 3 if i < half else 4, 5, 6, 7):
            parts[i].copy(j, *EDGES[j]).wait_send()
    for gather in spread:
        gather.finish()
    for copy in own_copies:
        copy.wait()


def finish(col, down, proj, d_w, small, n_tp, n_dp):
    size, block = col.shape
    tiles = size // 8
    cuts = [(8 * (tiles * i // 8), 8 * (tiles * (i + N1) // 8)) for i in range(8)]
    dma = pltpu.SemaphoreType.DMA
    shape = jax.ShapeDtypeStruct
    third = d_w.shape[N1:]
    kinds = len(EDGES)
    table, down_all, proj_all, qkv_all, total = pl.pallas_call(
        functools.partial(finish_kernel, n_tp, cuts),
        name='finish',
        out_shape=[shape((size, n_dp * block), F32)] + [shape((n_dp,) + src, F32) for src in (down.shape, proj.shape, third)] + [shape(small.shape, F32)],
        in_specs=[ANY] * 3 + [VMEM] * N2,
        out_specs=[ANY] * 4 + [VMEM],
        scratch_shapes=[pltpu.VMEM(lead + third[N1:], F32) for lead in ((4, N2), (4, N2), (N2, N2), (N2,), (N2,))] + [pltpu.VMEM((5,) + small.shape, F32), dma,
                        dma((8, kinds)), dma((8, kinds)), dma((3, kinds)), dma((3, kinds)), dma((4,))] + [dma((N2,))] * 5 + [dma((5,))] * N2,
        compiler_params=pltpu.CompilerParams(collective_id=N2, has_side_effects=True, vmem_limit_bytes=32 * N2 ** 20),
        cost_estimate=pl.CostEstimate(flops=10 * 10 ** 9, bytes_accessed=60 * N2 ** 20, transcendentals=N0),
    )(col, down, proj, d_w, small)
    return table, down_all.reshape(-N1, down.shape[N2]), proj_all.reshape(-N1, proj.shape[N2]), qkv_all.reshape(-N1, third[N2]), total


def dot(a, b, dims):
    return lax.dot_general(a, b, (dims, ((), ())), preferred_element_type=F32)


NT, TN, NN = ((1,), (1,)), ((0,), (0,)), ((1,), (0,))


def lane_head(shape, heads, halves):
    lane = lax.broadcasted_iota(jnp.int32, shape, 1)
    dims = shape[1] // halves
    return (lane % dims) // (dims // heads)


def turned(both, cos, sin):
    half = both.shape[1] // 2
    x1, x2 = both[:, :half], both[:, half:]
    return jnp.concatenate([x1 * cos - x2 * sin, x2 * cos + x1 * sin], axis=1)


def project(i, qb, emb, wq, bq, cos, sin, q, k, v):
    at_q = pl.ds(pl.multiple_of(i * qb, qb), qb)
    dims = q.shape[1]
    qkv = (dot(emb[at_q, :], wq[:], NN) + bq[:]).astype(BF)
    for ref, part in ((q, 0), (k, 1)):
        ref[at_q, :] = turned(qkv[:, part * dims:(part + 1) * dims].astype(F32), cos[at_q, :], sin[at_q, :]).astype(BF)
    v[at_q, :] = qkv[:, 2 * dims:]


def scores(i, j, kb, qb, scale, keys, q):
    s = dot(keys, q, NT) * scale
    key = j * kb + lax.broadcasted_iota(jnp.int32, (kb, qb), 0)
    query = i * qb + lax.broadcasted_iota(jnp.int32, (kb, qb), 1)
    return jnp.where(query >= key, s, -1e30)


def attend(i, h, heads, qb, q_ref, k_ref, v_ref, ctx_ref, top_ref, inv_ref, s_ref):
    kb = 2 * qb
    dims = q_ref.shape[1]
    scale = (dims // heads) ** -0.5
    at_q = pl.ds(pl.multiple_of(i * qb, qb), qb)
    q = jnp.where(lane_head((qb, dims), heads, 2) == h, q_ref[at_q, :].astype(F32), 0.0).astype(BF)
    count = (i + 2) // 2

    def at_key(j):
        return pl.ds(pl.multiple_of(j * kb, kb), kb)

    def first(j, top):
        s = scores(i, j, kb, qb, scale, k_ref[at_key(j), :], q)
        s_ref[at_key(j), :] = s
        return jnp.maximum(top, jnp.max(s, axis=0, keepdims=True))
    top = lax.fori_loop(0, count, first, jnp.full((1, qb), -1e30, F32))

    def weigh(j, total):
        e = jnp.exp(s_ref[at_key(j), :] - top)
        s_ref[at_key(j), :] = e
        return total + jnp.sum(e, axis=0, keepdims=True)
    inv = 1.0 / lax.fori_loop(0, count, weigh, jnp.zeros((1, qb), F32))

    def mix(j, acc):
        return acc + dot((s_ref[at_key(j), :] * inv).astype(BF), v_ref[at_key(j), :], TN)
    mixed = lax.fori_loop(0, count, mix, jnp.zeros((qb, dims), F32))
    ctx_ref[at_q, :] = jnp.where(lane_head((qb, dims), heads, 1) == h, mixed, ctx_ref[at_q, :])
    top_ref[pl.ds(h, 1), at_q] = top
    inv_ref[pl.ds(h, 1), at_q] = inv


def attend_grad(i, h, heads, qb, q_ref, k_ref, v_ref, ctx_ref, dctx_ref, top_ref, inv_ref, dq_ref, dk_ref, dv_ref):
    kb = 2 * qb
    dims = q_ref.shape[1]
    scale = (dims // heads) ** -0.5
    at_q = pl.ds(pl.multiple_of(i * qb, qb), qb)
    q = jnp.where(lane_head((qb, dims), heads, 2) == h, q_ref[at_q, :].astype(F32), 0.0).astype(BF)
    dc = jnp.where(lane_head((qb, dims), heads, 1) == h, dctx_ref[at_q, :], 0.0).astype(BF)
    ones = jnp.ones((8, dims), F32)
    mean = lax.dot_general(ones, dc.astype(F32) * ctx_ref[:], (NT, ((), ())), precision=lax.Precision.HIGHEST, preferred_element_type=F32)[:1]
    top, inv = top_ref[pl.ds(h, 1), at_q], inv_ref[pl.ds(h, 1), at_q]

    def step(j, dq):
        at_k = pl.ds(pl.multiple_of(j * kb, kb), kb)
        keys = k_ref[at_k, :]
        probs = (jnp.exp(scores(i, j, kb, qb, scale, keys, q) - top) * inv).astype(BF)
        ds = (probs.astype(F32) * (dot(v_ref[at_k, :], dc, NT) - mean) * scale).astype(BF)
        dv_ref[at_k, :] += dot(probs, dc, NN)
        dk_ref[at_k, :] += dot(ds, q, NN)
        return dq + dot(ds, keys, TN)
    dq = lax.fori_loop(0, (i + 2) // 2, step, jnp.zeros((qb, dims), F32))
    dq_ref[:] = jnp.where(lane_head((qb, dims), heads, 2) == h, dq, dq_ref[:])


def grad_rows(i, qb, cos, sin, dq, dk, dv, d_bias):
    at_q = pl.ds(pl.multiple_of(i * qb, qb), qb)
    back = [turned(values, cos, -sin) for values in (dq[:], dk[at_q, :])]
    rows = jnp.concatenate(back + [dv[at_q, :]], axis=1)
    d_bias[:] += jnp.sum(rows, axis=0, keepdims=True)
    return rows.astype(BF)


def standard(values):
    mean = jnp.mean(values, axis=1, keepdims=True)
    centered = values - mean
    scale = lax.rsqrt(jnp.mean(centered * centered, axis=1, keepdims=True) + EPS)
    return centered * scale, scale


def standard_grad(d_out, unit, scale):
    return scale * (d_out - jnp.mean(d_out, axis=1, keepdims=True) - unit * jnp.mean(d_out * unit, axis=1, keepdims=True))


def over_rows(values):
    return jnp.sum(values, axis=0, keepdims=True)


def layer_kernel(n, ctx, wo, emb, cot, vectors, gate_bias, lin_bias, wg, wl, wd, hidden, d_ffn, d_attn, resid, d_ctx, sums, inner, d_gate, d_lin, gate, lin, acc, unit1, scale1):
    i = pl.program_id(N0)
    t = i % n
    tile = 256 if acc.shape[N1] % 256 == N0 else acc.shape[N1]
    tiles = range(N0, acc.shape[N1], tile)
    b_out, gain1, bias1, b_down, gain2 = [vectors[pl.ds(j, N1), :] for j in range(5)]

    @pl.when(i == N0)
    def _():
        total = ALPHA * emb[:].astype(F32) + b_out
        for h in range(n):
            total = total + dot(ctx[h].astype(BF), wo[h], NN)
        unit, scale1[:] = standard(total)
        unit1[:] = unit
        hidden[:] = (unit * gain1 + bias1).astype(BF)
        acc[:] = jnp.zeros_like(acc)

    @pl.when(i < n)
    def _():
        for lo in tiles:
            cols = pl.ds(lo, tile)
            g = dot(hidden[:], wg[N0, :, cols], NN) + gate_bias[pl.ds(t, N1), cols]
            l = dot(hidden[:], wl[N0, :, cols], NN) + lin_bias[pl.ds(t, N1), cols]
            gate[t, :, cols] = g
            lin[t, :, cols] = l
            inner[N0, :, cols] = (0.5 * g * (1.0 + lax.erf(g * 0.5 ** 0.5)) * l).astype(BF)
        for lo in tiles:
            cols = pl.ds(lo, tile)
            acc[:, cols] += dot(inner[N0], wd[N0, :, cols], NN)

    @pl.when(i == n - N1)
    def _():
        unit, scale = standard(ALPHA * hidden[:].astype(F32) + acc[:] + b_down)
        g = cot[:].astype(F32)
        d_y = standard_grad(g * gain2, unit, scale)
        sums[pl.ds(N2 * n + 3, N1), :] = over_rows(d_y)
        sums[pl.ds(N2 * n + 4, N1), :] = over_rows(g * unit)
        d_ffn[:] = d_y.astype(BF)
        acc[:] = ALPHA * d_y

    @pl.when(i >= n)
    def _():
        for lo in tiles:
            cols = pl.ds(lo, tile)
            d_inner = dot(d_ffn[:], wd[N0, cols, :], NT).astype(BF).astype(F32)
            g, l = gate[t, :, cols], lin[t, :, cols]
            cdf = 0.5 * (1.0 + lax.erf(g * 0.5 ** 0.5))
            slope = cdf + g * (jnp.exp(-0.5 * g * g) * (N2 * np.pi) ** -0.5)
            d_l = d_inner * (g * cdf)
            d_g = d_inner * l * slope
            sums[pl.ds(t, N1), cols] = over_rows(d_g)
            sums[pl.ds(n + t, N1), cols] = over_rows(d_l)
            d_gate[N0, :, cols] = d_g.astype(BF)
            d_lin[N0, :, cols] = d_l.astype(BF)
        for lo in tiles:
            cols = pl.ds(lo, tile)
            acc[:, cols] += dot(d_gate[N0], wg[N0, cols, :], NT) + dot(d_lin[N0], wl[N0, cols, :], NT)

    @pl.when(i == N2 * n - N1)
    def _():
        d_h, unit = acc[:], unit1[:]
        d_x = standard_grad(d_h * gain1, unit, scale1[:])
        sums[pl.ds(N2 * n, N1), :] = over_rows(d_x)
        sums[pl.ds(N2 * n + N1, N1), :] = over_rows(d_h * unit)
        sums[pl.ds(N2 * n + N2, N1), :] = over_rows(d_h)
        resid[:] = ALPHA * d_x
        d_attn[:] = d_x.astype(BF)
        for h in range(n):
            d_ctx[h] = dot(d_attn[:], wo[h], NT)


def layer(ctx, wo, emb, cot, vectors, gate_bias, lin_bias, wg, wl, wd):
    n, own, dims = ctx.shape
    width = emb.shape[N1]
    ffn = wg.shape[N2]
    once = pl.BlockSpec(memory_space=pltpu.VMEM)
    weight = [pl.BlockSpec((N1,) + w.shape[N1:], lambda i: (i % n, N0, N0)) for w in (wg, wl, wd)]
    early = pl.BlockSpec((N1, own, ffn), lambda i: (jnp.minimum(i, n - N1), N0, N0))
    late = pl.BlockSpec((N1, own, ffn), lambda i: (jnp.maximum(i - n, N0), N0, N0))
    shape = jax.ShapeDtypeStruct
    slots = shape((n, own, ffn), BF)
    return pl.pallas_call(
        functools.partial(layer_kernel, n),
        name='layer',
        grid=(N2 * n,),
        in_specs=[once] * 7 + weight,
        out_specs=[once] * 6 + [early, late, late],
        out_shape=[shape((own, width), BF)] * 3 + [shape((own, width), F32), shape((n, own, dims), F32), shape((N2 * n + 8, width), F32), slots, slots, slots],
        scratch_shapes=[pltpu.VMEM((n, own, ffn), F32)] * N2 + [pltpu.VMEM((own, width), F32)] * N2 + [pltpu.VMEM((own, N1), F32)],
        compiler_params=pltpu.CompilerParams(dimension_semantics=('arbitrary',), vmem_limit_bytes=62 * N2 ** 20),
        cost_estimate=pl.CostEstimate(flops=15 * 10 ** 9, bytes_accessed=70 * N2 ** 20, transcendentals=N0),
    )(ctx, wo, emb, cot, vectors, gate_bias, lin_bias, wg, wl, wd)


def solution(mesh):
    n_tp, n_dp = mesh.shape['tp'], mesh.shape['dp']
    in_specs = (P('dp', None), P('dp', None, None), P('tp', None)) + WEIGHT_SPECS
    out_specs = (P('tp', None),) + WEIGHT_SPECS

    def device_step(tokens, cotangent, emb_table, *weights):
        (w_qkv, b_qkv, w_out, b_out, ln1_gain, ln1_bias, w_gate, b_gate, w_lin, b_lin, w_down, b_down, ln2_gain) = weights
        tp, dp = lax.axis_index('tp'), lax.axis_index('dp')
        tokens = tokens[N0]
        seq_len, width = tokens.shape[N0], emb_table.shape[N1]
        heads, head_dim = b_qkv.shape[N0], b_qkv.shape[N1] // 3
        own = seq_len // n_tp
        ffn = w_gate.shape[N1]
        rk, rf, ro = width // n_dp, ffn // n_dp, w_out.shape[N0] // n_dp

        def cut(weight):
            rows = weight.shape[N0] // n_dp
            return lax.dynamic_slice_in_dim(weight, dp * rows, rows, N0)
        bias_rows = jnp.concatenate([b_gate[None], b_lin[None], jnp.zeros((14, ffn), BF)], axis=N0)
        piece = jnp.concatenate([cut(w_gate), cut(w_lin), cut(w_down), cut(w_out), bias_rows], axis=N0).astype(F32)

        vocab_loc = emb_table.shape[N0]
        local_ids = tokens - tp * vocab_loc
        in_shard = (local_ids >= N0) & (local_ids < vocab_loc)
        safe_ids = jnp.where(in_shard, local_ids, N0)
        found = jnp.take(emb_table, safe_ids, axis=N0)
        dims = heads * head_dim
        place = column_order(heads, head_dim)
        swap = (jnp.arange(3 * dims)[:, None] == jnp.asarray(place)[None, :]).astype(BF)
        wq = jnp.dot(w_qkv, swap, preferred_element_type=F32).astype(BF)
        bq = jnp.dot(b_qkv.reshape(N1, -N1), swap, preferred_element_type=F32)
        cos_tab, sin_tab = rope_tables(seq_len, head_dim, heads)
        emb_bf, (wg_full, wl_full, wd_full, wo_full), biases, tok_all, ctx_own, saved = embed(found, in_shard[:, None].astype(F32), piece, tokens.reshape(-N1, min(128, seq_len // 8)), (w_gate, w_lin, w_down, w_out), wq, bq, cos_tab, sin_tab, heads, n_tp, n_dp)
        is_own = (jnp.arange(n_tp) == tp)[:, None]
        bg_full, bl_full = [jnp.where(is_own, b[None].astype(F32), biases[:, i]) for i, b in enumerate((b_gate, b_lin))]

        blocks = 8

        def owned(values):
            return lax.dynamic_index_in_dim(values.reshape(blocks, n_tp, -N1, width), tp, N1, keepdims=False).reshape(own, width)
        emb_own, cot_own = owned(emb_bf), owned(cotangent[N0])
        vectors = jnp.stack([b_out, ln1_gain, ln1_bias, b_down, ln2_gain] + [b_out] * 3).astype(F32)
        hidden, d_ffn_bf, d_attn_bf, resid, d_ctx, row_sums, inner_act, d_gate_bf, d_lin_bf = layer(
            ctx_own.reshape(n_tp, own, dims), wo_full, emb_own, cot_own, vectors, bg_full, bl_full, wg_full, wl_full, wd_full)

        def product(lhs, rhs, spec):
            return jnp.einsum(spec, lhs, rhs, preferred_element_type=F32).reshape(n_tp, n_dp, -N1, width)

        prod_down = product(inner_act, d_ffn_bf, 'tsc,sd->tcd')
        prod_gate = product(hidden, d_gate_bf, 'sk,tsc->tkc')
        prod_lin = product(hidden, d_lin_bf, 'sk,tsc->tkc')
        d_w_out = jnp.einsum('hse,sd->hed', ctx_own.reshape(n_tp, own, dims).astype(BF), d_attn_bf, preferred_element_type=F32)
        d_w_out = lax.psum_scatter(d_w_out.reshape(-N1, width), ALL, scatter_dimension=N0, tiled=True)
        d_w_qkv, d_b_qkv, d_cols, (d_w_gate, d_w_lin), d_w_down = backward(
            d_ctx.reshape(n_tp, blocks, own // blocks, dims), resid.reshape(blocks, own // blocks, width), saved, cos_tab, sin_tab, wq, swap.T, emb_bf,
            (prod_gate, prod_lin, prod_down), heads, n_tp, n_dp)
        d_w_gate, d_w_lin = d_w_gate.reshape(-N1, ffn), d_w_lin.reshape(-N1, ffn)
        d_b_qkv = jnp.dot(d_b_qkv, swap.astype(F32).T, precision=lax.Precision.HIGHEST)
        all_ids = tok_all.reshape(-N1) - tp * vocab_loc
        all_ids = jnp.where((all_ids >= N0) & (all_ids < vocab_loc), all_ids, vocab_loc)
        col = table_rows(all_ids, d_cols.reshape(n_dp * seq_len, -N1), vocab_loc)

        slot = (jnp.arange(n_tp) == tp).astype(F32)[:, None]
        d_bq_rows = jnp.pad(slot * d_b_qkv, ((N0, N0), (N0, ffn - 3 * dims)))
        kept = N2 * n_tp
        small = jnp.concatenate([row_sums[:kept], d_bq_rows, row_sums[kept:kept + 5], jnp.zeros((7, width), F32)], axis=N0)
        d_table, d_w_down, d_w_out, d_w_qkv, small = finish(
            col, d_w_down, d_w_out.reshape(N2, -N1, width), d_w_qkv.reshape(n_dp, N2, -N1, 3 * dims), small, n_tp, n_dp)
        d_b_gate = lax.dynamic_index_in_dim(small[:n_tp], tp, N0, keepdims=False)
        d_b_lin = lax.dynamic_index_in_dim(small[n_tp:N2 * n_tp], tp, N0, keepdims=False)
        d_b_qkv = lax.dynamic_index_in_dim(small[N2 * n_tp:3 * n_tp], tp, N0, keepdims=False)[:3 * dims].reshape(heads, 3 * head_dim)
        d_b_out, d_ln1_gain, d_ln1_bias, d_b_down, d_ln2_gain = [small[3 * n_tp + i] for i in range(5)]
        return (d_table, d_w_qkv, d_b_qkv, d_w_out, d_b_out, d_ln1_gain, d_ln1_bias, d_w_gate, d_b_gate, d_w_lin, d_b_lin, d_w_down, d_b_down, d_ln2_gain)

    return jax.shard_map(device_step, mesh=mesh, in_specs=in_specs, out_specs=out_specs, check_vma=False)
```

```python
import functools

import jax
import jax.numpy as jnp
import numpy as np
from jax import lax
from jax.experimental import pallas as pl
from jax.experimental.pallas import tpu as pltpu
from jax.sharding import PartitionSpec as P

ALPHA = 140.0 ** 0.5
EPS = 1e-5
SHRINK = 0.1
ROPE_BASE = 10000.0
WEIGHT_SPECS = (P(None, 'tp'), P('tp', None), P('tp', None), P(), P(), P(), P(None, 'tp'), P('tp'), P(None, 'tp'), P('tp'), P('tp', None), P(), P())
ALL = ('tp', 'dp')
BF = jnp.bfloat16
N0, N1, N2 = range(3)
F32 = jnp.float32
MESH = pl.DeviceIdType.MESH
ANY = pl.BlockSpec(memory_space=pl.ANY)
VMEM = pl.BlockSpec(memory_space=pltpu.VMEM)


def rope_tables(seq_len, head_dim, heads):
    half_dim = head_dim // 2
    inv_freq = (ROPE_BASE ** (-2.0 * np.arange(half_dim) / head_dim)).astype(np.float32)
    angles = np.arange(seq_len, dtype=np.float32)[:, None] * inv_freq[None, :]
    return [jnp.asarray(np.tile(table(angles), (1, heads))) for table in (np.cos, np.sin)]


def column_order(heads, head_dim):
    cols = np.arange(3 * heads * head_dim).reshape(heads, 3, 2, head_dim // 2)
    return np.concatenate([cols[:, part].transpose(1, 0, 2).ravel() for part in (0, 1)] + [cols[:, 2].ravel()])


def rcopy(src, dst, send, recv, **where):
    return pltpu.make_async_remote_copy(src_ref=src, dst_ref=dst, send_sem=send, recv_sem=recv, device_id=dict(where), device_id_type=MESH)


def plane():
    p = lax.axis_index('dp')
    y, x, c = p // 4, (p // 2) % 2, p % 2

    def at(rel):
        yy = 1 - y if rel & 4 else y
        xx = 1 - x if rel & 2 else x
        cc = 1 - c if rel & 1 else c
        return yy * 4 + xx * 2 + cc
    return p, at


def entry_barrier(z, n, at):
    bar = pltpu.get_barrier_semaphore()
    for rel in range(1, 8):
        pl.semaphore_signal(bar, inc=1, device_id={'dp': at(rel)}, device_id_type=MESH)
    for d in range(1, n):
        pl.semaphore_signal(bar, inc=1, device_id={'tp': (z + d) % n}, device_id_type=MESH)
    pl.semaphore_wait(bar, 7 + n - 1)


LAG = 3


def chain_sum(k, z, n, rows, chunks, part, left, right, done, send_r, send_l, recv_l, recv_r, place=lambda c: c):
    last = n - 1

    def at_rows(c):
        return pl.ds(pl.multiple_of(place(c) * rows, rows), rows)

    def cut(ref, c):
        return ref.at[at_rows(c)]

    def load(ref, c):
        return ref[at_rows(c)]

    def store(ref, c, value):
        ref[at_rows(c)] = value
    cl, cr = k - LAG * z, k - LAG * (last - z)
    okl, okr = (cl >= 0) & (cl < chunks), (cr >= 0) & (cr < chunks)

    @pl.when(okl & (z > 0))
    def _():
        rcopy(cut(left, cl), cut(left, cl), send_r, recv_l.at[cl], tp=z).wait_recv()

    @pl.when(okl & (z == last))
    def _():
        done(cl, load(left, cl) + load(part, cl))

    @pl.when(okl & (z > 0) & (z < last))
    def _():
        run = load(left, cl)

        @pl.when(z >= n // 2)
        def _():
            done(cl, run + load(right, cl))
        store(left, cl, run + load(part, cl))

    @pl.when(okr & (z < last))
    def _():
        rcopy(cut(right, cr), cut(right, cr), send_l, recv_r.at[cr], tp=z).wait_recv()

    @pl.when(okr & (z == 0))
    def _():
        done(cr, load(part, cr) + load(right, cr))

    @pl.when(okr & (z > 0) & (z < last))
    def _():
        run = load(right, cr)

        @pl.when(z < n // 2)
        def _():
            done(cr, load(left, cr) + run)
        store(right, cr, run + load(part, cr))

    @pl.when(okl & (z == 0))
    def _():
        rcopy(cut(part, cl), cut(left, cl), send_r, recv_l.at[cl], tp=z + 1).start()

    @pl.when(okl & (z > 0) & (z < last))
    def _():
        rcopy(cut(left, cl), cut(left, cl), send_r, recv_l.at[cl], tp=z + 1).start()

    @pl.when(okr & (z == last))
    def _():
        rcopy(cut(part, cr), cut(right, cr), send_l, recv_r.at[cr], tp=z - 1).start()

    @pl.when(okr & (z > 0) & (z < last))
    def _():
        rcopy(cut(right, cr), cut(right, cr), send_l, recv_r.at[cr], tp=z - 1).start()


def chain_drain(z, n, part, left, right, send_r, send_l, recv_l, recv_r):
    @pl.when(z < n - 1)
    def _():
        rcopy(part, left, send_r, recv_l.at[0], tp=z + 1).wait_send()

    @pl.when(z > 0)
    def _():
        rcopy(part, right, send_l, recv_r.at[0], tp=z - 1).wait_send()


EDGES = ((0, 0, 2), (0, 0, 4), (0, 0, 1), (2, 1, 4), (4, 2, 2), (2, 0, 1), (4, 0, 1), (6, 1, 1), (6, 2, 1))
CROSS, DIAGONAL, LAST = ((0, 3, 5), (1, 4, 6)), ((3, 7), (4, 8)), {1: (2,), 3: (5,), 5: (6,), 7: (7, 8)}
STEPS = (4, 10, 17, 21, 25, 29)
FIRST = 18
ORDER = (0, 2, 4, 1, 3, 5, 6, 7)


def emb_kernel(n, rows, chunks, cuts, heads, found, mask, wq, bq, cos, sin, piece, toks, *refs):
    m = len(cuts)
    local, outs = refs[:m], refs[m + N1:N2 * m + N1]
    out, (bias, tok_all, wall, ctx_own, q, k_all, v, ctx, top, inv, part, left, right, raw, low, weights, send_r, send_l, recv_l, recv_r, tsend, trecv, tself, zsend, zrecv, psend, precv, lsem, isem, osem, bsem, asend, arecv, aself) = refs[m], refs[N2 * m + N1:]
    blocks = 8
    qb = part.shape[N0] // blocks
    per = chunks // blocks
    z = lax.axis_index('tp')
    p, at = plane()
    entry_barrier(z, n, at)
    half = piece.shape[N0] // N2

    @pl.when(z < n - N1)
    def _():
        rcopy(piece, wall.at[z, p], zsend.at[z], zrecv.at[z], tp=z + N1).start()

    @pl.when(z > N0)
    def _():
        rcopy(piece, wall.at[z, p], bsem.at[N1], zrecv.at[z], tp=z - N1).start()
    mine = [pltpu.make_async_copy(toks, tok_all.at[p], tself)]
    mine += [pltpu.make_async_copy(src, dst.at[z], lsem.at[i]) for i, (src, dst) in enumerate(zip(local, outs))]
    for copy in mine:
        copy.start()
    for rel in range(N1, 8):
        rcopy(toks, tok_all.at[p], tsend.at[rel], trecv.at[rel], dp=at(rel)).start()

    def others(d, body):
        @pl.when(z >= d)
        def _():
            body(z - d, -N1)

        @pl.when(z + d < n)
        def _():
            body(z + d, N1)

    def region(t, rel, side):
        blk = wall.at[t, at(rel)]
        return blk if side == N0 else wall.at[t, at(rel), pl.ds((side - N1) * half, half)]

    def give(t, j):
        rel, side, to = EDGES[j]
        rcopy(region(t, rel, side), region(t, rel, side), psend.at[t, j], precv.at[t, j], dp=at(to)).start()

    def take(t, j):
        rel, side, to = EDGES[j]
        blk = region(t, rel ^ to, side)
        rcopy(blk, blk, psend.at[t, j], precv.at[t, j], dp=p).wait_recv()

    def gave(t, j):
        rel, side, to = EDGES[j]
        rcopy(region(t, rel, side), region(t, rel, side), psend.at[t, j], precv.at[t, j], dp=p).wait_send()

    def arrive(d):
        def body(t, sign):
            blk = wall.at[t, p]
            rcopy(blk, blk, zsend.at[t], zrecv.at[t], tp=z).wait_recv()

            @pl.when((z - sign >= N0) & (z - sign < n))
            def _():
                rcopy(blk, blk, zsend.at[t], zrecv.at[t], tp=z - sign).start()
            for j in range(3):
                give(t, j)
        others(d, body)

    def relay(d, moves):
        def body(t, sign):
            for first, *rest in moves:
                take(t, first)
                for j in rest:
                    give(t, j)
        others(d, body)

    k_all[:] = jnp.zeros_like(k_all)
    v[:] = jnp.zeros_like(v)
    arrive(N1)

    @pl.loop(N0, blocks)
    def _(i):
        at_i = pl.ds(pl.multiple_of(i * qb, qb), qb)
        part[at_i, :] = jnp.where(mask[at_i, :] > N0, found[at_i, :].astype(F32), 0.0)

    def done(c, value):
        out[pl.ds(pl.multiple_of(c * rows, rows), rows)] = value.astype(out.dtype)

    def other(i):
        return i + (i + n - z) // n

    def loaded(i, rel, slot):
        return pltpu.make_async_copy(wall.at[other(i), at(rel), pl.ds(N0, cuts[-N1][N1])], raw.at[slot], isem.at[slot])

    def stored(i, rel, slot):
        return [pltpu.make_async_copy(low.at[slot, pl.ds(lo, hi - lo)], dst.at[other(i), at(rel)], osem.at[slot, k]) for k, ((lo, hi), dst) in enumerate(zip(cuts, outs))]
    plan = [(i, rel) for rel in ORDER for i in range(n - N1)]

    def prefetch(s):
        i, rel = plan[s]
        for j in LAST.get(rel, ()):
            take(other(i), j)
        loaded(i, rel, s % N2).start()

    def convert(s):
        i, rel = plan[s]
        loaded(i, rel, s % N2).wait()
        if s >= N2:
            for copy in stored(*plan[s - N2], s % N2):
                copy.wait()
        low[s % N2] = raw[s % N2].astype(low.dtype)
        if s + N1 < len(plan):
            prefetch(s + N1)
        for copy in stored(i, rel, s % N2):
            copy.start()
    events = [(STEPS[d - N1], functools.partial(relay, d, CROSS)) for d in range(N1, n)] + [(STEPS[d + n - N2], functools.partial(relay, d, DIAGONAL)) for d in range(N1, n)]
    events += [(N2 * d - N2, functools.partial(arrive, d)) for d in range(N2, n)]
    events += [(FIRST - N1, functools.partial(prefetch, N0))] + [(FIRST + s, functools.partial(convert, s)) for s in range(len(plan))]

    start = per + LAG * (n - N1)

    share = qb // n

    def context(i, d):
        to = (z + d) % n
        src = ctx.at[pl.ds(pl.multiple_of(i * qb + to * share, share), share)]
        if d == N0:
            return pltpu.make_async_copy(src, ctx_own.at[z, i], aself)
        return rcopy(src, ctx_own.at[z, i], asend, arecv.at[z], tp=to)

    @pl.loop(N0, max(start + blocks * heads + N1, FIRST + len(plan)))
    def _(k):
        step = k - start
        i = step // heads - N1

        @pl.when((step > N0) & (step % heads == N0) & (step <= blocks * heads))
        def _():
            for d in range(n):
                context(i, d).start()
        chain_sum(k, z, n, rows, chunks, part, left, right, done, send_r, send_l, recv_l, recv_r)
        for at_step, event in events:
            pl.when(k == at_step)(event)

        @pl.when((step >= N0) & (step < blocks * heads))
        def _():
            @pl.when(step % heads == N0)
            def _():
                project(step // heads, qb, out, wq, bq, cos, sin, q, k_all, v)
            attend(step // heads, step % heads, heads, qb, q, k_all, v, ctx, top, inv, weights)

    pltpu.make_async_copy(ctx_own.at[z], ctx_own.at[z], aself).wait()
    for d in range(N1, n):
        src = (z + d) % n
        rcopy(ctx_own.at[src], ctx_own.at[src], asend, arecv.at[src], tp=z).wait()
    chain_drain(z, n, part, left, right, send_r, send_l, recv_l, recv_r)
    for s in (len(plan) - N2, len(plan) - N1):
        for copy in stored(*plan[s], s % N2):
            copy.wait()

    def finish(t, sign):
        for j in range(len(EDGES)):
            gave(t, j)
        tail = pltpu.make_async_copy(wall.at[t, p, pl.ds(cuts[-N1][N1], bias.shape[N1])], bias.at[t], bsem.at[N0])
        tail.start()
        tail.wait()

        @pl.when((z - sign >= N0) & (z - sign < n))
        def _():
            rcopy(wall.at[t, p], wall.at[t, p], zsend.at[t], zrecv.at[t], tp=z).wait_send()
    for d in range(N1, n):
        others(d, finish)
    for copy in mine:
        copy.wait()
    for rel in range(N1, 8):
        rcopy(toks, tok_all.at[at(rel)], tsend.at[rel], trecv.at[rel], dp=at(rel)).wait()

    @pl.when(z < n - N1)
    def _():
        rcopy(piece, wall.at[z, p], zsend.at[z], zrecv.at[z], tp=z + N1).wait_send()

    @pl.when(z > N0)
    def _():
        rcopy(piece, wall.at[z, p], bsem.at[N1], zrecv.at[z], tp=z - N1).wait_send()


def embed(found, mask, piece, toks, local, wq, bq, cos, sin, heads, n_tp, n_dp):
    seq, width = found.shape
    chunks = 32
    rows = seq // chunks
    dims = wq.shape[1] // 3
    cuts, lo = [], 0
    for weight in local:
        cuts.append((lo, lo + weight.shape[0] // n_dp))
        lo = cuts[-1][1]
    dma = pltpu.SemaphoreType.DMA
    shape = jax.ShapeDtypeStruct
    shapes = [shape((seq, width), BF)]
    shapes += [shape((n_tp, n_dp, w.shape[0] // n_dp, w.shape[1]), BF) for w in local]
    shapes += [shape((n_tp, piece.shape[0] - lo, width), F32), shape((n_dp,) + toks.shape, toks.dtype), shape((n_tp, n_dp) + piece.shape, F32), shape((n_tp, 8, seq // n_tp // 8, dims), F32)]
    shapes += [shape((seq, dims), BF)] * 3 + [shape((seq, dims), F32)] + [shape((heads, seq), F32)] * 2
    out = pl.pallas_call(
        functools.partial(emb_kernel, n_tp, rows, chunks, cuts, heads),
        name='embed',
        out_shape=shapes,
        in_specs=[VMEM] * 6 + [ANY] * (2 + len(local)),
        out_specs=[VMEM] + [ANY] * (4 + len(local)) + [VMEM] * 6,
        scratch_shapes=[pltpu.VMEM((seq, width), F32)] * 3 + [pltpu.VMEM((2, lo, width), F32), pltpu.VMEM((2, lo, width), BF), pltpu.VMEM((seq, seq // 8), F32), dma, dma, dma((chunks,)), dma((chunks,)),
                        dma((8,)), dma((8,)), dma, dma((n_tp,)), dma((n_tp,)), dma((n_tp, len(EDGES))), dma((n_tp, len(EDGES))), dma((len(local),)), dma((2,)), dma((2, len(local))), dma((2,)),
                        dma, dma((n_tp,)), dma],
        compiler_params=pltpu.CompilerParams(collective_id=0, has_side_effects=True, vmem_limit_bytes=60 * 2 ** 20),
        cost_estimate=pl.CostEstimate(flops=20 * 10 ** 9, bytes_accessed=80 * 2 ** 20, transcendentals=0),
    )(found, mask, wq, bq, cos, sin, piece, toks, *[w.reshape(n_dp, w.shape[0] // n_dp, w.shape[1]) for w in local])
    m = 1 + len(local)
    return out[0], [w.reshape(n_tp, -1, w.shape[3]) for w in out[1:m]], out[m], out[m + 1], out[m + 3], out[m + 4:]


RING = 4
HOLD, LIVE, PAIR = 4, 12, 4
ADD, LOAD, CROSSED, LAND, PLANE, HOP, BEAT = 1, 4, 5, 9, 10, 2, 4
GATHER = (37, 41)


def block_of(ref, at, rel, side):
    return ref.at[at(rel)] if side == 0 else ref.at[at(rel), side - 1]


class Spread:
    def __init__(self, at, block, send, recv, own=None):
        self.at, self.block, self.send, self.recv, self.own = at, block, send, recv, own

    def copy(self, j, rel, side, to):
        dst = self.block(rel, side)
        src = self.own if rel == 0 and self.own is not None else dst
        return rcopy(src, dst, self.send.at[j], self.recv.at[j], dp=self.at(to))

    def give(self, j):
        self.copy(j, *EDGES[j]).start()

    def take(self, j):
        rel, side, to = EDGES[j]
        self.copy(j, rel ^ to, side, 0).wait_recv()

    def start(self):
        for j in range(3):
            self.give(j)

    def relay(self, moves):
        for first, *rest in moves:
            self.take(first)
            for j in rest:
                self.give(j)

    def cross(self):
        self.relay(CROSS)

    def diagonal(self):
        self.relay(DIAGONAL)

    def finish(self):
        for j in (2, 5, 6, 7, 8):
            self.take(j)
        for j, (rel, side, _) in enumerate(EDGES):
            self.copy(j, rel, side, 0).wait_send()


def backward_kernel(n, rows, chunks, jobs, heads, d_ctx, resid, q, k_all, v, ctx, top, inv, cos, sin, wq, back, emb, *refs):
    prods = refs[:jobs]
    whole = refs[jobs:N2 * jobs - N1]
    out, grads, d_w, d_bias, landed, cross, last, part, left, right, total, dctx, dq, dk, dv, ctx_in, res_in, cos_in, sin_in, emb_in, q_in, work, fresh, xin, yin, keep, pass_on, along, final, *sems = refs[N2 * jobs - N1:]
    send_r, send_l, recv_l, recv_r, osend, orecv, csend, crecv, esem, fsem, xsend, xrecv, xsem, ysend, yrecv, ysem, ksem, zrecv, frecv, asend, arecv, aself, isem, gsend, grecv = sems
    z = lax.axis_index('tp')
    p, at = plane()
    entry_barrier(z, n, at)
    blocks = 8
    per = chunks // blocks
    qb = rows * per
    share = qb // n
    block = out.shape[N2]
    lead = jnp.maximum(z, n - N1 - z)
    span = N2 * n
    units = jobs * span
    size = work.shape[N2]

    def rows_of(i, to, count):
        return pl.ds(pl.multiple_of(i * qb + to * count, count), count)

    def exchange(i, d):
        to = (z + d) % n
        dst = dctx.at[rows_of(i, z, share)]
        if d == N0:
            return pltpu.make_async_copy(d_ctx.at[z, i], dst, aself.at[i])
        return rcopy(d_ctx.at[to, i], dst, asend, arecv.at[i], tp=to)

    @pl.loop(N0, blocks)
    def _(b):
        for d in range(n):
            exchange(blocks - N1 - b, d).start()

    def piece(m, u, rel):
        return prods[m].at[(u % span) // N2, at(rel), pl.ds(pl.multiple_of((u % N2) * size, size), size)]

    for m in range(jobs):
        @pl.loop(m * span, (m + N1) * span)
        def _(u, m=m):
            for i in range(4):
                rcopy(piece(m, u, N2 * i + N1), landed.at[u, i], csend, crecv.at[u], dp=at(N1)).start()

    def inputs(i):
        slot = i % N2
        at_q = rows_of(i, N0, qb)
        pairs = ((ctx.at[at_q], ctx_in), (resid.at[i], res_in), (cos.at[at_q], cos_in), (sin.at[at_q], sin_in), (emb.at[at_q], emb_in), (q.at[at_q], q_in))
        return [pltpu.make_async_copy(src, dst.at[slot], isem.at[j, slot]) for j, (src, dst) in enumerate(pairs)]

    dk[:] = jnp.zeros_like(dk)
    dv[:] = jnp.zeros_like(dv)
    d_w[:] = jnp.zeros_like(d_w)
    d_bias[:] = jnp.zeros_like(d_bias)
    for copy in inputs(blocks - N1):
        copy.start()

    def attention_step(b, h):
        i = blocks - N1 - b

        @pl.when(h == N0)
        def _():
            for copy in inputs(i):
                copy.wait()

            @pl.when(b + N1 < blocks)
            def _():
                for copy in inputs(i - N1):
                    copy.start()
            exchange(i, N0).wait()
            others = dctx.at[pl.ds(N0, (n - N1) * share)]
            rcopy(others, others, asend, arecv.at[i], tp=z).wait_recv()
        attend_grad(i, h, heads, qb, q_in.at[i % N2], k_all, v, ctx_in.at[i % N2], dctx, top, inv, dq, dk, dv)

        @pl.when(h == heads - N1)
        def _():
            slot = i % N2
            got = grad_rows(i, qb, cos_in[slot], sin_in[slot], dq, dk, dv, d_bias)
            d_w[:] += dot(emb_in[slot], dot(got, back[:], NN).astype(BF), TN)
            part[rows_of(i, N0, qb), :] = dot(got, wq[:], NT)
            part[rows_of(i, z, share), :] = part[rows_of(i, z, share), :] + res_in[i % N2]

    def sides(u):
        side = u % N2
        return side, at(N2) * (N1 - side) + at(4) * side, at(4) * (N1 - side) + at(N2) * side

    def fetch(u):
        slot = u % HOLD

        @pl.when(u >= HOLD)
        def _():
            rcopy(xin, cross.at[N0], xsend.at[slot], xrecv.at[N0], dp=p).wait_send()
        for m in range(jobs):
            @pl.when(u // span == m)
            def _(m=m):
                for i in range(4):
                    pltpu.make_async_copy(piece(m, u, N2 * i), work.at[slot, i], esem.at[slot]).start()
        rcopy(landed.at[u], landed.at[u], csend, crecv.at[u], dp=p).wait_recv()
        pltpu.make_async_copy(landed.at[u], fresh, fsem).start()

    def add(u):
        slot = u % HOLD
        pltpu.make_async_copy(landed.at[u], work.at[slot], esem.at[slot]).wait()
        pltpu.make_async_copy(landed.at[u], fresh, fsem).wait()
        for i in range(4):
            work[slot, i] = work[slot, i] + fresh[i]

    def add_send(u):
        slot = u % HOLD
        side, first, second = sides(u)
        rcopy(work.at[slot, N1 + side], cross.at[u, N0], xsend.at[slot], xrecv.at[u], dp=first).start()
        rcopy(work.at[slot, 3], cross.at[u, N1], xsend.at[slot], xrecv.at[u], dp=first).start()

    def load_cross(u):
        rcopy(cross.at[u], cross.at[u], xsend.at[N0], xrecv.at[u], dp=p).wait_recv()
        pltpu.make_async_copy(cross.at[u], xin, xsem).start()

    def crossed(u):
        slot = u % HOLD
        pltpu.make_async_copy(cross.at[u], xin, xsem).wait()

        @pl.when(u >= LIVE)
        def _():
            pltpu.make_async_copy(keep.at[u % LIVE], keep.at[u % LIVE], ksem.at[u % LIVE]).wait()

        @pl.when(u >= PAIR)
        def _():
            rcopy(pass_on.at[u % PAIR], last.at[u], ysend.at[u % PAIR], yrecv.at[u], dp=p).wait_send()
        keep[u % LIVE] = xin[N0] + work[slot, N0]
        pass_on[u % PAIR] = xin[N1] + work[slot, N2 - u % N2]

    def crossed_send(u):
        side, first, second = sides(u)
        rcopy(pass_on.at[u % PAIR], last.at[u], ysend.at[u % PAIR], yrecv.at[u], dp=second).start()

    def load_last(u):
        rcopy(last.at[u], last.at[u], ysend.at[N0], yrecv.at[u], dp=p).wait_recv()
        pltpu.make_async_copy(last.at[u], yin, ysem).start()

    def in_plane(u):
        pltpu.make_async_copy(last.at[u], yin, ysem).wait()
        keep[u % LIVE] = keep[u % LIVE] + yin[:]

    def unit(k):
        u = (k // BEAT) * (BEAT - N1) + k % BEAT
        return u, (k >= N0) & (k % BEAT < BEAT - N1) & (u < units)

    def along_tp(k, t, send):
        toward = jnp.where(z < t, z, n - N1 - z)
        late = HOP * jnp.where(z == t, max(t, n - N1 - t), toward)
        u, ok = unit(k - PLANE - N1 - late)
        mine = (u // span) * N2 + u % N2
        slot = u % LIVE
        ok = ok & ((u // N2) % n == t)

        def add_from(ref, sem):
            rcopy(ref, ref, csend, sem, tp=z).wait_recv()
            keep[slot] = keep[slot] + ref[:]
        if send:
            @pl.when(ok & (z < t))
            def _():
                rcopy(keep.at[slot], along.at[u], ksem.at[slot], zrecv.at[u], tp=z + N1).start()

            @pl.when(ok & (z > t + N1))
            def _():
                rcopy(keep.at[slot], along.at[u], ksem.at[slot], zrecv.at[u], tp=z - N1).start()

            @pl.when(ok & (z == t + N1))
            def _():
                rcopy(keep.at[slot], final.at[mine], ksem.at[slot], frecv.at[mine], tp=z - N1).start()

            for m in range(jobs):
                @pl.when(ok & (z == t) & (u // span == m))
                def _(m=m):
                    dst = whole[m].at[p, u % N2] if m < jobs - N1 else grads.at[u % N2]
                    pltpu.make_async_copy(keep.at[slot], dst, ksem.at[slot]).start()
        else:
            @pl.when(ok & (((z > N0) & (z <= t)) | ((z > t) & (z < n - N1))))
            def _():
                add_from(along.at[u], zrecv.at[u])
            if t < n - N1:
                @pl.when(ok & (z == t))
                def _():
                    add_from(final.at[mine], frecv.at[mine])

    spread = [Spread(at, functools.partial(block_of, whole[m], at), gsend.at[m], grecv.at[m]) for m in range(jobs - N1)]

    def settle(u):
        pltpu.make_async_copy(keep.at[u % LIVE], keep.at[u % LIVE], ksem.at[u % LIVE]).wait()

    def begin(m):
        for u in range(max(m * span, units - LIVE), (m + N1) * span):
            settle(u)
        spread[m].start()

    def place(c):
        return (blocks - N1 - c // per) * per + c % per

    def chunk(c):
        return total.at[c % RING]

    def done(c, value):
        @pl.when(c >= RING)
        def _():
            pltpu.make_async_copy(chunk(c), chunk(c), osend.at[c % RING]).wait()
        total[c % RING] = value

    def hand_out(c):
        where = out.at[p, pl.ds(pl.multiple_of(place(c) * rows, rows), rows)]
        for rel in range(8):
            src = total.at[c % RING, :, pl.ds(pl.multiple_of(at(rel) * block, block), block)]
            if rel == N0:
                pltpu.make_async_copy(src, where, osend.at[c % RING]).start()
            else:
                rcopy(src, where, osend.at[c % RING], orecv.at[rel], dp=at(rel)).start()

    def staged(k, offset, stage):
        u, ok = unit(k - offset)
        pl.when(ok)(functools.partial(stage, u))
    steps = max(heads + chunks + LAG * (n - N1) + N1, units // (BEAT - N1) * BEAT + PLANE + HOP * (n - N1), GATHER[-N1] + 7)

    @pl.loop(N0, steps)
    def _(k):
        c = k - heads - LAG * lead - N1

        @pl.when((c >= N0) & (c < chunks))
        def _():
            hand_out(c)
        chain_sum(k - heads, z, n, rows, chunks, part, left, right, done, send_r, send_l, recv_l, recv_r, place)
        for offset, stage in ((CROSSED, crossed), (ADD, add), (PLANE, in_plane)):
            staged(k, offset, stage)
        for t in range(n):
            along_tp(k, t, False)
        for offset, stage in ((N0, fetch), (LOAD, load_cross), (LAND, load_last)):
            staged(k, offset, stage)

        @pl.when(k < blocks * heads)
        def _():
            attention_step(k // heads, k % heads)
        for offset, stage in ((ADD, add_send), (CROSSED, crossed_send)):
            staged(k, offset, stage)
        for t in range(n):
            along_tp(k, t, True)
        for m, gather in enumerate(spread):
            for offset, stage in ((N0, functools.partial(begin, m)), (3, gather.cross), (6, gather.diagonal)):
                pl.when(k == GATHER[m] + offset)(stage)

    chain_drain(z, n, part, left, right, send_r, send_l, recv_l, recv_r)
    for c in range(max(N0, chunks - RING), chunks):
        pltpu.make_async_copy(chunk(c), chunk(c), osend.at[c % RING]).wait()
    for rel in range(N1, 8):
        rcopy(out.at[at(rel)], out.at[at(rel)], csend, orecv.at[rel], dp=p).wait_recv()
    for slot in range(HOLD):
        rcopy(xin, cross.at[N0], xsend.at[slot], xrecv.at[N0], dp=p).wait_send()
    for slot in range(PAIR):
        rcopy(pass_on.at[slot], last.at[N0], ysend.at[slot], yrecv.at[N0], dp=p).wait_send()
    for u in range(max((jobs - N1) * span, units - LIVE), units):
        settle(u)
    rcopy(landed, landed, csend, crecv.at[N0], dp=p).wait_send()
    for gather in spread:
        gather.finish()
    sent = dctx.at[pl.ds(N0, (n - N1) * share * blocks)]
    rcopy(sent, sent, asend, arecv.at[N0], tp=z).wait_send()


def backward(d_ctx, resid, saved, cos, sin, wq, back, emb, prods, heads, n_tp, n_dp):
    q, k, v, ctx, top, inv = saved
    seq, dims = q.shape
    width = wq.shape[0]
    chunks = 32
    rows = seq // chunks
    jobs = len(prods)
    piece = (prods[0].shape[2] // 2, prods[0].shape[3])
    units = jobs * 2 * n_tp
    dma = pltpu.SemaphoreType.DMA
    shape = jax.ShapeDtypeStruct
    qb = seq // 8
    vmem = [(seq, width)] * 3 + [(RING, rows, width), (seq, dims), (qb, dims), (seq, dims), (seq, dims), (2, qb, dims), (2, qb // n_tp, width)] + [(2, qb, dims // 2)] * 2 + [
            (HOLD, 4) + piece, (4,) + piece, (2,) + piece, piece, (LIVE,) + piece, (PAIR,) + piece, (units,) + piece, (2 * jobs,) + piece]
    sems = [(), (), (chunks,), (chunks,), (RING,), (8,), (), (units,), (HOLD,), (), (HOLD,), (units,), (), (PAIR,), (units,), (), (LIVE,), (units,), (2 * jobs,), (), (8,), (8,), (6, 2), (jobs - 1, len(EDGES)), (jobs - 1, len(EDGES))]
    scratch = [pltpu.VMEM(size, F32) for size in vmem]
    scratch[12:12] = [pltpu.VMEM((2, qb, width), BF), pltpu.VMEM((2, qb, dims), BF)]
    full = shape((n_dp, 2) + piece, F32)
    *whole, cols, grads, d_w, d_bias, _, _, _ = pl.pallas_call(
        functools.partial(backward_kernel, n_tp, rows, chunks, jobs, heads),
        name='backward',
        out_shape=[full] * (jobs - 1) + [shape((n_dp, seq, width // n_dp), F32), shape((2,) + piece, F32), shape((width, 3 * dims), F32), shape((1, 3 * dims), F32),
                   shape((units, 4) + piece, F32), shape((units, 2) + piece, F32), shape((units,) + piece, F32)],
        in_specs=[ANY] * 3 + [VMEM] * 2 + [ANY] + [VMEM] * 2 + [ANY] * 2 + [VMEM] * 2 + [ANY] * (1 + jobs),
        out_specs=[ANY] * (jobs - 1) + [ANY, ANY, VMEM, VMEM, ANY, ANY, ANY],
        scratch_shapes=scratch + [dma(size) for size in sems],
        compiler_params=pltpu.CompilerParams(collective_id=1, has_side_effects=True, vmem_limit_bytes=67_000_000),
        cost_estimate=pl.CostEstimate(flops=20 * 10 ** 9, bytes_accessed=100 * 2 ** 20, transcendentals=0),
    )(d_ctx, resid, q, k, v, ctx, top, inv, cos, sin, wq, back, emb, *prods)
    return d_w, d_bias, cols, whole, grads


WAYS = 4


def table_kernel(ids, rows_ref, out, *tables):
    step = pl.program_id(0)
    count = rows_ref.shape[0]
    part = count // WAYS

    @pl.when(step == 0)
    def _():
        for table in tables:
            table[:] = jnp.zeros_like(table)

    @pl.loop(0, part, unroll=4)
    def _(r):
        for way, table in enumerate(tables):
            row = way * part + r
            where = pl.ds(ids[step * count + row], 1)
            table[where, :] = table[where, :] + rows_ref[pl.ds(row, 1), :]

    @pl.when(step == pl.num_programs(0) - 1)
    def _():
        total = tables[0][:]
        for table in tables[1:]:
            total = total + table[:]
        out[:] = SHRINK * total[:out.shape[0]]


def table_rows(ids, rows, vocab_loc):
    count, block = rows.shape
    step = min(1024, count // 2)
    return pl.pallas_call(
        table_kernel,
        name='table_rows',
        grid_spec=pltpu.PrefetchScalarGridSpec(
            num_scalar_prefetch=1,
            grid=(count // step,),
            in_specs=[pl.BlockSpec((step, block), lambda i, ids: (i, 0))],
            out_specs=pl.BlockSpec((vocab_loc, block), lambda i, ids: (0, 0)),
            scratch_shapes=[pltpu.VMEM((vocab_loc + 8, block), F32)] * WAYS,
        ),
        out_shape=jax.ShapeDtypeStruct((vocab_loc, block), F32),
        compiler_params=pltpu.CompilerParams(dimension_semantics=('arbitrary',), vmem_limit_bytes=48 * 2 ** 20),
        cost_estimate=pl.CostEstimate(flops=3 * 10 ** 9, bytes_accessed=16 * 2 ** 20, transcendentals=0),
    )(ids, rows)


def finish_kernel(n, cuts, col, down, proj, d_w, small, table, down_all, proj_all, qkv_all, total, landed, work, cross, last, mine, inbox, sem, send, recv, dsend, drecv, osem, csem, xsend, xrecv, ysend, yrecv, rsend, rrecv):
    z = lax.axis_index('tp')
    p, at = plane()
    entry_barrier(z, n, at)
    block = col.shape[N1]
    half = len(cuts) // N2

    def part(i):
        def region(rel, side):
            return table.at[pl.ds(cuts[i][N0], cuts[i][N1] - cuts[i][N0]), pl.ds(pl.multiple_of(at(rel) * block, block), block)]
        return Spread(at, region, send.at[i], recv.at[i], col.at[pl.ds(cuts[i][N0], cuts[i][N1] - cuts[i][N0])])
    parts = [part(i) for i in range(len(cuts))]
    spread = [Spread(at, functools.partial(block_of, ref, at), dsend.at[i], drecv.at[i], own) for i, (ref, own) in enumerate(((down_all, down), (proj_all, proj), (qkv_all, mine)))]
    own_copies = [pltpu.make_async_copy(col, table.at[:, pl.ds(pl.multiple_of(p * block, block), block)], osem.at[N0])]
    own_copies += [pltpu.make_async_copy(src, dst.at[p], osem.at[i]) for i, (src, dst) in enumerate(((down, down_all), (proj, proj_all), (mine, qkv_all)), N1)]
    order = list(range(len(cuts)))
    flipped = order[half:] + order[:half]
    peers = [{'dp': at(N1)}, {'dp': at(N2)}, {'dp': at(4)}, {'tp': z + N1 - N2 * (z % N2)}, {'tp': (z + n // N2) % n}]

    def next_part(i):
        parts[order[i]].give(N0)
        parts[flipped[i]].give(N1)
        parts[order[i]].give(N2)

    def relay_part(i):
        one, two = order[i], flipped[i]
        parts[one].take(N0)
        if one < half:
            parts[one].give(3)
        parts[one].give(5)
        parts[two].take(N1)
        if two >= half:
            parts[two].give(4)
        parts[two].give(6)

    def exchange(r):
        return rcopy(total, inbox.at[r], rsend.at[r], rrecv.at[r], **peers[r])

    def round_end(r):
        exchange(r).wait()
        total[:] = total[:] + inbox[r]

    total[:] = small[:]
    for i in range(4):
        rcopy(d_w.at[at(N2 * i + N1)], landed.at[i], csem.at[N0], csem.at[N1], dp=at(N1)).start()
    for copy in own_copies[:3]:
        copy.start()
    next_part(N0)
    exchange(N0).start()
    spread[N0].start()
    spread[N1].start()
    next_part(N1)
    rcopy(landed, landed, csem.at[N0], csem.at[N1], dp=p).wait()
    for i in range(4):
        work[i] = d_w[at(N2 * i)] + landed[i]
    round_end(N0)
    for side, first in ((N0, N2), (N1, 4)):
        rcopy(work.at[N1 + side, side], cross.at[side, N0], xsend.at[side], xrecv.at[side], dp=at(first)).start()
        rcopy(work.at[3, side], cross.at[side, N1], xsend.at[side], xrecv.at[side], dp=at(first)).start()
    exchange(N1).start()
    next_part(N2)
    relay_part(N0)
    round_end(N1)
    for side, first in ((N0, N2), (N1, 4)):
        rcopy(cross.at[side], cross.at[side], xsend.at[side], xrecv.at[side], dp=p).wait()
        cross[side, N0] = cross[side, N0] + work[N0, side]
        cross[side, N1] = cross[side, N1] + work[N2 - side, side]
    exchange(N2).start()
    for side, second in ((N0, 4), (N1, N2)):
        rcopy(cross.at[side, N1], last.at[side], ysend.at[side], yrecv.at[side], dp=at(second)).start()
    next_part(3)
    spread[N0].cross()
    spread[N1].cross()
    relay_part(N1)
    round_end(N2)
    for side in range(N2):
        rcopy(last.at[side], last.at[side], ysend.at[side], yrecv.at[side], dp=p).wait()
        mine[side] = cross[side, N0] + last[side]
    exchange(3).start()
    next_part(4)
    spread[N2].start()
    own_copies[3].start()
    spread[N0].diagonal()
    spread[N1].diagonal()
    relay_part(N2)
    round_end(3)
    next_part(5)
    exchange(4).start()
    relay_part(3)
    spread[N2].cross()
    next_part(6)
    round_end(4)
    relay_part(4)
    next_part(7)
    spread[N2].diagonal()
    for i in range(5, len(cuts)):
        relay_part(i)
    for i in range(half):
        for via, where in ((3, i), (4, i + half)):
            parts[where].take(via)
            parts[where].give(7)
    for i in order:
        for j in (N2, 5, 6, 7):
            parts[i].take(j)
        for j in (N0, N1, N2, 3 if i < half else 4, 5, 6, 7):
            parts[i].copy(j, *EDGES[j]).wait_send()
    for gather in spread:
        gather.finish()
    for copy in own_copies:
        copy.wait()


def finish(col, down, proj, d_w, small, n_tp, n_dp):
    size, block = col.shape
    tiles = size // 8
    cuts = [(8 * (tiles * i // 8), 8 * (tiles * (i + N1) // 8)) for i in range(8)]
    dma = pltpu.SemaphoreType.DMA
    shape = jax.ShapeDtypeStruct
    third = d_w.shape[N1:]
    kinds = len(EDGES)
    table, down_all, proj_all, qkv_all, total = pl.pallas_call(
        functools.partial(finish_kernel, n_tp, cuts),
        name='finish',
        out_shape=[shape((size, n_dp * block), F32)] + [shape((n_dp,) + src, F32) for src in (down.shape, proj.shape, third)] + [shape(small.shape, F32)],
        in_specs=[ANY] * 3 + [VMEM] * N2,
        out_specs=[ANY] * 4 + [VMEM],
        scratch_shapes=[pltpu.VMEM(lead + third[N1:], F32) for lead in ((4, N2), (4, N2), (N2, N2), (N2,), (N2,))] + [pltpu.VMEM((5,) + small.shape, F32), dma,
                        dma((8, kinds)), dma((8, kinds)), dma((3, kinds)), dma((3, kinds)), dma((4,))] + [dma((N2,))] * 5 + [dma((5,))] * N2,
        compiler_params=pltpu.CompilerParams(collective_id=N2, has_side_effects=True, vmem_limit_bytes=32 * N2 ** 20),
        cost_estimate=pl.CostEstimate(flops=10 * 10 ** 9, bytes_accessed=60 * N2 ** 20, transcendentals=N0),
    )(col, down, proj, d_w, small)
    return table, down_all.reshape(-N1, down.shape[N2]), proj_all.reshape(-N1, proj.shape[N2]), qkv_all.reshape(-N1, third[N2]), total


def dot(a, b, dims):
    return lax.dot_general(a, b, (dims, ((), ())), preferred_element_type=F32)


NT, TN, NN = ((1,), (1,)), ((0,), (0,)), ((1,), (0,))


def lane_head(shape, heads, halves):
    lane = lax.broadcasted_iota(jnp.int32, shape, 1)
    dims = shape[1] // halves
    return (lane % dims) // (dims // heads)


def turned(both, cos, sin):
    half = both.shape[1] // 2
    x1, x2 = both[:, :half], both[:, half:]
    return jnp.concatenate([x1 * cos - x2 * sin, x2 * cos + x1 * sin], axis=1)


def project(i, qb, emb, wq, bq, cos, sin, q, k, v):
    at_q = pl.ds(pl.multiple_of(i * qb, qb), qb)
    dims = q.shape[1]
    qkv = (dot(emb[at_q, :], wq[:], NN) + bq[:]).astype(BF)
    for ref, part in ((q, 0), (k, 1)):
        ref[at_q, :] = turned(qkv[:, part * dims:(part + 1) * dims].astype(F32), cos[at_q, :], sin[at_q, :]).astype(BF)
    v[at_q, :] = qkv[:, 2 * dims:]


def scores(i, j, kb, qb, scale, keys, q):
    s = dot(keys, q, NT) * scale
    key = j * kb + lax.broadcasted_iota(jnp.int32, (kb, qb), 0)
    query = i * qb + lax.broadcasted_iota(jnp.int32, (kb, qb), 1)
    return jnp.where(query >= key, s, -1e30)


def attend(i, h, heads, qb, q_ref, k_ref, v_ref, ctx_ref, top_ref, inv_ref, s_ref):
    kb = 2 * qb
    dims = q_ref.shape[1]
    scale = (dims // heads) ** -0.5
    at_q = pl.ds(pl.multiple_of(i * qb, qb), qb)
    q = jnp.where(lane_head((qb, dims), heads, 2) == h, q_ref[at_q, :].astype(F32), 0.0).astype(BF)
    count = (i + 2) // 2

    def at_key(j):
        return pl.ds(pl.multiple_of(j * kb, kb), kb)

    def first(j, top):
        s = scores(i, j, kb, qb, scale, k_ref[at_key(j), :], q)
        s_ref[at_key(j), :] = s
        return jnp.maximum(top, jnp.max(s, axis=0, keepdims=True))
    top = lax.fori_loop(0, count, first, jnp.full((1, qb), -1e30, F32))

    def weigh(j, total):
        e = jnp.exp(s_ref[at_key(j), :] - top)
        s_ref[at_key(j), :] = e
        return total + jnp.sum(e, axis=0, keepdims=True)
    inv = 1.0 / lax.fori_loop(0, count, weigh, jnp.zeros((1, qb), F32))

    def mix(j, acc):
        return acc + dot((s_ref[at_key(j), :] * inv).astype(BF), v_ref[at_key(j), :], TN)
    mixed = lax.fori_loop(0, count, mix, jnp.zeros((qb, dims), F32))
    ctx_ref[at_q, :] = jnp.where(lane_head((qb, dims), heads, 1) == h, mixed, ctx_ref[at_q, :])
    top_ref[pl.ds(h, 1), at_q] = top
    inv_ref[pl.ds(h, 1), at_q] = inv


def attend_grad(i, h, heads, qb, q_ref, k_ref, v_ref, ctx_ref, dctx_ref, top_ref, inv_ref, dq_ref, dk_ref, dv_ref):
    kb = 2 * qb
    dims = dk_ref.shape[1]
    scale = (dims // heads) ** -0.5
    at_q = pl.ds(pl.multiple_of(i * qb, qb), qb)
    q = jnp.where(lane_head((qb, dims), heads, 2) == h, q_ref[:].astype(F32), 0.0).astype(BF)
    dc = jnp.where(lane_head((qb, dims), heads, 1) == h, dctx_ref[at_q, :], 0.0).astype(BF)
    ones = jnp.ones((8, dims), F32)
    mean = lax.dot_general(ones, dc.astype(F32) * ctx_ref[:], (NT, ((), ())), precision=lax.Precision.HIGHEST, preferred_element_type=F32)[:1]
    top, inv = top_ref[pl.ds(h, 1), at_q], inv_ref[pl.ds(h, 1), at_q]

    def step(j, dq):
        at_k = pl.ds(pl.multiple_of(j * kb, kb), kb)
        keys = k_ref[at_k, :]
        probs = (jnp.exp(scores(i, j, kb, qb, scale, keys, q) - top) * inv).astype(BF)
        ds = (probs.astype(F32) * (dot(v_ref[at_k, :], dc, NT) - mean) * scale).astype(BF)
        dv_ref[at_k, :] += dot(probs, dc, NN)
        dk_ref[at_k, :] += dot(ds, q, NN)
        return dq + dot(ds, keys, TN)
    dq = lax.fori_loop(0, (i + 2) // 2, step, jnp.zeros((qb, dims), F32))
    dq_ref[:] = jnp.where(lane_head((qb, dims), heads, 2) == h, dq, dq_ref[:])


def grad_rows(i, qb, cos, sin, dq, dk, dv, d_bias):
    at_q = pl.ds(pl.multiple_of(i * qb, qb), qb)
    back = [turned(values, cos, -sin) for values in (dq[:], dk[at_q, :])]
    rows = jnp.concatenate(back + [dv[at_q, :]], axis=1)
    d_bias[:] += jnp.sum(rows, axis=0, keepdims=True)
    return rows.astype(BF)


def standard(values):
    mean = jnp.mean(values, axis=1, keepdims=True)
    centered = values - mean
    scale = lax.rsqrt(jnp.mean(centered * centered, axis=1, keepdims=True) + EPS)
    return centered * scale, scale


def standard_grad(d_out, unit, scale):
    return scale * (d_out - jnp.mean(d_out, axis=1, keepdims=True) - unit * jnp.mean(d_out * unit, axis=1, keepdims=True))


def over_rows(values):
    return jnp.sum(values, axis=0, keepdims=True)


def layer_kernel(n, ctx, wo, emb, cot, vectors, gate_bias, lin_bias, wg, wl, wd, hidden, d_ffn, d_attn, resid, d_ctx, sums, inner, d_gate, d_lin, gate, lin, acc, unit1, scale1):
    i = pl.program_id(N0)
    t = i % n
    tile = 256 if acc.shape[N1] % 256 == N0 else acc.shape[N1]
    tiles = range(N0, acc.shape[N1], tile)
    b_out, gain1, bias1, b_down, gain2 = [vectors[pl.ds(j, N1), :] for j in range(5)]

    @pl.when(i == N0)
    def _():
        total = ALPHA * emb[:].astype(F32) + b_out
        for h in range(n):
            total = total + dot(ctx[h].astype(BF), wo[h], NN)
        unit, scale1[:] = standard(total)
        unit1[:] = unit
        hidden[:] = (unit * gain1 + bias1).astype(BF)
        acc[:] = jnp.zeros_like(acc)

    @pl.when(i < n)
    def _():
        for lo in tiles:
            cols = pl.ds(lo, tile)
            g = dot(hidden[:], wg[N0, :, cols], NN) + gate_bias[pl.ds(t, N1), cols]
            l = dot(hidden[:], wl[N0, :, cols], NN) + lin_bias[pl.ds(t, N1), cols]
            gate[t, :, cols] = g
            lin[t, :, cols] = l
            inner[N0, :, cols] = (0.5 * g * (1.0 + lax.erf(g * 0.5 ** 0.5)) * l).astype(BF)
        for lo in tiles:
            cols = pl.ds(lo, tile)
            acc[:, cols] += dot(inner[N0], wd[N0, :, cols], NN)

    @pl.when(i == n - N1)
    def _():
        unit, scale = standard(ALPHA * hidden[:].astype(F32) + acc[:] + b_down)
        g = cot[:].astype(F32)
        d_y = standard_grad(g * gain2, unit, scale)
        sums[pl.ds(N2 * n + 3, N1), :] = over_rows(d_y)
        sums[pl.ds(N2 * n + 4, N1), :] = over_rows(g * unit)
        d_ffn[:] = d_y.astype(BF)
        acc[:] = ALPHA * d_y

    @pl.when(i >= n)
    def _():
        for lo in tiles:
            cols = pl.ds(lo, tile)
            d_inner = dot(d_ffn[:], wd[N0, cols, :], NT).astype(BF).astype(F32)
            g, l = gate[t, :, cols], lin[t, :, cols]
            cdf = 0.5 * (1.0 + lax.erf(g * 0.5 ** 0.5))
            slope = cdf + g * (jnp.exp(-0.5 * g * g) * (N2 * np.pi) ** -0.5)
            d_l = d_inner * (g * cdf)
            d_g = d_inner * l * slope
            sums[pl.ds(t, N1), cols] = over_rows(d_g)
            sums[pl.ds(n + t, N1), cols] = over_rows(d_l)
            d_gate[N0, :, cols] = d_g.astype(BF)
            d_lin[N0, :, cols] = d_l.astype(BF)
        for lo in tiles:
            cols = pl.ds(lo, tile)
            acc[:, cols] += dot(d_gate[N0], wg[N0, cols, :], NT) + dot(d_lin[N0], wl[N0, cols, :], NT)

    @pl.when(i == N2 * n - N1)
    def _():
        d_h, unit = acc[:], unit1[:]
        d_x = standard_grad(d_h * gain1, unit, scale1[:])
        sums[pl.ds(N2 * n, N1), :] = over_rows(d_x)
        sums[pl.ds(N2 * n + N1, N1), :] = over_rows(d_h * unit)
        sums[pl.ds(N2 * n + N2, N1), :] = over_rows(d_h)
        resid[:] = ALPHA * d_x
        d_attn[:] = d_x.astype(BF)
        for h in range(n):
            d_ctx[h] = dot(d_attn[:], wo[h], NT)


def layer(ctx, wo, emb, cot, vectors, gate_bias, lin_bias, wg, wl, wd):
    n, own, dims = ctx.shape
    width = emb.shape[N1]
    ffn = wg.shape[N2]
    once = pl.BlockSpec(memory_space=pltpu.VMEM)
    weight = [pl.BlockSpec((N1,) + w.shape[N1:], lambda i: (i % n, N0, N0)) for w in (wg, wl, wd)]
    early = pl.BlockSpec((N1, own, ffn), lambda i: (jnp.minimum(i, n - N1), N0, N0))
    late = pl.BlockSpec((N1, own, ffn), lambda i: (jnp.maximum(i - n, N0), N0, N0))
    shape = jax.ShapeDtypeStruct
    slots = shape((n, own, ffn), BF)
    return pl.pallas_call(
        functools.partial(layer_kernel, n),
        name='layer',
        grid=(N2 * n,),
        in_specs=[once] * 7 + weight,
        out_specs=[once] * 6 + [early, late, late],
        out_shape=[shape((own, width), BF)] * 3 + [shape((own, width), F32), shape((n, own, dims), F32), shape((N2 * n + 8, width), F32), slots, slots, slots],
        scratch_shapes=[pltpu.VMEM((n, own, ffn), F32)] * N2 + [pltpu.VMEM((own, width), F32)] * N2 + [pltpu.VMEM((own, N1), F32)],
        compiler_params=pltpu.CompilerParams(dimension_semantics=('arbitrary',), vmem_limit_bytes=62 * N2 ** 20),
        cost_estimate=pl.CostEstimate(flops=15 * 10 ** 9, bytes_accessed=70 * N2 ** 20, transcendentals=N0),
    )(ctx, wo, emb, cot, vectors, gate_bias, lin_bias, wg, wl, wd)


def solution(mesh):
    n_tp, n_dp = mesh.shape['tp'], mesh.shape['dp']
    in_specs = (P('dp', None), P('dp', None, None), P('tp', None)) + WEIGHT_SPECS
    out_specs = (P('tp', None),) + WEIGHT_SPECS

    def device_step(tokens, cotangent, emb_table, *weights):
        (w_qkv, b_qkv, w_out, b_out, ln1_gain, ln1_bias, w_gate, b_gate, w_lin, b_lin, w_down, b_down, ln2_gain) = weights
        tp, dp = lax.axis_index('tp'), lax.axis_index('dp')
        tokens = tokens[N0]
        seq_len, width = tokens.shape[N0], emb_table.shape[N1]
        heads, head_dim = b_qkv.shape[N0], b_qkv.shape[N1] // 3
        own = seq_len // n_tp
        ffn = w_gate.shape[N1]
        rk, rf, ro = width // n_dp, ffn // n_dp, w_out.shape[N0] // n_dp

        def cut(weight):
            rows = weight.shape[N0] // n_dp
            return lax.dynamic_slice_in_dim(weight, dp * rows, rows, N0)
        bias_rows = jnp.concatenate([b_gate[None], b_lin[None], jnp.zeros((14, ffn), BF)], axis=N0)
        piece = jnp.concatenate([cut(w_gate), cut(w_lin), cut(w_down), cut(w_out), bias_rows], axis=N0).astype(F32)

        vocab_loc = emb_table.shape[N0]
        local_ids = tokens - tp * vocab_loc
        in_shard = (local_ids >= N0) & (local_ids < vocab_loc)
        safe_ids = jnp.where(in_shard, local_ids, N0)
        found = jnp.take(emb_table, safe_ids, axis=N0)
        dims = heads * head_dim
        place = column_order(heads, head_dim)
        swap = (jnp.arange(3 * dims)[:, None] == jnp.asarray(place)[None, :]).astype(BF)
        wq = jnp.dot(w_qkv, swap, preferred_element_type=F32).astype(BF)
        bq = jnp.dot(b_qkv.reshape(N1, -N1), swap, preferred_element_type=F32)
        cos_tab, sin_tab = rope_tables(seq_len, head_dim, heads)
        emb_bf, (wg_full, wl_full, wd_full, wo_full), biases, tok_all, ctx_own, saved = embed(found, in_shard[:, None].astype(F32), piece, tokens.reshape(-N1, min(128, seq_len // 8)), (w_gate, w_lin, w_down, w_out), wq, bq, cos_tab, sin_tab, heads, n_tp, n_dp)
        is_own = (jnp.arange(n_tp) == tp)[:, None]
        bg_full, bl_full = [jnp.where(is_own, b[None].astype(F32), biases[:, i]) for i, b in enumerate((b_gate, b_lin))]

        blocks = 8

        def owned(values):
            return lax.dynamic_index_in_dim(values.reshape(blocks, n_tp, -N1, width), tp, N1, keepdims=False).reshape(own, width)
        emb_own, cot_own = owned(emb_bf), owned(cotangent[N0])
        vectors = jnp.stack([b_out, ln1_gain, ln1_bias, b_down, ln2_gain] + [b_out] * 3).astype(F32)
        hidden, d_ffn_bf, d_attn_bf, resid, d_ctx, row_sums, inner_act, d_gate_bf, d_lin_bf = layer(
            ctx_own.reshape(n_tp, own, dims), wo_full, emb_own, cot_own, vectors, bg_full, bl_full, wg_full, wl_full, wd_full)

        def product(lhs, rhs, spec):
            return jnp.einsum(spec, lhs, rhs, preferred_element_type=F32).reshape(n_tp, n_dp, -N1, width)

        prod_down = product(inner_act, d_ffn_bf, 'tsc,sd->tcd')
        prod_gate = product(hidden, d_gate_bf, 'sk,tsc->tkc')
        prod_lin = product(hidden, d_lin_bf, 'sk,tsc->tkc')
        d_w_out = jnp.einsum('hse,sd->hed', ctx_own.reshape(n_tp, own, dims).astype(BF), d_attn_bf, preferred_element_type=F32)
        d_w_out = lax.psum_scatter(d_w_out.reshape(-N1, width), ALL, scatter_dimension=N0, tiled=True)
        d_w_qkv, d_b_qkv, d_cols, (d_w_gate, d_w_lin), d_w_down = backward(
            d_ctx.reshape(n_tp, blocks, own // blocks, dims), resid.reshape(blocks, own // blocks, width), saved, cos_tab, sin_tab, wq, swap.T, emb_bf,
            (prod_gate, prod_lin, prod_down), heads, n_tp, n_dp)
        d_w_gate, d_w_lin = d_w_gate.reshape(-N1, ffn), d_w_lin.reshape(-N1, ffn)
        d_b_qkv = jnp.dot(d_b_qkv, swap.astype(F32).T, precision=lax.Precision.HIGHEST)
        all_ids = tok_all.reshape(-N1) - tp * vocab_loc
        all_ids = jnp.where((all_ids >= N0) & (all_ids < vocab_loc), all_ids, vocab_loc)
        col = table_rows(all_ids, d_cols.reshape(n_dp * seq_len, -N1), vocab_loc)

        slot = (jnp.arange(n_tp) == tp).astype(F32)[:, None]
        d_bq_rows = jnp.pad(slot * d_b_qkv, ((N0, N0), (N0, ffn - 3 * dims)))
        kept = N2 * n_tp
        small = jnp.concatenate([row_sums[:kept], d_bq_rows, row_sums[kept:kept + 5], jnp.zeros((7, width), F32)], axis=N0)
        d_table, d_w_down, d_w_out, d_w_qkv, small = finish(
            col, d_w_down, d_w_out.reshape(N2, -N1, width), d_w_qkv.reshape(n_dp, N2, -N1, 3 * dims), small, n_tp, n_dp)
        d_b_gate = lax.dynamic_index_in_dim(small[:n_tp], tp, N0, keepdims=False)
        d_b_lin = lax.dynamic_index_in_dim(small[n_tp:N2 * n_tp], tp, N0, keepdims=False)
        d_b_qkv = lax.dynamic_index_in_dim(small[N2 * n_tp:3 * n_tp], tp, N0, keepdims=False)[:3 * dims].reshape(heads, 3 * head_dim)
        d_b_out, d_ln1_gain, d_ln1_bias, d_b_down, d_ln2_gain = [small[3 * n_tp + i] for i in range(5)]
        return (d_table, d_w_qkv, d_b_qkv, d_w_out, d_b_out, d_ln1_gain, d_ln1_bias, d_w_gate, d_b_gate, d_w_lin, d_b_lin, d_w_down, d_b_down, d_ln2_gain)

    return jax.shard_map(device_step, mesh=mesh, in_specs=in_specs, out_specs=out_specs, check_vma=False)
```

```python
import functools

import jax
import jax.numpy as jnp
import numpy as np
from jax import lax
from jax.experimental import pallas as pl
from jax.experimental.pallas import tpu as pltpu
from jax.sharding import PartitionSpec as P

ALPHA = 140.0 ** 0.5
EPS = 1e-5
SHRINK = 0.1
ROPE_BASE = 10000.0
WEIGHT_SPECS = (P(None, 'tp'), P('tp', None), P('tp', None), P(), P(), P(), P(None, 'tp'), P('tp'), P(None, 'tp'), P('tp'), P('tp', None), P(), P())
BF = jnp.bfloat16
N0, N1, N2 = range(3)
F32 = jnp.float32
MESH = pl.DeviceIdType.MESH
ANY = pl.BlockSpec(memory_space=pl.ANY)
VMEM = pl.BlockSpec(memory_space=pltpu.VMEM)


def rope_tables(seq_len, head_dim, heads):
    half_dim = head_dim // 2
    inv_freq = (ROPE_BASE ** (-2.0 * np.arange(half_dim) / head_dim)).astype(np.float32)
    angles = np.arange(seq_len, dtype=np.float32)[:, None] * inv_freq[None, :]
    return [jnp.asarray(np.tile(table(angles), (1, heads))) for table in (np.cos, np.sin)]


def column_order(heads, head_dim):
    cols = np.arange(3 * heads * head_dim).reshape(heads, 3, 2, head_dim // 2)
    return np.concatenate([cols[:, part].transpose(1, 0, 2).ravel() for part in (0, 1)] + [cols[:, 2].ravel()])


def rcopy(src, dst, send, recv, **where):
    return pltpu.make_async_remote_copy(src_ref=src, dst_ref=dst, send_sem=send, recv_sem=recv, device_id=dict(where), device_id_type=MESH)


def plane():
    p = lax.axis_index('dp')
    y, x, c = p // 4, (p // 2) % 2, p % 2

    def at(rel):
        yy = 1 - y if rel & 4 else y
        xx = 1 - x if rel & 2 else x
        cc = 1 - c if rel & 1 else c
        return yy * 4 + xx * 2 + cc
    return p, at


def entry_barrier(z, n, at):
    bar = pltpu.get_barrier_semaphore()
    for rel in range(1, 8):
        pl.semaphore_signal(bar, inc=1, device_id={'dp': at(rel)}, device_id_type=MESH)
    for d in range(1, n):
        pl.semaphore_signal(bar, inc=1, device_id={'tp': (z + d) % n}, device_id_type=MESH)
    pl.semaphore_wait(bar, 7 + n - 1)


LAG = 3


def chain_sum(k, z, n, rows, chunks, part, left, right, done, send_r, send_l, recv_l, recv_r, place=lambda c: c):
    last = n - 1

    def at_rows(c):
        return pl.ds(pl.multiple_of(place(c) * rows, rows), rows)

    def cut(ref, c):
        return ref.at[at_rows(c)]

    def load(ref, c):
        return ref[at_rows(c)]

    def store(ref, c, value):
        ref[at_rows(c)] = value
    cl, cr = k - LAG * z, k - LAG * (last - z)
    okl, okr = (cl >= 0) & (cl < chunks), (cr >= 0) & (cr < chunks)

    @pl.when(okl & (z > 0))
    def _():
        rcopy(cut(left, cl), cut(left, cl), send_r, recv_l.at[cl], tp=z).wait_recv()

    @pl.when(okl & (z == last))
    def _():
        done(cl, load(left, cl) + load(part, cl))

    @pl.when(okl & (z > 0) & (z < last))
    def _():
        run = load(left, cl)

        @pl.when(z >= n // 2)
        def _():
            done(cl, run + load(right, cl))
        store(left, cl, run + load(part, cl))

    @pl.when(okr & (z < last))
    def _():
        rcopy(cut(right, cr), cut(right, cr), send_l, recv_r.at[cr], tp=z).wait_recv()

    @pl.when(okr & (z == 0))
    def _():
        done(cr, load(part, cr) + load(right, cr))

    @pl.when(okr & (z > 0) & (z < last))
    def _():
        run = load(right, cr)

        @pl.when(z < n // 2)
        def _():
            done(cr, load(left, cr) + run)
        store(right, cr, run + load(part, cr))

    @pl.when(okl & (z == 0))
    def _():
        rcopy(cut(part, cl), cut(left, cl), send_r, recv_l.at[cl], tp=z + 1).start()

    @pl.when(okl & (z > 0) & (z < last))
    def _():
        rcopy(cut(left, cl), cut(left, cl), send_r, recv_l.at[cl], tp=z + 1).start()

    @pl.when(okr & (z == last))
    def _():
        rcopy(cut(part, cr), cut(right, cr), send_l, recv_r.at[cr], tp=z - 1).start()

    @pl.when(okr & (z > 0) & (z < last))
    def _():
        rcopy(cut(right, cr), cut(right, cr), send_l, recv_r.at[cr], tp=z - 1).start()


def chain_drain(z, n, part, left, right, send_r, send_l, recv_l, recv_r):
    @pl.when(z < n - 1)
    def _():
        rcopy(part, left, send_r, recv_l.at[0], tp=z + 1).wait_send()

    @pl.when(z > 0)
    def _():
        rcopy(part, right, send_l, recv_r.at[0], tp=z - 1).wait_send()


EDGES = ((0, 0, 2), (0, 0, 4), (0, 0, 1), (2, 1, 4), (4, 2, 2), (2, 0, 1), (4, 0, 1), (6, 1, 1), (6, 2, 1))
CROSS, DIAGONAL, LAST = ((0, 3, 5), (1, 4, 6)), ((3, 7), (4, 8)), {1: (2,), 3: (5,), 5: (6,), 7: (7, 8)}
STEPS = (4, 10, 17, 21, 25, 29)
FIRST = 18
ORDER = (0, 2, 4, 1, 3, 5, 6, 7)


def emb_kernel(n, rows, chunks, cuts, heads, found, mask, wq, bq, cos, sin, piece, toks, *refs):
    m = len(cuts)
    local, outs = refs[:m], refs[m + N1:N2 * m + N1]
    out, (bias, tok_all, wall, ctx_own, q, k_all, v, ctx, top, inv, part, left, right, raw, low, weights, send_r, send_l, recv_l, recv_r, tsend, trecv, tself, zsend, zrecv, psend, precv, lsem, isem, osem, bsem, asend, arecv, aself) = refs[m], refs[N2 * m + N1:]
    blocks = 8
    qb = part.shape[N0] // blocks
    per = chunks // blocks
    z = lax.axis_index('tp')
    p, at = plane()
    entry_barrier(z, n, at)
    half = piece.shape[N0] // N2

    @pl.when(z < n - N1)
    def _():
        rcopy(piece, wall.at[z, p], zsend.at[z], zrecv.at[z], tp=z + N1).start()

    @pl.when(z > N0)
    def _():
        rcopy(piece, wall.at[z, p], bsem.at[N1], zrecv.at[z], tp=z - N1).start()
    mine = [pltpu.make_async_copy(toks, tok_all.at[p], tself)]
    mine += [pltpu.make_async_copy(src, dst.at[z], lsem.at[i]) for i, (src, dst) in enumerate(zip(local, outs))]
    for copy in mine:
        copy.start()
    for rel in range(N1, 8):
        rcopy(toks, tok_all.at[p], tsend.at[rel], trecv.at[rel], dp=at(rel)).start()

    def others(d, body):
        @pl.when(z >= d)
        def _():
            body(z - d, -N1)

        @pl.when(z + d < n)
        def _():
            body(z + d, N1)

    def region(t, rel, side):
        blk = wall.at[t, at(rel)]
        return blk if side == N0 else wall.at[t, at(rel), pl.ds((side - N1) * half, half)]

    def give(t, j):
        rel, side, to = EDGES[j]
        rcopy(region(t, rel, side), region(t, rel, side), psend.at[t, j], precv.at[t, j], dp=at(to)).start()

    def take(t, j):
        rel, side, to = EDGES[j]
        blk = region(t, rel ^ to, side)
        rcopy(blk, blk, psend.at[t, j], precv.at[t, j], dp=p).wait_recv()

    def gave(t, j):
        rel, side, to = EDGES[j]
        rcopy(region(t, rel, side), region(t, rel, side), psend.at[t, j], precv.at[t, j], dp=p).wait_send()

    def arrive(d):
        def body(t, sign):
            blk = wall.at[t, p]
            rcopy(blk, blk, zsend.at[t], zrecv.at[t], tp=z).wait_recv()

            @pl.when((z - sign >= N0) & (z - sign < n))
            def _():
                rcopy(blk, blk, zsend.at[t], zrecv.at[t], tp=z - sign).start()
            for j in range(3):
                give(t, j)
        others(d, body)

    def relay(d, moves):
        def body(t, sign):
            for first, *rest in moves:
                take(t, first)
                for j in rest:
                    give(t, j)
        others(d, body)

    k_all[:] = jnp.zeros_like(k_all)
    v[:] = jnp.zeros_like(v)
    arrive(N1)

    @pl.loop(N0, blocks)
    def _(i):
        at_i = pl.ds(pl.multiple_of(i * qb, qb), qb)
        part[at_i, :] = jnp.where(mask[at_i, :] > N0, found[at_i, :].astype(F32), 0.0)

    def done(c, value):
        out[pl.ds(pl.multiple_of(c * rows, rows), rows)] = value.astype(out.dtype)

    def other(i):
        return i + (i + n - z) // n

    def loaded(i, rel, slot):
        return pltpu.make_async_copy(wall.at[other(i), at(rel), pl.ds(N0, cuts[-N1][N1])], raw.at[slot], isem.at[slot])

    def stored(i, rel, slot):
        return [pltpu.make_async_copy(low.at[slot, pl.ds(lo, hi - lo)], dst.at[other(i), at(rel)], osem.at[slot, k]) for k, ((lo, hi), dst) in enumerate(zip(cuts, outs))]
    plan = [(i, rel) for rel in ORDER for i in range(n - N1)]

    def prefetch(s):
        i, rel = plan[s]
        for j in LAST.get(rel, ()):
            take(other(i), j)
        loaded(i, rel, s % N2).start()

    def convert(s):
        i, rel = plan[s]
        loaded(i, rel, s % N2).wait()
        if s >= N2:
            for copy in stored(*plan[s - N2], s % N2):
                copy.wait()
        low[s % N2] = raw[s % N2].astype(low.dtype)
        if s + N1 < len(plan):
            prefetch(s + N1)
        for copy in stored(i, rel, s % N2):
            copy.start()
    events = [(STEPS[d - N1], functools.partial(relay, d, CROSS)) for d in range(N1, n)] + [(STEPS[d + n - N2], functools.partial(relay, d, DIAGONAL)) for d in range(N1, n)]
    events += [(N2 * d - N2, functools.partial(arrive, d)) for d in range(N2, n)]
    events += [(FIRST - N1, functools.partial(prefetch, N0))] + [(FIRST + s, functools.partial(convert, s)) for s in range(len(plan))]

    start = per + LAG * (n - N1)

    share = qb // n

    def context(i, d):
        to = (z + d) % n
        src = ctx.at[pl.ds(pl.multiple_of(i * qb + to * share, share), share)]
        if d == N0:
            return pltpu.make_async_copy(src, ctx_own.at[z, i], aself)
        return rcopy(src, ctx_own.at[z, i], asend, arecv.at[z], tp=to)

    @pl.loop(N0, max(start + blocks * heads + N1, FIRST + len(plan)))
    def _(k):
        step = k - start
        i = step // heads - N1

        @pl.when((step > N0) & (step % heads == N0) & (step <= blocks * heads))
        def _():
            for d in range(n):
                context(i, d).start()
        chain_sum(k, z, n, rows, chunks, part, left, right, done, send_r, send_l, recv_l, recv_r)
        for at_step, event in events:
            pl.when(k == at_step)(event)

        @pl.when((step >= N0) & (step < blocks * heads))
        def _():
            @pl.when(step % heads == N0)
            def _():
                project(step // heads, qb, out, wq, bq, cos, sin, q, k_all, v)
            attend(step // heads, step % heads, heads, qb, q, k_all, v, ctx, top, inv, weights)

    pltpu.make_async_copy(ctx_own.at[z], ctx_own.at[z], aself).wait()
    for d in range(N1, n):
        src = (z + d) % n
        rcopy(ctx_own.at[src], ctx_own.at[src], asend, arecv.at[src], tp=z).wait()
    chain_drain(z, n, part, left, right, send_r, send_l, recv_l, recv_r)
    for s in (len(plan) - N2, len(plan) - N1):
        for copy in stored(*plan[s], s % N2):
            copy.wait()

    def finish(t, sign):
        for j in range(len(EDGES)):
            gave(t, j)
        tail = pltpu.make_async_copy(wall.at[t, p, pl.ds(cuts[-N1][N1], bias.shape[N1])], bias.at[t], bsem.at[N0])
        tail.start()
        tail.wait()

        @pl.when((z - sign >= N0) & (z - sign < n))
        def _():
            rcopy(wall.at[t, p], wall.at[t, p], zsend.at[t], zrecv.at[t], tp=z).wait_send()
    for d in range(N1, n):
        others(d, finish)
    for copy in mine:
        copy.wait()
    for rel in range(N1, 8):
        rcopy(toks, tok_all.at[at(rel)], tsend.at[rel], trecv.at[rel], dp=at(rel)).wait()

    @pl.when(z < n - N1)
    def _():
        rcopy(piece, wall.at[z, p], zsend.at[z], zrecv.at[z], tp=z + N1).wait_send()

    @pl.when(z > N0)
    def _():
        rcopy(piece, wall.at[z, p], bsem.at[N1], zrecv.at[z], tp=z - N1).wait_send()


def embed(found, mask, piece, toks, local, wq, bq, cos, sin, heads, n_tp, n_dp):
    seq, width = found.shape
    chunks = 32
    rows = seq // chunks
    dims = wq.shape[N1] // 3
    cuts, lo = [], N0
    for weight in local:
        cuts.append((lo, lo + weight.shape[N0] // n_dp))
        lo = cuts[-N1][N1]
    dma = pltpu.SemaphoreType.DMA
    shape = jax.ShapeDtypeStruct
    shapes = [shape((seq, width), BF)]
    shapes += [shape((n_tp, n_dp, w.shape[N0] // n_dp, w.shape[N1]), BF) for w in local]
    shapes += [shape((n_tp, piece.shape[N0] - lo, width), F32), shape((n_dp,) + toks.shape, toks.dtype), shape((n_tp, n_dp) + piece.shape, F32), shape((n_tp, 8, seq // n_tp // 8, dims), F32)]
    shapes += [shape((seq, dims), BF)] * 3 + [shape((seq, dims), F32)] + [shape((heads, seq), F32)] * N2
    out = pl.pallas_call(
        functools.partial(emb_kernel, n_tp, rows, chunks, cuts, heads),
        name='embed',
        out_shape=shapes,
        in_specs=[VMEM] * 6 + [ANY] * (N2 + len(local)),
        out_specs=[VMEM] + [ANY] * (4 + len(local)) + [VMEM] * 6,
        scratch_shapes=[pltpu.VMEM((seq, width), F32)] * 3 + [pltpu.VMEM((N2, lo, width), F32), pltpu.VMEM((N2, lo, width), BF), pltpu.VMEM((seq, seq // 8), F32), dma, dma, dma((chunks,)), dma((chunks,)),
                        dma((8,)), dma((8,)), dma, dma((n_tp,)), dma((n_tp,)), dma((n_tp, len(EDGES))), dma((n_tp, len(EDGES))), dma((len(local),)), dma((N2,)), dma((N2, len(local))), dma((N2,)),
                        dma, dma((n_tp,)), dma],
        compiler_params=pltpu.CompilerParams(collective_id=N0, has_side_effects=True, vmem_limit_bytes=60 * N2 ** 20),
        cost_estimate=pl.CostEstimate(flops=20 * 10 ** 9, bytes_accessed=80 * N2 ** 20, transcendentals=N0),
    )(found, mask, wq, bq, cos, sin, piece, toks, *[w.reshape(n_dp, w.shape[N0] // n_dp, w.shape[N1]) for w in local])
    m = N1 + len(local)
    return out[N0], [w.reshape(n_tp, -N1, w.shape[3]) for w in out[N1:m]], out[m], out[m + N1], out[m + 3], out[m + 4:]


RING = 4
HOLD, LIVE, PAIR = 4, 12, 4
ADD, LOAD, CROSSED, LAND, PLANE, HOP, BEAT = 1, 4, 5, 9, 10, 2, 4
GATHER = (37, 41)


def block_of(ref, at, rel, side):
    return ref.at[at(rel)] if side == 0 else ref.at[at(rel), side - 1]


class Spread:
    def __init__(self, at, block, send, recv, own=None):
        self.at, self.block, self.send, self.recv, self.own = at, block, send, recv, own

    def copy(self, j, rel, side, to):
        dst = self.block(rel, side)
        src = self.own if rel == 0 and self.own is not None else dst
        return rcopy(src, dst, self.send.at[j], self.recv.at[j], dp=self.at(to))

    def give(self, j):
        self.copy(j, *EDGES[j]).start()

    def take(self, j):
        rel, side, to = EDGES[j]
        self.copy(j, rel ^ to, side, 0).wait_recv()

    def start(self):
        for j in range(3):
            self.give(j)

    def relay(self, moves):
        for first, *rest in moves:
            self.take(first)
            for j in rest:
                self.give(j)

    def cross(self):
        self.relay(CROSS)

    def diagonal(self):
        self.relay(DIAGONAL)

    def finish(self):
        for j in (2, 5, 6, 7, 8):
            self.take(j)
        for j, (rel, side, _) in enumerate(EDGES):
            self.copy(j, rel, side, 0).wait_send()


def backward_kernel(n, rows, chunks, jobs, heads, d_ctx, resid, q, k_all, v, ctx, top, inv, cos, sin, wq, back, emb, *refs):
    prods = refs[:jobs]
    whole = refs[jobs:N2 * jobs - N1]
    out, grads, d_w, d_bias, landed, cross, last, part, left, right, total, dctx, dq, dk, dv, ctx_in, res_in, cos_in, sin_in, emb_in, q_in, work, fresh, xin, yin, keep, pass_on, along, final, *sems = refs[N2 * jobs - N1:]
    send_r, send_l, recv_l, recv_r, osend, orecv, csend, crecv, esem, fsem, xsend, xrecv, xsem, ysend, yrecv, ysem, ksem, zrecv, frecv, asend, arecv, aself, isem, gsend, grecv = sems
    z = lax.axis_index('tp')
    p, at = plane()
    entry_barrier(z, n, at)
    blocks = 8
    per = chunks // blocks
    qb = rows * per
    share = qb // n
    block = out.shape[N2]
    lead = jnp.maximum(z, n - N1 - z)
    span = N2 * n
    units = jobs * span
    size = work.shape[N2]

    def rows_of(i, to, count):
        return pl.ds(pl.multiple_of(i * qb + to * count, count), count)

    def exchange(i, d):
        to = (z + d) % n
        dst = dctx.at[rows_of(i, z, share)]
        if d == N0:
            return pltpu.make_async_copy(d_ctx.at[z, i], dst, aself.at[i])
        return rcopy(d_ctx.at[to, i], dst, asend, arecv.at[i], tp=to)

    @pl.loop(N0, blocks)
    def _(b):
        for d in range(n):
            exchange(blocks - N1 - b, d).start()

    def piece(m, u, rel):
        return prods[m].at[(u % span) // N2, at(rel), pl.ds(pl.multiple_of((u % N2) * size, size), size)]

    for m in range(jobs):
        @pl.loop(m * span, (m + N1) * span)
        def _(u, m=m):
            for i in range(4):
                rcopy(piece(m, u, N2 * i + N1), landed.at[u, i], csend, crecv.at[u], dp=at(N1)).start()

    def inputs(i):
        slot = i % N2
        at_q = rows_of(i, N0, qb)
        pairs = ((ctx.at[at_q], ctx_in), (resid.at[i], res_in), (cos.at[at_q], cos_in), (sin.at[at_q], sin_in), (emb.at[at_q], emb_in), (q.at[at_q], q_in))
        return [pltpu.make_async_copy(src, dst.at[slot], isem.at[j, slot]) for j, (src, dst) in enumerate(pairs)]

    dk[:] = jnp.zeros_like(dk)
    dv[:] = jnp.zeros_like(dv)
    d_w[:] = jnp.zeros_like(d_w)
    d_bias[:] = jnp.zeros_like(d_bias)
    for copy in inputs(blocks - N1):
        copy.start()

    def attention_step(b, h):
        i = blocks - N1 - b

        @pl.when(h == N0)
        def _():
            for copy in inputs(i):
                copy.wait()

            @pl.when(b + N1 < blocks)
            def _():
                for copy in inputs(i - N1):
                    copy.start()
            exchange(i, N0).wait()
            others = dctx.at[pl.ds(N0, (n - N1) * share)]
            rcopy(others, others, asend, arecv.at[i], tp=z).wait_recv()
        attend_grad(i, h, heads, qb, q_in.at[i % N2], k_all, v, ctx_in.at[i % N2], dctx, top, inv, dq, dk, dv)

        @pl.when(h == heads - N1)
        def _():
            slot = i % N2
            got = grad_rows(i, qb, cos_in[slot], sin_in[slot], dq, dk, dv, d_bias)
            d_w[:] += dot(emb_in[slot], dot(got, back[:], NN).astype(BF), TN)
            part[rows_of(i, N0, qb), :] = dot(got, wq[:], NT)
            part[rows_of(i, z, share), :] = part[rows_of(i, z, share), :] + res_in[i % N2]

    def sides(u):
        side = u % N2
        return side, at(N2) * (N1 - side) + at(4) * side, at(4) * (N1 - side) + at(N2) * side

    def fetch(u):
        slot = u % HOLD

        @pl.when(u >= HOLD)
        def _():
            rcopy(xin, cross.at[N0], xsend.at[slot], xrecv.at[N0], dp=p).wait_send()
        for m in range(jobs):
            @pl.when(u // span == m)
            def _(m=m):
                for i in range(4):
                    pltpu.make_async_copy(piece(m, u, N2 * i), work.at[slot, i], esem.at[slot]).start()
        rcopy(landed.at[u], landed.at[u], csend, crecv.at[u], dp=p).wait_recv()
        pltpu.make_async_copy(landed.at[u], fresh, fsem).start()

    def add(u):
        slot = u % HOLD
        pltpu.make_async_copy(landed.at[u], work.at[slot], esem.at[slot]).wait()
        pltpu.make_async_copy(landed.at[u], fresh, fsem).wait()
        for i in range(4):
            work[slot, i] = work[slot, i] + fresh[i]

    def add_send(u):
        slot = u % HOLD
        side, first, second = sides(u)
        rcopy(work.at[slot, N1 + side], cross.at[u, N0], xsend.at[slot], xrecv.at[u], dp=first).start()
        rcopy(work.at[slot, 3], cross.at[u, N1], xsend.at[slot], xrecv.at[u], dp=first).start()

    def load_cross(u):
        rcopy(cross.at[u], cross.at[u], xsend.at[N0], xrecv.at[u], dp=p).wait_recv()
        pltpu.make_async_copy(cross.at[u], xin, xsem).start()

    def crossed(u):
        slot = u % HOLD
        pltpu.make_async_copy(cross.at[u], xin, xsem).wait()

        @pl.when(u >= LIVE)
        def _():
            pltpu.make_async_copy(keep.at[u % LIVE], keep.at[u % LIVE], ksem.at[u % LIVE]).wait()

        @pl.when(u >= PAIR)
        def _():
            rcopy(pass_on.at[u % PAIR], last.at[u], ysend.at[u % PAIR], yrecv.at[u], dp=p).wait_send()
        keep[u % LIVE] = xin[N0] + work[slot, N0]
        pass_on[u % PAIR] = xin[N1] + work[slot, N2 - u % N2]

    def crossed_send(u):
        side, first, second = sides(u)
        rcopy(pass_on.at[u % PAIR], last.at[u], ysend.at[u % PAIR], yrecv.at[u], dp=second).start()

    def load_last(u):
        rcopy(last.at[u], last.at[u], ysend.at[N0], yrecv.at[u], dp=p).wait_recv()
        pltpu.make_async_copy(last.at[u], yin, ysem).start()

    def in_plane(u):
        pltpu.make_async_copy(last.at[u], yin, ysem).wait()
        keep[u % LIVE] = keep[u % LIVE] + yin[:]

    def unit(k):
        u = (k // BEAT) * (BEAT - N1) + k % BEAT
        return u, (k >= N0) & (k % BEAT < BEAT - N1) & (u < units)

    def along_tp(k, t, send):
        toward = jnp.where(z < t, z, n - N1 - z)
        late = HOP * jnp.where(z == t, max(t, n - N1 - t), toward)
        u, ok = unit(k - PLANE - N1 - late)
        mine = (u // span) * N2 + u % N2
        slot = u % LIVE
        ok = ok & ((u // N2) % n == t)

        def add_from(ref, sem):
            rcopy(ref, ref, csend, sem, tp=z).wait_recv()
            keep[slot] = keep[slot] + ref[:]
        if send:
            @pl.when(ok & (z < t))
            def _():
                rcopy(keep.at[slot], along.at[u], ksem.at[slot], zrecv.at[u], tp=z + N1).start()

            @pl.when(ok & (z > t + N1))
            def _():
                rcopy(keep.at[slot], along.at[u], ksem.at[slot], zrecv.at[u], tp=z - N1).start()

            @pl.when(ok & (z == t + N1))
            def _():
                rcopy(keep.at[slot], final.at[mine], ksem.at[slot], frecv.at[mine], tp=z - N1).start()

            for m in range(jobs):
                @pl.when(ok & (z == t) & (u // span == m))
                def _(m=m):
                    dst = whole[m].at[p, u % N2] if m < jobs - N1 else grads.at[u % N2]
                    pltpu.make_async_copy(keep.at[slot], dst, ksem.at[slot]).start()
        else:
            @pl.when(ok & (((z > N0) & (z <= t)) | ((z > t) & (z < n - N1))))
            def _():
                add_from(along.at[u], zrecv.at[u])
            if t < n - N1:
                @pl.when(ok & (z == t))
                def _():
                    add_from(final.at[mine], frecv.at[mine])

    spread = [Spread(at, functools.partial(block_of, whole[m], at), gsend.at[m], grecv.at[m]) for m in range(jobs - N1)]

    def settle(u):
        pltpu.make_async_copy(keep.at[u % LIVE], keep.at[u % LIVE], ksem.at[u % LIVE]).wait()

    def begin(m):
        for u in range(max(m * span, units - LIVE), (m + N1) * span):
            settle(u)
        spread[m].start()

    def place(c):
        return (blocks - N1 - c // per) * per + c % per

    def chunk(c):
        return total.at[c % RING]

    def done(c, value):
        @pl.when(c >= RING)
        def _():
            pltpu.make_async_copy(chunk(c), chunk(c), osend.at[c % RING]).wait()
        total[c % RING] = value

    def hand_out(c):
        where = out.at[p, pl.ds(pl.multiple_of(place(c) * rows, rows), rows)]
        for rel in range(8):
            src = total.at[c % RING, :, pl.ds(pl.multiple_of(at(rel) * block, block), block)]
            if rel == N0:
                pltpu.make_async_copy(src, where, osend.at[c % RING]).start()
            else:
                rcopy(src, where, osend.at[c % RING], orecv.at[rel], dp=at(rel)).start()

    def staged(k, offset, stage):
        u, ok = unit(k - offset)
        pl.when(ok)(functools.partial(stage, u))
    steps = max(heads + chunks + LAG * (n - N1) + N1, units // (BEAT - N1) * BEAT + PLANE + HOP * (n - N1), GATHER[-N1] + 7)

    @pl.loop(N0, steps)
    def _(k):
        c = k - heads - LAG * lead - N1

        @pl.when((c >= N0) & (c < chunks))
        def _():
            hand_out(c)
        chain_sum(k - heads, z, n, rows, chunks, part, left, right, done, send_r, send_l, recv_l, recv_r, place)
        for offset, stage in ((CROSSED, crossed), (ADD, add), (PLANE, in_plane)):
            staged(k, offset, stage)
        for t in range(n):
            along_tp(k, t, False)
        for offset, stage in ((N0, fetch), (LOAD, load_cross), (LAND, load_last)):
            staged(k, offset, stage)

        @pl.when(k < blocks * heads)
        def _():
            attention_step(k // heads, k % heads)
        for offset, stage in ((ADD, add_send), (CROSSED, crossed_send)):
            staged(k, offset, stage)
        for t in range(n):
            along_tp(k, t, True)
        for m, gather in enumerate(spread):
            for offset, stage in ((N0, functools.partial(begin, m)), (3, gather.cross), (6, gather.diagonal)):
                pl.when(k == GATHER[m] + offset)(stage)

    chain_drain(z, n, part, left, right, send_r, send_l, recv_l, recv_r)
    for c in range(max(N0, chunks - RING), chunks):
        pltpu.make_async_copy(chunk(c), chunk(c), osend.at[c % RING]).wait()
    for rel in range(N1, 8):
        rcopy(out.at[at(rel)], out.at[at(rel)], csend, orecv.at[rel], dp=p).wait_recv()
    for slot in range(HOLD):
        rcopy(xin, cross.at[N0], xsend.at[slot], xrecv.at[N0], dp=p).wait_send()
    for slot in range(PAIR):
        rcopy(pass_on.at[slot], last.at[N0], ysend.at[slot], yrecv.at[N0], dp=p).wait_send()
    for u in range(max((jobs - N1) * span, units - LIVE), units):
        settle(u)
    rcopy(landed, landed, csend, crecv.at[N0], dp=p).wait_send()
    for gather in spread:
        gather.finish()
    sent = dctx.at[pl.ds(N0, (n - N1) * share * blocks)]
    rcopy(sent, sent, asend, arecv.at[N0], tp=z).wait_send()


def backward(d_ctx, resid, saved, cos, sin, wq, back, emb, prods, heads, n_tp, n_dp):
    q, k, v, ctx, top, inv = saved
    seq, dims = q.shape
    width = wq.shape[N0]
    chunks = 32
    rows = seq // chunks
    jobs = len(prods)
    piece = (prods[N0].shape[N2] // N2, prods[N0].shape[3])
    units = jobs * N2 * n_tp
    dma = pltpu.SemaphoreType.DMA
    shape = jax.ShapeDtypeStruct
    qb = seq // 8
    vmem = [(seq, width)] * 3 + [(RING, rows, width), (seq, dims), (qb, dims), (seq, dims), (seq, dims), (N2, qb, dims), (N2, qb // n_tp, width)] + [(N2, qb, dims // N2)] * N2 + [
            (HOLD, 4) + piece, (4,) + piece, (N2,) + piece, piece, (LIVE,) + piece, (PAIR,) + piece, (units,) + piece, (N2 * jobs,) + piece]
    sems = [(), (), (chunks,), (chunks,), (RING,), (8,), (), (units,), (HOLD,), (), (HOLD,), (units,), (), (PAIR,), (units,), (), (LIVE,), (units,), (N2 * jobs,), (), (8,), (8,), (6, N2), (jobs - N1, len(EDGES)), (jobs - N1, len(EDGES))]
    scratch = [pltpu.VMEM(size, F32) for size in vmem]
    scratch[12:12] = [pltpu.VMEM((N2, qb, width), BF), pltpu.VMEM((N2, qb, dims), BF)]
    full = shape((n_dp, N2) + piece, F32)
    *whole, cols, grads, d_w, d_bias, _, _, _ = pl.pallas_call(
        functools.partial(backward_kernel, n_tp, rows, chunks, jobs, heads),
        name='backward',
        out_shape=[full] * (jobs - N1) + [shape((n_dp, seq, width // n_dp), F32), shape((N2,) + piece, F32), shape((width, 3 * dims), F32), shape((N1, 3 * dims), F32),
                   shape((units, 4) + piece, F32), shape((units, N2) + piece, F32), shape((units,) + piece, F32)],
        in_specs=[ANY] * 3 + [VMEM] * N2 + [ANY] + [VMEM] * N2 + [ANY] * N2 + [VMEM] * N2 + [ANY] * (N1 + jobs),
        out_specs=[ANY] * (jobs - N1) + [ANY, ANY, VMEM, VMEM, ANY, ANY, ANY],
        scratch_shapes=scratch + [dma(size) for size in sems],
        compiler_params=pltpu.CompilerParams(collective_id=N1, has_side_effects=True, vmem_limit_bytes=67_000_000),
        cost_estimate=pl.CostEstimate(flops=20 * 10 ** 9, bytes_accessed=100 * N2 ** 20, transcendentals=N0),
    )(d_ctx, resid, q, k, v, ctx, top, inv, cos, sin, wq, back, emb, *prods)
    return d_w, d_bias, cols, whole, grads


WAYS = 4


def table_kernel(ids, rows_ref, out, *tables):
    step = pl.program_id(0)
    count = rows_ref.shape[0]
    part = count // WAYS

    @pl.when(step == 0)
    def _():
        for table in tables:
            table[:] = jnp.zeros_like(table)

    @pl.loop(0, part, unroll=4)
    def _(r):
        for way, table in enumerate(tables):
            row = way * part + r
            where = pl.ds(ids[step * count + row], 1)
            table[where, :] = table[where, :] + rows_ref[pl.ds(row, 1), :]

    @pl.when(step == pl.num_programs(0) - 1)
    def _():
        total = tables[0][:]
        for table in tables[1:]:
            total = total + table[:]
        out[:] = SHRINK * total[:out.shape[0]]


def table_rows(ids, rows, vocab_loc):
    count, block = rows.shape
    step = min(1024, count // 2)
    return pl.pallas_call(
        table_kernel,
        name='table_rows',
        grid_spec=pltpu.PrefetchScalarGridSpec(
            num_scalar_prefetch=1,
            grid=(count // step,),
            in_specs=[pl.BlockSpec((step, block), lambda i, ids: (i, 0))],
            out_specs=pl.BlockSpec((vocab_loc, block), lambda i, ids: (0, 0)),
            scratch_shapes=[pltpu.VMEM((vocab_loc + 8, block), F32)] * WAYS,
        ),
        out_shape=jax.ShapeDtypeStruct((vocab_loc, block), F32),
        compiler_params=pltpu.CompilerParams(dimension_semantics=('arbitrary',), vmem_limit_bytes=48 * 2 ** 20),
        cost_estimate=pl.CostEstimate(flops=3 * 10 ** 9, bytes_accessed=16 * 2 ** 20, transcendentals=0),
    )(ids, rows)


class PlaneSum:
    def __init__(self, at, block, landed, work, cross, last, mine, sems):
        self.at, self.block, self.landed, self.work, self.cross, self.last, self.mine, self.sems = at, block, landed, work, cross, last, mine, sems

    def copy(self, src, dst, kind, side, rel):
        return rcopy(src, dst, self.sems.at[kind, side, N0], self.sems.at[kind, side, N1], dp=self.at(rel))

    def start(self):
        for i in range(4):
            self.copy(self.block(N2 * i + N1), self.landed.at[i], N0, N0, N1).start()

    def first(self):
        self.copy(self.landed, self.landed, N0, N0, N0).wait()
        for i in range(4):
            self.work[i] = self.block(N2 * i)[:] + self.landed[i]

    def first_send(self):
        for side in range(N2):
            self.copy(self.work.at[N1 + side, side], self.cross.at[side, N0], N1, side, N2 * (N1 + side)).start()
            self.copy(self.work.at[3, side], self.cross.at[side, N1], N1, side, N2 * (N1 + side)).start()

    def second(self):
        for side in range(N2):
            self.copy(self.cross.at[side], self.cross.at[side], N1, side, N0).wait()
            self.cross[side, N0] = self.cross[side, N0] + self.work[N0, side]
            self.cross[side, N1] = self.cross[side, N1] + self.work[N2 - side, side]

    def second_send(self):
        for side in range(N2):
            self.copy(self.cross.at[side, N1], self.last.at[side], N2, side, N2 * (N2 - side)).start()

    def end(self):
        for side in range(N2):
            self.copy(self.last.at[side], self.last.at[side], N2, side, N0).wait()
            self.mine[side] = self.cross[side, N0] + self.last[side]


def finish_kernel(n, cuts, col, down, proj, d_w, small, table, down_all, proj_all, qkv_all, total, *refs):
    scratch, (summed, inbox, arrived, sem, send, recv, dsend, drecv, osem, psem, zsem, rsem) = refs[:10], refs[10:]
    z = lax.axis_index('tp')
    p, at = plane()
    entry_barrier(z, n, at)
    block = col.shape[N1]
    half = len(cuts) // N2

    def part(i):
        def region(rel, side):
            return table.at[pl.ds(cuts[i][N0], cuts[i][N1] - cuts[i][N0]), pl.ds(pl.multiple_of(at(rel) * block, block), block)]
        return Spread(at, region, send.at[i], recv.at[i], col.at[pl.ds(cuts[i][N0], cuts[i][N1] - cuts[i][N0])])
    parts = [part(i) for i in range(len(cuts))]
    qkv_sum = PlaneSum(at, lambda rel: d_w.at[at(rel)], *scratch[:5], psem.at[N0])
    proj_sum = PlaneSum(at, lambda rel: summed.at[at(rel)], *scratch[5:], psem.at[N1])
    pairs = ((down, down_all), (proj_sum.mine, proj_all), (qkv_sum.mine, qkv_all))
    spread = [Spread(at, functools.partial(block_of, ref, at), dsend.at[i], drecv.at[i], own) for i, (own, ref) in enumerate(pairs)]
    own_copies = [pltpu.make_async_copy(col, table.at[:, pl.ds(pl.multiple_of(p * block, block), block)], osem.at[N0])]
    own_copies += [pltpu.make_async_copy(src, dst.at[p], osem.at[i]) for i, (src, dst) in enumerate(pairs, N1)]
    order = list(range(len(cuts)))
    flipped = order[half:] + order[:half]
    peers = [{'dp': at(N1)}, {'dp': at(N2)}, {'dp': at(4)}, {'tp': z + N1 - N2 * (z % N2)}, {'tp': (z + n // N2) % n}]

    def next_part(i):
        parts[order[i]].give(N0)
        parts[flipped[i]].give(N1)
        parts[order[i]].give(N2)

    def relay_part(i):
        one, two = order[i], flipped[i]
        parts[one].take(N0)
        if one < half:
            parts[one].give(3)
        parts[one].give(5)
        parts[two].take(N1)
        if two >= half:
            parts[two].give(4)
        parts[two].give(6)

    def exchange(r):
        return rcopy(total, inbox.at[r], rsem.at[N0, r], rsem.at[N1, r], **peers[r])

    def round_end(r):
        exchange(r).wait()
        total[:] = total[:] + inbox[r]

    total[:] = small[:]
    for d in range(N1, n):
        to = (z + d) % n
        rcopy(proj.at[to], arrived.at[z], zsem.at[N0, to], zsem.at[N1, z], tp=to).start()
    qkv_sum.start()
    for copy in own_copies[:N2]:
        copy.start()
    next_part(N0)
    exchange(N0).start()
    spread[N0].start()
    next_part(N1)
    qkv_sum.first()
    round_end(N0)
    qkv_sum.first_send()
    exchange(N1).start()
    next_part(N2)
    relay_part(N0)
    round_end(N1)
    qkv_sum.second()
    exchange(N2).start()
    qkv_sum.second_send()
    next_part(3)
    spread[N0].cross()
    relay_part(N1)
    round_end(N2)
    qkv_sum.end()
    exchange(3).start()
    next_part(4)
    spread[N2].start()
    own_copies[3].start()
    spread[N0].diagonal()
    relay_part(N2)
    summed[:] = proj[z]
    for d in range(N1, n):
        src = (z + d) % n
        rcopy(proj.at[src], arrived.at[src], zsem.at[N0, src], zsem.at[N1, src], tp=src).wait()
        summed[:] = summed[:] + arrived[src]
    round_end(3)
    next_part(5)
    exchange(4).start()
    proj_sum.start()
    relay_part(3)
    spread[N2].cross()
    proj_sum.first()
    next_part(6)
    proj_sum.first_send()
    round_end(4)
    relay_part(4)
    proj_sum.second()
    next_part(7)
    proj_sum.second_send()
    spread[N2].diagonal()
    relay_part(5)
    proj_sum.end()
    relay_part(6)
    spread[N1].start()
    own_copies[N2].start()
    relay_part(7)
    spread[N1].cross()
    spread[N1].diagonal()
    for i in range(half):
        for via, where in ((3, i), (4, i + half)):
            parts[where].take(via)
            parts[where].give(7)
    for i in order:
        for j in (N2, 5, 6, 7):
            parts[i].take(j)
        for j in (N0, N1, N2, 3 if i < half else 4, 5, 6, 7):
            parts[i].copy(j, *EDGES[j]).wait_send()
    for gather in spread:
        gather.finish()
    for copy in own_copies:
        copy.wait()


def finish(col, down, proj, d_w, small, n_tp, n_dp):
    size, block = col.shape
    tiles = size // 8
    cuts = [(8 * (tiles * i // 8), 8 * (tiles * (i + N1) // 8)) for i in range(8)]
    dma = pltpu.SemaphoreType.DMA
    shape = jax.ShapeDtypeStruct
    ours = (d_w.shape[N1:], proj.shape[N2:])
    kinds = len(EDGES)
    vmem = [lead + src[N1:] for src in ours for lead in ((4, N2), (4, N2), (N2, N2), (N2,), (N2,))] + [proj.shape[N1:], (5,) + small.shape, proj.shape]
    sems = [(), (8, kinds), (8, kinds), (3, kinds), (3, kinds), (4,), (N2, 3, N2, N2), (N2, n_tp), (N2, 5)]
    table, down_all, proj_all, qkv_all, total = pl.pallas_call(
        functools.partial(finish_kernel, n_tp, cuts),
        name='finish',
        out_shape=[shape((size, n_dp * block), F32)] + [shape((n_dp,) + src, F32) for src in (down.shape, ours[N1], ours[N0])] + [shape(small.shape, F32)],
        in_specs=[ANY] * N2 + [VMEM] * 3,
        out_specs=[ANY] * 4 + [VMEM],
        scratch_shapes=[pltpu.VMEM(dims, F32) for dims in vmem] + [dma(dims) for dims in sems],
        compiler_params=pltpu.CompilerParams(collective_id=N2, has_side_effects=True, vmem_limit_bytes=48 * N2 ** 20),
        cost_estimate=pl.CostEstimate(flops=10 * 10 ** 9, bytes_accessed=60 * N2 ** 20, transcendentals=N0),
    )(col, down, proj, d_w, small)
    return [table] + [grad.reshape(-N1, grad.shape[3]) for grad in (down_all, proj_all, qkv_all)] + [total]


def dot(a, b, dims):
    return lax.dot_general(a, b, (dims, ((), ())), preferred_element_type=F32)


NT, TN, NN = ((1,), (1,)), ((0,), (0,)), ((1,), (0,))


def lane_head(shape, heads, halves):
    lane = lax.broadcasted_iota(jnp.int32, shape, 1)
    dims = shape[1] // halves
    return (lane % dims) // (dims // heads)


def turned(both, cos, sin):
    half = both.shape[1] // 2
    x1, x2 = both[:, :half], both[:, half:]
    return jnp.concatenate([x1 * cos - x2 * sin, x2 * cos + x1 * sin], axis=1)


def project(i, qb, emb, wq, bq, cos, sin, q, k, v):
    at_q = pl.ds(pl.multiple_of(i * qb, qb), qb)
    dims = q.shape[1]
    qkv = (dot(emb[at_q, :], wq[:], NN) + bq[:]).astype(BF)
    for ref, part in ((q, 0), (k, 1)):
        ref[at_q, :] = turned(qkv[:, part * dims:(part + 1) * dims].astype(F32), cos[at_q, :], sin[at_q, :]).astype(BF)
    v[at_q, :] = qkv[:, 2 * dims:]


def scores(i, j, kb, qb, scale, keys, q):
    s = dot(keys, q, NT) * scale
    key = j * kb + lax.broadcasted_iota(jnp.int32, (kb, qb), 0)
    query = i * qb + lax.broadcasted_iota(jnp.int32, (kb, qb), 1)
    return jnp.where(query >= key, s, -1e30)


def attend(i, h, heads, qb, q_ref, k_ref, v_ref, ctx_ref, top_ref, inv_ref, s_ref):
    kb = 2 * qb
    dims = q_ref.shape[1]
    scale = (dims // heads) ** -0.5
    at_q = pl.ds(pl.multiple_of(i * qb, qb), qb)
    q = jnp.where(lane_head((qb, dims), heads, 2) == h, q_ref[at_q, :].astype(F32), 0.0).astype(BF)
    count = (i + 2) // 2

    def at_key(j):
        return pl.ds(pl.multiple_of(j * kb, kb), kb)

    def first(j, top):
        s = scores(i, j, kb, qb, scale, k_ref[at_key(j), :], q)
        s_ref[at_key(j), :] = s
        return jnp.maximum(top, jnp.max(s, axis=0, keepdims=True))
    top = lax.fori_loop(0, count, first, jnp.full((1, qb), -1e30, F32))

    def weigh(j, total):
        e = jnp.exp(s_ref[at_key(j), :] - top)
        s_ref[at_key(j), :] = e
        return total + jnp.sum(e, axis=0, keepdims=True)
    inv = 1.0 / lax.fori_loop(0, count, weigh, jnp.zeros((1, qb), F32))

    def mix(j, acc):
        return acc + dot((s_ref[at_key(j), :] * inv).astype(BF), v_ref[at_key(j), :], TN)
    mixed = lax.fori_loop(0, count, mix, jnp.zeros((qb, dims), F32))
    ctx_ref[at_q, :] = jnp.where(lane_head((qb, dims), heads, 1) == h, mixed, ctx_ref[at_q, :])
    top_ref[pl.ds(h, 1), at_q] = top
    inv_ref[pl.ds(h, 1), at_q] = inv


def attend_grad(i, h, heads, qb, q_ref, k_ref, v_ref, ctx_ref, dctx_ref, top_ref, inv_ref, dq_ref, dk_ref, dv_ref):
    kb = 2 * qb
    dims = dk_ref.shape[1]
    scale = (dims // heads) ** -0.5
    at_q = pl.ds(pl.multiple_of(i * qb, qb), qb)
    q = jnp.where(lane_head((qb, dims), heads, 2) == h, q_ref[:].astype(F32), 0.0).astype(BF)
    dc = jnp.where(lane_head((qb, dims), heads, 1) == h, dctx_ref[at_q, :], 0.0).astype(BF)
    ones = jnp.ones((8, dims), F32)
    mean = lax.dot_general(ones, dc.astype(F32) * ctx_ref[:], (NT, ((), ())), precision=lax.Precision.HIGHEST, preferred_element_type=F32)[:1]
    top, inv = top_ref[pl.ds(h, 1), at_q], inv_ref[pl.ds(h, 1), at_q]

    def step(j, dq):
        at_k = pl.ds(pl.multiple_of(j * kb, kb), kb)
        keys = k_ref[at_k, :]
        probs = (jnp.exp(scores(i, j, kb, qb, scale, keys, q) - top) * inv).astype(BF)
        ds = (probs.astype(F32) * (dot(v_ref[at_k, :], dc, NT) - mean) * scale).astype(BF)
        dv_ref[at_k, :] += dot(probs, dc, NN)
        dk_ref[at_k, :] += dot(ds, q, NN)
        return dq + dot(ds, keys, TN)
    dq = lax.fori_loop(0, (i + 2) // 2, step, jnp.zeros((qb, dims), F32))
    dq_ref[:] = jnp.where(lane_head((qb, dims), heads, 2) == h, dq, dq_ref[:])


def grad_rows(i, qb, cos, sin, dq, dk, dv, d_bias):
    at_q = pl.ds(pl.multiple_of(i * qb, qb), qb)
    back = [turned(values, cos, -sin) for values in (dq[:], dk[at_q, :])]
    rows = jnp.concatenate(back + [dv[at_q, :]], axis=1)
    d_bias[:] += jnp.sum(rows, axis=0, keepdims=True)
    return rows.astype(BF)


def standard(values):
    mean = jnp.mean(values, axis=1, keepdims=True)
    centered = values - mean
    scale = lax.rsqrt(jnp.mean(centered * centered, axis=1, keepdims=True) + EPS)
    return centered * scale, scale


def standard_grad(d_out, unit, scale):
    return scale * (d_out - jnp.mean(d_out, axis=1, keepdims=True) - unit * jnp.mean(d_out * unit, axis=1, keepdims=True))


def over_rows(values):
    return jnp.sum(values, axis=0, keepdims=True)


def layer_kernel(n, ctx, wo, emb, cot, vectors, gate_bias, lin_bias, wg, wl, wd, hidden, d_ffn, d_attn, resid, d_ctx, sums, inner, d_gate, d_lin, gate, lin, acc, unit1, scale1):
    i = pl.program_id(N0)
    t = i % n
    tile = 256 if acc.shape[N1] % 256 == N0 else acc.shape[N1]
    tiles = range(N0, acc.shape[N1], tile)
    b_out, gain1, bias1, b_down, gain2 = [vectors[pl.ds(j, N1), :] for j in range(5)]

    @pl.when(i == N0)
    def _():
        total = ALPHA * emb[:].astype(F32) + b_out
        for h in range(n):
            total = total + dot(ctx[h].astype(BF), wo[h], NN)
        unit, scale1[:] = standard(total)
        unit1[:] = unit
        hidden[:] = (unit * gain1 + bias1).astype(BF)
        acc[:] = jnp.zeros_like(acc)

    @pl.when(i < n)
    def _():
        for lo in tiles:
            cols = pl.ds(lo, tile)
            g = dot(hidden[:], wg[N0, :, cols], NN) + gate_bias[pl.ds(t, N1), cols]
            l = dot(hidden[:], wl[N0, :, cols], NN) + lin_bias[pl.ds(t, N1), cols]
            gate[t, :, cols] = g
            lin[t, :, cols] = l
            inner[N0, :, cols] = (0.5 * g * (1.0 + lax.erf(g * 0.5 ** 0.5)) * l).astype(BF)
        for lo in tiles:
            cols = pl.ds(lo, tile)
            acc[:, cols] += dot(inner[N0], wd[N0, :, cols], NN)

    @pl.when(i == n - N1)
    def _():
        unit, scale = standard(ALPHA * hidden[:].astype(F32) + acc[:] + b_down)
        g = cot[:].astype(F32)
        d_y = standard_grad(g * gain2, unit, scale)
        sums[pl.ds(N2 * n + 3, N1), :] = over_rows(d_y)
        sums[pl.ds(N2 * n + 4, N1), :] = over_rows(g * unit)
        d_ffn[:] = d_y.astype(BF)
        acc[:] = ALPHA * d_y

    @pl.when(i >= n)
    def _():
        for lo in tiles:
            cols = pl.ds(lo, tile)
            d_inner = dot(d_ffn[:], wd[N0, cols, :], NT).astype(BF).astype(F32)
            g, l = gate[t, :, cols], lin[t, :, cols]
            cdf = 0.5 * (1.0 + lax.erf(g * 0.5 ** 0.5))
            slope = cdf + g * (jnp.exp(-0.5 * g * g) * (N2 * np.pi) ** -0.5)
            d_l = d_inner * (g * cdf)
            d_g = d_inner * l * slope
            sums[pl.ds(t, N1), cols] = over_rows(d_g)
            sums[pl.ds(n + t, N1), cols] = over_rows(d_l)
            d_gate[N0, :, cols] = d_g.astype(BF)
            d_lin[N0, :, cols] = d_l.astype(BF)
        for lo in tiles:
            cols = pl.ds(lo, tile)
            acc[:, cols] += dot(d_gate[N0], wg[N0, cols, :], NT) + dot(d_lin[N0], wl[N0, cols, :], NT)

    @pl.when(i == N2 * n - N1)
    def _():
        d_h, unit = acc[:], unit1[:]
        d_x = standard_grad(d_h * gain1, unit, scale1[:])
        sums[pl.ds(N2 * n, N1), :] = over_rows(d_x)
        sums[pl.ds(N2 * n + N1, N1), :] = over_rows(d_h * unit)
        sums[pl.ds(N2 * n + N2, N1), :] = over_rows(d_h)
        resid[:] = ALPHA * d_x
        d_attn[:] = d_x.astype(BF)
        for h in range(n):
            d_ctx[h] = dot(d_attn[:], wo[h], NT)


def layer(ctx, wo, emb, cot, vectors, gate_bias, lin_bias, wg, wl, wd):
    n, own, dims = ctx.shape
    width = emb.shape[N1]
    ffn = wg.shape[N2]
    once = pl.BlockSpec(memory_space=pltpu.VMEM)
    weight = [pl.BlockSpec((N1,) + w.shape[N1:], lambda i: (i % n, N0, N0)) for w in (wg, wl, wd)]
    early = pl.BlockSpec((N1, own, ffn), lambda i: (jnp.minimum(i, n - N1), N0, N0))
    late = pl.BlockSpec((N1, own, ffn), lambda i: (jnp.maximum(i - n, N0), N0, N0))
    shape = jax.ShapeDtypeStruct
    slots = shape((n, own, ffn), BF)
    return pl.pallas_call(
        functools.partial(layer_kernel, n),
        name='layer',
        grid=(N2 * n,),
        in_specs=[once] * 7 + weight,
        out_specs=[once] * 6 + [early, late, late],
        out_shape=[shape((own, width), BF)] * 3 + [shape((own, width), F32), shape((n, own, dims), F32), shape((N2 * n + 8, width), F32), slots, slots, slots],
        scratch_shapes=[pltpu.VMEM((n, own, ffn), F32)] * N2 + [pltpu.VMEM((own, width), F32)] * N2 + [pltpu.VMEM((own, N1), F32)],
        compiler_params=pltpu.CompilerParams(dimension_semantics=('arbitrary',), vmem_limit_bytes=62 * N2 ** 20),
        cost_estimate=pl.CostEstimate(flops=15 * 10 ** 9, bytes_accessed=70 * N2 ** 20, transcendentals=N0),
    )(ctx, wo, emb, cot, vectors, gate_bias, lin_bias, wg, wl, wd)


def solution(mesh):
    n_tp, n_dp = mesh.shape['tp'], mesh.shape['dp']
    in_specs = (P('dp', None), P('dp', None, None), P('tp', None)) + WEIGHT_SPECS
    out_specs = (P('tp', None),) + WEIGHT_SPECS

    def device_step(tokens, cotangent, emb_table, *weights):
        (w_qkv, b_qkv, w_out, b_out, ln1_gain, ln1_bias, w_gate, b_gate, w_lin, b_lin, w_down, b_down, ln2_gain) = weights
        tp, dp = lax.axis_index('tp'), lax.axis_index('dp')
        tokens = tokens[N0]
        seq_len, width = tokens.shape[N0], emb_table.shape[N1]
        heads, head_dim = b_qkv.shape[N0], b_qkv.shape[N1] // 3
        own = seq_len // n_tp
        ffn = w_gate.shape[N1]
        rk, rf, ro = width // n_dp, ffn // n_dp, w_out.shape[N0] // n_dp

        def cut(weight):
            rows = weight.shape[N0] // n_dp
            return lax.dynamic_slice_in_dim(weight, dp * rows, rows, N0)
        bias_rows = jnp.concatenate([b_gate[None], b_lin[None], jnp.zeros((14, ffn), BF)], axis=N0)
        piece = jnp.concatenate([cut(w_gate), cut(w_lin), cut(w_down), cut(w_out), bias_rows], axis=N0).astype(F32)

        vocab_loc = emb_table.shape[N0]
        local_ids = tokens - tp * vocab_loc
        in_shard = (local_ids >= N0) & (local_ids < vocab_loc)
        safe_ids = jnp.where(in_shard, local_ids, N0)
        found = jnp.take(emb_table, safe_ids, axis=N0, mode='clip')
        dims = heads * head_dim
        place = column_order(heads, head_dim)
        swap = (jnp.arange(3 * dims)[:, None] == jnp.asarray(place)[None, :]).astype(BF)
        wq = jnp.dot(w_qkv, swap, preferred_element_type=F32).astype(BF)
        bq = jnp.dot(b_qkv.reshape(N1, -N1), swap, preferred_element_type=F32)
        cos_tab, sin_tab = rope_tables(seq_len, head_dim, heads)
        emb_bf, (wg_full, wl_full, wd_full, wo_full), biases, tok_all, ctx_own, saved = embed(found, in_shard[:, None].astype(F32), piece, tokens.reshape(-N1, min(128, seq_len // 8)), (w_gate, w_lin, w_down, w_out), wq, bq, cos_tab, sin_tab, heads, n_tp, n_dp)
        is_own = (jnp.arange(n_tp) == tp)[:, None]
        bg_full, bl_full = [jnp.where(is_own, b[None].astype(F32), biases[:, i]) for i, b in enumerate((b_gate, b_lin))]

        blocks = 8

        def owned(values):
            return lax.dynamic_index_in_dim(values.reshape(blocks, n_tp, -N1, width), tp, N1, keepdims=False).reshape(own, width)
        emb_own, cot_own = owned(emb_bf), owned(cotangent[N0])
        vectors = jnp.stack([b_out, ln1_gain, ln1_bias, b_down, ln2_gain] + [b_out] * 3).astype(F32)
        hidden, d_ffn_bf, d_attn_bf, resid, d_ctx, row_sums, inner_act, d_gate_bf, d_lin_bf = layer(
            ctx_own.reshape(n_tp, own, dims), wo_full, emb_own, cot_own, vectors, bg_full, bl_full, wg_full, wl_full, wd_full)

        def product(lhs, rhs, spec):
            return jnp.einsum(spec, lhs, rhs, preferred_element_type=F32).reshape(n_tp, n_dp, -N1, width)

        prod_down = product(inner_act, d_ffn_bf, 'tsc,sd->tcd')
        prod_gate = product(hidden, d_gate_bf, 'sk,tsc->tkc')
        prod_lin = product(hidden, d_lin_bf, 'sk,tsc->tkc')
        d_w_out = jnp.einsum('hse,sd->hed', ctx_own.reshape(n_tp, own, dims).astype(BF), d_attn_bf, preferred_element_type=F32)
        d_w_qkv, d_b_qkv, d_cols, (d_w_gate, d_w_lin), d_w_down = backward(
            d_ctx.reshape(n_tp, blocks, own // blocks, dims), resid.reshape(blocks, own // blocks, width), saved, cos_tab, sin_tab, wq, swap.T, emb_bf,
            (prod_gate, prod_lin, prod_down), heads, n_tp, n_dp)
        d_w_gate, d_w_lin = d_w_gate.reshape(-N1, ffn), d_w_lin.reshape(-N1, ffn)
        d_b_qkv = jnp.dot(d_b_qkv, swap.astype(F32).T, precision=lax.Precision.HIGHEST)
        all_ids = tok_all.reshape(-N1) - tp * vocab_loc
        all_ids = jnp.where((all_ids >= N0) & (all_ids < vocab_loc), all_ids, vocab_loc)
        col = table_rows(all_ids, d_cols.reshape(n_dp * seq_len, -N1), vocab_loc)

        slot = (jnp.arange(n_tp) == tp).astype(F32)[:, None]
        d_bq_rows = jnp.pad(slot * d_b_qkv, ((N0, N0), (N0, ffn - 3 * dims)))
        kept = N2 * n_tp
        small = jnp.concatenate([row_sums[:kept], d_bq_rows, row_sums[kept:kept + 5], jnp.zeros((7, width), F32)], axis=N0)
        d_table, d_w_down, d_w_out, d_w_qkv, small = finish(
            col, d_w_down, d_w_out.reshape(n_tp, n_dp, N2, -N1, width), d_w_qkv.reshape(n_dp, N2, -N1, 3 * dims), small, n_tp, n_dp)
        d_b_gate = lax.dynamic_index_in_dim(small[:n_tp], tp, N0, keepdims=False)
        d_b_lin = lax.dynamic_index_in_dim(small[n_tp:N2 * n_tp], tp, N0, keepdims=False)
        d_b_qkv = lax.dynamic_index_in_dim(small[N2 * n_tp:3 * n_tp], tp, N0, keepdims=False)[:3 * dims].reshape(heads, 3 * head_dim)
        d_b_out, d_ln1_gain, d_ln1_bias, d_b_down, d_ln2_gain = [small[3 * n_tp + i] for i in range(5)]
        return (d_table, d_w_qkv, d_b_qkv, d_w_out, d_b_out, d_ln1_gain, d_ln1_bias, d_w_gate, d_b_gate, d_w_lin, d_b_lin, d_w_down, d_b_down, d_ln2_gain)

    return jax.shard_map(device_step, mesh=mesh, in_specs=in_specs, out_specs=out_specs, check_vma=False)
```

```python
import functools

import jax
import jax.numpy as jnp
import numpy as np
from jax import lax
from jax.experimental import pallas as pl
from jax.experimental.pallas import tpu as pltpu
from jax.sharding import PartitionSpec as P

ALPHA = 140.0 ** 0.5
EPS = 1e-5
SHRINK = 0.1
ROPE_BASE = 10000.0
WEIGHT_SPECS = (P(None, 'tp'), P('tp', None), P('tp', None), P(), P(), P(), P(None, 'tp'), P('tp'), P(None, 'tp'), P('tp'), P('tp', None), P(), P())
BF = jnp.bfloat16
N0, N1, N2 = range(3)
F32 = jnp.float32
MESH = pl.DeviceIdType.MESH
ANY = pl.BlockSpec(memory_space=pl.ANY)
VMEM = pl.BlockSpec(memory_space=pltpu.VMEM)


def rope_tables(seq_len, head_dim, heads):
    half_dim = head_dim // 2
    inv_freq = (ROPE_BASE ** (-2.0 * np.arange(half_dim) / head_dim)).astype(np.float32)
    angles = np.arange(seq_len, dtype=np.float32)[:, None] * inv_freq[None, :]
    return [jnp.asarray(np.tile(table(angles), (1, heads))) for table in (np.cos, np.sin)]


def column_order(heads, head_dim):
    cols = np.arange(3 * heads * head_dim).reshape(heads, 3, 2, head_dim // 2)
    return np.concatenate([cols[:, part].transpose(1, 0, 2).ravel() for part in (0, 1)] + [cols[:, 2].ravel()])


def rcopy(src, dst, send, recv, **where):
    return pltpu.make_async_remote_copy(src_ref=src, dst_ref=dst, send_sem=send, recv_sem=recv, device_id=dict(where), device_id_type=MESH)


def plane():
    p = lax.axis_index('dp')
    y, x, c = p // 4, (p // 2) % 2, p % 2

    def at(rel):
        yy = 1 - y if rel & 4 else y
        xx = 1 - x if rel & 2 else x
        cc = 1 - c if rel & 1 else c
        return yy * 4 + xx * 2 + cc
    return p, at


def entry_barrier(z, n, at):
    bar = pltpu.get_barrier_semaphore()
    for rel in range(1, 8):
        pl.semaphore_signal(bar, inc=1, device_id={'dp': at(rel)}, device_id_type=MESH)
    for d in range(1, n):
        pl.semaphore_signal(bar, inc=1, device_id={'tp': (z + d) % n}, device_id_type=MESH)
    pl.semaphore_wait(bar, 7 + n - 1)


LAG = 3


def chain_sum(k, z, n, rows, chunks, part, left, right, done, send_r, send_l, recv_l, recv_r, place=lambda c: c):
    last = n - 1

    def at_rows(c):
        return pl.ds(pl.multiple_of(place(c) * rows, rows), rows)

    def cut(ref, c):
        return ref.at[at_rows(c)]

    def load(ref, c):
        return ref[at_rows(c)]

    def store(ref, c, value):
        ref[at_rows(c)] = value
    cl, cr = k - LAG * z, k - LAG * (last - z)
    okl, okr = (cl >= 0) & (cl < chunks), (cr >= 0) & (cr < chunks)

    @pl.when(okl & (z > 0))
    def _():
        rcopy(cut(left, cl), cut(left, cl), send_r, recv_l.at[cl], tp=z).wait_recv()

    @pl.when(okl & (z == last))
    def _():
        done(cl, load(left, cl) + load(part, cl))

    @pl.when(okl & (z > 0) & (z < last))
    def _():
        run = load(left, cl)

        @pl.when(z >= n // 2)
        def _():
            done(cl, run + load(right, cl))
        store(left, cl, run + load(part, cl))

    @pl.when(okr & (z < last))
    def _():
        rcopy(cut(right, cr), cut(right, cr), send_l, recv_r.at[cr], tp=z).wait_recv()

    @pl.when(okr & (z == 0))
    def _():
        done(cr, load(part, cr) + load(right, cr))

    @pl.when(okr & (z > 0) & (z < last))
    def _():
        run = load(right, cr)

        @pl.when(z < n // 2)
        def _():
            done(cr, load(left, cr) + run)
        store(right, cr, run + load(part, cr))

    @pl.when(okl & (z == 0))
    def _():
        rcopy(cut(part, cl), cut(left, cl), send_r, recv_l.at[cl], tp=z + 1).start()

    @pl.when(okl & (z > 0) & (z < last))
    def _():
        rcopy(cut(left, cl), cut(left, cl), send_r, recv_l.at[cl], tp=z + 1).start()

    @pl.when(okr & (z == last))
    def _():
        rcopy(cut(part, cr), cut(right, cr), send_l, recv_r.at[cr], tp=z - 1).start()

    @pl.when(okr & (z > 0) & (z < last))
    def _():
        rcopy(cut(right, cr), cut(right, cr), send_l, recv_r.at[cr], tp=z - 1).start()


def chain_drain(z, n, part, left, right, send_r, send_l, recv_l, recv_r):
    @pl.when(z < n - 1)
    def _():
        rcopy(part, left, send_r, recv_l.at[0], tp=z + 1).wait_send()

    @pl.when(z > 0)
    def _():
        rcopy(part, right, send_l, recv_r.at[0], tp=z - 1).wait_send()


EDGES = ((0, 0, 2), (0, 0, 4), (0, 0, 1), (2, 1, 4), (4, 2, 2), (2, 0, 1), (4, 0, 1), (6, 1, 1), (6, 2, 1))
CROSS, DIAGONAL, LAST = ((0, 3, 5), (1, 4, 6)), ((3, 7), (4, 8)), {1: (2,), 3: (5,), 5: (6,), 7: (7, 8)}
STEPS = (4, 10, 17, 21, 25, 29)
FIRST = 18
ORDER = (0, 2, 4, 1, 3, 5, 6, 7)


def emb_kernel(n, rows, chunks, cuts, heads, found, mask, wq, bq, cos, sin, piece, toks, *refs):
    m = len(cuts)
    local, outs = refs[:m], refs[m + N1:N2 * m + N1]
    out, (bias, tok_all, wall, ctx_own, q, k_all, v, ctx, top, inv, part, left, right, raw, low, weights, send_r, send_l, recv_l, recv_r, tsend, trecv, tself, zsend, zrecv, psend, precv, lsem, isem, osem, bsem, asend, arecv, aself) = refs[m], refs[N2 * m + N1:]
    blocks = 8
    qb = part.shape[N0] // blocks
    per = chunks // blocks
    z = lax.axis_index('tp')
    p, at = plane()
    entry_barrier(z, n, at)
    half = piece.shape[N0] // N2

    @pl.when(z < n - N1)
    def _():
        rcopy(piece, wall.at[z, p], zsend.at[z], zrecv.at[z], tp=z + N1).start()

    @pl.when(z > N0)
    def _():
        rcopy(piece, wall.at[z, p], bsem.at[N1], zrecv.at[z], tp=z - N1).start()
    mine = [pltpu.make_async_copy(toks, tok_all.at[p], tself)]
    mine += [pltpu.make_async_copy(src, dst.at[z], lsem.at[i]) for i, (src, dst) in enumerate(zip(local, outs))]
    for copy in mine:
        copy.start()
    for rel in range(N1, 8):
        rcopy(toks, tok_all.at[p], tsend.at[rel], trecv.at[rel], dp=at(rel)).start()

    def others(d, body):
        @pl.when(z >= d)
        def _():
            body(z - d, -N1)

        @pl.when(z + d < n)
        def _():
            body(z + d, N1)

    def region(t, rel, side):
        blk = wall.at[t, at(rel)]
        return blk if side == N0 else wall.at[t, at(rel), pl.ds((side - N1) * half, half)]

    def give(t, j):
        rel, side, to = EDGES[j]
        rcopy(region(t, rel, side), region(t, rel, side), psend.at[t, j], precv.at[t, j], dp=at(to)).start()

    def take(t, j):
        rel, side, to = EDGES[j]
        blk = region(t, rel ^ to, side)
        rcopy(blk, blk, psend.at[t, j], precv.at[t, j], dp=p).wait_recv()

    def gave(t, j):
        rel, side, to = EDGES[j]
        rcopy(region(t, rel, side), region(t, rel, side), psend.at[t, j], precv.at[t, j], dp=p).wait_send()

    def arrive(d):
        def body(t, sign):
            blk = wall.at[t, p]
            rcopy(blk, blk, zsend.at[t], zrecv.at[t], tp=z).wait_recv()

            @pl.when((z - sign >= N0) & (z - sign < n))
            def _():
                rcopy(blk, blk, zsend.at[t], zrecv.at[t], tp=z - sign).start()
            for j in range(3):
                give(t, j)
        others(d, body)

    def relay(d, moves):
        def body(t, sign):
            for first, *rest in moves:
                take(t, first)
                for j in rest:
                    give(t, j)
        others(d, body)

    k_all[:] = jnp.zeros_like(k_all)
    v[:] = jnp.zeros_like(v)
    arrive(N1)

    @pl.loop(N0, blocks)
    def _(i):
        at_i = pl.ds(pl.multiple_of(i * qb, qb), qb)
        part[at_i, :] = jnp.where(mask[at_i, :] > N0, found[at_i, :].astype(F32), 0.0)

    def done(c, value):
        out[pl.ds(pl.multiple_of(c * rows, rows), rows)] = value.astype(out.dtype)

    def other(i):
        return i + (i + n - z) // n

    def loaded(i, rel, slot):
        return pltpu.make_async_copy(wall.at[other(i), at(rel), pl.ds(N0, cuts[-N1][N1])], raw.at[slot], isem.at[slot])

    def stored(i, rel, slot):
        return [pltpu.make_async_copy(low.at[slot, pl.ds(lo, hi - lo)], dst.at[other(i), at(rel)], osem.at[slot, k]) for k, ((lo, hi), dst) in enumerate(zip(cuts, outs))]
    plan = [(i, rel) for rel in ORDER for i in range(n - N1)]

    def prefetch(s):
        i, rel = plan[s]
        for j in LAST.get(rel, ()):
            take(other(i), j)
        loaded(i, rel, s % N2).start()

    def convert(s):
        i, rel = plan[s]
        loaded(i, rel, s % N2).wait()
        if s >= N2:
            for copy in stored(*plan[s - N2], s % N2):
                copy.wait()
        low[s % N2] = raw[s % N2].astype(low.dtype)
        if s + N1 < len(plan):
            prefetch(s + N1)
        for copy in stored(i, rel, s % N2):
            copy.start()
    events = [(STEPS[d - N1], functools.partial(relay, d, CROSS)) for d in range(N1, n)] + [(STEPS[d + n - N2], functools.partial(relay, d, DIAGONAL)) for d in range(N1, n)]
    events += [(N2 * d - N2, functools.partial(arrive, d)) for d in range(N2, n)]
    events += [(FIRST - N1, functools.partial(prefetch, N0))] + [(FIRST + s, functools.partial(convert, s)) for s in range(len(plan))]

    start = per + LAG * (n - N1)

    share = qb // n

    def context(i, d):
        to = (z + d) % n
        src = ctx.at[pl.ds(pl.multiple_of(i * qb + to * share, share), share)]
        if d == N0:
            return pltpu.make_async_copy(src, ctx_own.at[z, i], aself)
        return rcopy(src, ctx_own.at[z, i], asend, arecv.at[z], tp=to)

    @pl.loop(N0, max(start + blocks * heads + N1, FIRST + len(plan)))
    def _(k):
        step = k - start
        i = step // heads - N1

        @pl.when((step > N0) & (step % heads == N0) & (step <= blocks * heads))
        def _():
            for d in range(n):
                context(i, d).start()
        chain_sum(k, z, n, rows, chunks, part, left, right, done, send_r, send_l, recv_l, recv_r)
        for at_step, event in events:
            pl.when(k == at_step)(event)

        @pl.when((step >= N0) & (step < blocks * heads))
        def _():
            @pl.when(step % heads == N0)
            def _():
                project(step // heads, qb, out, wq, bq, cos, sin, q, k_all, v)
            attend(step // heads, step % heads, heads, qb, q, k_all, v, ctx, top, inv, weights)

    pltpu.make_async_copy(ctx_own.at[z], ctx_own.at[z], aself).wait()
    for d in range(N1, n):
        src = (z + d) % n
        rcopy(ctx_own.at[src], ctx_own.at[src], asend, arecv.at[src], tp=z).wait()
    chain_drain(z, n, part, left, right, send_r, send_l, recv_l, recv_r)
    for s in (len(plan) - N2, len(plan) - N1):
        for copy in stored(*plan[s], s % N2):
            copy.wait()

    def finish(t, sign):
        for j in range(len(EDGES)):
            gave(t, j)
        tail = pltpu.make_async_copy(wall.at[t, p, pl.ds(cuts[-N1][N1], bias.shape[N1])], bias.at[t], bsem.at[N0])
        tail.start()
        tail.wait()

        @pl.when((z - sign >= N0) & (z - sign < n))
        def _():
            rcopy(wall.at[t, p], wall.at[t, p], zsend.at[t], zrecv.at[t], tp=z).wait_send()
    for d in range(N1, n):
        others(d, finish)
    for copy in mine:
        copy.wait()
    for rel in range(N1, 8):
        rcopy(toks, tok_all.at[at(rel)], tsend.at[rel], trecv.at[rel], dp=at(rel)).wait()

    @pl.when(z < n - N1)
    def _():
        rcopy(piece, wall.at[z, p], zsend.at[z], zrecv.at[z], tp=z + N1).wait_send()

    @pl.when(z > N0)
    def _():
        rcopy(piece, wall.at[z, p], bsem.at[N1], zrecv.at[z], tp=z - N1).wait_send()


def embed(found, mask, piece, toks, local, wq, bq, cos, sin, heads, n_tp, n_dp):
    seq, width = found.shape
    chunks = 32
    rows = seq // chunks
    dims = wq.shape[N1] // 3
    cuts, lo = [], N0
    for weight in local:
        cuts.append((lo, lo + weight.shape[N0] // n_dp))
        lo = cuts[-N1][N1]
    dma = pltpu.SemaphoreType.DMA
    shape = jax.ShapeDtypeStruct
    shapes = [shape((seq, width), BF)]
    shapes += [shape((n_tp, n_dp, w.shape[N0] // n_dp, w.shape[N1]), BF) for w in local]
    shapes += [shape((n_tp, piece.shape[N0] - lo, width), F32), shape((n_dp,) + toks.shape, toks.dtype), shape((n_tp, n_dp) + piece.shape, F32), shape((n_tp, 8, seq // n_tp // 8, dims), F32)]
    shapes += [shape((seq, dims), BF)] * 3 + [shape((seq, dims), F32)] + [shape((heads, seq), F32)] * N2
    out = pl.pallas_call(
        functools.partial(emb_kernel, n_tp, rows, chunks, cuts, heads),
        name='embed',
        out_shape=shapes,
        in_specs=[VMEM] * 6 + [ANY] * (N2 + len(local)),
        out_specs=[VMEM] + [ANY] * (4 + len(local)) + [VMEM] * 6,
        scratch_shapes=[pltpu.VMEM((seq, width), F32)] * 3 + [pltpu.VMEM((N2, lo, width), F32), pltpu.VMEM((N2, lo, width), BF), pltpu.VMEM((seq, seq // 8), F32), dma, dma, dma((chunks,)), dma((chunks,)),
                        dma((8,)), dma((8,)), dma, dma((n_tp,)), dma((n_tp,)), dma((n_tp, len(EDGES))), dma((n_tp, len(EDGES))), dma((len(local),)), dma((N2,)), dma((N2, len(local))), dma((N2,)),
                        dma, dma((n_tp,)), dma],
        compiler_params=pltpu.CompilerParams(collective_id=N0, has_side_effects=True, vmem_limit_bytes=60 * N2 ** 20),
        cost_estimate=pl.CostEstimate(flops=20 * 10 ** 9, bytes_accessed=80 * N2 ** 20, transcendentals=N0),
    )(found, mask, wq, bq, cos, sin, piece, toks, *[w.reshape(n_dp, w.shape[N0] // n_dp, w.shape[N1]) for w in local])
    m = N1 + len(local)
    return out[N0], [w.reshape(n_tp, -N1, w.shape[3]) for w in out[N1:m]], out[m], out[m + N1], out[m + 3], out[m + 4:]


RING = 4
HOLD, LIVE, PAIR = 4, 12, 4
ADD, LOAD, CROSSED, LAND, PLANE, HOP, BEAT = 1, 4, 5, 9, 10, 2, 4
GATHER = (37, 41)


def block_of(ref, at, rel, side):
    return ref.at[at(rel)] if side == 0 else ref.at[at(rel), side - 1]


class Spread:
    def __init__(self, at, block, send, recv, own=None):
        self.at, self.block, self.send, self.recv, self.own = at, block, send, recv, own

    def copy(self, j, rel, side, to):
        dst = self.block(rel, side)
        src = self.own if rel == 0 and self.own is not None else dst
        return rcopy(src, dst, self.send.at[j], self.recv.at[j], dp=self.at(to))

    def give(self, j):
        self.copy(j, *EDGES[j]).start()

    def take(self, j):
        rel, side, to = EDGES[j]
        self.copy(j, rel ^ to, side, 0).wait_recv()

    def start(self):
        for j in range(3):
            self.give(j)

    def relay(self, moves):
        for first, *rest in moves:
            self.take(first)
            for j in rest:
                self.give(j)

    def cross(self):
        self.relay(CROSS)

    def diagonal(self):
        self.relay(DIAGONAL)

    def finish(self):
        for j in (2, 5, 6, 7, 8):
            self.take(j)
        for j, (rel, side, _) in enumerate(EDGES):
            self.copy(j, rel, side, 0).wait_send()


def backward_kernel(n, rows, chunks, jobs, heads, d_ctx, resid, q, k_all, v, ctx, top, inv, cos, sin, wq, back, emb, *refs):
    prods = refs[:jobs]
    whole = refs[jobs:N2 * jobs - N1]
    out, grads, d_w, d_bias, landed, cross, last, part, left, right, total, dctx, dq, dk, dv, ctx_in, res_in, cos_in, sin_in, emb_in, q_in, work, fresh, xin, yin, keep, pass_on, along, final, *sems = refs[N2 * jobs - N1:]
    send_r, send_l, recv_l, recv_r, osend, orecv, csend, crecv, esem, fsem, xsend, xrecv, xsem, ysend, yrecv, ysem, ksem, zrecv, frecv, asend, arecv, aself, isem, gsend, grecv = sems
    z = lax.axis_index('tp')
    p, at = plane()
    entry_barrier(z, n, at)
    blocks = 8
    per = chunks // blocks
    qb = rows * per
    share = qb // n
    block = out.shape[N2]
    lead = jnp.maximum(z, n - N1 - z)
    span = N2 * n
    units = jobs * span
    size = work.shape[N2]

    def rows_of(i, to, count):
        return pl.ds(pl.multiple_of(i * qb + to * count, count), count)

    def exchange(i, d):
        to = (z + d) % n
        dst = dctx.at[rows_of(i, z, share)]
        if d == N0:
            return pltpu.make_async_copy(d_ctx.at[z, i], dst, aself.at[i])
        return rcopy(d_ctx.at[to, i], dst, asend, arecv.at[i], tp=to)

    @pl.loop(N0, blocks)
    def _(b):
        for d in range(n):
            exchange(blocks - N1 - b, d).start()

    def piece(m, u, rel):
        return prods[m].at[(u % span) // N2, at(rel), pl.ds(pl.multiple_of((u % N2) * size, size), size)]

    for m in range(jobs):
        @pl.loop(m * span, (m + N1) * span)
        def _(u, m=m):
            for i in range(4):
                rcopy(piece(m, u, N2 * i + N1), landed.at[u, i], csend, crecv.at[u], dp=at(N1)).start()

    def inputs(i):
        slot = i % N2
        at_q = rows_of(i, N0, qb)
        pairs = ((ctx.at[at_q], ctx_in), (resid.at[i], res_in), (cos.at[at_q], cos_in), (sin.at[at_q], sin_in), (emb.at[at_q], emb_in), (q.at[at_q], q_in))
        return [pltpu.make_async_copy(src, dst.at[slot], isem.at[j, slot]) for j, (src, dst) in enumerate(pairs)]

    dk[:] = jnp.zeros_like(dk)
    dv[:] = jnp.zeros_like(dv)
    d_w[:] = jnp.zeros_like(d_w)
    d_bias[:] = jnp.zeros_like(d_bias)
    for copy in inputs(blocks - N1):
        copy.start()

    def attention_step(b, h):
        i = blocks - N1 - b

        @pl.when(h == N0)
        def _():
            for copy in inputs(i):
                copy.wait()

            @pl.when(b + N1 < blocks)
            def _():
                for copy in inputs(i - N1):
                    copy.start()
            exchange(i, N0).wait()
            others = dctx.at[pl.ds(N0, (n - N1) * share)]
            rcopy(others, others, asend, arecv.at[i], tp=z).wait_recv()
        attend_grad(i, h, heads, qb, q_in.at[i % N2], k_all, v, ctx_in.at[i % N2], dctx, top, inv, dq, dk, dv)

        @pl.when(h == heads - N1)
        def _():
            slot = i % N2
            got = grad_rows(i, qb, cos_in[slot], sin_in[slot], dq, dk, dv, d_bias)
            d_w[:] += dot(emb_in[slot], dot(got, back[:], NN).astype(BF), TN)
            part[rows_of(i, N0, qb), :] = dot(got, wq[:], NT)
            part[rows_of(i, z, share), :] = part[rows_of(i, z, share), :] + res_in[i % N2]

    def sides(u):
        side = u % N2
        return side, at(N2) * (N1 - side) + at(4) * side, at(4) * (N1 - side) + at(N2) * side

    def fetch(u):
        slot = u % HOLD

        @pl.when(u >= HOLD)
        def _():
            rcopy(xin, cross.at[N0], xsend.at[slot], xrecv.at[N0], dp=p).wait_send()
        for m in range(jobs):
            @pl.when(u // span == m)
            def _(m=m):
                for i in range(4):
                    pltpu.make_async_copy(piece(m, u, N2 * i), work.at[slot, i], esem.at[slot]).start()
        rcopy(landed.at[u], landed.at[u], csend, crecv.at[u], dp=p).wait_recv()
        pltpu.make_async_copy(landed.at[u], fresh, fsem).start()

    def add(u):
        slot = u % HOLD
        pltpu.make_async_copy(landed.at[u], work.at[slot], esem.at[slot]).wait()
        pltpu.make_async_copy(landed.at[u], fresh, fsem).wait()
        for i in range(4):
            work[slot, i] = work[slot, i] + fresh[i]

    def add_send(u):
        slot = u % HOLD
        side, first, second = sides(u)
        rcopy(work.at[slot, N1 + side], cross.at[u, N0], xsend.at[slot], xrecv.at[u], dp=first).start()
        rcopy(work.at[slot, 3], cross.at[u, N1], xsend.at[slot], xrecv.at[u], dp=first).start()

    def load_cross(u):
        rcopy(cross.at[u], cross.at[u], xsend.at[N0], xrecv.at[u], dp=p).wait_recv()
        pltpu.make_async_copy(cross.at[u], xin, xsem).start()

    def crossed(u):
        slot = u % HOLD
        pltpu.make_async_copy(cross.at[u], xin, xsem).wait()

        @pl.when(u >= LIVE)
        def _():
            pltpu.make_async_copy(keep.at[u % LIVE], keep.at[u % LIVE], ksem.at[u % LIVE]).wait()

        @pl.when(u >= PAIR)
        def _():
            rcopy(pass_on.at[u % PAIR], last.at[u], ysend.at[u % PAIR], yrecv.at[u], dp=p).wait_send()
        keep[u % LIVE] = xin[N0] + work[slot, N0]
        pass_on[u % PAIR] = xin[N1] + work[slot, N2 - u % N2]

    def crossed_send(u):
        side, first, second = sides(u)
        rcopy(pass_on.at[u % PAIR], last.at[u], ysend.at[u % PAIR], yrecv.at[u], dp=second).start()

    def load_last(u):
        rcopy(last.at[u], last.at[u], ysend.at[N0], yrecv.at[u], dp=p).wait_recv()
        pltpu.make_async_copy(last.at[u], yin, ysem).start()

    def in_plane(u):
        pltpu.make_async_copy(last.at[u], yin, ysem).wait()
        keep[u % LIVE] = keep[u % LIVE] + yin[:]

    def unit(k):
        u = (k // BEAT) * (BEAT - N1) + k % BEAT
        return u, (k >= N0) & (k % BEAT < BEAT - N1) & (u < units)

    def along_tp(k, t, send):
        toward = jnp.where(z < t, z, n - N1 - z)
        late = HOP * jnp.where(z == t, max(t, n - N1 - t), toward)
        u, ok = unit(k - PLANE - N1 - late)
        mine = (u // span) * N2 + u % N2
        slot = u % LIVE
        ok = ok & ((u // N2) % n == t)

        def add_from(ref, sem):
            rcopy(ref, ref, csend, sem, tp=z).wait_recv()
            keep[slot] = keep[slot] + ref[:]
        if send:
            @pl.when(ok & (z < t))
            def _():
                rcopy(keep.at[slot], along.at[u], ksem.at[slot], zrecv.at[u], tp=z + N1).start()

            @pl.when(ok & (z > t + N1))
            def _():
                rcopy(keep.at[slot], along.at[u], ksem.at[slot], zrecv.at[u], tp=z - N1).start()

            @pl.when(ok & (z == t + N1))
            def _():
                rcopy(keep.at[slot], final.at[mine], ksem.at[slot], frecv.at[mine], tp=z - N1).start()

            for m in range(jobs):
                @pl.when(ok & (z == t) & (u // span == m))
                def _(m=m):
                    dst = whole[m].at[p, u % N2] if m < jobs - N1 else grads.at[u % N2]
                    pltpu.make_async_copy(keep.at[slot], dst, ksem.at[slot]).start()
        else:
            @pl.when(ok & (((z > N0) & (z <= t)) | ((z > t) & (z < n - N1))))
            def _():
                add_from(along.at[u], zrecv.at[u])
            if t < n - N1:
                @pl.when(ok & (z == t))
                def _():
                    add_from(final.at[mine], frecv.at[mine])

    spread = [Spread(at, functools.partial(block_of, whole[m], at), gsend.at[m], grecv.at[m]) for m in range(jobs - N1)]

    def settle(u):
        pltpu.make_async_copy(keep.at[u % LIVE], keep.at[u % LIVE], ksem.at[u % LIVE]).wait()

    def begin(m):
        for u in range(max(m * span, units - LIVE), (m + N1) * span):
            settle(u)
        spread[m].start()

    def place(c):
        return (blocks - N1 - c // per) * per + c % per

    def chunk(c):
        return total.at[c % RING]

    def done(c, value):
        @pl.when(c >= RING)
        def _():
            pltpu.make_async_copy(chunk(c), chunk(c), osend.at[c % RING]).wait()
        total[c % RING] = value

    def hand_out(c):
        where = out.at[p, pl.ds(pl.multiple_of(place(c) * rows, rows), rows)]
        for rel in range(8):
            src = total.at[c % RING, :, pl.ds(pl.multiple_of(at(rel) * block, block), block)]
            if rel == N0:
                pltpu.make_async_copy(src, where, osend.at[c % RING]).start()
            else:
                rcopy(src, where, osend.at[c % RING], orecv.at[rel], dp=at(rel)).start()

    def staged(k, offset, stage):
        u, ok = unit(k - offset)
        pl.when(ok)(functools.partial(stage, u))
    steps = max(heads + chunks + LAG * (n - N1) + N1, units // (BEAT - N1) * BEAT + PLANE + HOP * (n - N1), GATHER[-N1] + 7)

    @pl.loop(N0, steps)
    def _(k):
        c = k - heads - LAG * lead - N1

        @pl.when((c >= N0) & (c < chunks))
        def _():
            hand_out(c)
        chain_sum(k - heads, z, n, rows, chunks, part, left, right, done, send_r, send_l, recv_l, recv_r, place)
        for offset, stage in ((CROSSED, crossed), (ADD, add), (PLANE, in_plane)):
            staged(k, offset, stage)
        for t in range(n):
            along_tp(k, t, False)
        for offset, stage in ((N0, fetch), (LOAD, load_cross), (LAND, load_last)):
            staged(k, offset, stage)

        @pl.when(k < blocks * heads)
        def _():
            attention_step(k // heads, k % heads)
        for offset, stage in ((ADD, add_send), (CROSSED, crossed_send)):
            staged(k, offset, stage)
        for t in range(n):
            along_tp(k, t, True)
        for m, gather in enumerate(spread):
            for offset, stage in ((N0, functools.partial(begin, m)), (3, gather.cross), (6, gather.diagonal)):
                pl.when(k == GATHER[m] + offset)(stage)

    chain_drain(z, n, part, left, right, send_r, send_l, recv_l, recv_r)
    for c in range(max(N0, chunks - RING), chunks):
        pltpu.make_async_copy(chunk(c), chunk(c), osend.at[c % RING]).wait()
    for rel in range(N1, 8):
        rcopy(out.at[at(rel)], out.at[at(rel)], csend, orecv.at[rel], dp=p).wait_recv()
    for slot in range(HOLD):
        rcopy(xin, cross.at[N0], xsend.at[slot], xrecv.at[N0], dp=p).wait_send()
    for slot in range(PAIR):
        rcopy(pass_on.at[slot], last.at[N0], ysend.at[slot], yrecv.at[N0], dp=p).wait_send()
    for u in range(max((jobs - N1) * span, units - LIVE), units):
        settle(u)
    rcopy(landed, landed, csend, crecv.at[N0], dp=p).wait_send()
    for gather in spread:
        gather.finish()
    sent = dctx.at[pl.ds(N0, (n - N1) * share * blocks)]
    rcopy(sent, sent, asend, arecv.at[N0], tp=z).wait_send()


def backward(d_ctx, resid, saved, cos, sin, wq, back, emb, prods, heads, n_tp, n_dp):
    q, k, v, ctx, top, inv = saved
    seq, dims = q.shape
    width = wq.shape[N0]
    chunks = 32
    rows = seq // chunks
    jobs = len(prods)
    piece = (prods[N0].shape[N2] // N2, prods[N0].shape[3])
    units = jobs * N2 * n_tp
    dma = pltpu.SemaphoreType.DMA
    shape = jax.ShapeDtypeStruct
    qb = seq // 8
    vmem = [(seq, width)] * 3 + [(RING, rows, width), (seq, dims), (qb, dims), (seq, dims), (seq, dims), (N2, qb, dims), (N2, qb // n_tp, width)] + [(N2, qb, dims // N2)] * N2 + [
            (HOLD, 4) + piece, (4,) + piece, (N2,) + piece, piece, (LIVE,) + piece, (PAIR,) + piece, (units,) + piece, (N2 * jobs,) + piece]
    sems = [(), (), (chunks,), (chunks,), (RING,), (8,), (), (units,), (HOLD,), (), (HOLD,), (units,), (), (PAIR,), (units,), (), (LIVE,), (units,), (N2 * jobs,), (), (8,), (8,), (6, N2), (jobs - N1, len(EDGES)), (jobs - N1, len(EDGES))]
    scratch = [pltpu.VMEM(size, F32) for size in vmem]
    scratch[12:12] = [pltpu.VMEM((N2, qb, width), BF), pltpu.VMEM((N2, qb, dims), BF)]
    full = shape((n_dp, N2) + piece, F32)
    *whole, cols, grads, d_w, d_bias, _, _, _ = pl.pallas_call(
        functools.partial(backward_kernel, n_tp, rows, chunks, jobs, heads),
        name='backward',
        out_shape=[full] * (jobs - N1) + [shape((n_dp, seq, width // n_dp), F32), shape((N2,) + piece, F32), shape((width, 3 * dims), F32), shape((N1, 3 * dims), F32),
                   shape((units, 4) + piece, F32), shape((units, N2) + piece, F32), shape((units,) + piece, F32)],
        in_specs=[ANY] * 3 + [VMEM] * N2 + [ANY] + [VMEM] * N2 + [ANY] * N2 + [VMEM] * N2 + [ANY] * (N1 + jobs),
        out_specs=[ANY] * (jobs - N1) + [ANY, ANY, VMEM, VMEM, ANY, ANY, ANY],
        scratch_shapes=scratch + [dma(size) for size in sems],
        compiler_params=pltpu.CompilerParams(collective_id=N1, has_side_effects=True, vmem_limit_bytes=67_000_000),
        cost_estimate=pl.CostEstimate(flops=20 * 10 ** 9, bytes_accessed=100 * N2 ** 20, transcendentals=N0),
    )(d_ctx, resid, q, k, v, ctx, top, inv, cos, sin, wq, back, emb, *prods)
    return d_w, d_bias, cols, whole, grads


WAYS = 4


def table_kernel(ids, rows_ref, out, *tables):
    step = pl.program_id(0)
    count = rows_ref.shape[0]
    part = count // WAYS

    @pl.when(step == 0)
    def _():
        for table in tables:
            table[:] = jnp.zeros_like(table)

    @pl.loop(0, part, unroll=4)
    def _(r):
        for way, table in enumerate(tables):
            row = way * part + r
            where = pl.ds(ids[step * count + row], 1)
            table[where, :] = table[where, :] + rows_ref[pl.ds(row, 1), :]

    @pl.when(step == pl.num_programs(0) - 1)
    def _():
        total = tables[0][:]
        for table in tables[1:]:
            total = total + table[:]
        out[:] = SHRINK * total[:out.shape[0]]


def table_rows(ids, rows, vocab_loc):
    count, block = rows.shape
    step = min(1024, count // 2)
    return pl.pallas_call(
        table_kernel,
        name='table_rows',
        grid_spec=pltpu.PrefetchScalarGridSpec(
            num_scalar_prefetch=1,
            grid=(count // step,),
            in_specs=[pl.BlockSpec((step, block), lambda i, ids: (i, 0))],
            out_specs=pl.BlockSpec((vocab_loc, block), lambda i, ids: (0, 0)),
            scratch_shapes=[pltpu.VMEM((vocab_loc + 8, block), F32)] * WAYS,
        ),
        out_shape=jax.ShapeDtypeStruct((vocab_loc, block), F32),
        compiler_params=pltpu.CompilerParams(dimension_semantics=('arbitrary',), vmem_limit_bytes=48 * 2 ** 20),
        cost_estimate=pl.CostEstimate(flops=3 * 10 ** 9, bytes_accessed=16 * 2 ** 20, transcendentals=0),
    )(ids, rows)


class PlaneSum:
    def __init__(self, at, block, landed, work, cross, last, mine, sems):
        self.at, self.block, self.landed, self.work, self.cross, self.last, self.mine, self.sems = at, block, landed, work, cross, last, mine, sems

    def copy(self, src, dst, kind, side, rel):
        return rcopy(src, dst, self.sems.at[kind, side, N0], self.sems.at[kind, side, N1], dp=self.at(rel))

    def start(self):
        for i in range(4):
            self.copy(self.block(N2 * i + N1), self.landed.at[i], N0, N0, N1).start()

    def first(self):
        self.copy(self.landed, self.landed, N0, N0, N0).wait()
        for i in range(4):
            self.work[i] = self.block(N2 * i)[:] + self.landed[i]

    def first_send(self):
        for side in range(N2):
            self.copy(self.work.at[N1 + side, side], self.cross.at[side, N0], N1, side, N2 * (N1 + side)).start()
            self.copy(self.work.at[3, side], self.cross.at[side, N1], N1, side, N2 * (N1 + side)).start()

    def second(self):
        for side in range(N2):
            self.copy(self.cross.at[side], self.cross.at[side], N1, side, N0).wait()
            self.cross[side, N0] = self.cross[side, N0] + self.work[N0, side]
            self.cross[side, N1] = self.cross[side, N1] + self.work[N2 - side, side]

    def second_send(self):
        for side in range(N2):
            self.copy(self.cross.at[side, N1], self.last.at[side], N2, side, N2 * (N2 - side)).start()

    def end(self):
        for side in range(N2):
            self.copy(self.last.at[side], self.last.at[side], N2, side, N0).wait()
            self.mine[side] = self.cross[side, N0] + self.last[side]


def finish_kernel(n, cuts, col, down, proj, d_w, small, table, down_all, proj_all, qkv_all, total, *refs):
    scratch, (summed, inbox, arrived, sem, send, recv, dsend, drecv, osem, psem, zsem, rsem) = refs[:10], refs[10:]
    z = lax.axis_index('tp')
    p, at = plane()
    entry_barrier(z, n, at)
    block = col.shape[N1]
    half = len(cuts) // N2

    def part(i):
        def region(rel, side):
            return table.at[pl.ds(cuts[i][N0], cuts[i][N1] - cuts[i][N0]), pl.ds(pl.multiple_of(at(rel) * block, block), block)]
        return Spread(at, region, send.at[i], recv.at[i], col.at[pl.ds(cuts[i][N0], cuts[i][N1] - cuts[i][N0])])
    parts = [part(i) for i in range(len(cuts))]
    qkv_sum = PlaneSum(at, lambda rel: d_w.at[at(rel)], *scratch[:5], psem.at[N0])
    proj_sum = PlaneSum(at, lambda rel: summed.at[at(rel)], *scratch[5:], psem.at[N1])
    pairs = ((down, down_all), (proj_sum.mine, proj_all), (qkv_sum.mine, qkv_all))
    spread = [Spread(at, functools.partial(block_of, ref, at), dsend.at[i], drecv.at[i], own) for i, (own, ref) in enumerate(pairs)]
    own_copies = [pltpu.make_async_copy(col, table.at[:, pl.ds(pl.multiple_of(p * block, block), block)], osem.at[N0])]
    own_copies += [pltpu.make_async_copy(src, dst.at[p], osem.at[i]) for i, (src, dst) in enumerate(pairs, N1)]
    order = list(range(len(cuts)))
    flipped = order[half:] + order[:half]
    peers = [{'dp': at(N1)}, {'dp': at(N2)}, {'dp': at(4)}, {'tp': z + N1 - N2 * (z % N2)}, {'tp': (z + n // N2) % n}]

    def next_part(i):
        parts[order[i]].give(N0)
        parts[flipped[i]].give(N1)
        parts[order[i]].give(N2)

    def relay_part(i):
        one, two = order[i], flipped[i]
        parts[one].take(N0)
        if one < half:
            parts[one].give(3)
        parts[one].give(5)
        parts[two].take(N1)
        if two >= half:
            parts[two].give(4)
        parts[two].give(6)

    def exchange(r):
        return rcopy(total, inbox.at[r], rsem.at[N0, r], rsem.at[N1, r], **peers[r])

    def round_end(r):
        exchange(r).wait()
        total[:] = total[:] + inbox[r]

    total[:] = small[:]
    for d in range(N1, n):
        to = (z + d) % n
        rcopy(proj.at[to], arrived.at[z], zsem.at[N0, to], zsem.at[N1, z], tp=to).start()
    qkv_sum.start()
    for copy in own_copies[:N2]:
        copy.start()
    next_part(N0)
    exchange(N0).start()
    spread[N0].start()
    next_part(N1)
    qkv_sum.first()
    round_end(N0)
    qkv_sum.first_send()
    exchange(N1).start()
    next_part(N2)
    relay_part(N0)
    round_end(N1)
    qkv_sum.second()
    exchange(N2).start()
    qkv_sum.second_send()
    next_part(3)
    spread[N0].cross()
    relay_part(N1)
    round_end(N2)
    qkv_sum.end()
    exchange(3).start()
    next_part(4)
    spread[N2].start()
    own_copies[3].start()
    spread[N0].diagonal()
    relay_part(N2)
    summed[:] = proj[z]
    for d in range(N1, n):
        src = (z + d) % n
        rcopy(proj.at[src], arrived.at[src], zsem.at[N0, src], zsem.at[N1, src], tp=src).wait()
        summed[:] = summed[:] + arrived[src]
    round_end(3)
    next_part(5)
    exchange(4).start()
    proj_sum.start()
    relay_part(3)
    spread[N2].cross()
    proj_sum.first()
    next_part(6)
    proj_sum.first_send()
    round_end(4)
    relay_part(4)
    proj_sum.second()
    next_part(7)
    proj_sum.second_send()
    spread[N2].diagonal()
    relay_part(5)
    proj_sum.end()
    relay_part(6)
    spread[N1].start()
    own_copies[N2].start()
    relay_part(7)
    spread[N1].cross()
    spread[N1].diagonal()
    for i in range(half):
        for via, where in ((3, i), (4, i + half)):
            parts[where].take(via)
            parts[where].give(7)
    for i in order:
        for j in (N2, 5, 6, 7):
            parts[i].take(j)
        for j in (N0, N1, N2, 3 if i < half else 4, 5, 6, 7):
            parts[i].copy(j, *EDGES[j]).wait_send()
    for gather in spread:
        gather.finish()
    for copy in own_copies:
        copy.wait()


def finish(col, down, proj, d_w, small, n_tp, n_dp):
    size, block = col.shape
    tiles = size // 8
    cuts = [(8 * (tiles * i // 8), 8 * (tiles * (i + N1) // 8)) for i in range(8)]
    dma = pltpu.SemaphoreType.DMA
    shape = jax.ShapeDtypeStruct
    ours = (d_w.shape[N1:], proj.shape[N2:])
    kinds = len(EDGES)
    vmem = [lead + src[N1:] for src in ours for lead in ((4, N2), (4, N2), (N2, N2), (N2,), (N2,))] + [proj.shape[N1:], (5,) + small.shape, proj.shape]
    sems = [(), (8, kinds), (8, kinds), (3, kinds), (3, kinds), (4,), (N2, 3, N2, N2), (N2, n_tp), (N2, 5)]
    table, down_all, proj_all, qkv_all, total = pl.pallas_call(
        functools.partial(finish_kernel, n_tp, cuts),
        name='finish',
        out_shape=[shape((size, n_dp * block), F32)] + [shape((n_dp,) + src, F32) for src in (down.shape, ours[N1], ours[N0])] + [shape(small.shape, F32)],
        in_specs=[ANY] * N2 + [VMEM] * 3,
        out_specs=[ANY] * 4 + [VMEM],
        scratch_shapes=[pltpu.VMEM(dims, F32) for dims in vmem] + [dma(dims) for dims in sems],
        compiler_params=pltpu.CompilerParams(collective_id=N2, has_side_effects=True, vmem_limit_bytes=48 * N2 ** 20),
        cost_estimate=pl.CostEstimate(flops=10 * 10 ** 9, bytes_accessed=60 * N2 ** 20, transcendentals=N0),
    )(col, down, proj, d_w, small)
    return [table] + [grad.reshape(-N1, grad.shape[3]) for grad in (down_all, proj_all, qkv_all)] + [total]


def dot(a, b, dims):
    return lax.dot_general(a, b, (dims, ((), ())), preferred_element_type=F32)


NT, TN, NN = ((1,), (1,)), ((0,), (0,)), ((1,), (0,))


def lane_head(shape, heads, halves):
    lane = lax.broadcasted_iota(jnp.int32, shape, 1)
    dims = shape[1] // halves
    return (lane % dims) // (dims // heads)


def turned(both, cos, sin):
    half = both.shape[1] // 2
    x1, x2 = both[:, :half], both[:, half:]
    return jnp.concatenate([x1 * cos - x2 * sin, x2 * cos + x1 * sin], axis=1)


def project(i, qb, emb, wq, bq, cos, sin, q, k, v):
    at_q = pl.ds(pl.multiple_of(i * qb, qb), qb)
    dims = q.shape[1]
    qkv = (dot(emb[at_q, :], wq[:], NN) + bq[:]).astype(BF)
    for ref, part in ((q, 0), (k, 1)):
        ref[at_q, :] = turned(qkv[:, part * dims:(part + 1) * dims].astype(F32), cos[at_q, :], sin[at_q, :]).astype(BF)
    v[at_q, :] = qkv[:, 2 * dims:]


def scores(i, j, kb, qb, scale, keys, q):
    s = dot(keys, q, NT) * scale
    key = j * kb + lax.broadcasted_iota(jnp.int32, (kb, qb), 0)
    query = i * qb + lax.broadcasted_iota(jnp.int32, (kb, qb), 1)
    return jnp.where(query >= key, s, -1e30)


def attend(i, h, heads, qb, q_ref, k_ref, v_ref, ctx_ref, top_ref, inv_ref, s_ref):
    kb = 2 * qb
    dims = q_ref.shape[1]
    scale = (dims // heads) ** -0.5
    at_q = pl.ds(pl.multiple_of(i * qb, qb), qb)
    q = jnp.where(lane_head((qb, dims), heads, 2) == h, q_ref[at_q, :].astype(F32), 0.0).astype(BF)
    count = (i + 2) // 2

    def at_key(j):
        return pl.ds(pl.multiple_of(j * kb, kb), kb)

    def first(j, top):
        s = scores(i, j, kb, qb, scale, k_ref[at_key(j), :], q)
        s_ref[at_key(j), :] = s
        return jnp.maximum(top, jnp.max(s, axis=0, keepdims=True))
    top = lax.fori_loop(0, count, first, jnp.full((1, qb), -1e30, F32))

    def weigh(j, total):
        e = jnp.exp(s_ref[at_key(j), :] - top)
        s_ref[at_key(j), :] = e
        return total + jnp.sum(e, axis=0, keepdims=True)
    inv = 1.0 / lax.fori_loop(0, count, weigh, jnp.zeros((1, qb), F32))

    def mix(j, acc):
        return acc + dot((s_ref[at_key(j), :] * inv).astype(BF), v_ref[at_key(j), :], TN)
    mixed = lax.fori_loop(0, count, mix, jnp.zeros((qb, dims), F32))
    ctx_ref[at_q, :] = jnp.where(lane_head((qb, dims), heads, 1) == h, mixed, ctx_ref[at_q, :])
    top_ref[pl.ds(h, 1), at_q] = top
    inv_ref[pl.ds(h, 1), at_q] = inv


def attend_grad(i, h, heads, qb, q_ref, k_ref, v_ref, ctx_ref, dctx_ref, top_ref, inv_ref, dq_ref, dk_ref, dv_ref):
    kb = 2 * qb
    dims = dk_ref.shape[1]
    scale = (dims // heads) ** -0.5
    at_q = pl.ds(pl.multiple_of(i * qb, qb), qb)
    q = jnp.where(lane_head((qb, dims), heads, 2) == h, q_ref[:].astype(F32), 0.0).astype(BF)
    dc = jnp.where(lane_head((qb, dims), heads, 1) == h, dctx_ref[at_q, :], 0.0).astype(BF)
    ones = jnp.ones((8, dims), F32)
    mean = lax.dot_general(ones, dc.astype(F32) * ctx_ref[:], (NT, ((), ())), precision=lax.Precision.HIGHEST, preferred_element_type=F32)[:1]
    top, inv = top_ref[pl.ds(h, 1), at_q], inv_ref[pl.ds(h, 1), at_q]

    def step(j, dq):
        at_k = pl.ds(pl.multiple_of(j * kb, kb), kb)
        keys = k_ref[at_k, :]
        probs = (jnp.exp(scores(i, j, kb, qb, scale, keys, q) - top) * inv).astype(BF)
        ds = (probs.astype(F32) * (dot(v_ref[at_k, :], dc, NT) - mean) * scale).astype(BF)
        dv_ref[at_k, :] += dot(probs, dc, NN)
        dk_ref[at_k, :] += dot(ds, q, NN)
        return dq + dot(ds, keys, TN)
    dq = lax.fori_loop(0, (i + 2) // 2, step, jnp.zeros((qb, dims), F32))
    dq_ref[:] = jnp.where(lane_head((qb, dims), heads, 2) == h, dq, dq_ref[:])


def grad_rows(i, qb, cos, sin, dq, dk, dv, d_bias):
    at_q = pl.ds(pl.multiple_of(i * qb, qb), qb)
    back = [turned(values, cos, -sin) for values in (dq[:], dk[at_q, :])]
    rows = jnp.concatenate(back + [dv[at_q, :]], axis=1)
    d_bias[:] += jnp.sum(rows, axis=0, keepdims=True)
    return rows.astype(BF)


def standard(values):
    mean = jnp.mean(values, axis=1, keepdims=True)
    centered = values - mean
    scale = lax.rsqrt(jnp.mean(centered * centered, axis=1, keepdims=True) + EPS)
    return centered * scale, scale


def standard_grad(d_out, unit, scale):
    return scale * (d_out - jnp.mean(d_out, axis=1, keepdims=True) - unit * jnp.mean(d_out * unit, axis=1, keepdims=True))


def over_rows(values):
    return jnp.sum(values, axis=0, keepdims=True)


def layer_kernel(n, ctx, wo, emb, cot, vectors, gate_bias, lin_bias, wg, wl, wd, hidden, d_ffn, d_attn, resid, d_ctx, sums, inner, d_gate, d_lin, gate, lin, acc, unit1, scale1):
    i = pl.program_id(N0)
    t = i % n
    tile = 256 if acc.shape[N1] % 256 == N0 else acc.shape[N1]
    tiles = range(N0, acc.shape[N1], tile)
    b_out, gain1, bias1, b_down, gain2 = [vectors[pl.ds(j, N1), :] for j in range(5)]

    @pl.when(i == N0)
    def _():
        total = ALPHA * emb[:].astype(F32) + b_out
        for h in range(n):
            total = total + dot(ctx[h].astype(BF), wo[h], NN)
        unit, scale1[:] = standard(total)
        unit1[:] = unit
        hidden[:] = (unit * gain1 + bias1).astype(BF)
        acc[:] = jnp.zeros_like(acc)

    @pl.when(i < n)
    def _():
        for lo in tiles:
            cols = pl.ds(lo, tile)
            g = dot(hidden[:], wg[N0, :, cols], NN) + gate_bias[pl.ds(t, N1), cols]
            l = dot(hidden[:], wl[N0, :, cols], NN) + lin_bias[pl.ds(t, N1), cols]
            gate[t, :, cols] = g
            lin[t, :, cols] = l
            inner[N0, :, cols] = (0.5 * g * (1.0 + lax.erf(g * 0.5 ** 0.5)) * l).astype(BF)
        for lo in tiles:
            cols = pl.ds(lo, tile)
            acc[:, cols] += dot(inner[N0], wd[N0, :, cols], NN)

    @pl.when(i == n - N1)
    def _():
        unit, scale = standard(ALPHA * hidden[:].astype(F32) + acc[:] + b_down)
        g = cot[:].astype(F32)
        d_y = standard_grad(g * gain2, unit, scale)
        sums[pl.ds(N2 * n + 3, N1), :] = over_rows(d_y)
        sums[pl.ds(N2 * n + 4, N1), :] = over_rows(g * unit)
        d_ffn[:] = d_y.astype(BF)
        acc[:] = ALPHA * d_y

    @pl.when(i >= n)
    def _():
        for lo in tiles:
            cols = pl.ds(lo, tile)
            d_inner = dot(d_ffn[:], wd[N0, cols, :], NT).astype(BF).astype(F32)
            g, l = gate[t, :, cols], lin[t, :, cols]
            cdf = 0.5 * (1.0 + lax.erf(g * 0.5 ** 0.5))
            slope = cdf + g * (jnp.exp(-0.5 * g * g) * (N2 * np.pi) ** -0.5)
            d_l = d_inner * (g * cdf)
            d_g = d_inner * l * slope
            sums[pl.ds(t, N1), cols] = over_rows(d_g)
            sums[pl.ds(n + t, N1), cols] = over_rows(d_l)
            d_gate[N0, :, cols] = d_g.astype(BF)
            d_lin[N0, :, cols] = d_l.astype(BF)
        for lo in tiles:
            cols = pl.ds(lo, tile)
            acc[:, cols] += dot(d_gate[N0], wg[N0, cols, :], NT) + dot(d_lin[N0], wl[N0, cols, :], NT)

    @pl.when(i == N2 * n - N1)
    def _():
        d_h, unit = acc[:], unit1[:]
        d_x = standard_grad(d_h * gain1, unit, scale1[:])
        sums[pl.ds(N2 * n, N1), :] = over_rows(d_x)
        sums[pl.ds(N2 * n + N1, N1), :] = over_rows(d_h * unit)
        sums[pl.ds(N2 * n + N2, N1), :] = over_rows(d_h)
        resid[:] = ALPHA * d_x
        d_attn[:] = d_x.astype(BF)
        for h in range(n):
            d_ctx[h] = dot(d_attn[:], wo[h], NT)


def layer(ctx, wo, emb, cot, vectors, gate_bias, lin_bias, wg, wl, wd):
    n, own, dims = ctx.shape
    width = emb.shape[N1]
    ffn = wg.shape[N2]
    once = pl.BlockSpec(memory_space=pltpu.VMEM)
    weight = [pl.BlockSpec((N1,) + w.shape[N1:], lambda i: (i % n, N0, N0)) for w in (wg, wl, wd)]
    early = pl.BlockSpec((N1, own, ffn), lambda i: (jnp.minimum(i, n - N1), N0, N0))
    late = pl.BlockSpec((N1, own, ffn), lambda i: (jnp.maximum(i - n, N0), N0, N0))
    shape = jax.ShapeDtypeStruct
    slots = shape((n, own, ffn), BF)
    return pl.pallas_call(
        functools.partial(layer_kernel, n),
        name='layer',
        grid=(N2 * n,),
        in_specs=[once] * 7 + weight,
        out_specs=[once] * 6 + [early, late, late],
        out_shape=[shape((own, width), BF)] * 3 + [shape((own, width), F32), shape((n, own, dims), F32), shape((N2 * n + 8, width), F32), slots, slots, slots],
        scratch_shapes=[pltpu.VMEM((n, own, ffn), F32)] * N2 + [pltpu.VMEM((own, width), F32)] * N2 + [pltpu.VMEM((own, N1), F32)],
        compiler_params=pltpu.CompilerParams(dimension_semantics=('arbitrary',), vmem_limit_bytes=62 * N2 ** 20),
        cost_estimate=pl.CostEstimate(flops=15 * 10 ** 9, bytes_accessed=70 * N2 ** 20, transcendentals=N0),
    )(ctx, wo, emb, cot, vectors, gate_bias, lin_bias, wg, wl, wd)


def products_kernel(n, hidden, d_ffn, inner, d_gate, d_lin, gate, lin, down, turned_hidden):
    i = pl.program_id(N0)
    size = hidden.shape[N1]
    tile = 256 if size % 256 == N0 else size

    @pl.when(i == N0)
    def _():
        turned_hidden[:] = hidden[:].T

    def fill(out, lhs, rhs, dims):
        for lo in range(N0, size, tile):
            cols = pl.ds(lo, tile)
            out[N0, :, cols] = dot(lhs, rhs[:, cols], dims)
    pl.when(i < n)(lambda: fill(gate, turned_hidden[:], d_gate.at[N0], NN))
    pl.when((i >= n) & (i < N2 * n))(lambda: fill(lin, turned_hidden[:], d_lin.at[N0], NN))

    @pl.when(i >= N2 * n)
    def _():
        fill(down, inner[N0].T, d_ffn, NN)


def products(hidden, d_ffn, inner, d_gate, d_lin):
    n, own, ffn = inner.shape
    width = hidden.shape[N1]
    once = pl.BlockSpec(memory_space=pltpu.VMEM)

    def slot(rows, first):
        return pl.BlockSpec((N1, rows, ffn), lambda i: (jnp.clip(i - first * n, N0, n - N1), N0, N0))
    shape = jax.ShapeDtypeStruct((n, width, ffn), F32)
    return pl.pallas_call(
        functools.partial(products_kernel, n),
        name='products',
        grid=(3 * n,),
        in_specs=[once, once, slot(own, N2), slot(own, N0), slot(own, N1)],
        out_specs=[slot(width, N0), slot(width, N1), slot(width, N2)],
        out_shape=[shape] * 3,
        scratch_shapes=[pltpu.VMEM((width, own), BF)],
        compiler_params=pltpu.CompilerParams(dimension_semantics=('arbitrary',), vmem_limit_bytes=58 * N2 ** 20),
        cost_estimate=pl.CostEstimate(flops=12 * 10 ** 9, bytes_accessed=70 * N2 ** 20, transcendentals=N0),
    )(hidden, d_ffn, inner, d_gate, d_lin)


def solution(mesh):
    n_tp, n_dp = mesh.shape['tp'], mesh.shape['dp']
    in_specs = (P('dp', None), P('dp', None, None), P('tp', None)) + WEIGHT_SPECS
    out_specs = (P('tp', None),) + WEIGHT_SPECS

    def device_step(tokens, cotangent, emb_table, *weights):
        (w_qkv, b_qkv, w_out, b_out, ln1_gain, ln1_bias, w_gate, b_gate, w_lin, b_lin, w_down, b_down, ln2_gain) = weights
        tp, dp = lax.axis_index('tp'), lax.axis_index('dp')
        tokens = tokens[N0]
        seq_len, width = tokens.shape[N0], emb_table.shape[N1]
        heads, head_dim = b_qkv.shape[N0], b_qkv.shape[N1] // 3
        own = seq_len // n_tp
        ffn = w_gate.shape[N1]
        rk, rf, ro = width // n_dp, ffn // n_dp, w_out.shape[N0] // n_dp

        def cut(weight):
            rows = weight.shape[N0] // n_dp
            return lax.dynamic_slice_in_dim(weight, dp * rows, rows, N0)
        bias_rows = jnp.concatenate([b_gate[None], b_lin[None], jnp.zeros((14, ffn), BF)], axis=N0)
        piece = jnp.concatenate([cut(w_gate), cut(w_lin), cut(w_down), cut(w_out), bias_rows], axis=N0).astype(F32)

        vocab_loc = emb_table.shape[N0]
        local_ids = tokens - tp * vocab_loc
        in_shard = (local_ids >= N0) & (local_ids < vocab_loc)
        safe_ids = jnp.where(in_shard, local_ids, N0)
        found = jnp.take(emb_table, safe_ids, axis=N0, mode='clip')
        dims = heads * head_dim
        place = column_order(heads, head_dim)
        swap = (jnp.arange(3 * dims)[:, None] == jnp.asarray(place)[None, :]).astype(BF)
        wq = jnp.dot(w_qkv, swap, preferred_element_type=F32).astype(BF)
        bq = jnp.dot(b_qkv.reshape(N1, -N1), swap, preferred_element_type=F32)
        cos_tab, sin_tab = rope_tables(seq_len, head_dim, heads)
        emb_bf, (wg_full, wl_full, wd_full, wo_full), biases, tok_all, ctx_own, saved = embed(found, in_shard[:, None].astype(F32), piece, tokens.reshape(-N1, min(128, seq_len // 8)), (w_gate, w_lin, w_down, w_out), wq, bq, cos_tab, sin_tab, heads, n_tp, n_dp)
        is_own = (jnp.arange(n_tp) == tp)[:, None]
        bg_full, bl_full = [jnp.where(is_own, b[None].astype(F32), biases[:, i]) for i, b in enumerate((b_gate, b_lin))]

        blocks = 8

        def owned(values):
            return lax.dynamic_index_in_dim(values.reshape(blocks, n_tp, -N1, width), tp, N1, keepdims=False).reshape(own, width)
        emb_own, cot_own = owned(emb_bf), owned(cotangent[N0])
        vectors = jnp.stack([b_out, ln1_gain, ln1_bias, b_down, ln2_gain] + [b_out] * 3).astype(F32)
        hidden, d_ffn_bf, d_attn_bf, resid, d_ctx, row_sums, inner_act, d_gate_bf, d_lin_bf = layer(
            ctx_own.reshape(n_tp, own, dims), wo_full, emb_own, cot_own, vectors, bg_full, bl_full, wg_full, wl_full, wd_full)

        prods = [grad.reshape(n_tp, n_dp, -N1, width) for grad in products(hidden, d_ffn_bf, inner_act, d_gate_bf, d_lin_bf)]
        d_w_out = jnp.einsum('hse,sd->hed', ctx_own.reshape(n_tp, own, dims).astype(BF), d_attn_bf, preferred_element_type=F32)
        d_w_qkv, d_b_qkv, d_cols, (d_w_gate, d_w_lin), d_w_down = backward(
            d_ctx.reshape(n_tp, blocks, own // blocks, dims), resid.reshape(blocks, own // blocks, width), saved, cos_tab, sin_tab, wq, swap.T, emb_bf,
            prods, heads, n_tp, n_dp)
        d_w_gate, d_w_lin = d_w_gate.reshape(-N1, ffn), d_w_lin.reshape(-N1, ffn)
        d_b_qkv = jnp.dot(d_b_qkv, swap.astype(F32).T, precision=lax.Precision.HIGHEST)
        all_ids = tok_all.reshape(-N1) - tp * vocab_loc
        all_ids = jnp.where((all_ids >= N0) & (all_ids < vocab_loc), all_ids, vocab_loc)
        col = table_rows(all_ids, d_cols.reshape(n_dp * seq_len, -N1), vocab_loc)

        slot = (jnp.arange(n_tp) == tp).astype(F32)[:, None]
        d_bq_rows = jnp.pad(slot * d_b_qkv, ((N0, N0), (N0, ffn - 3 * dims)))
        kept = N2 * n_tp
        small = jnp.concatenate([row_sums[:kept], d_bq_rows, row_sums[kept:kept + 5], jnp.zeros((7, width), F32)], axis=N0)
        d_table, d_w_down, d_w_out, d_w_qkv, small = finish(
            col, d_w_down, d_w_out.reshape(n_tp, n_dp, N2, -N1, width), d_w_qkv.reshape(n_dp, N2, -N1, 3 * dims), small, n_tp, n_dp)
        d_b_gate = lax.dynamic_index_in_dim(small[:n_tp], tp, N0, keepdims=False)
        d_b_lin = lax.dynamic_index_in_dim(small[n_tp:N2 * n_tp], tp, N0, keepdims=False)
        d_b_qkv = lax.dynamic_index_in_dim(small[N2 * n_tp:3 * n_tp], tp, N0, keepdims=False)[:3 * dims].reshape(heads, 3 * head_dim)
        d_b_out, d_ln1_gain, d_ln1_bias, d_b_down, d_ln2_gain = [small[3 * n_tp + i] for i in range(5)]
        return (d_table, d_w_qkv, d_b_qkv, d_w_out, d_b_out, d_ln1_gain, d_ln1_bias, d_w_gate, d_b_gate, d_w_lin, d_b_lin, d_w_down, d_b_down, d_ln2_gain)

    return jax.shard_map(device_step, mesh=mesh, in_specs=in_specs, out_specs=out_specs, check_vma=False)
```

```python
import functools

import jax
import jax.numpy as jnp
import numpy as np
from jax import lax
from jax.experimental import pallas as pl
from jax.experimental.pallas import tpu as pltpu
from jax.sharding import PartitionSpec as P

ALPHA = 140.0 ** 0.5
EPS = 1e-5
SHRINK = 0.1
ROPE_BASE = 10000.0
WEIGHT_SPECS = (P(None, 'tp'), P('tp', None), P('tp', None), P(), P(), P(), P(None, 'tp'), P('tp'), P(None, 'tp'), P('tp'), P('tp', None), P(), P())
BF = jnp.bfloat16
N0, N1, N2 = range(3)
F32 = jnp.float32
MESH = pl.DeviceIdType.MESH
ANY = pl.BlockSpec(memory_space=pl.ANY)
VMEM = pl.BlockSpec(memory_space=pltpu.VMEM)


def rope_tables(seq_len, head_dim, heads):
    half_dim = head_dim // 2
    inv_freq = (ROPE_BASE ** (-2.0 * np.arange(half_dim) / head_dim)).astype(np.float32)
    angles = np.arange(seq_len, dtype=np.float32)[:, None] * inv_freq[None, :]
    return [jnp.asarray(np.tile(table(angles), (1, heads))) for table in (np.cos, np.sin)]


def column_order(heads, head_dim):
    cols = np.arange(3 * heads * head_dim).reshape(heads, 3, 2, head_dim // 2)
    return np.concatenate([cols[:, part].transpose(1, 0, 2).ravel() for part in (0, 1)] + [cols[:, 2].ravel()])


def rcopy(src, dst, send, recv, **where):
    return pltpu.make_async_remote_copy(src_ref=src, dst_ref=dst, send_sem=send, recv_sem=recv, device_id=dict(where), device_id_type=MESH)


def plane():
    p = lax.axis_index('dp')
    y, x, c = p // 4, (p // 2) % 2, p % 2

    def at(rel):
        yy = 1 - y if rel & 4 else y
        xx = 1 - x if rel & 2 else x
        cc = 1 - c if rel & 1 else c
        return yy * 4 + xx * 2 + cc
    return p, at


def entry_barrier(z, n, at):
    bar = pltpu.get_barrier_semaphore()
    for rel in range(1, 8):
        pl.semaphore_signal(bar, inc=1, device_id={'dp': at(rel)}, device_id_type=MESH)
    for d in range(1, n):
        pl.semaphore_signal(bar, inc=1, device_id={'tp': (z + d) % n}, device_id_type=MESH)
    pl.semaphore_wait(bar, 7 + n - 1)


LAG = 3


def chain_sum(k, z, n, rows, chunks, part, left, right, done, send_r, send_l, recv_l, recv_r, place=lambda c: c, lag=LAG):
    last = n - 1

    def at_rows(c):
        return pl.ds(pl.multiple_of(place(c) * rows, rows), rows)

    def cut(ref, c):
        return ref.at[at_rows(c)]

    def load(ref, c):
        return ref[at_rows(c)]

    def store(ref, c, value):
        ref[at_rows(c)] = value
    cl, cr = k - lag * z, k - lag * (last - z)
    okl, okr = (cl >= 0) & (cl < chunks), (cr >= 0) & (cr < chunks)

    @pl.when(okl & (z > 0))
    def _():
        rcopy(cut(left, cl), cut(left, cl), send_r, recv_l.at[cl], tp=z).wait_recv()

    @pl.when(okl & (z == last))
    def _():
        done(cl, load(left, cl) + load(part, cl))

    @pl.when(okl & (z > 0) & (z < last))
    def _():
        run = load(left, cl)

        @pl.when(z >= n // 2)
        def _():
            done(cl, run + load(right, cl))
        store(left, cl, run + load(part, cl))

    @pl.when(okr & (z < last))
    def _():
        rcopy(cut(right, cr), cut(right, cr), send_l, recv_r.at[cr], tp=z).wait_recv()

    @pl.when(okr & (z == 0))
    def _():
        done(cr, load(part, cr) + load(right, cr))

    @pl.when(okr & (z > 0) & (z < last))
    def _():
        run = load(right, cr)

        @pl.when(z < n // 2)
        def _():
            done(cr, load(left, cr) + run)
        store(right, cr, run + load(part, cr))

    @pl.when(okl & (z == 0))
    def _():
        rcopy(cut(part, cl), cut(left, cl), send_r, recv_l.at[cl], tp=z + 1).start()

    @pl.when(okl & (z > 0) & (z < last))
    def _():
        rcopy(cut(left, cl), cut(left, cl), send_r, recv_l.at[cl], tp=z + 1).start()

    @pl.when(okr & (z == last))
    def _():
        rcopy(cut(part, cr), cut(right, cr), send_l, recv_r.at[cr], tp=z - 1).start()

    @pl.when(okr & (z > 0) & (z < last))
    def _():
        rcopy(cut(right, cr), cut(right, cr), send_l, recv_r.at[cr], tp=z - 1).start()


def chain_drain(z, n, part, left, right, send_r, send_l, recv_l, recv_r):
    @pl.when(z < n - 1)
    def _():
        rcopy(part, left, send_r, recv_l.at[0], tp=z + 1).wait_send()

    @pl.when(z > 0)
    def _():
        rcopy(part, right, send_l, recv_r.at[0], tp=z - 1).wait_send()


EDGES = ((0, 0, 2), (0, 0, 4), (0, 0, 1), (2, 1, 4), (4, 2, 2), (2, 0, 1), (4, 0, 1), (6, 1, 1), (6, 2, 1))
CROSS, DIAGONAL, LAST = ((0, 3, 5), (1, 4, 6)), ((3, 7), (4, 8)), {1: (2,), 3: (5,), 5: (6,), 7: (7, 8)}
STEPS = (8, 14, 20, 24, 28, 32)
ARRIVE = {2: 2, 3: 8}
EMB_LAG = 4
FIRST = 18
ORDER = (0, 2, 4, 1, 3, 5, 6, 7)


def emb_kernel(n, rows, chunks, cuts, heads, found, mask, wq, bq, cos, sin, piece, toks, *refs):
    m = len(cuts)
    local, outs = refs[:m], refs[m + N1:N2 * m + N1]
    out, (bias, tok_all, wall, ctx_own, q, k_all, v, ctx, top, inv, part, left, right, raw, low, weights, send_r, send_l, recv_l, recv_r, tsend, trecv, tself, zsend, zrecv, psend, precv, lsem, isem, osem, bsem, asend, arecv, aself) = refs[m], refs[N2 * m + N1:]
    blocks = 8
    qb = part.shape[N0] // blocks
    per = chunks // blocks
    z = lax.axis_index('tp')
    p, at = plane()
    entry_barrier(z, n, at)
    half = piece.shape[N0] // N2

    @pl.when(z < n - N1)
    def _():
        rcopy(piece, wall.at[z, p], zsend.at[z], zrecv.at[z], tp=z + N1).start()

    @pl.when(z > N0)
    def _():
        rcopy(piece, wall.at[z, p], bsem.at[N1], zrecv.at[z], tp=z - N1).start()
    mine = [pltpu.make_async_copy(toks, tok_all.at[p], tself)]
    mine += [pltpu.make_async_copy(src, dst.at[z], lsem.at[i]) for i, (src, dst) in enumerate(zip(local, outs))]
    for copy in mine:
        copy.start()
    for rel in range(N1, 8):
        rcopy(toks, tok_all.at[p], tsend.at[rel], trecv.at[rel], dp=at(rel)).start()

    def others(d, body):
        @pl.when(z >= d)
        def _():
            body(z - d, -N1)

        @pl.when(z + d < n)
        def _():
            body(z + d, N1)

    def region(t, rel, side):
        blk = wall.at[t, at(rel)]
        return blk if side == N0 else wall.at[t, at(rel), pl.ds((side - N1) * half, half)]

    def give(t, j):
        rel, side, to = EDGES[j]
        rcopy(region(t, rel, side), region(t, rel, side), psend.at[t, j], precv.at[t, j], dp=at(to)).start()

    def take(t, j):
        rel, side, to = EDGES[j]
        blk = region(t, rel ^ to, side)
        rcopy(blk, blk, psend.at[t, j], precv.at[t, j], dp=p).wait_recv()

    def gave(t, j):
        rel, side, to = EDGES[j]
        rcopy(region(t, rel, side), region(t, rel, side), psend.at[t, j], precv.at[t, j], dp=p).wait_send()

    def arrive(d):
        def body(t, sign):
            blk = wall.at[t, p]
            rcopy(blk, blk, zsend.at[t], zrecv.at[t], tp=z).wait_recv()

            @pl.when((z - sign >= N0) & (z - sign < n))
            def _():
                rcopy(blk, blk, zsend.at[t], zrecv.at[t], tp=z - sign).start()
            for j in range(3):
                give(t, j)
        others(d, body)

    def relay(d, moves):
        def body(t, sign):
            for first, *rest in moves:
                take(t, first)
                for j in rest:
                    give(t, j)
        others(d, body)

    k_all[:] = jnp.zeros_like(k_all)
    v[:] = jnp.zeros_like(v)
    arrive(N1)

    @pl.loop(N0, blocks)
    def _(i):
        at_i = pl.ds(pl.multiple_of(i * qb, qb), qb)
        part[at_i, :] = jnp.where(mask[at_i, :] > N0, found[at_i, :].astype(F32), 0.0)

    def done(c, value):
        out[pl.ds(pl.multiple_of(c * rows, rows), rows)] = value.astype(out.dtype)

    def other(i):
        return i + (i + n - z) // n

    def loaded(i, rel, slot):
        return pltpu.make_async_copy(wall.at[other(i), at(rel), pl.ds(N0, cuts[-N1][N1])], raw.at[slot], isem.at[slot])

    def stored(i, rel, slot):
        return [pltpu.make_async_copy(low.at[slot, pl.ds(lo, hi - lo)], dst.at[other(i), at(rel)], osem.at[slot, k]) for k, ((lo, hi), dst) in enumerate(zip(cuts, outs))]
    plan = [(i, rel) for rel in ORDER for i in range(n - N1)]

    def prefetch(s):
        i, rel = plan[s]
        for j in LAST.get(rel, ()):
            take(other(i), j)
        loaded(i, rel, s % N2).start()

    def convert(s):
        i, rel = plan[s]
        loaded(i, rel, s % N2).wait()
        if s >= N2:
            for copy in stored(*plan[s - N2], s % N2):
                copy.wait()
        low[s % N2] = raw[s % N2].astype(low.dtype)
        if s + N1 < len(plan):
            prefetch(s + N1)
        for copy in stored(i, rel, s % N2):
            copy.start()
    events = [(STEPS[d - N1], functools.partial(relay, d, CROSS)) for d in range(N1, n)] + [(STEPS[d + n - N2], functools.partial(relay, d, DIAGONAL)) for d in range(N1, n)]
    events += [(ARRIVE[d], functools.partial(arrive, d)) for d in range(N2, n)]
    events += [(FIRST - N1, functools.partial(prefetch, N0))] + [(FIRST + s, functools.partial(convert, s)) for s in range(len(plan))]

    start = per + EMB_LAG * (n - N1)

    share = qb // n

    def context(i, d):
        to = (z + d) % n
        src = ctx.at[pl.ds(pl.multiple_of(i * qb + to * share, share), share)]
        if d == N0:
            return pltpu.make_async_copy(src, ctx_own.at[z, i], aself)
        return rcopy(src, ctx_own.at[z, i], asend, arecv.at[z], tp=to)

    @pl.loop(N0, max(start + blocks * heads + N1, FIRST + len(plan)))
    def _(k):
        step = k - start
        i = step // heads - N1

        @pl.when((step > N0) & (step % heads == N0) & (step <= blocks * heads))
        def _():
            for d in range(n):
                context(i, d).start()
        chain_sum(k, z, n, rows, chunks, part, left, right, done, send_r, send_l, recv_l, recv_r, lag=EMB_LAG)
        for at_step, event in events:
            pl.when(k == at_step)(event)

        @pl.when((step >= N0) & (step < blocks * heads))
        def _():
            @pl.when(step % heads == N0)
            def _():
                project(step // heads, qb, out, wq, bq, cos, sin, q, k_all, v)
            attend(step // heads, step % heads, heads, qb, q, k_all, v, ctx, top, inv, weights)

    pltpu.make_async_copy(ctx_own.at[z], ctx_own.at[z], aself).wait()
    for d in range(N1, n):
        src = (z + d) % n
        rcopy(ctx_own.at[src], ctx_own.at[src], asend, arecv.at[src], tp=z).wait()
    chain_drain(z, n, part, left, right, send_r, send_l, recv_l, recv_r)
    for s in (len(plan) - N2, len(plan) - N1):
        for copy in stored(*plan[s], s % N2):
            copy.wait()

    def finish(t, sign):
        for j in range(len(EDGES)):
            gave(t, j)
        tail = pltpu.make_async_copy(wall.at[t, p, pl.ds(cuts[-N1][N1], bias.shape[N1])], bias.at[t], bsem.at[N0])
        tail.start()
        tail.wait()

        @pl.when((z - sign >= N0) & (z - sign < n))
        def _():
            rcopy(wall.at[t, p], wall.at[t, p], zsend.at[t], zrecv.at[t], tp=z).wait_send()
    for d in range(N1, n):
        others(d, finish)
    for copy in mine:
        copy.wait()
    for rel in range(N1, 8):
        rcopy(toks, tok_all.at[at(rel)], tsend.at[rel], trecv.at[rel], dp=at(rel)).wait()

    @pl.when(z < n - N1)
    def _():
        rcopy(piece, wall.at[z, p], zsend.at[z], zrecv.at[z], tp=z + N1).wait_send()

    @pl.when(z > N0)
    def _():
        rcopy(piece, wall.at[z, p], bsem.at[N1], zrecv.at[z], tp=z - N1).wait_send()


def embed(found, mask, piece, toks, local, wq, bq, cos, sin, heads, n_tp, n_dp):
    seq, width = found.shape
    chunks = 32
    rows = seq // chunks
    dims = wq.shape[N1] // 3
    cuts, lo = [], N0
    for weight in local:
        cuts.append((lo, lo + weight.shape[N0] // n_dp))
        lo = cuts[-N1][N1]
    dma = pltpu.SemaphoreType.DMA
    shape = jax.ShapeDtypeStruct
    shapes = [shape((seq, width), BF)]
    shapes += [shape((n_tp, n_dp, w.shape[N0] // n_dp, w.shape[N1]), BF) for w in local]
    shapes += [shape((n_tp, piece.shape[N0] - lo, width), F32), shape((n_dp,) + toks.shape, toks.dtype), shape((n_tp, n_dp) + piece.shape, F32), shape((n_tp, 8, seq // n_tp // 8, dims), F32)]
    shapes += [shape((seq, dims), BF)] * 3 + [shape((seq, dims), F32)] + [shape((heads, seq), F32)] * N2
    out = pl.pallas_call(
        functools.partial(emb_kernel, n_tp, rows, chunks, cuts, heads),
        name='embed',
        out_shape=shapes,
        in_specs=[VMEM] * 6 + [ANY] * (N2 + len(local)),
        out_specs=[VMEM] + [ANY] * (4 + len(local)) + [VMEM] * 6,
        scratch_shapes=[pltpu.VMEM((seq, width), F32)] * 3 + [pltpu.VMEM((N2, lo, width), F32), pltpu.VMEM((N2, lo, width), BF), pltpu.VMEM((seq, seq // 8), F32), dma, dma, dma((chunks,)), dma((chunks,)),
                        dma((8,)), dma((8,)), dma, dma((n_tp,)), dma((n_tp,)), dma((n_tp, len(EDGES))), dma((n_tp, len(EDGES))), dma((len(local),)), dma((N2,)), dma((N2, len(local))), dma((N2,)),
                        dma, dma((n_tp,)), dma],
        compiler_params=pltpu.CompilerParams(collective_id=N0, has_side_effects=True, vmem_limit_bytes=60 * N2 ** 20),
        cost_estimate=pl.CostEstimate(flops=20 * 10 ** 9, bytes_accessed=80 * N2 ** 20, transcendentals=N0),
    )(found, mask, wq, bq, cos, sin, piece, toks, *[w.reshape(n_dp, w.shape[N0] // n_dp, w.shape[N1]) for w in local])
    m = N1 + len(local)
    return out[N0], [w.reshape(n_tp, -N1, w.shape[3]) for w in out[N1:m]], out[m], out[m + N1], out[m + 3], out[m + 4:]


RING = 4
HOLD, LIVE, PAIR = 4, 12, 4
ADD, LOAD, CROSSED, LAND, PLANE, HOP, BEAT = 1, 4, 5, 9, 10, 2, 4
GATHER = (37, 41)


def block_of(ref, at, rel, side):
    return ref.at[at(rel)] if side == 0 else ref.at[at(rel), side - 1]


class Spread:
    def __init__(self, at, block, send, recv, own=None):
        self.at, self.block, self.send, self.recv, self.own = at, block, send, recv, own

    def copy(self, j, rel, side, to):
        dst = self.block(rel, side)
        src = self.own if rel == 0 and self.own is not None else dst
        return rcopy(src, dst, self.send.at[j], self.recv.at[j], dp=self.at(to))

    def give(self, j):
        self.copy(j, *EDGES[j]).start()

    def take(self, j):
        rel, side, to = EDGES[j]
        self.copy(j, rel ^ to, side, 0).wait_recv()

    def start(self):
        for j in range(3):
            self.give(j)

    def relay(self, moves):
        for first, *rest in moves:
            self.take(first)
            for j in rest:
                self.give(j)

    def cross(self):
        self.relay(CROSS)

    def diagonal(self):
        self.relay(DIAGONAL)

    def finish(self):
        for j in (2, 5, 6, 7, 8):
            self.take(j)
        for j, (rel, side, _) in enumerate(EDGES):
            self.copy(j, rel, side, 0).wait_send()


def backward_kernel(n, rows, chunks, jobs, heads, d_ctx, resid, q, k_all, v, ctx, top, inv, cos, sin, wq, back, emb, *refs):
    prods = refs[:jobs]
    whole = refs[jobs:N2 * jobs - N1]
    out, grads, d_w, d_bias, landed, cross, last, part, left, right, total, dctx, dq, dk, dv, ctx_in, res_in, cos_in, sin_in, emb_in, q_in, work, fresh, xin, yin, keep, pass_on, along, final, *sems = refs[N2 * jobs - N1:]
    send_r, send_l, recv_l, recv_r, osend, orecv, csend, crecv, esem, fsem, xsend, xrecv, xsem, ysend, yrecv, ysem, ksem, zrecv, frecv, asend, arecv, aself, isem, gsend, grecv = sems
    z = lax.axis_index('tp')
    p, at = plane()
    entry_barrier(z, n, at)
    blocks = 8
    per = chunks // blocks
    qb = rows * per
    share = qb // n
    block = out.shape[N2]
    lead = jnp.maximum(z, n - N1 - z)
    span = N2 * n
    units = jobs * span
    size = work.shape[N2]

    def rows_of(i, to, count):
        return pl.ds(pl.multiple_of(i * qb + to * count, count), count)

    def exchange(i, d):
        to = (z + d) % n
        dst = dctx.at[rows_of(i, z, share)]
        if d == N0:
            return pltpu.make_async_copy(d_ctx.at[z, i], dst, aself.at[i])
        return rcopy(d_ctx.at[to, i], dst, asend, arecv.at[i], tp=to)

    @pl.loop(N0, blocks)
    def _(b):
        for d in range(n):
            exchange(blocks - N1 - b, d).start()

    def piece(m, u, rel):
        return prods[m].at[(u % span) // N2, at(rel), pl.ds(pl.multiple_of((u % N2) * size, size), size)]

    for m in range(jobs):
        @pl.loop(m * span, (m + N1) * span)
        def _(u, m=m):
            for i in range(4):
                rcopy(piece(m, u, N2 * i + N1), landed.at[u, i], csend, crecv.at[u], dp=at(N1)).start()

    def inputs(i):
        slot = i % N2
        at_q = rows_of(i, N0, qb)
        pairs = ((ctx.at[at_q], ctx_in), (resid.at[i], res_in), (cos.at[at_q], cos_in), (sin.at[at_q], sin_in), (emb.at[at_q], emb_in), (q.at[at_q], q_in))
        return [pltpu.make_async_copy(src, dst.at[slot], isem.at[j, slot]) for j, (src, dst) in enumerate(pairs)]

    dk[:] = jnp.zeros_like(dk)
    dv[:] = jnp.zeros_like(dv)
    d_w[:] = jnp.zeros_like(d_w)
    d_bias[:] = jnp.zeros_like(d_bias)
    for copy in inputs(blocks - N1):
        copy.start()

    def attention_step(b, h):
        i = blocks - N1 - b

        @pl.when(h == N0)
        def _():
            for copy in inputs(i):
                copy.wait()

            @pl.when(b + N1 < blocks)
            def _():
                for copy in inputs(i - N1):
                    copy.start()
            exchange(i, N0).wait()
            others = dctx.at[pl.ds(N0, (n - N1) * share)]
            rcopy(others, others, asend, arecv.at[i], tp=z).wait_recv()
        attend_grad(i, h, heads, qb, q_in.at[i % N2], k_all, v, ctx_in.at[i % N2], dctx, top, inv, dq, dk, dv)

        @pl.when(h == heads - N1)
        def _():
            slot = i % N2
            got = grad_rows(i, qb, cos_in[slot], sin_in[slot], dq, dk, dv, d_bias)
            d_w[:] += dot(emb_in[slot], dot(got, back[:], NN).astype(BF), TN)
            part[rows_of(i, N0, qb), :] = dot(got, wq[:], NT)
            part[rows_of(i, z, share), :] = part[rows_of(i, z, share), :] + res_in[i % N2]

    def sides(u):
        side = u % N2
        return side, at(N2) * (N1 - side) + at(4) * side, at(4) * (N1 - side) + at(N2) * side

    def fetch(u):
        slot = u % HOLD

        @pl.when(u >= HOLD)
        def _():
            rcopy(xin, cross.at[N0], xsend.at[slot], xrecv.at[N0], dp=p).wait_send()
        for m in range(jobs):
            @pl.when(u // span == m)
            def _(m=m):
                for i in range(4):
                    pltpu.make_async_copy(piece(m, u, N2 * i), work.at[slot, i], esem.at[slot]).start()
        rcopy(landed.at[u], landed.at[u], csend, crecv.at[u], dp=p).wait_recv()
        pltpu.make_async_copy(landed.at[u], fresh, fsem).start()

    def add(u):
        slot = u % HOLD
        pltpu.make_async_copy(landed.at[u], work.at[slot], esem.at[slot]).wait()
        pltpu.make_async_copy(landed.at[u], fresh, fsem).wait()
        for i in range(4):
            work[slot, i] = work[slot, i] + fresh[i]

    def add_send(u):
        slot = u % HOLD
        side, first, second = sides(u)
        rcopy(work.at[slot, N1 + side], cross.at[u, N0], xsend.at[slot], xrecv.at[u], dp=first).start()
        rcopy(work.at[slot, 3], cross.at[u, N1], xsend.at[slot], xrecv.at[u], dp=first).start()

    def load_cross(u):
        rcopy(cross.at[u], cross.at[u], xsend.at[N0], xrecv.at[u], dp=p).wait_recv()
        pltpu.make_async_copy(cross.at[u], xin, xsem).start()

    def crossed(u):
        slot = u % HOLD
        pltpu.make_async_copy(cross.at[u], xin, xsem).wait()

        @pl.when(u >= LIVE)
        def _():
            pltpu.make_async_copy(keep.at[u % LIVE], keep.at[u % LIVE], ksem.at[u % LIVE]).wait()

        @pl.when(u >= PAIR)
        def _():
            rcopy(pass_on.at[u % PAIR], last.at[u], ysend.at[u % PAIR], yrecv.at[u], dp=p).wait_send()
        keep[u % LIVE] = xin[N0] + work[slot, N0]
        pass_on[u % PAIR] = xin[N1] + work[slot, N2 - u % N2]

    def crossed_send(u):
        side, first, second = sides(u)
        rcopy(pass_on.at[u % PAIR], last.at[u], ysend.at[u % PAIR], yrecv.at[u], dp=second).start()

    def load_last(u):
        rcopy(last.at[u], last.at[u], ysend.at[N0], yrecv.at[u], dp=p).wait_recv()
        pltpu.make_async_copy(last.at[u], yin, ysem).start()

    def in_plane(u):
        pltpu.make_async_copy(last.at[u], yin, ysem).wait()
        keep[u % LIVE] = keep[u % LIVE] + yin[:]

    def unit(k):
        u = (k // BEAT) * (BEAT - N1) + k % BEAT
        return u, (k >= N0) & (k % BEAT < BEAT - N1) & (u < units)

    def along_tp(k, t, send):
        toward = jnp.where(z < t, z, n - N1 - z)
        late = HOP * jnp.where(z == t, max(t, n - N1 - t), toward)
        u, ok = unit(k - PLANE - N1 - late)
        mine = (u // span) * N2 + u % N2
        slot = u % LIVE
        ok = ok & ((u // N2) % n == t)

        def add_from(ref, sem):
            rcopy(ref, ref, csend, sem, tp=z).wait_recv()
            keep[slot] = keep[slot] + ref[:]
        if send:
            @pl.when(ok & (z < t))
            def _():
                rcopy(keep.at[slot], along.at[u], ksem.at[slot], zrecv.at[u], tp=z + N1).start()

            @pl.when(ok & (z > t + N1))
            def _():
                rcopy(keep.at[slot], along.at[u], ksem.at[slot], zrecv.at[u], tp=z - N1).start()

            @pl.when(ok & (z == t + N1))
            def _():
                rcopy(keep.at[slot], final.at[mine], ksem.at[slot], frecv.at[mine], tp=z - N1).start()

            for m in range(jobs):
                @pl.when(ok & (z == t) & (u // span == m))
                def _(m=m):
                    dst = whole[m].at[p, u % N2] if m < jobs - N1 else grads.at[u % N2]
                    pltpu.make_async_copy(keep.at[slot], dst, ksem.at[slot]).start()
        else:
            @pl.when(ok & (((z > N0) & (z <= t)) | ((z > t) & (z < n - N1))))
            def _():
                add_from(along.at[u], zrecv.at[u])
            if t < n - N1:
                @pl.when(ok & (z == t))
                def _():
                    add_from(final.at[mine], frecv.at[mine])

    spread = [Spread(at, functools.partial(block_of, whole[m], at), gsend.at[m], grecv.at[m]) for m in range(jobs - N1)]

    def settle(u):
        pltpu.make_async_copy(keep.at[u % LIVE], keep.at[u % LIVE], ksem.at[u % LIVE]).wait()

    def begin(m):
        for u in range(max(m * span, units - LIVE), (m + N1) * span):
            settle(u)
        spread[m].start()

    def place(c):
        return (blocks - N1 - c // per) * per + c % per

    def chunk(c):
        return total.at[c % RING]

    def done(c, value):
        @pl.when(c >= RING)
        def _():
            pltpu.make_async_copy(chunk(c), chunk(c), osend.at[c % RING]).wait()
        total[c % RING] = value

    def hand_out(c):
        where = out.at[p, pl.ds(pl.multiple_of(place(c) * rows, rows), rows)]
        for rel in range(8):
            src = total.at[c % RING, :, pl.ds(pl.multiple_of(at(rel) * block, block), block)]
            if rel == N0:
                pltpu.make_async_copy(src, where, osend.at[c % RING]).start()
            else:
                rcopy(src, where, osend.at[c % RING], orecv.at[rel], dp=at(rel)).start()

    def staged(k, offset, stage):
        u, ok = unit(k - offset)
        pl.when(ok)(functools.partial(stage, u))
    steps = max(heads + chunks + LAG * (n - N1) + N1, units // (BEAT - N1) * BEAT + PLANE + HOP * (n - N1), GATHER[-N1] + 7)

    @pl.loop(N0, steps)
    def _(k):
        c = k - heads - LAG * lead - N1

        @pl.when((c >= N0) & (c < chunks))
        def _():
            hand_out(c)
        chain_sum(k - heads, z, n, rows, chunks, part, left, right, done, send_r, send_l, recv_l, recv_r, place)
        for offset, stage in ((CROSSED, crossed), (ADD, add), (PLANE, in_plane)):
            staged(k, offset, stage)
        for t in range(n):
            along_tp(k, t, False)
        for offset, stage in ((N0, fetch), (LOAD, load_cross), (LAND, load_last)):
            staged(k, offset, stage)

        @pl.when(k < blocks * heads)
        def _():
            attention_step(k // heads, k % heads)
        for offset, stage in ((ADD, add_send), (CROSSED, crossed_send)):
            staged(k, offset, stage)
        for t in range(n):
            along_tp(k, t, True)
        for m, gather in enumerate(spread):
            for offset, stage in ((N0, functools.partial(begin, m)), (3, gather.cross), (6, gather.diagonal)):
                pl.when(k == GATHER[m] + offset)(stage)

    chain_drain(z, n, part, left, right, send_r, send_l, recv_l, recv_r)
    for c in range(max(N0, chunks - RING), chunks):
        pltpu.make_async_copy(chunk(c), chunk(c), osend.at[c % RING]).wait()
    for rel in range(N1, 8):
        rcopy(out.at[at(rel)], out.at[at(rel)], csend, orecv.at[rel], dp=p).wait_recv()
    for slot in range(HOLD):
        rcopy(xin, cross.at[N0], xsend.at[slot], xrecv.at[N0], dp=p).wait_send()
    for slot in range(PAIR):
        rcopy(pass_on.at[slot], last.at[N0], ysend.at[slot], yrecv.at[N0], dp=p).wait_send()
    for u in range(max((jobs - N1) * span, units - LIVE), units):
        settle(u)
    rcopy(landed, landed, csend, crecv.at[N0], dp=p).wait_send()
    for gather in spread:
        gather.finish()
    sent = dctx.at[pl.ds(N0, (n - N1) * share * blocks)]
    rcopy(sent, sent, asend, arecv.at[N0], tp=z).wait_send()


def backward(d_ctx, resid, saved, cos, sin, wq, back, emb, prods, heads, n_tp, n_dp):
    q, k, v, ctx, top, inv = saved
    seq, dims = q.shape
    width = wq.shape[N0]
    chunks = 32
    rows = seq // chunks
    jobs = len(prods)
    piece = (prods[N0].shape[N2] // N2, prods[N0].shape[3])
    units = jobs * N2 * n_tp
    dma = pltpu.SemaphoreType.DMA
    shape = jax.ShapeDtypeStruct
    qb = seq // 8
    vmem = [(seq, width)] * 3 + [(RING, rows, width), (seq, dims), (qb, dims), (seq, dims), (seq, dims), (N2, qb, dims), (N2, qb // n_tp, width)] + [(N2, qb, dims // N2)] * N2 + [
            (HOLD, 4) + piece, (4,) + piece, (N2,) + piece, piece, (LIVE,) + piece, (PAIR,) + piece, (units,) + piece, (N2 * jobs,) + piece]
    sems = [(), (), (chunks,), (chunks,), (RING,), (8,), (), (units,), (HOLD,), (), (HOLD,), (units,), (), (PAIR,), (units,), (), (LIVE,), (units,), (N2 * jobs,), (), (8,), (8,), (6, N2), (jobs - N1, len(EDGES)), (jobs - N1, len(EDGES))]
    scratch = [pltpu.VMEM(size, F32) for size in vmem]
    scratch[12:12] = [pltpu.VMEM((N2, qb, width), BF), pltpu.VMEM((N2, qb, dims), BF)]
    full = shape((n_dp, N2) + piece, F32)
    *whole, cols, grads, d_w, d_bias, _, _, _ = pl.pallas_call(
        functools.partial(backward_kernel, n_tp, rows, chunks, jobs, heads),
        name='backward',
        out_shape=[full] * (jobs - N1) + [shape((n_dp, seq, width // n_dp), F32), shape((N2,) + piece, F32), shape((width, 3 * dims), F32), shape((N1, 3 * dims), F32),
                   shape((units, 4) + piece, F32), shape((units, N2) + piece, F32), shape((units,) + piece, F32)],
        in_specs=[ANY] * 3 + [VMEM] * N2 + [ANY] + [VMEM] * N2 + [ANY] * N2 + [VMEM] * N2 + [ANY] * (N1 + jobs),
        out_specs=[ANY] * (jobs - N1) + [ANY, ANY, VMEM, VMEM, ANY, ANY, ANY],
        scratch_shapes=scratch + [dma(size) for size in sems],
        compiler_params=pltpu.CompilerParams(collective_id=N1, has_side_effects=True, vmem_limit_bytes=67_000_000),
        cost_estimate=pl.CostEstimate(flops=20 * 10 ** 9, bytes_accessed=100 * N2 ** 20, transcendentals=N0),
    )(d_ctx, resid, q, k, v, ctx, top, inv, cos, sin, wq, back, emb, *prods)
    return d_w, d_bias, cols, whole, grads


WAYS = 4


def table_kernel(ids, rows_ref, out, *tables):
    step = pl.program_id(0)
    count = rows_ref.shape[0]
    part = count // WAYS

    @pl.when(step == 0)
    def _():
        for table in tables:
            table[:] = jnp.zeros_like(table)

    @pl.loop(0, part, unroll=4)
    def _(r):
        for way, table in enumerate(tables):
            row = way * part + r
            where = pl.ds(ids[step * count + row], 1)
            table[where, :] = table[where, :] + rows_ref[pl.ds(row, 1), :]

    @pl.when(step == pl.num_programs(0) - 1)
    def _():
        total = tables[0][:]
        for table in tables[1:]:
            total = total + table[:]
        out[:] = SHRINK * total[:out.shape[0]]


def table_rows(ids, rows, vocab_loc):
    count, block = rows.shape
    step = min(1024, count // 2)
    return pl.pallas_call(
        table_kernel,
        name='table_rows',
        grid_spec=pltpu.PrefetchScalarGridSpec(
            num_scalar_prefetch=1,
            grid=(count // step,),
            in_specs=[pl.BlockSpec((step, block), lambda i, ids: (i, 0))],
            out_specs=pl.BlockSpec((vocab_loc, block), lambda i, ids: (0, 0)),
            scratch_shapes=[pltpu.VMEM((vocab_loc + 8, block), F32)] * WAYS,
        ),
        out_shape=jax.ShapeDtypeStruct((vocab_loc, block), F32),
        compiler_params=pltpu.CompilerParams(dimension_semantics=('arbitrary',), vmem_limit_bytes=48 * 2 ** 20),
        cost_estimate=pl.CostEstimate(flops=3 * 10 ** 9, bytes_accessed=16 * 2 ** 20, transcendentals=0),
    )(ids, rows)


class PlaneSum:
    def __init__(self, at, block, landed, work, cross, last, mine, sems):
        self.at, self.block, self.landed, self.work, self.cross, self.last, self.mine, self.sems = at, block, landed, work, cross, last, mine, sems

    def copy(self, src, dst, kind, side, rel):
        return rcopy(src, dst, self.sems.at[kind, side, N0], self.sems.at[kind, side, N1], dp=self.at(rel))

    def start(self):
        for i in range(4):
            self.copy(self.block(N2 * i + N1), self.landed.at[i], N0, N0, N1).start()

    def first(self):
        self.copy(self.landed, self.landed, N0, N0, N0).wait()
        for i in range(4):
            self.work[i] = self.block(N2 * i)[:] + self.landed[i]

    def first_send(self):
        for side in range(N2):
            self.copy(self.work.at[N1 + side, side], self.cross.at[side, N0], N1, side, N2 * (N1 + side)).start()
            self.copy(self.work.at[3, side], self.cross.at[side, N1], N1, side, N2 * (N1 + side)).start()

    def second(self):
        for side in range(N2):
            self.copy(self.cross.at[side], self.cross.at[side], N1, side, N0).wait()
            self.cross[side, N0] = self.cross[side, N0] + self.work[N0, side]
            self.cross[side, N1] = self.cross[side, N1] + self.work[N2 - side, side]

    def second_send(self):
        for side in range(N2):
            self.copy(self.cross.at[side, N1], self.last.at[side], N2, side, N2 * (N2 - side)).start()

    def end(self):
        for side in range(N2):
            self.copy(self.last.at[side], self.last.at[side], N2, side, N0).wait()
            self.mine[side] = self.cross[side, N0] + self.last[side]


def finish_kernel(n, cuts, col, down, proj, d_w, small, table, down_all, proj_all, qkv_all, total, *refs):
    scratch, (summed, inbox, arrived, sem, send, recv, dsend, drecv, osem, psem, zsem, rsem) = refs[:10], refs[10:]
    z = lax.axis_index('tp')
    p, at = plane()
    entry_barrier(z, n, at)
    block = col.shape[N1]
    half = len(cuts) // N2

    def part(i):
        def region(rel, side):
            return table.at[pl.ds(cuts[i][N0], cuts[i][N1] - cuts[i][N0]), pl.ds(pl.multiple_of(at(rel) * block, block), block)]
        return Spread(at, region, send.at[i], recv.at[i], col.at[pl.ds(cuts[i][N0], cuts[i][N1] - cuts[i][N0])])
    parts = [part(i) for i in range(len(cuts))]
    qkv_sum = PlaneSum(at, lambda rel: d_w.at[at(rel)], *scratch[:5], psem.at[N0])
    proj_sum = PlaneSum(at, lambda rel: summed.at[at(rel)], *scratch[5:], psem.at[N1])
    pairs = ((down, down_all), (proj_sum.mine, proj_all), (qkv_sum.mine, qkv_all))
    spread = [Spread(at, functools.partial(block_of, ref, at), dsend.at[i], drecv.at[i], own) for i, (own, ref) in enumerate(pairs)]
    own_copies = [pltpu.make_async_copy(col, table.at[:, pl.ds(pl.multiple_of(p * block, block), block)], osem.at[N0])]
    own_copies += [pltpu.make_async_copy(src, dst.at[p], osem.at[i]) for i, (src, dst) in enumerate(pairs, N1)]
    order = list(range(len(cuts)))
    flipped = order[half:] + order[:half]
    peers = [{'dp': at(N1)}, {'dp': at(N2)}, {'dp': at(4)}, {'tp': z + N1 - N2 * (z % N2)}, {'tp': (z + n // N2) % n}]

    def next_part(i):
        parts[order[i]].give(N0)
        parts[flipped[i]].give(N1)
        parts[order[i]].give(N2)

    def relay_part(i):
        one, two = order[i], flipped[i]
        parts[one].take(N0)
        if one < half:
            parts[one].give(3)
        parts[one].give(5)
        parts[two].take(N1)
        if two >= half:
            parts[two].give(4)
        parts[two].give(6)

    def exchange(r):
        return rcopy(total, inbox.at[r], rsem.at[N0, r], rsem.at[N1, r], **peers[r])

    def round_end(r):
        exchange(r).wait()
        total[:] = total[:] + inbox[r]

    total[:] = small[:]
    for d in range(N1, n):
        to = (z + d) % n
        rcopy(proj.at[to], arrived.at[z], zsem.at[N0, to], zsem.at[N1, z], tp=to).start()
    qkv_sum.start()
    for copy in own_copies[:N2]:
        copy.start()
    next_part(N0)
    exchange(N0).start()
    spread[N0].start()
    next_part(N1)
    qkv_sum.first()
    round_end(N0)
    qkv_sum.first_send()
    exchange(N1).start()
    next_part(N2)
    relay_part(N0)
    round_end(N1)
    qkv_sum.second()
    exchange(N2).start()
    qkv_sum.second_send()
    next_part(3)
    spread[N0].cross()
    relay_part(N1)
    round_end(N2)
    qkv_sum.end()
    exchange(3).start()
    next_part(4)
    spread[N2].start()
    own_copies[3].start()
    spread[N0].diagonal()
    relay_part(N2)
    summed[:] = proj[z]
    for d in range(N1, n):
        src = (z + d) % n
        rcopy(proj.at[src], arrived.at[src], zsem.at[N0, src], zsem.at[N1, src], tp=src).wait()
        summed[:] = summed[:] + arrived[src]
    round_end(3)
    next_part(5)
    exchange(4).start()
    proj_sum.start()
    relay_part(3)
    spread[N2].cross()
    proj_sum.first()
    next_part(6)
    proj_sum.first_send()
    round_end(4)
    relay_part(4)
    proj_sum.second()
    next_part(7)
    proj_sum.second_send()
    spread[N2].diagonal()
    relay_part(5)
    proj_sum.end()
    relay_part(6)
    spread[N1].start()
    own_copies[N2].start()
    relay_part(7)
    spread[N1].cross()
    spread[N1].diagonal()
    for i in range(half):
        for via, where in ((3, i), (4, i + half)):
            parts[where].take(via)
            parts[where].give(7)
    for i in order:
        for j in (N2, 5, 6, 7):
            parts[i].take(j)
        for j in (N0, N1, N2, 3 if i < half else 4, 5, 6, 7):
            parts[i].copy(j, *EDGES[j]).wait_send()
    for gather in spread:
        gather.finish()
    for copy in own_copies:
        copy.wait()


def finish(col, down, proj, d_w, small, n_tp, n_dp):
    size, block = col.shape
    tiles = size // 8
    cuts = [(8 * (tiles * i // 8), 8 * (tiles * (i + N1) // 8)) for i in range(8)]
    dma = pltpu.SemaphoreType.DMA
    shape = jax.ShapeDtypeStruct
    ours = (d_w.shape[N1:], proj.shape[N2:])
    kinds = len(EDGES)
    vmem = [lead + src[N1:] for src in ours for lead in ((4, N2), (4, N2), (N2, N2), (N2,), (N2,))] + [proj.shape[N1:], (5,) + small.shape, proj.shape]
    sems = [(), (8, kinds), (8, kinds), (3, kinds), (3, kinds), (4,), (N2, 3, N2, N2), (N2, n_tp), (N2, 5)]
    table, down_all, proj_all, qkv_all, total = pl.pallas_call(
        functools.partial(finish_kernel, n_tp, cuts),
        name='finish',
        out_shape=[shape((size, n_dp * block), F32)] + [shape((n_dp,) + src, F32) for src in (down.shape, ours[N1], ours[N0])] + [shape(small.shape, F32)],
        in_specs=[ANY] * N2 + [VMEM] * 3,
        out_specs=[ANY] * 4 + [VMEM],
        scratch_shapes=[pltpu.VMEM(dims, F32) for dims in vmem] + [dma(dims) for dims in sems],
        compiler_params=pltpu.CompilerParams(collective_id=N2, has_side_effects=True, vmem_limit_bytes=48 * N2 ** 20),
        cost_estimate=pl.CostEstimate(flops=10 * 10 ** 9, bytes_accessed=60 * N2 ** 20, transcendentals=N0),
    )(col, down, proj, d_w, small)
    return [table] + [grad.reshape(-N1, grad.shape[3]) for grad in (down_all, proj_all, qkv_all)] + [total]


def dot(a, b, dims):
    return lax.dot_general(a, b, (dims, ((), ())), preferred_element_type=F32)


NT, TN, NN = ((1,), (1,)), ((0,), (0,)), ((1,), (0,))


def lane_head(shape, heads, halves):
    lane = lax.broadcasted_iota(jnp.int32, shape, 1)
    dims = shape[1] // halves
    return (lane % dims) // (dims // heads)


def turned(both, cos, sin):
    half = both.shape[1] // 2
    x1, x2 = both[:, :half], both[:, half:]
    return jnp.concatenate([x1 * cos - x2 * sin, x2 * cos + x1 * sin], axis=1)


def project(i, qb, emb, wq, bq, cos, sin, q, k, v):
    at_q = pl.ds(pl.multiple_of(i * qb, qb), qb)
    dims = q.shape[1]
    qkv = (dot(emb[at_q, :], wq[:], NN) + bq[:]).astype(BF)
    for ref, part in ((q, 0), (k, 1)):
        ref[at_q, :] = turned(qkv[:, part * dims:(part + 1) * dims].astype(F32), cos[at_q, :], sin[at_q, :]).astype(BF)
    v[at_q, :] = qkv[:, 2 * dims:]


def scores(i, j, kb, qb, scale, keys, q):
    s = dot(keys, q, NT) * scale
    key = j * kb + lax.broadcasted_iota(jnp.int32, (kb, qb), 0)
    query = i * qb + lax.broadcasted_iota(jnp.int32, (kb, qb), 1)
    return jnp.where(query >= key, s, -1e30)


def attend(i, h, heads, qb, q_ref, k_ref, v_ref, ctx_ref, top_ref, inv_ref, s_ref):
    kb = 2 * qb
    dims = q_ref.shape[1]
    scale = (dims // heads) ** -0.5
    at_q = pl.ds(pl.multiple_of(i * qb, qb), qb)
    q = jnp.where(lane_head((qb, dims), heads, 2) == h, q_ref[at_q, :].astype(F32), 0.0).astype(BF)
    count = (i + 2) // 2

    def at_key(j):
        return pl.ds(pl.multiple_of(j * kb, kb), kb)

    def first(j, top):
        s = scores(i, j, kb, qb, scale, k_ref[at_key(j), :], q)
        s_ref[at_key(j), :] = s
        return jnp.maximum(top, jnp.max(s, axis=0, keepdims=True))
    top = lax.fori_loop(0, count, first, jnp.full((1, qb), -1e30, F32))

    def weigh(j, total):
        e = jnp.exp(s_ref[at_key(j), :] - top)
        s_ref[at_key(j), :] = e
        return total + jnp.sum(e, axis=0, keepdims=True)
    inv = 1.0 / lax.fori_loop(0, count, weigh, jnp.zeros((1, qb), F32))

    def mix(j, acc):
        return acc + dot((s_ref[at_key(j), :] * inv).astype(BF), v_ref[at_key(j), :], TN)
    mixed = lax.fori_loop(0, count, mix, jnp.zeros((qb, dims), F32))
    ctx_ref[at_q, :] = jnp.where(lane_head((qb, dims), heads, 1) == h, mixed, ctx_ref[at_q, :])
    top_ref[pl.ds(h, 1), at_q] = top
    inv_ref[pl.ds(h, 1), at_q] = inv


def attend_grad(i, h, heads, qb, q_ref, k_ref, v_ref, ctx_ref, dctx_ref, top_ref, inv_ref, dq_ref, dk_ref, dv_ref):
    kb = 2 * qb
    dims = dk_ref.shape[1]
    scale = (dims // heads) ** -0.5
    at_q = pl.ds(pl.multiple_of(i * qb, qb), qb)
    q = jnp.where(lane_head((qb, dims), heads, 2) == h, q_ref[:].astype(F32), 0.0).astype(BF)
    dc = jnp.where(lane_head((qb, dims), heads, 1) == h, dctx_ref[at_q, :], 0.0).astype(BF)
    ones = jnp.ones((8, dims), F32)
    mean = lax.dot_general(ones, dc.astype(F32) * ctx_ref[:], (NT, ((), ())), precision=lax.Precision.HIGHEST, preferred_element_type=F32)[:1]
    top, inv = top_ref[pl.ds(h, 1), at_q], inv_ref[pl.ds(h, 1), at_q]

    def step(j, dq):
        at_k = pl.ds(pl.multiple_of(j * kb, kb), kb)
        keys = k_ref[at_k, :]
        probs = (jnp.exp(scores(i, j, kb, qb, scale, keys, q) - top) * inv).astype(BF)
        ds = (probs.astype(F32) * (dot(v_ref[at_k, :], dc, NT) - mean) * scale).astype(BF)
        dv_ref[at_k, :] += dot(probs, dc, NN)
        dk_ref[at_k, :] += dot(ds, q, NN)
        return dq + dot(ds, keys, TN)
    dq = lax.fori_loop(0, (i + 2) // 2, step, jnp.zeros((qb, dims), F32))
    dq_ref[:] = jnp.where(lane_head((qb, dims), heads, 2) == h, dq, dq_ref[:])


def grad_rows(i, qb, cos, sin, dq, dk, dv, d_bias):
    at_q = pl.ds(pl.multiple_of(i * qb, qb), qb)
    back = [turned(values, cos, -sin) for values in (dq[:], dk[at_q, :])]
    rows = jnp.concatenate(back + [dv[at_q, :]], axis=1)
    d_bias[:] += jnp.sum(rows, axis=0, keepdims=True)
    return rows.astype(BF)


def standard(values):
    mean = jnp.mean(values, axis=1, keepdims=True)
    centered = values - mean
    scale = lax.rsqrt(jnp.mean(centered * centered, axis=1, keepdims=True) + EPS)
    return centered * scale, scale


def standard_grad(d_out, unit, scale):
    return scale * (d_out - jnp.mean(d_out, axis=1, keepdims=True) - unit * jnp.mean(d_out * unit, axis=1, keepdims=True))


def over_rows(values):
    return jnp.sum(values, axis=0, keepdims=True)


def layer_kernel(n, ctx, wo, emb, cot, vectors, gate_bias, lin_bias, wg, wl, wd, hidden, d_ffn, d_attn, resid, d_ctx, sums, inner, d_gate, d_lin, gate, lin, acc, unit1, scale1, emb_own, cot_own, sem):
    i = pl.program_id(N0)
    t = i % n
    tile = 256 if acc.shape[N1] % 256 == N0 else acc.shape[N1]
    tiles = range(N0, acc.shape[N1], tile)
    b_out, gain1, bias1, b_down, gain2 = [vectors[pl.ds(j, N1), :] for j in range(5)]

    def owned(src, dst, j):
        return pltpu.make_async_copy(src.at[:, lax.axis_index('tp')], dst, sem.at[j])

    @pl.when(i == N0)
    def _():
        owned(emb, emb_own, N0).start()
        owned(cot, cot_own, N1).start()
        owned(emb, emb_own, N0).wait()
        total = ALPHA * emb_own[:].reshape(acc.shape).astype(F32) + b_out
        for h in range(n):
            total = total + dot(ctx[h].astype(BF), wo[h], NN)
        unit, scale1[:] = standard(total)
        unit1[:] = unit
        hidden[:] = (unit * gain1 + bias1).astype(BF)
        acc[:] = jnp.zeros_like(acc)

    @pl.when(i < n)
    def _():
        for lo in tiles:
            cols = pl.ds(lo, tile)
            g = dot(hidden[:], wg[N0, :, cols], NN) + gate_bias[pl.ds(t, N1), cols]
            l = dot(hidden[:], wl[N0, :, cols], NN) + lin_bias[pl.ds(t, N1), cols]
            gate[t, :, cols] = g
            lin[t, :, cols] = l
            inner[N0, :, cols] = (0.5 * g * (1.0 + lax.erf(g * 0.5 ** 0.5)) * l).astype(BF)
        for lo in tiles:
            cols = pl.ds(lo, tile)
            acc[:, cols] += dot(inner[N0], wd[N0, :, cols], NN)

    @pl.when(i == n - N1)
    def _():
        unit, scale = standard(ALPHA * hidden[:].astype(F32) + acc[:] + b_down)
        owned(cot, cot_own, N1).wait()
        g = cot_own[:].reshape(acc.shape).astype(F32)
        d_y = standard_grad(g * gain2, unit, scale)
        sums[pl.ds(N2 * n + 3, N1), :] = over_rows(d_y)
        sums[pl.ds(N2 * n + 4, N1), :] = over_rows(g * unit)
        d_ffn[:] = d_y.astype(BF)
        acc[:] = ALPHA * d_y

    @pl.when(i >= n)
    def _():
        for lo in tiles:
            cols = pl.ds(lo, tile)
            d_inner = dot(d_ffn[:], wd[N0, cols, :], NT).astype(BF).astype(F32)
            g, l = gate[t, :, cols], lin[t, :, cols]
            cdf = 0.5 * (1.0 + lax.erf(g * 0.5 ** 0.5))
            slope = cdf + g * (jnp.exp(-0.5 * g * g) * (N2 * np.pi) ** -0.5)
            d_l = d_inner * (g * cdf)
            d_g = d_inner * l * slope
            sums[pl.ds(t, N1), cols] = over_rows(d_g)
            sums[pl.ds(n + t, N1), cols] = over_rows(d_l)
            d_gate[N0, :, cols] = d_g.astype(BF)
            d_lin[N0, :, cols] = d_l.astype(BF)
        for lo in tiles:
            cols = pl.ds(lo, tile)
            acc[:, cols] += dot(d_gate[N0], wg[N0, cols, :], NT) + dot(d_lin[N0], wl[N0, cols, :], NT)

    @pl.when(i == N2 * n - N1)
    def _():
        d_h, unit = acc[:], unit1[:]
        d_x = standard_grad(d_h * gain1, unit, scale1[:])
        sums[pl.ds(N2 * n, N1), :] = over_rows(d_x)
        sums[pl.ds(N2 * n + N1, N1), :] = over_rows(d_h * unit)
        sums[pl.ds(N2 * n + N2, N1), :] = over_rows(d_h)
        resid[:] = ALPHA * d_x
        d_attn[:] = d_x.astype(BF)
        for h in range(n):
            d_ctx[h] = dot(d_attn[:], wo[h], NT)


def layer(ctx, wo, emb, cot, vectors, gate_bias, lin_bias, wg, wl, wd):
    n, own, dims = ctx.shape
    width = emb.shape[-1]
    ffn = wg.shape[N2]
    once = pl.BlockSpec(memory_space=pltpu.VMEM)
    weight = [pl.BlockSpec((N1,) + w.shape[N1:], lambda i: (i % n, N0, N0)) for w in (wg, wl, wd)]
    early = pl.BlockSpec((N1, own, ffn), lambda i: (jnp.minimum(i, n - N1), N0, N0))
    late = pl.BlockSpec((N1, own, ffn), lambda i: (jnp.maximum(i - n, N0), N0, N0))
    shape = jax.ShapeDtypeStruct
    slots = shape((n, own, ffn), BF)
    return pl.pallas_call(
        functools.partial(layer_kernel, n),
        name='layer',
        grid=(N2 * n,),
        in_specs=[once] * 2 + [ANY] * 2 + [once] * 3 + weight,
        out_specs=[once] * 6 + [early, late, late],
        out_shape=[shape((own, width), BF)] * 3 + [shape((own, width), F32), shape((n, own, dims), F32), shape((N2 * n + 8, width), F32), slots, slots, slots],
        scratch_shapes=[pltpu.VMEM((n, own, ffn), F32)] * N2 + [pltpu.VMEM((own, width), F32)] * N2 + [pltpu.VMEM((own, N1), F32)] + [pltpu.VMEM((emb.shape[0],) + emb.shape[2:], BF)] * 2 + [pltpu.SemaphoreType.DMA((2,))],
        compiler_params=pltpu.CompilerParams(dimension_semantics=('arbitrary',), vmem_limit_bytes=62 * N2 ** 20),
        cost_estimate=pl.CostEstimate(flops=15 * 10 ** 9, bytes_accessed=70 * N2 ** 20, transcendentals=N0),
    )(ctx, wo, emb, cot, vectors, gate_bias, lin_bias, wg, wl, wd)


def products_kernel(n, hidden, d_ffn, inner, d_gate, d_lin, gate, lin, down, turned_hidden):
    i = pl.program_id(N0)
    size = hidden.shape[N1]
    tile = 256 if size % 256 == N0 else size

    @pl.when(i == N0)
    def _():
        turned_hidden[:] = hidden[:].T

    def fill(out, lhs, rhs, dims):
        for lo in range(N0, size, tile):
            cols = pl.ds(lo, tile)
            out[N0, :, cols] = dot(lhs, rhs[:, cols], dims)
    pl.when(i < n)(lambda: fill(gate, turned_hidden[:], d_gate.at[N0], NN))
    pl.when((i >= n) & (i < N2 * n))(lambda: fill(lin, turned_hidden[:], d_lin.at[N0], NN))

    @pl.when(i >= N2 * n)
    def _():
        fill(down, inner[N0].T, d_ffn, NN)


def products(hidden, d_ffn, inner, d_gate, d_lin):
    n, own, ffn = inner.shape
    width = hidden.shape[N1]
    once = pl.BlockSpec(memory_space=pltpu.VMEM)

    def slot(rows, first):
        return pl.BlockSpec((N1, rows, ffn), lambda i: (jnp.clip(i - first * n, N0, n - N1), N0, N0))
    shape = jax.ShapeDtypeStruct((n, width, ffn), F32)
    return pl.pallas_call(
        functools.partial(products_kernel, n),
        name='products',
        grid=(3 * n,),
        in_specs=[once, once, slot(own, N2), slot(own, N0), slot(own, N1)],
        out_specs=[slot(width, N0), slot(width, N1), slot(width, N2)],
        out_shape=[shape] * 3,
        scratch_shapes=[pltpu.VMEM((width, own), BF)],
        compiler_params=pltpu.CompilerParams(dimension_semantics=('arbitrary',), vmem_limit_bytes=58 * N2 ** 20),
        cost_estimate=pl.CostEstimate(flops=12 * 10 ** 9, bytes_accessed=70 * N2 ** 20, transcendentals=N0),
    )(hidden, d_ffn, inner, d_gate, d_lin)


def solution(mesh):
    n_tp, n_dp = mesh.shape['tp'], mesh.shape['dp']
    in_specs = (P('dp', None), P('dp', None, None), P('tp', None)) + WEIGHT_SPECS
    out_specs = (P('tp', None),) + WEIGHT_SPECS

    def device_step(tokens, cotangent, emb_table, *weights):
        (w_qkv, b_qkv, w_out, b_out, ln1_gain, ln1_bias, w_gate, b_gate, w_lin, b_lin, w_down, b_down, ln2_gain) = weights
        tp, dp = lax.axis_index('tp'), lax.axis_index('dp')
        tokens = tokens[N0]
        seq_len, width = tokens.shape[N0], emb_table.shape[N1]
        heads, head_dim = b_qkv.shape[N0], b_qkv.shape[N1] // 3
        own = seq_len // n_tp
        ffn = w_gate.shape[N1]
        rk, rf, ro = width // n_dp, ffn // n_dp, w_out.shape[N0] // n_dp

        def cut(weight):
            rows = weight.shape[N0] // n_dp
            return lax.dynamic_slice_in_dim(weight, dp * rows, rows, N0)
        bias_rows = jnp.concatenate([b_gate[None], b_lin[None], jnp.zeros((14, ffn), BF)], axis=N0)
        piece = jnp.concatenate([cut(w_gate), cut(w_lin), cut(w_down), cut(w_out), bias_rows], axis=N0).astype(F32)

        vocab_loc = emb_table.shape[N0]
        local_ids = tokens - tp * vocab_loc
        in_shard = (local_ids >= N0) & (local_ids < vocab_loc)
        safe_ids = jnp.where(in_shard, local_ids, N0)
        found = jnp.take(emb_table, safe_ids, axis=N0, mode='clip')
        dims = heads * head_dim
        place = column_order(heads, head_dim)
        swap = (jnp.arange(3 * dims)[:, None] == jnp.asarray(place)[None, :]).astype(BF)
        wq = jnp.dot(w_qkv, swap, preferred_element_type=F32).astype(BF)
        bq = jnp.dot(b_qkv.reshape(N1, -N1), swap, preferred_element_type=F32)
        cos_tab, sin_tab = rope_tables(seq_len, head_dim, heads)
        emb_bf, (wg_full, wl_full, wd_full, wo_full), biases, tok_all, ctx_own, saved = embed(found, in_shard[:, None].astype(F32), piece, tokens.reshape(-N1, min(128, seq_len // 8)), (w_gate, w_lin, w_down, w_out), wq, bq, cos_tab, sin_tab, heads, n_tp, n_dp)
        is_own = (jnp.arange(n_tp) == tp)[:, None]
        bg_full, bl_full = [jnp.where(is_own, b[None].astype(F32), biases[:, i]) for i, b in enumerate((b_gate, b_lin))]

        blocks = 8

        def by_owner(values):
            return values.reshape(blocks, n_tp, -N1, width)

        vectors = jnp.stack([b_out, ln1_gain, ln1_bias, b_down, ln2_gain] + [b_out] * 3).astype(F32)
        hidden, d_ffn_bf, d_attn_bf, resid, d_ctx, row_sums, inner_act, d_gate_bf, d_lin_bf = layer(
            ctx_own.reshape(n_tp, own, dims), wo_full, by_owner(emb_bf), by_owner(cotangent[N0]), vectors, bg_full, bl_full, wg_full, wl_full, wd_full)

        prods = [grad.reshape(n_tp, n_dp, -N1, width) for grad in products(hidden, d_ffn_bf, inner_act, d_gate_bf, d_lin_bf)]
        d_w_out = jnp.einsum('hse,sd->hed', ctx_own.reshape(n_tp, own, dims).astype(BF), d_attn_bf, preferred_element_type=F32)
        d_w_qkv, d_b_qkv, d_cols, (d_w_gate, d_w_lin), d_w_down = backward(
            d_ctx.reshape(n_tp, blocks, own // blocks, dims), resid.reshape(blocks, own // blocks, width), saved, cos_tab, sin_tab, wq, swap.T, emb_bf,
            prods, heads, n_tp, n_dp)
        d_w_gate, d_w_lin = d_w_gate.reshape(-N1, ffn), d_w_lin.reshape(-N1, ffn)
        d_b_qkv = jnp.dot(d_b_qkv, swap.astype(F32).T, precision=lax.Precision.HIGHEST)
        all_ids = tok_all.reshape(-N1) - tp * vocab_loc
        all_ids = jnp.where((all_ids >= N0) & (all_ids < vocab_loc), all_ids, vocab_loc)
        col = table_rows(all_ids, d_cols.reshape(n_dp * seq_len, -N1), vocab_loc)

        slot = (jnp.arange(n_tp) == tp).astype(F32)[:, None]
        d_bq_rows = jnp.pad(slot * d_b_qkv, ((N0, N0), (N0, ffn - 3 * dims)))
        kept = N2 * n_tp
        small = jnp.concatenate([row_sums[:kept], d_bq_rows, row_sums[kept:kept + 5], jnp.zeros((7, width), F32)], axis=N0)
        d_table, d_w_down, d_w_out, d_w_qkv, small = finish(
            col, d_w_down, d_w_out.reshape(n_tp, n_dp, N2, -N1, width), d_w_qkv.reshape(n_dp, N2, -N1, 3 * dims), small, n_tp, n_dp)
        d_b_gate = lax.dynamic_index_in_dim(small[:n_tp], tp, N0, keepdims=False)
        d_b_lin = lax.dynamic_index_in_dim(small[n_tp:N2 * n_tp], tp, N0, keepdims=False)
        d_b_qkv = lax.dynamic_index_in_dim(small[N2 * n_tp:3 * n_tp], tp, N0, keepdims=False)[:3 * dims].reshape(heads, 3 * head_dim)
        d_b_out, d_ln1_gain, d_ln1_bias, d_b_down, d_ln2_gain = [small[3 * n_tp + i] for i in range(5)]
        return (d_table, d_w_qkv, d_b_qkv, d_w_out, d_b_out, d_ln1_gain, d_ln1_bias, d_w_gate, d_b_gate, d_w_lin, d_b_lin, d_w_down, d_b_down, d_ln2_gain)

    return jax.shard_map(device_step, mesh=mesh, in_specs=in_specs, out_specs=out_specs, check_vma=False)
```

```python
import functools

import jax
import jax.numpy as jnp
import numpy as np
from jax import lax
from jax.experimental import pallas as pl
from jax.experimental.pallas import tpu as pltpu
from jax.sharding import PartitionSpec as P

ALPHA = 140.0 ** 0.5
EPS = 1e-5
SHRINK = 0.1
ROPE_BASE = 10000.0
WEIGHT_SPECS = (P(None, 'tp'), P('tp', None), P('tp', None), P(), P(), P(), P(None, 'tp'), P('tp'), P(None, 'tp'), P('tp'), P('tp', None), P(), P())
BF = jnp.bfloat16
N0, N1, N2 = range(3)
F32 = jnp.float32
MESH = pl.DeviceIdType.MESH
ANY = pl.BlockSpec(memory_space=pl.ANY)
VMEM = pl.BlockSpec(memory_space=pltpu.VMEM)


def rope_tables(seq_len, head_dim, heads):
    half_dim = head_dim // 2
    inv_freq = (ROPE_BASE ** (-2.0 * np.arange(half_dim) / head_dim)).astype(np.float32)
    angles = np.arange(seq_len, dtype=np.float32)[:, None] * inv_freq[None, :]
    return [jnp.asarray(np.tile(table(angles), (1, heads))) for table in (np.cos, np.sin)]


def column_order(heads, head_dim):
    cols = np.arange(3 * heads * head_dim).reshape(heads, 3, 2, head_dim // 2)
    return np.concatenate([cols[:, part].transpose(1, 0, 2).ravel() for part in (0, 1)] + [cols[:, 2].ravel()])


def rcopy(src, dst, send, recv, **where):
    return pltpu.make_async_remote_copy(src_ref=src, dst_ref=dst, send_sem=send, recv_sem=recv, device_id=dict(where), device_id_type=MESH)


def plane():
    p = lax.axis_index('dp')
    y, x, c = p // 4, (p // 2) % 2, p % 2

    def at(rel):
        yy = 1 - y if rel & 4 else y
        xx = 1 - x if rel & 2 else x
        cc = 1 - c if rel & 1 else c
        return yy * 4 + xx * 2 + cc
    return p, at


def entry_barrier(z, n, at):
    bar = pltpu.get_barrier_semaphore()
    for rel in range(1, 8):
        pl.semaphore_signal(bar, inc=1, device_id={'dp': at(rel)}, device_id_type=MESH)
    for d in range(1, n):
        pl.semaphore_signal(bar, inc=1, device_id={'tp': (z + d) % n}, device_id_type=MESH)
    pl.semaphore_wait(bar, 7 + n - 1)


LAG = 3


def chain_sum(k, z, n, rows, chunks, part, left, right, done, send_r, send_l, recv_l, recv_r, place=lambda c: c, lag=LAG):
    last = n - 1

    def at_rows(c):
        return pl.ds(pl.multiple_of(place(c) * rows, rows), rows)

    def cut(ref, c):
        return ref.at[at_rows(c)]

    def load(ref, c):
        return ref[at_rows(c)]

    def store(ref, c, value):
        ref[at_rows(c)] = value
    cl, cr = k - lag * z, k - lag * (last - z)
    okl, okr = (cl >= 0) & (cl < chunks), (cr >= 0) & (cr < chunks)

    @pl.when(okl & (z > 0))
    def _():
        rcopy(cut(left, cl), cut(left, cl), send_r, recv_l.at[cl], tp=z).wait_recv()

    @pl.when(okl & (z == last))
    def _():
        done(cl, load(left, cl) + load(part, cl))

    @pl.when(okl & (z > 0) & (z < last))
    def _():
        run = load(left, cl)

        @pl.when(z >= n // 2)
        def _():
            done(cl, run + load(right, cl))
        store(left, cl, run + load(part, cl))

    @pl.when(okr & (z < last))
    def _():
        rcopy(cut(right, cr), cut(right, cr), send_l, recv_r.at[cr], tp=z).wait_recv()

    @pl.when(okr & (z == 0))
    def _():
        done(cr, load(part, cr) + load(right, cr))

    @pl.when(okr & (z > 0) & (z < last))
    def _():
        run = load(right, cr)

        @pl.when(z < n // 2)
        def _():
            done(cr, load(left, cr) + run)
        store(right, cr, run + load(part, cr))

    @pl.when(okl & (z == 0))
    def _():
        rcopy(cut(part, cl), cut(left, cl), send_r, recv_l.at[cl], tp=z + 1).start()

    @pl.when(okl & (z > 0) & (z < last))
    def _():
        rcopy(cut(left, cl), cut(left, cl), send_r, recv_l.at[cl], tp=z + 1).start()

    @pl.when(okr & (z == last))
    def _():
        rcopy(cut(part, cr), cut(right, cr), send_l, recv_r.at[cr], tp=z - 1).start()

    @pl.when(okr & (z > 0) & (z < last))
    def _():
        rcopy(cut(right, cr), cut(right, cr), send_l, recv_r.at[cr], tp=z - 1).start()


def chain_drain(z, n, part, left, right, send_r, send_l, recv_l, recv_r):
    @pl.when(z < n - 1)
    def _():
        rcopy(part, left, send_r, recv_l.at[0], tp=z + 1).wait_send()

    @pl.when(z > 0)
    def _():
        rcopy(part, right, send_l, recv_r.at[0], tp=z - 1).wait_send()


EDGES = ((0, 0, 2), (0, 0, 4), (0, 0, 1), (2, 1, 4), (4, 2, 2), (2, 0, 1), (4, 0, 1), (6, 1, 1), (6, 2, 1))
CROSS, DIAGONAL, LAST = ((0, 3, 5), (1, 4, 6)), ((3, 7), (4, 8)), {1: (2,), 3: (5,), 5: (6,), 7: (7, 8)}
STEPS = (8, 14, 20, 24, 28, 32)
ARRIVE = {2: 2, 3: 8}
EMB_LAG = 4
FIRST = 18
ORDER = (0, 2, 4, 1, 3, 5, 6, 7)


def emb_kernel(n, rows, chunks, cuts, heads, found, mask, wq, bq, cos, sin, piece, toks, *refs):
    m = len(cuts)
    local, outs = refs[:m], refs[m + N1:N2 * m + N1]
    out, (bias, tok_all, wall, ctx_own, q, k_all, v, ctx, top, inv, part, left, right, raw, low, weights, send_r, send_l, recv_l, recv_r, tsend, trecv, tself, zsend, zrecv, psend, precv, lsem, isem, osem, bsem, asend, arecv, aself) = refs[m], refs[N2 * m + N1:]
    blocks = 8
    qb = part.shape[N0] // blocks
    per = chunks // blocks
    z = lax.axis_index('tp')
    p, at = plane()
    entry_barrier(z, n, at)
    half = piece.shape[N0] // N2

    @pl.when(z < n - N1)
    def _():
        rcopy(piece, wall.at[z, p], zsend.at[z], zrecv.at[z], tp=z + N1).start()

    @pl.when(z > N0)
    def _():
        rcopy(piece, wall.at[z, p], bsem.at[N1], zrecv.at[z], tp=z - N1).start()
    mine = [pltpu.make_async_copy(toks, tok_all.at[p], tself)]
    mine += [pltpu.make_async_copy(src, dst.at[z], lsem.at[i]) for i, (src, dst) in enumerate(zip(local, outs))]
    for copy in mine:
        copy.start()
    for rel in range(N1, 8):
        rcopy(toks, tok_all.at[p], tsend.at[rel], trecv.at[rel], dp=at(rel)).start()

    def others(d, body):
        @pl.when(z >= d)
        def _():
            body(z - d, -N1)

        @pl.when(z + d < n)
        def _():
            body(z + d, N1)

    def region(t, rel, side):
        blk = wall.at[t, at(rel)]
        return blk if side == N0 else wall.at[t, at(rel), pl.ds((side - N1) * half, half)]

    def give(t, j):
        rel, side, to = EDGES[j]
        rcopy(region(t, rel, side), region(t, rel, side), psend.at[t, j], precv.at[t, j], dp=at(to)).start()

    def take(t, j):
        rel, side, to = EDGES[j]
        blk = region(t, rel ^ to, side)
        rcopy(blk, blk, psend.at[t, j], precv.at[t, j], dp=p).wait_recv()

    def gave(t, j):
        rel, side, to = EDGES[j]
        rcopy(region(t, rel, side), region(t, rel, side), psend.at[t, j], precv.at[t, j], dp=p).wait_send()

    def arrive(d):
        def body(t, sign):
            blk = wall.at[t, p]
            rcopy(blk, blk, zsend.at[t], zrecv.at[t], tp=z).wait_recv()

            @pl.when((z - sign >= N0) & (z - sign < n))
            def _():
                rcopy(blk, blk, zsend.at[t], zrecv.at[t], tp=z - sign).start()
            for j in range(3):
                give(t, j)
        others(d, body)

    def relay(d, moves):
        def body(t, sign):
            for first, *rest in moves:
                take(t, first)
                for j in rest:
                    give(t, j)
        others(d, body)

    k_all[:] = jnp.zeros_like(k_all)
    v[:] = jnp.zeros_like(v)
    arrive(N1)

    @pl.loop(N0, blocks)
    def _(i):
        at_i = pl.ds(pl.multiple_of(i * qb, qb), qb)
        part[at_i, :] = jnp.where(mask[at_i, :] > N0, found[at_i, :].astype(F32), 0.0)

    def done(c, value):
        out[pl.ds(pl.multiple_of(c * rows, rows), rows)] = value.astype(out.dtype)

    def other(i):
        return i + (i + n - z) // n

    def loaded(i, rel, slot):
        return pltpu.make_async_copy(wall.at[other(i), at(rel), pl.ds(N0, cuts[-N1][N1])], raw.at[slot], isem.at[slot])

    def stored(i, rel, slot):
        return [pltpu.make_async_copy(low.at[slot, pl.ds(lo, hi - lo)], dst.at[other(i), at(rel)], osem.at[slot, k]) for k, ((lo, hi), dst) in enumerate(zip(cuts, outs))]
    plan = [(i, rel) for rel in ORDER for i in range(n - N1)]

    def prefetch(s):
        i, rel = plan[s]
        for j in LAST.get(rel, ()):
            take(other(i), j)
        loaded(i, rel, s % N2).start()

    def convert(s):
        i, rel = plan[s]
        loaded(i, rel, s % N2).wait()
        if s >= N2:
            for copy in stored(*plan[s - N2], s % N2):
                copy.wait()
        low[s % N2] = raw[s % N2].astype(low.dtype)
        if s + N1 < len(plan):
            prefetch(s + N1)
        for copy in stored(i, rel, s % N2):
            copy.start()
    events = [(STEPS[d - N1], functools.partial(relay, d, CROSS)) for d in range(N1, n)] + [(STEPS[d + n - N2], functools.partial(relay, d, DIAGONAL)) for d in range(N1, n)]
    events += [(ARRIVE[d], functools.partial(arrive, d)) for d in range(N2, n)]
    events += [(FIRST - N1, functools.partial(prefetch, N0))] + [(FIRST + s, functools.partial(convert, s)) for s in range(len(plan))]

    start = per + EMB_LAG * (n - N1)

    share = qb // n

    def context(i, d):
        to = (z + d) % n
        src = ctx.at[pl.ds(pl.multiple_of(i * qb + to * share, share), share)]
        if d == N0:
            return pltpu.make_async_copy(src, ctx_own.at[z, i], aself)
        return rcopy(src, ctx_own.at[z, i], asend, arecv.at[z], tp=to)

    @pl.loop(N0, max(start + blocks * heads + N1, FIRST + len(plan)))
    def _(k):
        step = k - start
        i = step // heads - N1

        @pl.when((step > N0) & (step % heads == N0) & (step <= blocks * heads))
        def _():
            for d in range(n):
                context(i, d).start()
        chain_sum(k, z, n, rows, chunks, part, left, right, done, send_r, send_l, recv_l, recv_r, lag=EMB_LAG)
        for at_step, event in events:
            pl.when(k == at_step)(event)

        @pl.when((step >= N0) & (step < blocks * heads))
        def _():
            @pl.when(step % heads == N0)
            def _():
                project(step // heads, qb, out, wq, bq, cos, sin, q, k_all, v)
            attend(step // heads, step % heads, heads, qb, q, k_all, v, ctx, top, inv, weights)

    pltpu.make_async_copy(ctx_own.at[z], ctx_own.at[z], aself).wait()
    for d in range(N1, n):
        src = (z + d) % n
        rcopy(ctx_own.at[src], ctx_own.at[src], asend, arecv.at[src], tp=z).wait()
    chain_drain(z, n, part, left, right, send_r, send_l, recv_l, recv_r)
    for s in (len(plan) - N2, len(plan) - N1):
        for copy in stored(*plan[s], s % N2):
            copy.wait()

    def finish(t, sign):
        for j in range(len(EDGES)):
            gave(t, j)
        tail = pltpu.make_async_copy(wall.at[t, p, pl.ds(cuts[-N1][N1], bias.shape[N1])], bias.at[t], bsem.at[N0])
        tail.start()
        tail.wait()

        @pl.when((z - sign >= N0) & (z - sign < n))
        def _():
            rcopy(wall.at[t, p], wall.at[t, p], zsend.at[t], zrecv.at[t], tp=z).wait_send()
    for d in range(N1, n):
        others(d, finish)
    for copy in mine:
        copy.wait()
    for rel in range(N1, 8):
        rcopy(toks, tok_all.at[at(rel)], tsend.at[rel], trecv.at[rel], dp=at(rel)).wait()

    @pl.when(z < n - N1)
    def _():
        rcopy(piece, wall.at[z, p], zsend.at[z], zrecv.at[z], tp=z + N1).wait_send()

    @pl.when(z > N0)
    def _():
        rcopy(piece, wall.at[z, p], bsem.at[N1], zrecv.at[z], tp=z - N1).wait_send()


def embed(found, mask, piece, toks, local, wq, bq, cos, sin, heads, n_tp, n_dp):
    seq, width = found.shape
    chunks = 32
    rows = seq // chunks
    dims = wq.shape[N1] // 3
    cuts, lo = [], N0
    for weight in local:
        cuts.append((lo, lo + weight.shape[N0] // n_dp))
        lo = cuts[-N1][N1]
    dma = pltpu.SemaphoreType.DMA
    shape = jax.ShapeDtypeStruct
    shapes = [shape((seq, width), BF)]
    shapes += [shape((n_tp, n_dp, w.shape[N0] // n_dp, w.shape[N1]), BF) for w in local]
    shapes += [shape((n_tp, piece.shape[N0] - lo, width), F32), shape((n_dp,) + toks.shape, toks.dtype), shape((n_tp, n_dp) + piece.shape, F32), shape((n_tp, 8, seq // n_tp // 8, dims), F32)]
    shapes += [shape((seq, dims), BF)] * 3 + [shape((seq, dims), F32)] + [shape((heads, seq), F32)] * N2
    out = pl.pallas_call(
        functools.partial(emb_kernel, n_tp, rows, chunks, cuts, heads),
        name='embed',
        out_shape=shapes,
        in_specs=[VMEM] * 6 + [ANY] * (N2 + len(local)),
        out_specs=[VMEM] + [ANY] * (4 + len(local)) + [VMEM] * 6,
        scratch_shapes=[pltpu.VMEM((seq, width), F32)] * 3 + [pltpu.VMEM((N2, lo, width), F32), pltpu.VMEM((N2, lo, width), BF), pltpu.VMEM((seq, seq // 8), F32), dma, dma, dma((chunks,)), dma((chunks,)),
                        dma((8,)), dma((8,)), dma, dma((n_tp,)), dma((n_tp,)), dma((n_tp, len(EDGES))), dma((n_tp, len(EDGES))), dma((len(local),)), dma((N2,)), dma((N2, len(local))), dma((N2,)),
                        dma, dma((n_tp,)), dma],
        compiler_params=pltpu.CompilerParams(collective_id=N0, has_side_effects=True, vmem_limit_bytes=60 * N2 ** 20),
        cost_estimate=pl.CostEstimate(flops=20 * 10 ** 9, bytes_accessed=80 * N2 ** 20, transcendentals=N0),
    )(found, mask, wq, bq, cos, sin, piece, toks, *[w.reshape(n_dp, w.shape[N0] // n_dp, w.shape[N1]) for w in local])
    m = N1 + len(local)
    return out[N0], [w.reshape(n_tp, -N1, w.shape[3]) for w in out[N1:m]], out[m], out[m + N1], out[m + 3], out[m + 4:]


RING = 4
HOLD, LIVE, PAIR = 4, 12, 4
ADD, LOAD, CROSSED, LAND, PLANE, HOP, BEAT = 1, 4, 5, 9, 10, 2, 4
GATHER = (37, 41)


def block_of(ref, at, rel, side):
    return ref.at[at(rel)] if side == 0 else ref.at[at(rel), side - 1]


class Spread:
    def __init__(self, at, block, send, recv, own=None):
        self.at, self.block, self.send, self.recv, self.own = at, block, send, recv, own

    def copy(self, j, rel, side, to):
        dst = self.block(rel, side)
        src = self.own if rel == 0 and self.own is not None else dst
        return rcopy(src, dst, self.send.at[j], self.recv.at[j], dp=self.at(to))

    def give(self, j):
        self.copy(j, *EDGES[j]).start()

    def take(self, j):
        rel, side, to = EDGES[j]
        self.copy(j, rel ^ to, side, 0).wait_recv()

    def start(self):
        for j in range(3):
            self.give(j)

    def relay(self, moves):
        for first, *rest in moves:
            self.take(first)
            for j in rest:
                self.give(j)

    def cross(self):
        self.relay(CROSS)

    def diagonal(self):
        self.relay(DIAGONAL)

    def finish(self):
        for j in (2, 5, 6, 7, 8):
            self.take(j)
        for j, (rel, side, _) in enumerate(EDGES):
            self.copy(j, rel, side, 0).wait_send()


def backward_kernel(n, rows, chunks, jobs, heads, d_ctx, resid, q, k_all, v, ctx, top, inv, cos, sin, wq, back, emb, *refs):
    prods = refs[:jobs]
    whole = refs[jobs:N2 * jobs - N1]
    out, grads, d_w, d_bias, landed, cross, last, part, left, right, total, dctx, dq, dk, dv, ctx_in, res_in, cos_in, sin_in, emb_in, q_in, work, fresh, xin, yin, keep, pass_on, along, final, *sems = refs[N2 * jobs - N1:]
    send_r, send_l, recv_l, recv_r, osend, orecv, csend, crecv, esem, fsem, xsend, xrecv, xsem, ysend, yrecv, ysem, ksem, zrecv, frecv, asend, arecv, aself, isem, gsend, grecv = sems
    z = lax.axis_index('tp')
    p, at = plane()
    entry_barrier(z, n, at)
    blocks = 8
    per = chunks // blocks
    qb = rows * per
    share = qb // n
    block = out.shape[N2]
    lead = jnp.maximum(z, n - N1 - z)
    span = N2 * n
    units = jobs * span
    size = work.shape[N2]

    def rows_of(i, to, count):
        return pl.ds(pl.multiple_of(i * qb + to * count, count), count)

    def exchange(i, d):
        to = (z + d) % n
        dst = dctx.at[rows_of(i, z, share)]
        if d == N0:
            return pltpu.make_async_copy(d_ctx.at[z, i], dst, aself.at[i])
        return rcopy(d_ctx.at[to, i], dst, asend, arecv.at[i], tp=to)

    @pl.loop(N0, blocks)
    def _(b):
        for d in range(n):
            exchange(blocks - N1 - b, d).start()

    def piece(m, u, rel):
        return prods[m].at[(u % span) // N2, at(rel), pl.ds(pl.multiple_of((u % N2) * size, size), size)]

    for m in range(jobs):
        @pl.loop(m * span, (m + N1) * span)
        def _(u, m=m):
            for i in range(4):
                rcopy(piece(m, u, N2 * i + N1), landed.at[u, i], csend, crecv.at[u], dp=at(N1)).start()

    def inputs(i):
        slot = i % N2
        at_q = rows_of(i, N0, qb)
        pairs = ((ctx.at[at_q], ctx_in), (resid.at[i], res_in), (cos.at[at_q], cos_in), (sin.at[at_q], sin_in), (emb.at[at_q], emb_in), (q.at[at_q], q_in))
        return [pltpu.make_async_copy(src, dst.at[slot], isem.at[j, slot]) for j, (src, dst) in enumerate(pairs)]

    dk[:] = jnp.zeros_like(dk)
    dv[:] = jnp.zeros_like(dv)
    d_w[:] = jnp.zeros_like(d_w)
    d_bias[:] = jnp.zeros_like(d_bias)
    for copy in inputs(blocks - N1):
        copy.start()

    def attention_step(b, h):
        i = blocks - N1 - b

        @pl.when(h == N0)
        def _():
            for copy in inputs(i):
                copy.wait()

            @pl.when(b + N1 < blocks)
            def _():
                for copy in inputs(i - N1):
                    copy.start()
            exchange(i, N0).wait()
            others = dctx.at[pl.ds(N0, (n - N1) * share)]
            rcopy(others, others, asend, arecv.at[i], tp=z).wait_recv()
        attend_grad(i, h, heads, qb, q_in.at[i % N2], k_all, v, ctx_in.at[i % N2], dctx, top, inv, dq, dk, dv)

        @pl.when(h == heads - N1)
        def _():
            slot = i % N2
            got = grad_rows(i, qb, cos_in[slot], sin_in[slot], dq, dk, dv, d_bias)
            d_w[:] += dot(emb_in[slot], dot(got, back[:], NN).astype(BF), TN)
            part[rows_of(i, N0, qb), :] = dot(got, wq[:], NT)
            part[rows_of(i, z, share), :] = part[rows_of(i, z, share), :] + res_in[i % N2]

    def sides(u):
        side = u % N2
        return side, at(N2) * (N1 - side) + at(4) * side, at(4) * (N1 - side) + at(N2) * side

    def fetch(u):
        slot = u % HOLD

        @pl.when(u >= HOLD)
        def _():
            rcopy(xin, cross.at[N0], xsend.at[slot], xrecv.at[N0], dp=p).wait_send()
        for m in range(jobs):
            @pl.when(u // span == m)
            def _(m=m):
                for i in range(4):
                    pltpu.make_async_copy(piece(m, u, N2 * i), work.at[slot, i], esem.at[slot]).start()
        rcopy(landed.at[u], landed.at[u], csend, crecv.at[u], dp=p).wait_recv()
        pltpu.make_async_copy(landed.at[u], fresh, fsem).start()

    def add(u):
        slot = u % HOLD
        pltpu.make_async_copy(landed.at[u], work.at[slot], esem.at[slot]).wait()
        pltpu.make_async_copy(landed.at[u], fresh, fsem).wait()
        for i in range(4):
            work[slot, i] = work[slot, i] + fresh[i]

    def add_send(u):
        slot = u % HOLD
        side, first, second = sides(u)
        rcopy(work.at[slot, N1 + side], cross.at[u, N0], xsend.at[slot], xrecv.at[u], dp=first).start()
        rcopy(work.at[slot, 3], cross.at[u, N1], xsend.at[slot], xrecv.at[u], dp=first).start()

    def load_cross(u):
        rcopy(cross.at[u], cross.at[u], xsend.at[N0], xrecv.at[u], dp=p).wait_recv()
        pltpu.make_async_copy(cross.at[u], xin, xsem).start()

    def crossed(u):
        slot = u % HOLD
        pltpu.make_async_copy(cross.at[u], xin, xsem).wait()

        @pl.when(u >= LIVE)
        def _():
            pltpu.make_async_copy(keep.at[u % LIVE], keep.at[u % LIVE], ksem.at[u % LIVE]).wait()

        @pl.when(u >= PAIR)
        def _():
            rcopy(pass_on.at[u % PAIR], last.at[u], ysend.at[u % PAIR], yrecv.at[u], dp=p).wait_send()
        keep[u % LIVE] = xin[N0] + work[slot, N0]
        pass_on[u % PAIR] = xin[N1] + work[slot, N2 - u % N2]

    def crossed_send(u):
        side, first, second = sides(u)
        rcopy(pass_on.at[u % PAIR], last.at[u], ysend.at[u % PAIR], yrecv.at[u], dp=second).start()

    def load_last(u):
        rcopy(last.at[u], last.at[u], ysend.at[N0], yrecv.at[u], dp=p).wait_recv()
        pltpu.make_async_copy(last.at[u], yin, ysem).start()

    def in_plane(u):
        pltpu.make_async_copy(last.at[u], yin, ysem).wait()
        keep[u % LIVE] = keep[u % LIVE] + yin[:]

    def unit(k):
        u = (k // BEAT) * (BEAT - N1) + k % BEAT
        return u, (k >= N0) & (k % BEAT < BEAT - N1) & (u < units)

    def along_tp(k, t, send):
        toward = jnp.where(z < t, z, n - N1 - z)
        late = HOP * jnp.where(z == t, max(t, n - N1 - t), toward)
        u, ok = unit(k - PLANE - N1 - late)
        mine = (u // span) * N2 + u % N2
        slot = u % LIVE
        ok = ok & ((u // N2) % n == t)

        def add_from(ref, sem):
            rcopy(ref, ref, csend, sem, tp=z).wait_recv()
            keep[slot] = keep[slot] + ref[:]
        if send:
            @pl.when(ok & (z < t))
            def _():
                rcopy(keep.at[slot], along.at[u], ksem.at[slot], zrecv.at[u], tp=z + N1).start()

            @pl.when(ok & (z > t + N1))
            def _():
                rcopy(keep.at[slot], along.at[u], ksem.at[slot], zrecv.at[u], tp=z - N1).start()

            @pl.when(ok & (z == t + N1))
            def _():
                rcopy(keep.at[slot], final.at[mine], ksem.at[slot], frecv.at[mine], tp=z - N1).start()

            for m in range(jobs):
                @pl.when(ok & (z == t) & (u // span == m))
                def _(m=m):
                    dst = whole[m].at[p, u % N2] if m < jobs - N1 else grads.at[u % N2]
                    pltpu.make_async_copy(keep.at[slot], dst, ksem.at[slot]).start()
        else:
            @pl.when(ok & (((z > N0) & (z <= t)) | ((z > t) & (z < n - N1))))
            def _():
                add_from(along.at[u], zrecv.at[u])
            if t < n - N1:
                @pl.when(ok & (z == t))
                def _():
                    add_from(final.at[mine], frecv.at[mine])

    spread = [Spread(at, functools.partial(block_of, whole[m], at), gsend.at[m], grecv.at[m]) for m in range(jobs - N1)]

    def settle(u):
        pltpu.make_async_copy(keep.at[u % LIVE], keep.at[u % LIVE], ksem.at[u % LIVE]).wait()

    def begin(m):
        for u in range(max(m * span, units - LIVE), (m + N1) * span):
            settle(u)
        spread[m].start()

    def place(c):
        return (blocks - N1 - c // per) * per + c % per

    def chunk(c):
        return total.at[c % RING]

    def done(c, value):
        @pl.when(c >= RING)
        def _():
            pltpu.make_async_copy(chunk(c), chunk(c), osend.at[c % RING]).wait()
        total[c % RING] = value

    def hand_out(c):
        where = out.at[p, pl.ds(pl.multiple_of(place(c) * rows, rows), rows)]
        for rel in range(8):
            src = total.at[c % RING, :, pl.ds(pl.multiple_of(at(rel) * block, block), block)]
            if rel == N0:
                pltpu.make_async_copy(src, where, osend.at[c % RING]).start()
            else:
                rcopy(src, where, osend.at[c % RING], orecv.at[rel], dp=at(rel)).start()

    def staged(k, offset, stage):
        u, ok = unit(k - offset)
        pl.when(ok)(functools.partial(stage, u))
    steps = max(heads + chunks + LAG * (n - N1) + N1, units // (BEAT - N1) * BEAT + PLANE + HOP * (n - N1), GATHER[-N1] + 7)

    @pl.loop(N0, steps)
    def _(k):
        c = k - heads - LAG * lead - N1

        @pl.when((c >= N0) & (c < chunks))
        def _():
            hand_out(c)
        chain_sum(k - heads, z, n, rows, chunks, part, left, right, done, send_r, send_l, recv_l, recv_r, place)
        for offset, stage in ((CROSSED, crossed), (ADD, add), (PLANE, in_plane)):
            staged(k, offset, stage)
        for t in range(n):
            along_tp(k, t, False)
        for offset, stage in ((N0, fetch), (LOAD, load_cross), (LAND, load_last)):
            staged(k, offset, stage)

        @pl.when(k < blocks * heads)
        def _():
            attention_step(k // heads, k % heads)
        for offset, stage in ((ADD, add_send), (CROSSED, crossed_send)):
            staged(k, offset, stage)
        for t in range(n):
            along_tp(k, t, True)
        for m, gather in enumerate(spread):
            for offset, stage in ((N0, functools.partial(begin, m)), (3, gather.cross), (6, gather.diagonal)):
                pl.when(k == GATHER[m] + offset)(stage)

    chain_drain(z, n, part, left, right, send_r, send_l, recv_l, recv_r)
    for c in range(max(N0, chunks - RING), chunks):
        pltpu.make_async_copy(chunk(c), chunk(c), osend.at[c % RING]).wait()
    for rel in range(N1, 8):
        rcopy(out.at[at(rel)], out.at[at(rel)], csend, orecv.at[rel], dp=p).wait_recv()
    for slot in range(HOLD):
        rcopy(xin, cross.at[N0], xsend.at[slot], xrecv.at[N0], dp=p).wait_send()
    for slot in range(PAIR):
        rcopy(pass_on.at[slot], last.at[N0], ysend.at[slot], yrecv.at[N0], dp=p).wait_send()
    for u in range(max((jobs - N1) * span, units - LIVE), units):
        settle(u)
    rcopy(landed, landed, csend, crecv.at[N0], dp=p).wait_send()
    for gather in spread:
        gather.finish()
    sent = dctx.at[pl.ds(N0, (n - N1) * share * blocks)]
    rcopy(sent, sent, asend, arecv.at[N0], tp=z).wait_send()


def backward(d_ctx, resid, saved, cos, sin, wq, back, emb, prods, heads, n_tp, n_dp):
    q, k, v, ctx, top, inv = saved
    seq, dims = q.shape
    width = wq.shape[N0]
    chunks = 32
    rows = seq // chunks
    jobs = len(prods)
    piece = (prods[N0].shape[N2] // N2, prods[N0].shape[3])
    units = jobs * N2 * n_tp
    dma = pltpu.SemaphoreType.DMA
    shape = jax.ShapeDtypeStruct
    qb = seq // 8
    vmem = [(seq, width)] * 3 + [(RING, rows, width), (seq, dims), (qb, dims), (seq, dims), (seq, dims), (N2, qb, dims), (N2, qb // n_tp, width)] + [(N2, qb, dims // N2)] * N2 + [
            (HOLD, 4) + piece, (4,) + piece, (N2,) + piece, piece, (LIVE,) + piece, (PAIR,) + piece, (units,) + piece, (N2 * jobs,) + piece]
    sems = [(), (), (chunks,), (chunks,), (RING,), (8,), (), (units,), (HOLD,), (), (HOLD,), (units,), (), (PAIR,), (units,), (), (LIVE,), (units,), (N2 * jobs,), (), (8,), (8,), (6, N2), (jobs - N1, len(EDGES)), (jobs - N1, len(EDGES))]
    scratch = [pltpu.VMEM(size, F32) for size in vmem]
    scratch[12:12] = [pltpu.VMEM((N2, qb, width), BF), pltpu.VMEM((N2, qb, dims), BF)]
    full = shape((n_dp, N2) + piece, F32)
    *whole, cols, grads, d_w, d_bias, _, _, _ = pl.pallas_call(
        functools.partial(backward_kernel, n_tp, rows, chunks, jobs, heads),
        name='backward',
        out_shape=[full] * (jobs - N1) + [shape((n_dp, seq, width // n_dp), F32), shape((N2,) + piece, F32), shape((width, 3 * dims), F32), shape((N1, 3 * dims), F32),
                   shape((units, 4) + piece, F32), shape((units, N2) + piece, F32), shape((units,) + piece, F32)],
        in_specs=[ANY] * 3 + [VMEM] * N2 + [ANY] + [VMEM] * N2 + [ANY] * N2 + [VMEM] * N2 + [ANY] * (N1 + jobs),
        out_specs=[ANY] * (jobs - N1) + [ANY, ANY, VMEM, VMEM, ANY, ANY, ANY],
        scratch_shapes=scratch + [dma(size) for size in sems],
        compiler_params=pltpu.CompilerParams(collective_id=N1, has_side_effects=True, vmem_limit_bytes=67_000_000),
        cost_estimate=pl.CostEstimate(flops=20 * 10 ** 9, bytes_accessed=100 * N2 ** 20, transcendentals=N0),
    )(d_ctx, resid, q, k, v, ctx, top, inv, cos, sin, wq, back, emb, *prods)
    return d_w, d_bias, cols, whole, grads


WAYS = 4


def table_kernel(ids, rows_ref, one, two, out, one_out, two_out, *tables):
    one_out[:] = one[:]
    two_out[:] = two[:]
    step = pl.program_id(0)
    count = rows_ref.shape[0]
    part = count // WAYS

    @pl.when(step == 0)
    def _():
        for table in tables:
            table[:] = jnp.zeros_like(table)

    @pl.loop(0, part, unroll=4)
    def _(r):
        for way, table in enumerate(tables):
            row = way * part + r
            where = pl.ds(ids[step * count + row], 1)
            table[where, :] = table[where, :] + rows_ref[pl.ds(row, 1), :]

    @pl.when(step == pl.num_programs(0) - 1)
    def _():
        total = tables[0][:]
        for table in tables[1:]:
            total = total + table[:]
        out[:] = SHRINK * total[:out.shape[0]]


def table_rows(ids, rows, vocab_loc, one, two):
    count, block = rows.shape
    step = min(1024, count // 2)
    tall = pl.BlockSpec((one.shape[0] // (count // step), one.shape[1]), lambda i, ids: (i, 0))
    same = jax.ShapeDtypeStruct(one.shape, F32)
    return pl.pallas_call(
        table_kernel,
        name='table_rows',
        grid_spec=pltpu.PrefetchScalarGridSpec(
            num_scalar_prefetch=1,
            grid=(count // step,),
            in_specs=[pl.BlockSpec((step, block), lambda i, ids: (i, 0)), tall, tall],
            out_specs=[pl.BlockSpec((vocab_loc, block), lambda i, ids: (0, 0)), tall, tall],
            scratch_shapes=[pltpu.VMEM((vocab_loc + 8, block), F32)] * WAYS,
        ),
        out_shape=[jax.ShapeDtypeStruct((vocab_loc, block), F32), same, same],
        compiler_params=pltpu.CompilerParams(dimension_semantics=('arbitrary',), vmem_limit_bytes=48 * 2 ** 20),
        cost_estimate=pl.CostEstimate(flops=3 * 10 ** 9, bytes_accessed=16 * 2 ** 20, transcendentals=0),
    )(ids, rows, one, two)


class PlaneSum:
    def __init__(self, at, block, landed, work, cross, last, mine, sems):
        self.at, self.block, self.landed, self.work, self.cross, self.last, self.mine, self.sems = at, block, landed, work, cross, last, mine, sems

    def copy(self, src, dst, kind, side, rel):
        return rcopy(src, dst, self.sems.at[kind, side, N0], self.sems.at[kind, side, N1], dp=self.at(rel))

    def start(self):
        for i in range(4):
            self.copy(self.block(N2 * i + N1), self.landed.at[i], N0, N0, N1).start()

    def first(self):
        self.copy(self.landed, self.landed, N0, N0, N0).wait()
        for i in range(4):
            self.work[i] = self.block(N2 * i)[:] + self.landed[i]

    def first_send(self):
        for side in range(N2):
            self.copy(self.work.at[N1 + side, side], self.cross.at[side, N0], N1, side, N2 * (N1 + side)).start()
            self.copy(self.work.at[3, side], self.cross.at[side, N1], N1, side, N2 * (N1 + side)).start()

    def second(self):
        for side in range(N2):
            self.copy(self.cross.at[side], self.cross.at[side], N1, side, N0).wait()
            self.cross[side, N0] = self.cross[side, N0] + self.work[N0, side]
            self.cross[side, N1] = self.cross[side, N1] + self.work[N2 - side, side]

    def second_send(self):
        for side in range(N2):
            self.copy(self.cross.at[side, N1], self.last.at[side], N2, side, N2 * (N2 - side)).start()

    def end(self):
        for side in range(N2):
            self.copy(self.last.at[side], self.last.at[side], N2, side, N0).wait()
            self.mine[side] = self.cross[side, N0] + self.last[side]


def finish_kernel(n, cuts, col, down, proj, d_w, small, table, down_all, proj_all, qkv_all, total, *refs):
    scratch, (summed, inbox, arrived, sem, send, recv, dsend, drecv, osem, psem, zsem, rsem) = refs[:10], refs[10:]
    z = lax.axis_index('tp')
    p, at = plane()
    entry_barrier(z, n, at)
    block = col.shape[N1]
    half = len(cuts) // N2

    def part(i):
        def region(rel, side):
            return table.at[pl.ds(cuts[i][N0], cuts[i][N1] - cuts[i][N0]), pl.ds(pl.multiple_of(at(rel) * block, block), block)]
        return Spread(at, region, send.at[i], recv.at[i], col.at[pl.ds(cuts[i][N0], cuts[i][N1] - cuts[i][N0])])
    parts = [part(i) for i in range(len(cuts))]
    qkv_sum = PlaneSum(at, lambda rel: d_w.at[at(rel)], *scratch[:5], psem.at[N0])
    proj_sum = PlaneSum(at, lambda rel: summed.at[at(rel)], *scratch[5:], psem.at[N1])
    pairs = ((down, down_all), (proj_sum.mine, proj_all), (qkv_sum.mine, qkv_all))
    spread = [Spread(at, functools.partial(block_of, ref, at), dsend.at[i], drecv.at[i], own) for i, (own, ref) in enumerate(pairs)]
    own_copies = [pltpu.make_async_copy(col, table.at[:, pl.ds(pl.multiple_of(p * block, block), block)], osem.at[N0])]
    own_copies += [pltpu.make_async_copy(src, dst.at[p], osem.at[i]) for i, (src, dst) in enumerate(pairs, N1)]
    order = list(range(len(cuts)))
    flipped = order[half:] + order[:half]
    peers = [{'dp': at(N1)}, {'dp': at(N2)}, {'dp': at(4)}, {'tp': z + N1 - N2 * (z % N2)}, {'tp': (z + n // N2) % n}]

    def next_part(i):
        parts[order[i]].give(N0)
        parts[flipped[i]].give(N1)
        parts[order[i]].give(N2)

    def relay_part(i):
        one, two = order[i], flipped[i]
        parts[one].take(N0)
        if one < half:
            parts[one].give(3)
        parts[one].give(5)
        parts[two].take(N1)
        if two >= half:
            parts[two].give(4)
        parts[two].give(6)

    def exchange(r):
        return rcopy(total, inbox.at[r], rsem.at[N0, r], rsem.at[N1, r], **peers[r])

    def round_end(r):
        exchange(r).wait()
        total[:] = total[:] + inbox[r]

    total[:] = small[:]
    for d in range(N1, n):
        to = (z + d) % n
        rcopy(proj.at[to], arrived.at[z], zsem.at[N0, to], zsem.at[N1, z], tp=to).start()
    qkv_sum.start()
    for copy in own_copies[:N2]:
        copy.start()
    next_part(N0)
    exchange(N0).start()
    spread[N0].start()
    next_part(N1)
    qkv_sum.first()
    round_end(N0)
    qkv_sum.first_send()
    exchange(N1).start()
    next_part(N2)
    relay_part(N0)
    round_end(N1)
    qkv_sum.second()
    exchange(N2).start()
    qkv_sum.second_send()
    next_part(3)
    spread[N0].cross()
    relay_part(N1)
    round_end(N2)
    qkv_sum.end()
    exchange(3).start()
    next_part(4)
    spread[N2].start()
    own_copies[3].start()
    spread[N0].diagonal()
    relay_part(N2)
    summed[:] = proj[z]
    for d in range(N1, n):
        src = (z + d) % n
        rcopy(proj.at[src], arrived.at[src], zsem.at[N0, src], zsem.at[N1, src], tp=src).wait()
        summed[:] = summed[:] + arrived[src]
    round_end(3)
    next_part(5)
    exchange(4).start()
    proj_sum.start()
    relay_part(3)
    spread[N2].cross()
    proj_sum.first()
    next_part(6)
    proj_sum.first_send()
    round_end(4)
    relay_part(4)
    proj_sum.second()
    next_part(7)
    proj_sum.second_send()
    spread[N2].diagonal()
    relay_part(5)
    proj_sum.end()
    relay_part(6)
    spread[N1].start()
    own_copies[N2].start()
    relay_part(7)
    spread[N1].cross()
    spread[N1].diagonal()
    for i in range(half):
        for via, where in ((3, i), (4, i + half)):
            parts[where].take(via)
            parts[where].give(7)
    for i in order:
        for j in (N2, 5, 6, 7):
            parts[i].take(j)
        for j in (N0, N1, N2, 3 if i < half else 4, 5, 6, 7):
            parts[i].copy(j, *EDGES[j]).wait_send()
    for gather in spread:
        gather.finish()
    for copy in own_copies:
        copy.wait()


def finish(col, down, proj, d_w, small, n_tp, n_dp):
    size, block = col.shape
    tiles = size // 8
    cuts = [(8 * (tiles * i // 8), 8 * (tiles * (i + N1) // 8)) for i in range(8)]
    dma = pltpu.SemaphoreType.DMA
    shape = jax.ShapeDtypeStruct
    ours = (d_w.shape[N1:], proj.shape[N2:])
    kinds = len(EDGES)
    vmem = [lead + src[N1:] for src in ours for lead in ((4, N2), (4, N2), (N2, N2), (N2,), (N2,))] + [proj.shape[N1:], (5,) + small.shape, proj.shape]
    sems = [(), (8, kinds), (8, kinds), (3, kinds), (3, kinds), (4,), (N2, 3, N2, N2), (N2, n_tp), (N2, 5)]
    table, down_all, proj_all, qkv_all, total = pl.pallas_call(
        functools.partial(finish_kernel, n_tp, cuts),
        name='finish',
        out_shape=[shape((size, n_dp * block), F32)] + [shape((n_dp,) + src, F32) for src in (down.shape, ours[N1], ours[N0])] + [shape(small.shape, F32)],
        in_specs=[ANY] * N2 + [VMEM] * 3,
        out_specs=[ANY] * 4 + [VMEM],
        scratch_shapes=[pltpu.VMEM(dims, F32) for dims in vmem] + [dma(dims) for dims in sems],
        compiler_params=pltpu.CompilerParams(collective_id=N2, has_side_effects=True, vmem_limit_bytes=48 * N2 ** 20),
        cost_estimate=pl.CostEstimate(flops=10 * 10 ** 9, bytes_accessed=60 * N2 ** 20, transcendentals=N0),
    )(col, down, proj, d_w, small)
    return [table] + [grad.reshape(-N1, grad.shape[3]) for grad in (down_all, proj_all, qkv_all)] + [total]


def dot(a, b, dims):
    return lax.dot_general(a, b, (dims, ((), ())), preferred_element_type=F32)


NT, TN, NN = ((1,), (1,)), ((0,), (0,)), ((1,), (0,))


def lane_head(shape, heads, halves):
    lane = lax.broadcasted_iota(jnp.int32, shape, 1)
    dims = shape[1] // halves
    return (lane % dims) // (dims // heads)


def turned(both, cos, sin):
    half = both.shape[1] // 2
    x1, x2 = both[:, :half], both[:, half:]
    return jnp.concatenate([x1 * cos - x2 * sin, x2 * cos + x1 * sin], axis=1)


def project(i, qb, emb, wq, bq, cos, sin, q, k, v):
    at_q = pl.ds(pl.multiple_of(i * qb, qb), qb)
    dims = q.shape[1]
    qkv = (dot(emb[at_q, :], wq[:], NN) + bq[:]).astype(BF)
    for ref, part in ((q, 0), (k, 1)):
        ref[at_q, :] = turned(qkv[:, part * dims:(part + 1) * dims].astype(F32), cos[at_q, :], sin[at_q, :]).astype(BF)
    v[at_q, :] = qkv[:, 2 * dims:]


def scores(i, j, kb, qb, scale, keys, q, diagonal):
    s = dot(keys, q, NT) * scale
    if not diagonal:
        return s
    key = j * kb + lax.broadcasted_iota(jnp.int32, (kb, qb), 0)
    query = i * qb + lax.broadcasted_iota(jnp.int32, (kb, qb), 1)
    return jnp.where(query >= key, s, -1e30)


def attend(i, h, heads, qb, q_ref, k_ref, v_ref, ctx_ref, top_ref, inv_ref, s_ref):
    kb = 2 * qb
    dims = q_ref.shape[1]
    scale = (dims // heads) ** -0.5
    at_q = pl.ds(pl.multiple_of(i * qb, qb), qb)
    q = jnp.where(lane_head((qb, dims), heads, 2) == h, q_ref[at_q, :].astype(F32), 0.0).astype(BF)
    count = (i + 2) // 2

    def at_key(j):
        return pl.ds(pl.multiple_of(j * kb, kb), kb)

    def first(diagonal, j, top):
        s = scores(i, j, kb, qb, scale, k_ref[at_key(j), :], q, diagonal)
        s_ref[at_key(j), :] = s
        return jnp.maximum(top, jnp.max(s, axis=0, keepdims=True))
    top = lax.fori_loop(0, count - 1, functools.partial(first, False), jnp.full((1, qb), -1e30, F32))
    top = first(True, count - 1, top)

    def weigh(j, total):
        e = jnp.exp(s_ref[at_key(j), :] - top)
        s_ref[at_key(j), :] = e
        return total + jnp.sum(e, axis=0, keepdims=True)
    inv = 1.0 / lax.fori_loop(0, count, weigh, jnp.zeros((1, qb), F32))

    def mix(j, acc):
        return acc + dot((s_ref[at_key(j), :] * inv).astype(BF), v_ref[at_key(j), :], TN)
    mixed = lax.fori_loop(0, count, mix, jnp.zeros((qb, dims), F32))
    ctx_ref[at_q, :] = jnp.where(lane_head((qb, dims), heads, 1) == h, mixed, ctx_ref[at_q, :])
    top_ref[pl.ds(h, 1), at_q] = top
    inv_ref[pl.ds(h, 1), at_q] = inv


def attend_grad(i, h, heads, qb, q_ref, k_ref, v_ref, ctx_ref, dctx_ref, top_ref, inv_ref, dq_ref, dk_ref, dv_ref):
    kb = 2 * qb
    dims = dk_ref.shape[1]
    scale = (dims // heads) ** -0.5
    at_q = pl.ds(pl.multiple_of(i * qb, qb), qb)
    q = jnp.where(lane_head((qb, dims), heads, 2) == h, q_ref[:].astype(F32), 0.0).astype(BF)
    dc = jnp.where(lane_head((qb, dims), heads, 1) == h, dctx_ref[at_q, :], 0.0).astype(BF)
    ones = jnp.ones((8, dims), F32)
    mean = lax.dot_general(ones, dc.astype(F32) * ctx_ref[:], (NT, ((), ())), precision=lax.Precision.HIGHEST, preferred_element_type=F32)[:1]
    top, inv = top_ref[pl.ds(h, 1), at_q], inv_ref[pl.ds(h, 1), at_q]

    def step(diagonal, j, dq):
        at_k = pl.ds(pl.multiple_of(j * kb, kb), kb)
        keys = k_ref[at_k, :]
        probs = (jnp.exp(scores(i, j, kb, qb, scale, keys, q, diagonal) - top) * inv).astype(BF)
        ds = (probs.astype(F32) * (dot(v_ref[at_k, :], dc, NT) - mean) * scale).astype(BF)
        dv_ref[at_k, :] += dot(probs, dc, NN)
        dk_ref[at_k, :] += dot(ds, q, NN)
        return dq + dot(ds, keys, TN)
    last = (i + 2) // 2 - 1
    dq = step(True, last, lax.fori_loop(0, last, functools.partial(step, False), jnp.zeros((qb, dims), F32)))
    dq_ref[:] = jnp.where(lane_head((qb, dims), heads, 2) == h, dq, dq_ref[:])


def grad_rows(i, qb, cos, sin, dq, dk, dv, d_bias):
    at_q = pl.ds(pl.multiple_of(i * qb, qb), qb)
    back = [turned(values, cos, -sin) for values in (dq[:], dk[at_q, :])]
    rows = jnp.concatenate(back + [dv[at_q, :]], axis=1)
    d_bias[:] += jnp.sum(rows, axis=0, keepdims=True)
    return rows.astype(BF)


def standard(values):
    mean = jnp.mean(values, axis=1, keepdims=True)
    centered = values - mean
    scale = lax.rsqrt(jnp.mean(centered * centered, axis=1, keepdims=True) + EPS)
    return centered * scale, scale


def standard_grad(d_out, unit, scale):
    return scale * (d_out - jnp.mean(d_out, axis=1, keepdims=True) - unit * jnp.mean(d_out * unit, axis=1, keepdims=True))


def over_rows(values):
    return jnp.sum(values, axis=0, keepdims=True)


def layer_kernel(n, ctx, wo, emb, cot, vectors, gate_bias, lin_bias, wg, wl, wd, hidden, d_ffn, d_attn, resid, d_ctx, sums, inner, d_gate, d_lin, gate, lin, acc, unit1, scale1, emb_own, cot_own, sem):
    i = pl.program_id(N0)
    t = i % n
    tile = 256 if acc.shape[N1] % 256 == N0 else acc.shape[N1]
    tiles = range(N0, acc.shape[N1], tile)
    b_out, gain1, bias1, b_down, gain2 = [vectors[pl.ds(j, N1), :] for j in range(5)]

    def owned(src, dst, j):
        return pltpu.make_async_copy(src.at[:, lax.axis_index('tp')], dst, sem.at[j])

    @pl.when(i == N0)
    def _():
        owned(emb, emb_own, N0).start()
        owned(cot, cot_own, N1).start()
        owned(emb, emb_own, N0).wait()
        total = ALPHA * emb_own[:].reshape(acc.shape).astype(F32) + b_out
        for h in range(n):
            total = total + dot(ctx[h].astype(BF), wo[h], NN)
        unit, scale1[:] = standard(total)
        unit1[:] = unit
        hidden[:] = (unit * gain1 + bias1).astype(BF)
        acc[:] = jnp.zeros_like(acc)

    @pl.when(i < n)
    def _():
        for lo in tiles:
            cols = pl.ds(lo, tile)
            g = dot(hidden[:], wg[N0, :, cols], NN) + gate_bias[pl.ds(t, N1), cols]
            l = dot(hidden[:], wl[N0, :, cols], NN) + lin_bias[pl.ds(t, N1), cols]
            gate[t, :, cols] = g
            lin[t, :, cols] = l
            inner[N0, :, cols] = (0.5 * g * (1.0 + lax.erf(g * 0.5 ** 0.5)) * l).astype(BF)
        for lo in tiles:
            cols = pl.ds(lo, tile)
            acc[:, cols] += dot(inner[N0], wd[N0, :, cols], NN)

    @pl.when(i == n - N1)
    def _():
        unit, scale = standard(ALPHA * hidden[:].astype(F32) + acc[:] + b_down)
        owned(cot, cot_own, N1).wait()
        g = cot_own[:].reshape(acc.shape).astype(F32)
        d_y = standard_grad(g * gain2, unit, scale)
        sums[pl.ds(N2 * n + 3, N1), :] = over_rows(d_y)
        sums[pl.ds(N2 * n + 4, N1), :] = over_rows(g * unit)
        d_ffn[:] = d_y.astype(BF)
        acc[:] = ALPHA * d_y

    @pl.when(i >= n)
    def _():
        for lo in tiles:
            cols = pl.ds(lo, tile)
            d_inner = dot(d_ffn[:], wd[N0, cols, :], NT).astype(BF).astype(F32)
            g, l = gate[t, :, cols], lin[t, :, cols]
            cdf = 0.5 * (1.0 + lax.erf(g * 0.5 ** 0.5))
            slope = cdf + g * (jnp.exp(-0.5 * g * g) * (N2 * np.pi) ** -0.5)
            d_l = d_inner * (g * cdf)
            d_g = d_inner * l * slope
            sums[pl.ds(t, N1), cols] = over_rows(d_g)
            sums[pl.ds(n + t, N1), cols] = over_rows(d_l)
            d_gate[N0, :, cols] = d_g.astype(BF)
            d_lin[N0, :, cols] = d_l.astype(BF)
        for lo in tiles:
            cols = pl.ds(lo, tile)
            acc[:, cols] += dot(d_gate[N0], wg[N0, cols, :], NT) + dot(d_lin[N0], wl[N0, cols, :], NT)

    @pl.when(i == N2 * n - N1)
    def _():
        d_h, unit = acc[:], unit1[:]
        d_x = standard_grad(d_h * gain1, unit, scale1[:])
        sums[pl.ds(N2 * n, N1), :] = over_rows(d_x)
        sums[pl.ds(N2 * n + N1, N1), :] = over_rows(d_h * unit)
        sums[pl.ds(N2 * n + N2, N1), :] = over_rows(d_h)
        resid[:] = ALPHA * d_x
        d_attn[:] = d_x.astype(BF)
        for h in range(n):
            d_ctx[h] = dot(d_attn[:], wo[h], NT)


def layer(ctx, wo, emb, cot, vectors, gate_bias, lin_bias, wg, wl, wd):
    n, own, dims = ctx.shape
    width = emb.shape[-1]
    ffn = wg.shape[N2]
    once = pl.BlockSpec(memory_space=pltpu.VMEM)
    weight = [pl.BlockSpec((N1,) + w.shape[N1:], lambda i: (i % n, N0, N0)) for w in (wg, wl, wd)]
    early = pl.BlockSpec((N1, own, ffn), lambda i: (jnp.minimum(i, n - N1), N0, N0))
    late = pl.BlockSpec((N1, own, ffn), lambda i: (jnp.maximum(i - n, N0), N0, N0))
    shape = jax.ShapeDtypeStruct
    slots = shape((n, own, ffn), BF)
    return pl.pallas_call(
        functools.partial(layer_kernel, n),
        name='layer',
        grid=(N2 * n,),
        in_specs=[once] * 2 + [ANY] * 2 + [once] * 3 + weight,
        out_specs=[once] * 6 + [early, late, late],
        out_shape=[shape((own, width), BF)] * 3 + [shape((own, width), F32), shape((n, own, dims), F32), shape((N2 * n + 8, width), F32), slots, slots, slots],
        scratch_shapes=[pltpu.VMEM((n, own, ffn), F32)] * N2 + [pltpu.VMEM((own, width), F32)] * N2 + [pltpu.VMEM((own, N1), F32)] + [pltpu.VMEM((emb.shape[0],) + emb.shape[2:], BF)] * 2 + [pltpu.SemaphoreType.DMA((2,))],
        compiler_params=pltpu.CompilerParams(dimension_semantics=('arbitrary',), vmem_limit_bytes=62 * N2 ** 20),
        cost_estimate=pl.CostEstimate(flops=15 * 10 ** 9, bytes_accessed=70 * N2 ** 20, transcendentals=N0),
    )(ctx, wo, emb, cot, vectors, gate_bias, lin_bias, wg, wl, wd)


def products_kernel(n, hidden, d_ffn, inner, d_gate, d_lin, gate, lin, down, turned_hidden):
    i = pl.program_id(N0)
    size = hidden.shape[N1]
    tile = 256 if size % 256 == N0 else size

    @pl.when(i == N0)
    def _():
        turned_hidden[:] = hidden[:].T

    def fill(out, lhs, rhs, dims):
        for lo in range(N0, size, tile):
            cols = pl.ds(lo, tile)
            out[N0, :, cols] = dot(lhs, rhs[:, cols], dims)
    pl.when(i < n)(lambda: fill(gate, turned_hidden[:], d_gate.at[N0], NN))
    pl.when((i >= n) & (i < N2 * n))(lambda: fill(lin, turned_hidden[:], d_lin.at[N0], NN))

    @pl.when(i >= N2 * n)
    def _():
        fill(down, inner[N0].T, d_ffn, NN)


def products(hidden, d_ffn, inner, d_gate, d_lin):
    n, own, ffn = inner.shape
    width = hidden.shape[N1]
    once = pl.BlockSpec(memory_space=pltpu.VMEM)

    def slot(rows, first):
        return pl.BlockSpec((N1, rows, ffn), lambda i: (jnp.clip(i - first * n, N0, n - N1), N0, N0))
    shape = jax.ShapeDtypeStruct((n, width, ffn), F32)
    return pl.pallas_call(
        functools.partial(products_kernel, n),
        name='products',
        grid=(3 * n,),
        in_specs=[once, once, slot(own, N2), slot(own, N0), slot(own, N1)],
        out_specs=[slot(width, N0), slot(width, N1), slot(width, N2)],
        out_shape=[shape] * 3,
        scratch_shapes=[pltpu.VMEM((width, own), BF)],
        compiler_params=pltpu.CompilerParams(dimension_semantics=('arbitrary',), vmem_limit_bytes=58 * N2 ** 20),
        cost_estimate=pl.CostEstimate(flops=12 * 10 ** 9, bytes_accessed=70 * N2 ** 20, transcendentals=N0),
    )(hidden, d_ffn, inner, d_gate, d_lin)


def solution(mesh):
    n_tp, n_dp = mesh.shape['tp'], mesh.shape['dp']
    in_specs = (P('dp', None), P('dp', None, None), P('tp', None)) + WEIGHT_SPECS
    out_specs = (P('tp', None),) + WEIGHT_SPECS

    def device_step(tokens, cotangent, emb_table, *weights):
        (w_qkv, b_qkv, w_out, b_out, ln1_gain, ln1_bias, w_gate, b_gate, w_lin, b_lin, w_down, b_down, ln2_gain) = weights
        tp, dp = lax.axis_index('tp'), lax.axis_index('dp')
        tokens = tokens[N0]
        seq_len, width = tokens.shape[N0], emb_table.shape[N1]
        heads, head_dim = b_qkv.shape[N0], b_qkv.shape[N1] // 3
        own = seq_len // n_tp
        ffn = w_gate.shape[N1]
        rk, rf, ro = width // n_dp, ffn // n_dp, w_out.shape[N0] // n_dp

        def cut(weight):
            rows = weight.shape[N0] // n_dp
            return lax.dynamic_slice_in_dim(weight, dp * rows, rows, N0)
        bias_rows = jnp.concatenate([b_gate[None], b_lin[None], jnp.zeros((14, ffn), BF)], axis=N0)
        piece = jnp.concatenate([cut(w_gate), cut(w_lin), cut(w_down), cut(w_out), bias_rows], axis=N0).astype(F32)

        vocab_loc = emb_table.shape[N0]
        local_ids = tokens - tp * vocab_loc
        in_shard = (local_ids >= N0) & (local_ids < vocab_loc)
        safe_ids = jnp.where(in_shard, local_ids, N0)
        found = jnp.take(emb_table, safe_ids, axis=N0, mode='clip')
        dims = heads * head_dim
        place = column_order(heads, head_dim)
        swap = (jnp.arange(3 * dims)[:, None] == jnp.asarray(place)[None, :]).astype(BF)
        wq = jnp.dot(w_qkv, swap, preferred_element_type=F32).astype(BF)
        bq = jnp.dot(b_qkv.reshape(N1, -N1), swap, preferred_element_type=F32)
        cos_tab, sin_tab = rope_tables(seq_len, head_dim, heads)
        emb_bf, (wg_full, wl_full, wd_full, wo_full), biases, tok_all, ctx_own, saved = embed(found, in_shard[:, None].astype(F32), piece, tokens.reshape(-N1, min(128, seq_len // 8)), (w_gate, w_lin, w_down, w_out), wq, bq, cos_tab, sin_tab, heads, n_tp, n_dp)
        is_own = (jnp.arange(n_tp) == tp)[:, None]
        bg_full, bl_full = [jnp.where(is_own, b[None].astype(F32), biases[:, i]) for i, b in enumerate((b_gate, b_lin))]

        blocks = 8

        def by_owner(values):
            return values.reshape(blocks, n_tp, -N1, width)

        vectors = jnp.stack([b_out, ln1_gain, ln1_bias, b_down, ln2_gain] + [b_out] * 3).astype(F32)
        hidden, d_ffn_bf, d_attn_bf, resid, d_ctx, row_sums, inner_act, d_gate_bf, d_lin_bf = layer(
            ctx_own.reshape(n_tp, own, dims), wo_full, by_owner(emb_bf), by_owner(cotangent[N0]), vectors, bg_full, bl_full, wg_full, wl_full, wd_full)

        prods = [grad.reshape(n_tp, n_dp, -N1, width) for grad in products(hidden, d_ffn_bf, inner_act, d_gate_bf, d_lin_bf)]
        d_w_out = jnp.einsum('hse,sd->hed', ctx_own.reshape(n_tp, own, dims).astype(BF), d_attn_bf, preferred_element_type=F32)
        d_w_qkv, d_b_qkv, d_cols, (d_w_gate, d_w_lin), d_w_down = backward(
            d_ctx.reshape(n_tp, blocks, own // blocks, dims), resid.reshape(blocks, own // blocks, width), saved, cos_tab, sin_tab, wq, swap.T, emb_bf,
            prods, heads, n_tp, n_dp)
        d_w_gate, d_w_lin = d_w_gate.reshape(-N1, ffn), d_w_lin.reshape(-N1, ffn)
        d_b_qkv = jnp.dot(d_b_qkv, swap.astype(F32).T, precision=lax.Precision.HIGHEST)
        all_ids = tok_all.reshape(-N1) - tp * vocab_loc
        all_ids = jnp.where((all_ids >= N0) & (all_ids < vocab_loc), all_ids, vocab_loc)
        col, d_w_gate, d_w_lin = table_rows(all_ids, d_cols.reshape(n_dp * seq_len, -N1), vocab_loc, d_w_gate, d_w_lin)

        slot = (jnp.arange(n_tp) == tp).astype(F32)[:, None]
        d_bq_rows = jnp.pad(slot * d_b_qkv, ((N0, N0), (N0, ffn - 3 * dims)))
        kept = N2 * n_tp
        small = jnp.concatenate([row_sums[:kept], d_bq_rows, row_sums[kept:kept + 5], jnp.zeros((7, width), F32)], axis=N0)
        d_table, d_w_down, d_w_out, d_w_qkv, small = finish(
            col, d_w_down, d_w_out.reshape(n_tp, n_dp, N2, -N1, width), d_w_qkv.reshape(n_dp, N2, -N1, 3 * dims), small, n_tp, n_dp)
        d_b_gate = lax.dynamic_index_in_dim(small[:n_tp], tp, N0, keepdims=False)
        d_b_lin = lax.dynamic_index_in_dim(small[n_tp:N2 * n_tp], tp, N0, keepdims=False)
        d_b_qkv = lax.dynamic_index_in_dim(small[N2 * n_tp:3 * n_tp], tp, N0, keepdims=False)[:3 * dims].reshape(heads, 3 * head_dim)
        d_b_out, d_ln1_gain, d_ln1_bias, d_b_down, d_ln2_gain = [small[3 * n_tp + i] for i in range(5)]
        return (d_table, d_w_qkv, d_b_qkv, d_w_out, d_b_out, d_ln1_gain, d_ln1_bias, d_w_gate, d_b_gate, d_w_lin, d_b_lin, d_w_down, d_b_down, d_ln2_gain)

    return jax.shard_map(device_step, mesh=mesh, in_specs=in_specs, out_specs=out_specs, check_vma=False)
```
